8 devices in a mesh: dp: 2 (over z, y), tp: 4 (over x, core).
Axes of the slice: x: 2, y: 2, z: 1, core: 2. Of those that a mesh axis runs over, the one named last changes fastest.
Arguments:
- x: bfloat16 [2, 96, 1536], P('dp', 'tp'), parts along dimension 0
- ln1_gamma: float32 [1536], replicated
- ln1_beta: float32 [1536], replicated
- w_qkv: bfloat16 [1536, 16, 3, 96], P(None, 'tp')
- b_qkv: float32 [16, 3, 96], P('tp')
- w_out: bfloat16 [1536, 1536], P('tp')
- b_out: float32 [1536], replicated
- ln2_gamma: float32 [1536], replicated
- ln2_beta: float32 [1536], replicated
- w_up: bfloat16 [1536, 6144], P(None, 'tp')
- b_up: float32 [6144], P('tp')
- w_down: bfloat16 [6144, 1536], P('tp')
- b_down: float32 [1536], replicated
- grad_y: bfloat16 [2, 96, 1536], P('dp', 'tp'), parts along dimension 0
Outputs:
- output 1: bfloat16 [2, 96, 1536], P('dp', 'tp'), parts along dimension 0
- output 2: bfloat16 [2, 96, 1536], P('dp', 'tp'), parts along dimension 0
- output 3: float32 [3072], P('dp'), parts along dimension 0
- output 4: float32 [3072], P('dp'), parts along dimension 0
- output 5: bfloat16 [3072, 16, 3, 96], P('dp', 'tp'), parts along dimension 0
- output 6: float32 [32, 3, 96], P(('dp', 'tp')), parts along dimension 0
- output 7: bfloat16 [3072, 1536], P(('dp', 'tp')), parts along dimension 0
- output 8: float32 [3072], P('dp'), parts along dimension 0
- output 9: float32 [3072], P('dp'), parts along dimension 0
- output 10: float32 [3072], P('dp'), parts along dimension 0
- output 11: bfloat16 [3072, 6144], P('dp', 'tp'), parts along dimension 0
- output 12: float32 [12288], P(('dp', 'tp')), parts along dimension 0
- output 13: bfloat16 [12288, 1536], P(('dp', 'tp')), parts along dimension 0
- output 14: float32 [3072], P('dp'), parts along dimension 0
There are 2 independent parts. The reference program is written for one: setup_inputs(seed, part) draws one part's arguments, and reference() takes and returns one part's arrays. A program takes and returns all parts, laid end to end along the dimension named above; an argument that names none is the same for every part.
All inputs are finite; a program needn't handle non-finite values.
Results may differ from the reference program's by a relative error of at most 0.0173697.
Values are sent between devices in bfloat16 or wider.
A program may use at most 1 GiB of HBM per device.

```python
import math
import jax
import jax.numpy as jnp
from jax import lax

BATCH = 1
SEQ = 96
D = 1536
HEADS = 16
HEAD = 96
FF = 6144
EPS = 1e-5
MASK_VALUE = -1e30


def alibi_slopes(n_heads):
    closest = 2 ** int(math.floor(math.log2(n_heads)))
    base_ratio = 2.0 ** (-8.0 / closest)
    extra_ratio = 2.0 ** (-4.0 / closest)
    remaining = min(closest, n_heads - closest)
    slopes = [base_ratio ** (i + 1) for i in range(closest)]
    slopes = slopes + [extra_ratio ** (2 * i + 1) for i in range(remaining)]
    return jnp.array(slopes, dtype=jnp.float32)


def layer_norm(values, ln_gain, ln_bias):
    row_mean = jnp.mean(values, axis=-1, keepdims=True)
    centered = values - row_mean
    variance = jnp.mean(centered * centered, axis=-1, keepdims=True)
    return centered * lax.rsqrt(variance + EPS) * ln_gain + ln_bias


def layer_forward(x, ln1_gamma, ln1_beta, w_qkv, b_qkv, w_out, b_out, ln2_gamma, ln2_beta, w_up, b_up, w_down, b_down):
    positions = jnp.arange(SEQ)
    causal = positions[None, :] <= positions[:, None]
    key_pos = positions.astype(jnp.float32)
    x_f = x.astype(jnp.float32)
    h_norm = layer_norm(x_f, ln1_gamma, ln1_beta).astype(jnp.bfloat16)
    qkv_vals = (jnp.einsum('bsd,dhte->bshte', h_norm.astype(jnp.float32), w_qkv.astype(jnp.float32)) + b_qkv).astype(jnp.bfloat16)
    per_head = jnp.moveaxis(qkv_vals, 2, 0)

    def head_attention(operands):
        head_qkv, head_slope = operands
        q_one = head_qkv[:, :, 0].astype(jnp.float32)
        k_one = head_qkv[:, :, 1].astype(jnp.float32)
        v_one = head_qkv[:, :, 2].astype(jnp.float32)
        scores = jnp.einsum('bie,bje->bij', q_one, k_one) * (HEAD ** -0.5) + head_slope * key_pos
        scores = jnp.where(causal, scores, MASK_VALUE)
        prob_bf = jax.nn.softmax(scores, axis=-1).astype(jnp.bfloat16)
        return jnp.einsum('bij,bje->bie', prob_bf.astype(jnp.float32), v_one).astype(jnp.bfloat16)

    context = lax.map(jax.checkpoint(head_attention), (per_head, alibi_slopes(HEADS)))
    context_flat = jnp.moveaxis(context, 0, 2).reshape(BATCH, SEQ, D)
    attn_out = jnp.einsum('bsc,cd->bsd', context_flat.astype(jnp.float32), w_out.astype(jnp.float32)).astype(jnp.bfloat16)
    x_mid = x_f + attn_out.astype(jnp.float32) + b_out
    g_norm = layer_norm(x_mid, ln2_gamma, ln2_beta).astype(jnp.bfloat16)
    pre_act = jnp.einsum('bsd,df->bsf', g_norm.astype(jnp.float32), w_up.astype(jnp.float32)) + b_up
    activated = jax.nn.gelu(pre_act, approximate=True).astype(jnp.bfloat16)
    mlp_out = jnp.einsum('bsf,fd->bsd', activated.astype(jnp.float32), w_down.astype(jnp.float32)).astype(jnp.bfloat16)
    return (x_mid + mlp_out.astype(jnp.float32) + b_down).astype(jnp.bfloat16)


def setup_inputs(seed: int = 0, part: int = 0) -> dict:
    key_list = jax.random.split(jax.random.key(seed), 14)

    def normal(rng_key, out_shape, std_dev):
        return std_dev * jax.random.normal(rng_key, out_shape, jnp.float32)

    return {
        'x': normal(jax.random.fold_in(key_list[0], part), (BATCH, SEQ, D), 1.0).astype(jnp.bfloat16),
        'ln1_gamma': 1.0 + normal(key_list[1], (D,), 0.2),
        'ln1_beta': normal(key_list[2], (D,), 0.2),
        'w_qkv': normal(key_list[3], (D, HEADS, 3, HEAD), D ** -0.5).astype(jnp.bfloat16),
        'b_qkv': normal(key_list[4], (HEADS, 3, HEAD), 0.5),
        'w_out': normal(key_list[5], (D, D), D ** -0.5).astype(jnp.bfloat16),
        'b_out': normal(key_list[6], (D,), 0.5),
        'ln2_gamma': 1.0 + normal(key_list[7], (D,), 0.2),
        'ln2_beta': normal(key_list[8], (D,), 0.2),
        'w_up': normal(key_list[9], (D, FF), D ** -0.5).astype(jnp.bfloat16),
        'b_up': normal(key_list[10], (FF,), 0.5),
        'w_down': normal(key_list[11], (FF, D), FF ** -0.5).astype(jnp.bfloat16),
        'b_down': normal(key_list[12], (D,), 0.5),
        'grad_y': normal(jax.random.fold_in(key_list[13], part), (BATCH, SEQ, D), 1.0).astype(jnp.bfloat16),
    }


def reference(x, ln1_gamma, ln1_beta, w_qkv, b_qkv, w_out, b_out, ln2_gamma, ln2_beta, w_up, b_up, w_down, b_down, grad_y):
    y, pullback = jax.vjp(layer_forward, x, ln1_gamma, ln1_beta, w_qkv, b_qkv, w_out, b_out, ln2_gamma, ln2_beta, w_up, b_up, w_down, b_down)
    (grad_x, grad_ln1_gamma, grad_ln1_beta, grad_w_qkv, grad_b_qkv, grad_w_out, grad_b_out,
     grad_ln2_gamma, grad_ln2_beta, grad_w_up, grad_b_up, grad_w_down, grad_b_down) = pullback(grad_y)
    return (y, grad_x, grad_ln1_gamma, grad_ln1_beta, grad_w_qkv, grad_b_qkv, grad_w_out, grad_b_out,
            grad_ln2_gamma, grad_ln2_beta, grad_w_up, grad_b_up, grad_w_down, grad_b_down)
```

```python
import functools
import math

import jax
import jax.numpy as jnp
from jax import lax
from jax.experimental import pallas as pl
from jax.experimental.pallas import tpu as pltpu
from jax.sharding import PartitionSpec as P

EPS = 1e-5
MASK_VALUE = -1e30
BF = jnp.bfloat16
F32 = jnp.float32
MESH = pl.DeviceIdType.MESH

D = 1536
S = 96
SL = 24
TP = 4
HL = 4
HD = 96
FL = 1536
CW = 256
NCH = D // CW
HCH = NCH // 2


def alibi_slopes(n_heads):
    closest = 2 ** int(math.floor(math.log2(n_heads)))
    base_ratio = 2.0 ** (-8.0 / closest)
    extra_ratio = 2.0 ** (-4.0 / closest)
    remaining = min(closest, n_heads - closest)
    slopes = [base_ratio ** (i + 1) for i in range(closest)]
    return slopes + [extra_ratio ** (2 * i + 1) for i in range(remaining)]


def dot(a, b, ca, cb):
    return lax.dot_general(a, b, (((ca,), (cb,)), ((), ())), preferred_element_type=F32)


def gelu_parts(u):
    k = math.sqrt(2.0 / math.pi)
    u2 = u * u
    th = jnp.tanh(k * (u + 0.044715 * (u2 * u)))
    half = 0.5 * (1.0 + th)
    dk = k * (1.0 + 3.0 * 0.044715 * u2)
    return u * half, half + 0.5 * u * (1.0 - th * th) * dk


def rows_stats(v):
    mean = jnp.mean(v, axis=-1, keepdims=True)
    cen = v - mean
    var = jnp.mean(cen * cen, axis=-1, keepdims=True)
    return cen, lax.rsqrt(var + EPS)


def block_kernel(x_ref, gy_ref, g1_ref, be1_ref, g2_ref, be2_ref, bo_ref, bd_ref, bqkv_ref, bup_ref,
                 wqkv_hbm, wout_hbm, wup_hbm, wdn_hbm,
                 y_ref, gx_ref, vec_ref, gbqkv_ref, h_ref, gqkv_ref, ctx_ref, gmid_ref, g_ref, gpre_ref, act_ref, gyf_ref,
                 wqkv, wout, wup, wdn, xg, gyg, xf, xhat, rstd_s, biasT, qkvT, probs,
                 a_ps, a_pr, a_hs, a_hr, a_cr, a_fr, b_ps, b_pr, b_hs, b_hr, b_cr, b_fr,
                 gact, ghp, m_pr, m_hs, m_cr, r_pr, r_hs, r_cr, gm_f, ln_x, gg_f,
                 wsem, ssem, rsem):
    t = lax.axis_index('tp')
    core = t % 2
    pt = t + 1 - 2 * core
    ct = (t + 2) % TP
    qt = (pt + 2) % TP

    started = []
    counter = [0]

    def send(src, dst, dev):
        i = counter[0]
        counter[0] += 1
        c = pltpu.make_async_remote_copy(src_ref=src, dst_ref=dst, send_sem=ssem.at[i], recv_sem=rsem.at[i],
                                         device_id={'tp': dev}, device_id_type=MESH)
        c.start()
        started.append(c)
        return c

    w_cps = {}
    w_cps['qkv'] = [pltpu.make_async_copy(wqkv_hbm, wqkv, wsem.at[0])]
    w_cps['out'] = [pltpu.make_async_copy(wout_hbm.at[:, pl.ds(k * CW, CW)], wout.at[k], wsem.at[1 + k]) for k in range(NCH)]
    w_cps['dn'] = [pltpu.make_async_copy(wdn_hbm, wdn, wsem.at[7])]
    w_cps['up'] = [pltpu.make_async_copy(wup_hbm, wup, wsem.at[8])]

    barrier = pltpu.get_barrier_semaphore()
    for dev in (pt, ct):
        pl.semaphore_signal(barrier, inc=1, device_id={'tp': dev}, device_id_type=MESH)
    for name in ('qkv', 'out', 'dn', 'up'):
        for c in w_cps[name]:
            c.start()
    pl.semaphore_wait(barrier, 2)

    x_c = send(x_ref, xg.at[t], ct)
    x_p = send(x_ref, xg.at[t], pt)
    y_c = send(gy_ref, gyg.at[t], ct)
    y_p = send(gy_ref, gyg.at[t], pt)
    xg[t] = x_ref[...]
    gyg[t] = gy_ref[...]

    for h in range(HL):
        for e in range(3):
            row = jnp.broadcast_to(bqkv_ref[e, h:h + 1, :], (S, HD))
            biasT[pl.ds((h * 3 + e) * HD, HD), :] = row.T

    x_c.wait_recv()
    x_f = send(xg.at[ct], xg.at[ct], pt)
    x_p.wait_recv()
    x_f.wait_recv()

    for i in range(TP):
        xf[pl.ds(i * SL, SL), :] = xg[i].astype(F32)
    for r in range(0, S, 32):
        cen, rstd = rows_stats(xf[r:r + 32, :])
        xh = cen * rstd
        xhat[r:r + 32, :] = xh
        rstd_s[r:r + 32, :] = jnp.broadcast_to(rstd, (32, 128))
        h_ref[r:r + 32, :] = (xh * g1_ref[...] + be1_ref[...]).astype(BF)

    y_c.wait_recv()
    y_f = send(gyg.at[ct], gyg.at[ct], pt)

    w_cps['qkv'][0].wait()
    hv = h_ref[...]
    for h in range(HL):
        rows = slice(h * 3 * HD, (h + 1) * 3 * HD)
        qkvT[rows, :] = (dot(wqkv[rows, :], hv, 1, 1) + biasT[rows, :]).astype(BF)

    scale = HD ** -0.5
    slopes = alibi_slopes(HL * TP)
    j_pos = lax.broadcasted_iota(jnp.int32, (S, S), 0)
    i_pos = lax.broadcasted_iota(jnp.int32, (S, S), 1)
    causal = j_pos <= i_pos
    j_f = j_pos.astype(F32)

    def head(h, e):
        return qkvT[(h * 3 + e) * HD:(h * 3 + e + 1) * HD, :]

    for h in range(HL):
        slope = jnp.where(t == 0, slopes[h], jnp.where(t == 1, slopes[HL + h], jnp.where(t == 2, slopes[2 * HL + h], slopes[3 * HL + h]))).astype(F32)
        s = dot(head(h, 1), head(h, 0), 0, 0) * scale + slope * j_f
        s = jnp.where(causal, s, MASK_VALUE)
        p = jnp.exp(s - jnp.max(s, axis=0, keepdims=True))
        p = p / jnp.sum(p, axis=0, keepdims=True)
        probs[h] = p
        ctx_ref[h * HD:(h + 1) * HD, :] = dot(head(h, 2), p.astype(BF), 1, 0).astype(BF)

    def exchange(part, ps, pr, hs, hr, cr):
        firsts = []
        for k in range(HCH):
            ps[k] = part((1 - core) * HCH + k).astype(BF)
            firsts.append(send(ps.at[k], pr.at[k], pt))
        outs = []
        for k in range(HCH):
            own = part(core * HCH + k)
            firsts[k].wait_recv()
            hs[k] = (own + pr[k].astype(F32)).astype(BF)
            outs.append((send(hs.at[k], cr.at[k], ct), send(hs.at[k], hr.at[k], pt)))
        return outs

    def forward(outs, cr, fr):
        fwd = []
        for k in range(HCH):
            outs[k][0].wait_recv()
            fwd.append(send(cr.at[k], fr.at[k], pt))
        return fwd

    for c in w_cps['out']:
        c.wait()
    ctxT = ctx_ref[...]
    a_outs = exchange(lambda kk: dot(ctxT, wout[kk], 0, 0), a_ps, a_pr, a_hs, a_hr, a_cr)

    y_p.wait_recv()
    y_f.wait_recv()
    for i in range(TP):
        gm_f[pl.ds(i * SL, SL), :] = gyg[i].astype(F32)
    for r in range(0, S, 32):
        gyf_ref[r:r + 32, :] = gm_f[r:r + 32, :].astype(BF)
    w_cps['dn'][0].wait()
    gyv = gyf_ref[...]
    for n in range(NCH):
        gact[:, n * CW:(n + 1) * CW] = dot(gyv, wdn[n * CW:(n + 1) * CW, :], 1, 1).astype(BF)
    vec_ref[0:1, :] = jnp.sum(gm_f[...], axis=0, keepdims=True)

    def gathered(outs, fwd, hs, hr, cr, fr, put):
        for k in range(HCH):
            put(core * HCH + k, (hs[k].astype(F32) + cr[k].astype(F32)).astype(BF).astype(F32))
        for k in range(HCH):
            outs[k][1].wait_recv()
            fwd[k].wait_recv()
            put((1 - core) * HCH + k, (hr[k].astype(F32) + fr[k].astype(F32)).astype(BF).astype(F32))

    a_fwd = forward(a_outs, a_cr, a_fr)

    def put_x(kk, val):
        cols = pl.ds(pl.multiple_of(kk * CW, CW), CW)
        xf[:, cols] = xf[:, cols] + val + bo_ref[:, cols]

    gathered(a_outs, a_fwd, a_hs, a_hr, a_cr, a_fr, put_x)

    for r in range(0, S, 32):
        cen, rstd = rows_stats(xf[r:r + 32, :])
        g_ref[r:r + 32, :] = (cen * rstd * g2_ref[...] + be2_ref[...]).astype(BF)

    w_cps['up'][0].wait()
    gv = g_ref[...]
    for n in range(NCH):
        cols = slice(n * CW, (n + 1) * CW)
        pre = dot(gv, wup[:, cols], 1, 0) + bup_ref[:, cols]
        val, der = gelu_parts(pre)
        act_ref[:, cols] = val.astype(BF)
        gp = gact[:, cols].astype(F32) * der
        vec_ref[1:2, cols] = jnp.sum(gp, axis=0, keepdims=True)
        gpre_ref[:, cols] = gp.astype(BF)

    gprev = gpre_ref[...]

    def part_g(kk):
        return dot(gprev, wup[pl.ds(pl.multiple_of(kk * CW, CW), CW), :], 1, 1)

    g_outs = exchange(part_g, b_ps, b_pr, b_hs, b_hr, b_cr)

    def scatter_first(part, buf, pr, extra=None):
        for n in range(NCH):
            cols = slice(n * CW, (n + 1) * CW)
            v = part(n)
            for i in range(TP):
                buf[i, :, cols] = v[i * SL:(i + 1) * SL, :].astype(BF)
            if extra is not None:
                extra(n, v)
        return (send(buf.at[qt], pr.at[1], pt), send(buf.at[pt], pr.at[0], pt))

    actv = act_ref[...]
    m_first = scatter_first(lambda n: dot(actv, wdn[:, n * CW:(n + 1) * CW], 1, 0), ghp.at[0], m_pr)

    g_fwd = forward(g_outs, b_cr, b_fr)

    m_first[0].wait_recv()
    m_hs[...] = (ghp[0, ct].astype(F32) + m_pr[1].astype(F32)).astype(BF)
    m_out = send(m_hs, m_cr, ct)

    def put_g(kk, val):
        gg_f[:, pl.ds(pl.multiple_of(kk * CW, CW), CW)] = val

    gathered(g_outs, g_fwd, b_hs, b_hr, b_cr, b_fr, put_g)

    gg2 = jnp.zeros((1, D), F32)
    gb2 = jnp.zeros((1, D), F32)
    gbo = jnp.zeros((1, D), F32)
    for r in range(0, S, 32):
        cen, rstd = rows_stats(xf[r:r + 32, :])
        xh = cen * rstd
        gg = gg_f[r:r + 32, :]
        gg2 = gg2 + jnp.sum(gg * xh, axis=0, keepdims=True)
        gb2 = gb2 + jnp.sum(gg, axis=0, keepdims=True)
        dxh = gg * g2_ref[...]
        m1 = jnp.mean(dxh, axis=-1, keepdims=True)
        m2 = jnp.mean(dxh * xh, axis=-1, keepdims=True)
        gm = gm_f[r:r + 32, :] + rstd * (dxh - m1 - xh * m2)
        gm_f[r:r + 32, :] = gm
        gbo = gbo + jnp.sum(gm, axis=0, keepdims=True)
        gmid_ref[r:r + 32, :] = gm.astype(BF)
    vec_ref[2:3, :] = gg2
    vec_ref[3:4, :] = gb2
    vec_ref[4:5, :] = gbo

    gmv = gmid_ref[...]
    gctxT = dot(wout[0], gmv[:, :CW], 1, 1)
    for k in range(1, NCH):
        gctxT = gctxT + dot(wout[k], gmv[:, k * CW:(k + 1) * CW], 1, 1)
    gctxT = gctxT.astype(BF)
    ones = jnp.ones((8, S), BF)
    for h in range(HL):
        go = gctxT[h * HD:(h + 1) * HD, :]
        p = probs[h]
        gp = dot(head(h, 2), go, 0, 0).astype(BF).astype(F32)
        gv_ = dot(go, p.astype(BF), 1, 1).astype(BF)
        gs = (p * (gp - jnp.sum(gp * p, axis=0, keepdims=True))).astype(BF)
        gq = (dot(head(h, 1), gs, 1, 0) * scale).astype(BF)
        gk = (dot(head(h, 0), gs, 1, 1) * scale).astype(BF)
        for e, val in enumerate((gq, gk, gv_)):
            gqkv_ref[(h * 3 + e) * HD:(h * 3 + e + 1) * HD, :] = val
            gbqkv_ref[e, h:h + 1, :] = dot(ones, val, 1, 1)[0:1, :]

    gqv = gqkv_ref[...]

    def ln1_sums(n, v):
        cols = slice(n * CW, (n + 1) * CW)
        v = v.astype(BF).astype(F32)
        ln_s[0:1, cols] = jnp.sum(v * xhat[:, cols], axis=0, keepdims=True)
        ln_s[1:2, cols] = jnp.sum(v, axis=0, keepdims=True)

    ln_s, ln_pr, ln_hs, ln_cr = ln_x.at[0], ln_x.at[1], ln_x.at[2], ln_x.at[3]
    r_first = scatter_first(lambda n: dot(gqv, wqkv[:, n * CW:(n + 1) * CW], 0, 0), ghp.at[1], r_pr, ln1_sums)
    l_first = send(ln_s, ln_pr, pt)

    r_first[0].wait_recv()
    r_hs[...] = (ghp[1, ct].astype(F32) + r_pr[1].astype(F32)).astype(BF)
    r_out = send(r_hs, r_cr, ct)
    l_first.wait_recv()
    ln_hs[...] = ln_s[...] + ln_pr[...]
    l_out = send(ln_hs, ln_cr, ct)

    own = pl.ds(pl.multiple_of(t * SL, 8), SL)
    m_first[1].wait_recv()
    m_out.wait_recv()
    m_sum = (ghp[0, t].astype(F32) + m_pr[0].astype(F32)).astype(BF).astype(F32) + m_cr[...].astype(F32)
    y_ref[...] = (xf[own, :] + m_sum.astype(BF).astype(F32) + bd_ref[...]).astype(BF)

    r_first[1].wait_recv()
    mine = (ghp[1, t].astype(F32) + r_pr[0].astype(F32)).astype(BF).astype(F32)
    r_out.wait_recv()
    gh = (mine + r_cr[...].astype(F32)).astype(BF).astype(F32)
    xh = xhat[own, :]
    dxh = gh * g1_ref[...]
    m1 = jnp.mean(dxh, axis=-1, keepdims=True)
    m2 = jnp.mean(dxh * xh, axis=-1, keepdims=True)
    gx_ref[...] = (gm_f[own, :] + rstd_s[own, 0:1] * (dxh - m1 - xh * m2)).astype(BF)
    l_out.wait_recv()
    vec_ref[6:8, :] = ln_hs[...] + ln_cr[...]
    for c in started:
        c.wait_send()


N_SEND = 38


def grads_kernel(h_ref, gqkv_ref, ctx_ref, gmid_ref, g_ref, gpre_ref, act_ref, gyf_ref, yi_ref, gxi_ref, vec_ref, gbi_ref,
                 y_ref, gx_ref, gl1_ref, bl1_ref, gwqkv_ref, gbqkv_ref, gwout_ref, gbo_ref, gl2_ref, bl2_ref,
                 gwup_ref, gbup_ref, gwdn_ref, gbd_ref, s_qkv, s_out, s_up, s_dn, sem):
    cps = []

    def out(src, dst):
        c = pltpu.make_async_copy(src, dst, sem.at[len(cps)])
        c.start()
        cps.append(c)

    y_ref[...] = yi_ref[...]
    gx_ref[...] = gxi_ref[...]
    gbqkv_ref[...] = gbi_ref[...]
    for i, r in enumerate((gbd_ref, gbup_ref, gl2_ref, bl2_ref, gbo_ref, None, gl1_ref, bl1_ref)):
        if r is not None:
            r[...] = vec_ref[i, :]

    gyv = gyf_ref[...]
    gpv = gpre_ref[...]
    for n in range(NCH):
        rows = pl.ds(n * CW, CW)
        s_dn[rows, :] = dot(act_ref[:, n * CW:(n + 1) * CW], gyv, 0, 0).astype(BF)
        out(s_dn.at[rows], gwdn_ref.at[rows])
    for n in range(NCH):
        rows = pl.ds(n * CW, CW)
        s_up[rows, :] = dot(g_ref[:, n * CW:(n + 1) * CW], gpv, 0, 0).astype(BF)
        out(s_up.at[rows], gwup_ref.at[rows])
    hv = h_ref[...]
    for n in range(HL):
        rows = pl.ds(n * 3 * HD, 3 * HD)
        s_qkv[rows, :] = dot(gqkv_ref[n * 3 * HD:(n + 1) * 3 * HD, :], hv, 1, 0).astype(BF)
        out(s_qkv.at[rows], gwqkv_ref.at[rows])
    s_out[...] = dot(ctx_ref[...], gmid_ref[...], 1, 0).astype(BF)
    out(s_out, gwout_ref)
    for c in cps:
        c.wait()


def solution(mesh):
    VM = pl.BlockSpec(memory_space=pltpu.VMEM)
    ANY = pl.BlockSpec(memory_space=pl.ANY)

    def sds(shape, dt):
        return jax.ShapeDtypeStruct(shape, dt)

    def local_step(x, g1, be1, w_qkv, b_qkv, w_out, b_out, g2, be2, w_up, b_up, w_down, b_down, grad_y):
        wq = jnp.transpose(w_qkv, (1, 2, 3, 0)).reshape(3 * HL * HD, D)
        bq = jnp.transpose(b_qkv, (1, 0, 2))
        row = lambda v: v.reshape(1, -1)
        half = pltpu.VMEM((HCH, S, CW), BF)
        mids = pl.pallas_call(
            block_kernel,
            out_shape=(sds((SL, D), BF), sds((SL, D), BF), sds((8, D), F32), sds((3, HL, HD), F32), sds((S, D), BF),
                       sds((3 * HL * HD, S), BF), sds((HL * HD, S), BF), sds((S, D), BF), sds((S, D), BF), sds((S, FL), BF),
                       sds((S, FL), BF), sds((S, D), BF)),
            in_specs=[VM] * 10 + [ANY] * 4,
            out_specs=(VM,) * 12,
            scratch_shapes=[
                pltpu.VMEM((3 * HL * HD, D), BF), pltpu.VMEM((NCH, HL * HD, CW), BF), pltpu.VMEM((D, FL), BF), pltpu.VMEM((FL, D), BF),
                pltpu.VMEM((TP, SL, D), BF), pltpu.VMEM((TP, SL, D), BF), pltpu.VMEM((S, D), F32), pltpu.VMEM((S, D), F32),
                pltpu.VMEM((S, 128), F32), pltpu.VMEM((3 * HL * HD, S), F32), pltpu.VMEM((3 * HL * HD, S), BF), pltpu.VMEM((HL, S, S), F32),
                half, half, half, half, half, half, half, half, half, half, half, half,
                pltpu.VMEM((S, FL), BF), pltpu.VMEM((2, TP, SL, D), BF),
                pltpu.VMEM((2, SL, D), BF), pltpu.VMEM((SL, D), BF), pltpu.VMEM((SL, D), BF),
                pltpu.VMEM((2, SL, D), BF), pltpu.VMEM((SL, D), BF), pltpu.VMEM((SL, D), BF),
                pltpu.VMEM((S, D), F32), pltpu.VMEM((4, 2, D), F32), pltpu.VMEM((S, D), F32),
                pltpu.SemaphoreType.DMA((9,)), pltpu.SemaphoreType.DMA((N_SEND,)), pltpu.SemaphoreType.DMA((N_SEND,)),
            ],
            compiler_params=pltpu.CompilerParams(collective_id=0, has_side_effects=True),
            name='block',
        )(x.reshape(SL, D), grad_y.reshape(SL, D), row(g1), row(be1), row(g2), row(be2), row(b_out), row(b_down), bq, row(b_up),
          wq, w_out, w_up, w_down)
        y, gx, vec, gb, h, gqkv, ctx, gmid, g, gpre, act, gyf = mids
        vec1 = sds((D,), F32)
        outs = pl.pallas_call(
            grads_kernel,
            out_shape=(sds((SL, D), BF), sds((SL, D), BF), vec1, vec1, sds((3 * HL * HD, D), BF), sds((3, HL, HD), F32),
                       sds((HL * HD, D), BF), vec1, vec1, vec1, sds((D, FL), BF), vec1, sds((FL, D), BF), vec1),
            in_specs=[VM] * 12,
            out_specs=(VM, VM, VM, VM, ANY, VM, ANY, VM, VM, VM, ANY, VM, ANY, VM),
            scratch_shapes=[pltpu.VMEM((3 * HL * HD, D), BF), pltpu.VMEM((HL * HD, D), BF), pltpu.VMEM((D, FL), BF), pltpu.VMEM((FL, D), BF),
                            pltpu.SemaphoreType.DMA((32,))],
            name='grads',
        )(h, gqkv, ctx, gmid, g, gpre, act, gyf, y, gx, vec, gb)
        (y, gx, gl1, bl1, gwqkv, gbqkv, gwout, gbo, gl2, bl2, gwup, gbup, gwdn, gbd) = outs
        gwqkv = jnp.transpose(gwqkv.reshape(HL, 3, HD, D), (3, 0, 1, 2))
        gbqkv = jnp.transpose(gbqkv, (1, 0, 2))
        return (y.reshape(1, SL, D), gx.reshape(1, SL, D), gl1, bl1, gwqkv, gbqkv, gwout, gbo, gl2, bl2, gwup, gbup, gwdn, gbd)

    row_spec = P('dp', 'tp', None)
    in_specs = (row_spec, P(), P(), P(None, 'tp', None, None), P('tp', None, None), P('tp', None), P(), P(), P(),
                P(None, 'tp'), P('tp'), P('tp', None), P(), row_spec)
    out_specs = (row_spec, row_spec, P('dp'), P('dp'), P('dp', 'tp', None, None), P(('dp', 'tp'), None, None),
                 P(('dp', 'tp'), None), P('dp'), P('dp'), P('dp'), P('dp', 'tp'), P(('dp', 'tp')), P(('dp', 'tp'), None), P('dp'))
    return jax.shard_map(local_step, mesh=mesh, in_specs=in_specs, out_specs=out_specs, check_vma=False)
```

```python
import functools
import math

import jax
import jax.numpy as jnp
from jax import lax
from jax.experimental import pallas as pl
from jax.experimental.pallas import tpu as pltpu
from jax.sharding import PartitionSpec as P

EPS = 1e-5
MASK_VALUE = -1e30
BF = jnp.bfloat16
F32 = jnp.float32
MESH = pl.DeviceIdType.MESH

D = 1536
S = 96
SL = 24
TP = 4
HL = 4
HD = 96
FL = 1536
CW = 256
NCH = D // CW
HCH = NCH // 2


def alibi_slopes(n_heads):
    closest = 2 ** int(math.floor(math.log2(n_heads)))
    base_ratio = 2.0 ** (-8.0 / closest)
    extra_ratio = 2.0 ** (-4.0 / closest)
    remaining = min(closest, n_heads - closest)
    slopes = [base_ratio ** (i + 1) for i in range(closest)]
    return slopes + [extra_ratio ** (2 * i + 1) for i in range(remaining)]


def dot(a, b, ca, cb):
    return lax.dot_general(a, b, (((ca,), (cb,)), ((), ())), preferred_element_type=F32)


def gelu_parts(u):
    k = math.sqrt(2.0 / math.pi)
    u2 = u * u
    th = jnp.tanh(k * (u + 0.044715 * (u2 * u)))
    half = 0.5 * (1.0 + th)
    dk = k * (1.0 + 3.0 * 0.044715 * u2)
    return u * half, half + 0.5 * u * (1.0 - th * th) * dk


def rows_stats(v):
    mean = jnp.mean(v, axis=-1, keepdims=True)
    cen = v - mean
    var = jnp.mean(cen * cen, axis=-1, keepdims=True)
    return cen, lax.rsqrt(var + EPS)


def block_kernel(x_ref, gy_ref, g1_in, be1_in, g2_in, be2_in, bo_in, bd_in, bqkv_ref, bup_in,
                 wqkv_hbm, wout_hbm, wup_hbm, wdn_hbm,
                 y_ref, gx_ref, vec_ref, gbqkv_ref, h_ref, gqkv_ref, ctx_ref, gmid_ref, g_ref, gpre_ref, act_ref, gyf_ref,
                 wqkv, wout, wup, wdn, xg, gyg, xf, xhat, rstd_s, biasT, qkvT, probs,
                 a_ps, a_pr, a_hs, a_hr, a_cr, a_fr, b_ps, b_pr, b_hs, b_hr, b_cr, b_fr,
                 gact, ghp, m_pr, m_hs, m_cr, r_pr, r_hs, r_cr, gm_f, ln_x, gg_f, par,
                 wsem, ssem, rsem):
    t = lax.axis_index('tp')
    core = t % 2
    pt = t + 1 - 2 * core
    ct = (t + 2) % TP
    qt = (pt + 2) % TP

    started = []
    counter = [0]

    def send(src, dst, dev):
        i = counter[0]
        counter[0] += 1
        c = pltpu.make_async_remote_copy(src_ref=src, dst_ref=dst, send_sem=ssem.at[i], recv_sem=rsem.at[i],
                                         device_id={'tp': dev}, device_id_type=MESH)
        c.start()
        started.append(c)
        return c

    w_cps = {}
    w_cps['qkv'] = [pltpu.make_async_copy(wqkv_hbm, wqkv, wsem.at[0])]
    w_cps['out'] = [pltpu.make_async_copy(wout_hbm.at[:, pl.ds(k * CW, CW)], wout.at[k], wsem.at[1 + k]) for k in range(NCH)]
    w_cps['dn'] = [pltpu.make_async_copy(wdn_hbm, wdn, wsem.at[7])]
    w_cps['up'] = [pltpu.make_async_copy(wup_hbm, wup, wsem.at[8])]

    barrier = pltpu.get_barrier_semaphore()
    for dev in (pt, ct):
        pl.semaphore_signal(barrier, inc=1, device_id={'tp': dev}, device_id_type=MESH)
    for name in ('qkv', 'out', 'dn', 'up'):
        for c in w_cps[name]:
            c.start()
    pl.semaphore_wait(barrier, 2)

    x_c = send(x_ref, xg.at[t], ct)
    x_p = send(x_ref, xg.at[t], pt)
    y_c = send(gy_ref, gyg.at[t], ct)
    y_p = send(gy_ref, gyg.at[t], pt)
    xg[t] = x_ref[...]
    gyg[t] = gy_ref[...]

    for i, r in enumerate((g1_in, be1_in, g2_in, be2_in, bo_in, bd_in, bup_in)):
        par[i, :] = r[...]
    g1_ref, be1_ref, g2_ref, be2_ref, bo_ref, bd_ref, bup_ref = (par.at[i:i + 1] for i in range(7))

    for h in range(HL):
        for e in range(3):
            row = jnp.broadcast_to(bqkv_ref[e, h:h + 1, :], (S, HD))
            biasT[pl.ds((h * 3 + e) * HD, HD), :] = row.T

    x_c.wait_recv()
    x_f = send(xg.at[ct], xg.at[ct], pt)
    x_p.wait_recv()
    x_f.wait_recv()

    for i in range(TP):
        xf[pl.ds(i * SL, SL), :] = xg[i].astype(F32)
    for r in range(0, S, 32):
        cen, rstd = rows_stats(xf[r:r + 32, :])
        xh = cen * rstd
        xhat[r:r + 32, :] = xh
        rstd_s[r:r + 32, :] = jnp.broadcast_to(rstd, (32, 128))
        h_ref[r:r + 32, :] = (xh * g1_ref[...] + be1_ref[...]).astype(BF)

    y_c.wait_recv()
    y_f = send(gyg.at[ct], gyg.at[ct], pt)

    w_cps['qkv'][0].wait()
    hv = h_ref[...]
    for h in range(HL):
        rows = slice(h * 3 * HD, (h + 1) * 3 * HD)
        qkvT[rows, :] = (dot(wqkv[rows, :], hv, 1, 1) + biasT[rows, :]).astype(BF)

    scale = HD ** -0.5
    slopes = alibi_slopes(HL * TP)
    j_pos = lax.broadcasted_iota(jnp.int32, (S, S), 0)
    i_pos = lax.broadcasted_iota(jnp.int32, (S, S), 1)
    causal = j_pos <= i_pos
    j_f = j_pos.astype(F32)

    def head(h, e):
        return qkvT[(h * 3 + e) * HD:(h * 3 + e + 1) * HD, :]

    for h in range(HL):
        slope = jnp.where(t == 0, slopes[h], jnp.where(t == 1, slopes[HL + h], jnp.where(t == 2, slopes[2 * HL + h], slopes[3 * HL + h]))).astype(F32)
        s = dot(head(h, 1), head(h, 0), 0, 0) * scale + slope * j_f
        s = jnp.where(causal, s, MASK_VALUE)
        p = jnp.exp(s - jnp.max(s, axis=0, keepdims=True))
        p = p / jnp.sum(p, axis=0, keepdims=True)
        probs[h] = p
        ctx_ref[h * HD:(h + 1) * HD, :] = dot(head(h, 2), p.astype(BF), 1, 0).astype(BF)

    def exchange(part, ps, pr, hs, hr, cr):
        firsts = []
        for k in range(HCH):
            ps[k] = part((1 - core) * HCH + k).astype(BF)
            firsts.append(send(ps.at[k], pr.at[k], pt))
        outs = []
        for k in range(HCH):
            own = part(core * HCH + k)
            firsts[k].wait_recv()
            hs[k] = (own + pr[k].astype(F32)).astype(BF)
            outs.append((send(hs.at[k], cr.at[k], ct), send(hs.at[k], hr.at[k], pt)))
        return outs

    def forward(outs, cr, fr):
        fwd = []
        for k in range(HCH):
            outs[k][0].wait_recv()
            fwd.append(send(cr.at[k], fr.at[k], pt))
        return fwd

    for c in w_cps['out']:
        c.wait()
    ctxT = ctx_ref[...]
    a_outs = exchange(lambda kk: dot(ctxT, wout[kk], 0, 0), a_ps, a_pr, a_hs, a_hr, a_cr)

    y_p.wait_recv()
    y_f.wait_recv()
    for i in range(TP):
        gm_f[pl.ds(i * SL, SL), :] = gyg[i].astype(F32)
    for r in range(0, S, 32):
        gyf_ref[r:r + 32, :] = gm_f[r:r + 32, :].astype(BF)
    w_cps['dn'][0].wait()
    gyv = gyf_ref[...]
    for n in range(NCH):
        gact[:, n * CW:(n + 1) * CW] = dot(gyv, wdn[n * CW:(n + 1) * CW, :], 1, 1).astype(BF)
    vec_ref[0:1, :] = jnp.sum(gm_f[...], axis=0, keepdims=True)

    def gathered(outs, fwd, hs, hr, cr, fr, put):
        for k in range(HCH):
            put(core * HCH + k, (hs[k].astype(F32) + cr[k].astype(F32)).astype(BF).astype(F32))
        for k in range(HCH):
            outs[k][1].wait_recv()
            fwd[k].wait_recv()
            put((1 - core) * HCH + k, (hr[k].astype(F32) + fr[k].astype(F32)).astype(BF).astype(F32))

    a_fwd = forward(a_outs, a_cr, a_fr)

    def put_x(kk, val):
        cols = pl.ds(pl.multiple_of(kk * CW, CW), CW)
        xf[:, cols] = xf[:, cols] + val + bo_ref[:, cols]

    gathered(a_outs, a_fwd, a_hs, a_hr, a_cr, a_fr, put_x)

    for r in range(0, S, 32):
        cen, rstd = rows_stats(xf[r:r + 32, :])
        g_ref[r:r + 32, :] = (cen * rstd * g2_ref[...] + be2_ref[...]).astype(BF)

    w_cps['up'][0].wait()
    gv = g_ref[...]
    for n in range(NCH):
        cols = slice(n * CW, (n + 1) * CW)
        pre = dot(gv, wup[:, cols], 1, 0) + bup_ref[:, cols]
        val, der = gelu_parts(pre)
        act_ref[:, cols] = val.astype(BF)
        gp = gact[:, cols].astype(F32) * der
        vec_ref[1:2, cols] = jnp.sum(gp, axis=0, keepdims=True)
        gpre_ref[:, cols] = gp.astype(BF)

    gprev = gpre_ref[...]

    def part_g(kk):
        return dot(gprev, wup[pl.ds(pl.multiple_of(kk * CW, CW), CW), :], 1, 1)

    g_outs = exchange(part_g, b_ps, b_pr, b_hs, b_hr, b_cr)

    def scatter_first(part, buf, pr, extra=None):
        for n in range(NCH):
            cols = slice(n * CW, (n + 1) * CW)
            v = part(n)
            for i in range(TP):
                buf[i, :, cols] = v[i * SL:(i + 1) * SL, :].astype(BF)
            if extra is not None:
                extra(n, v)
        return (send(buf.at[qt], pr.at[1], pt), send(buf.at[pt], pr.at[0], pt))

    actv = act_ref[...]
    m_first = scatter_first(lambda n: dot(actv, wdn[:, n * CW:(n + 1) * CW], 1, 0), ghp.at[0], m_pr)

    g_fwd = forward(g_outs, b_cr, b_fr)

    m_first[0].wait_recv()
    m_hs[...] = (ghp[0, ct].astype(F32) + m_pr[1].astype(F32)).astype(BF)
    m_out = send(m_hs, m_cr, ct)

    def put_g(kk, val):
        gg_f[:, pl.ds(pl.multiple_of(kk * CW, CW), CW)] = val

    gathered(g_outs, g_fwd, b_hs, b_hr, b_cr, b_fr, put_g)

    gg2 = jnp.zeros((1, D), F32)
    gb2 = jnp.zeros((1, D), F32)
    gbo = jnp.zeros((1, D), F32)
    for r in range(0, S, 32):
        cen, rstd = rows_stats(xf[r:r + 32, :])
        xh = cen * rstd
        gg = gg_f[r:r + 32, :]
        gg2 = gg2 + jnp.sum(gg * xh, axis=0, keepdims=True)
        gb2 = gb2 + jnp.sum(gg, axis=0, keepdims=True)
        dxh = gg * g2_ref[...]
        m1 = jnp.mean(dxh, axis=-1, keepdims=True)
        m2 = jnp.mean(dxh * xh, axis=-1, keepdims=True)
        gm = gm_f[r:r + 32, :] + rstd * (dxh - m1 - xh * m2)
        gm_f[r:r + 32, :] = gm
        gbo = gbo + jnp.sum(gm, axis=0, keepdims=True)
        gmid_ref[r:r + 32, :] = gm.astype(BF)
    vec_ref[2:3, :] = gg2
    vec_ref[3:4, :] = gb2
    vec_ref[4:5, :] = gbo

    gmv = gmid_ref[...]
    gctxT = dot(wout[0], gmv[:, :CW], 1, 1)
    for k in range(1, NCH):
        gctxT = gctxT + dot(wout[k], gmv[:, k * CW:(k + 1) * CW], 1, 1)
    gctxT = gctxT.astype(BF)
    ones = jnp.ones((8, S), BF)
    for h in range(HL):
        go = gctxT[h * HD:(h + 1) * HD, :]
        p = probs[h]
        gp = dot(head(h, 2), go, 0, 0).astype(BF).astype(F32)
        gv_ = dot(go, p.astype(BF), 1, 1).astype(BF)
        gs = (p * (gp - jnp.sum(gp * p, axis=0, keepdims=True))).astype(BF)
        gq = (dot(head(h, 1), gs, 1, 0) * scale).astype(BF)
        gk = (dot(head(h, 0), gs, 1, 1) * scale).astype(BF)
        for e, val in enumerate((gq, gk, gv_)):
            gqkv_ref[(h * 3 + e) * HD:(h * 3 + e + 1) * HD, :] = val
            gbqkv_ref[e, h:h + 1, :] = dot(ones, val, 1, 1)[0:1, :]

    gqv = gqkv_ref[...]

    def ln1_sums(n, v):
        cols = slice(n * CW, (n + 1) * CW)
        v = v.astype(BF).astype(F32)
        ln_s[0:1, cols] = jnp.sum(v * xhat[:, cols], axis=0, keepdims=True)
        ln_s[1:2, cols] = jnp.sum(v, axis=0, keepdims=True)

    ln_s, ln_pr, ln_hs, ln_cr = ln_x.at[0], ln_x.at[1], ln_x.at[2], ln_x.at[3]
    r_first = scatter_first(lambda n: dot(gqv, wqkv[:, n * CW:(n + 1) * CW], 0, 0), ghp.at[1], r_pr, ln1_sums)
    l_first = send(ln_s, ln_pr, pt)

    r_first[0].wait_recv()
    r_hs[...] = (ghp[1, ct].astype(F32) + r_pr[1].astype(F32)).astype(BF)
    r_out = send(r_hs, r_cr, ct)
    l_first.wait_recv()
    ln_hs[...] = ln_s[...] + ln_pr[...]
    l_out = send(ln_hs, ln_cr, ct)

    own = pl.ds(pl.multiple_of(t * SL, 8), SL)
    m_first[1].wait_recv()
    m_out.wait_recv()
    m_sum = (ghp[0, t].astype(F32) + m_pr[0].astype(F32)).astype(BF).astype(F32) + m_cr[...].astype(F32)
    y_ref[...] = (xf[own, :] + m_sum.astype(BF).astype(F32) + bd_ref[...]).astype(BF)

    r_first[1].wait_recv()
    mine = (ghp[1, t].astype(F32) + r_pr[0].astype(F32)).astype(BF).astype(F32)
    r_out.wait_recv()
    gh = (mine + r_cr[...].astype(F32)).astype(BF).astype(F32)
    xh = xhat[own, :]
    dxh = gh * g1_ref[...]
    m1 = jnp.mean(dxh, axis=-1, keepdims=True)
    m2 = jnp.mean(dxh * xh, axis=-1, keepdims=True)
    gx_ref[...] = (gm_f[own, :] + rstd_s[own, 0:1] * (dxh - m1 - xh * m2)).astype(BF)
    l_out.wait_recv()
    vec_ref[6:8, :] = ln_hs[...] + ln_cr[...]
    for c in started:
        c.wait_send()


N_SEND = 38


def grads_kernel(h_ref, gqkv_ref, ctx_ref, gmid_ref, g_ref, gpre_ref, act_ref, gyf_ref, yi_ref, gxi_ref, vec_ref, gbi_ref,
                 y_ref, gx_ref, gl1_ref, bl1_ref, gwqkv_ref, gbqkv_ref, gwout_ref, gbo_ref, gl2_ref, bl2_ref,
                 gwup_ref, gbup_ref, gwdn_ref, gbd_ref, s_qkv, s_out, s_up, s_dn, sem):
    cps = []

    def out(src, dst):
        c = pltpu.make_async_copy(src, dst, sem.at[len(cps)])
        c.start()
        cps.append(c)

    y_ref[...] = yi_ref[...]
    gx_ref[...] = gxi_ref[...]
    gbqkv_ref[...] = gbi_ref[...]
    for i, r in enumerate((gbd_ref, gbup_ref, gl2_ref, bl2_ref, gbo_ref, None, gl1_ref, bl1_ref)):
        if r is not None:
            r[...] = vec_ref[i, :]

    gyv = gyf_ref[...]
    gpv = gpre_ref[...]
    for n in range(NCH):
        rows = pl.ds(n * CW, CW)
        s_dn[rows, :] = dot(act_ref[:, n * CW:(n + 1) * CW], gyv, 0, 0).astype(BF)
        out(s_dn.at[rows], gwdn_ref.at[rows])
    for n in range(NCH):
        rows = pl.ds(n * CW, CW)
        s_up[rows, :] = dot(g_ref[:, n * CW:(n + 1) * CW], gpv, 0, 0).astype(BF)
        out(s_up.at[rows], gwup_ref.at[rows])
    hv = h_ref[...]
    for n in range(HL):
        rows = pl.ds(n * 3 * HD, 3 * HD)
        s_qkv[rows, :] = dot(gqkv_ref[n * 3 * HD:(n + 1) * 3 * HD, :], hv, 1, 0).astype(BF)
        out(s_qkv.at[rows], gwqkv_ref.at[rows])
    s_out[...] = dot(ctx_ref[...], gmid_ref[...], 1, 0).astype(BF)
    out(s_out, gwout_ref)
    for c in cps:
        c.wait()


def solution(mesh):
    VM = pl.BlockSpec(memory_space=pltpu.VMEM)
    ANY = pl.BlockSpec(memory_space=pltpu.HBM)

    def sds(shape, dt):
        return jax.ShapeDtypeStruct(shape, dt)

    def local_step(x, g1, be1, w_qkv, b_qkv, w_out, b_out, g2, be2, w_up, b_up, w_down, b_down, grad_y):
        wq = jnp.transpose(w_qkv, (1, 2, 3, 0)).reshape(3 * HL * HD, D)
        bq = jnp.transpose(b_qkv, (1, 0, 2))
        half = pltpu.VMEM((HCH, S, CW), BF)
        mids = pl.pallas_call(
            block_kernel,
            out_shape=(sds((SL, D), BF), sds((SL, D), BF), sds((8, D), F32), sds((3, HL, HD), F32), sds((S, D), BF),
                       sds((3 * HL * HD, S), BF), sds((HL * HD, S), BF), sds((S, D), BF), sds((S, D), BF), sds((S, FL), BF),
                       sds((S, FL), BF), sds((S, D), BF)),
            in_specs=[VM] * 10 + [ANY] * 4,
            out_specs=(VM,) * 12,
            scratch_shapes=[
                pltpu.VMEM((3 * HL * HD, D), BF), pltpu.VMEM((NCH, HL * HD, CW), BF), pltpu.VMEM((D, FL), BF), pltpu.VMEM((FL, D), BF),
                pltpu.VMEM((TP, SL, D), BF), pltpu.VMEM((TP, SL, D), BF), pltpu.VMEM((S, D), F32), pltpu.VMEM((S, D), F32),
                pltpu.VMEM((S, 128), F32), pltpu.VMEM((3 * HL * HD, S), F32), pltpu.VMEM((3 * HL * HD, S), BF), pltpu.VMEM((HL, S, S), F32),
                half, half, half, half, half, half, half, half, half, half, half, half,
                pltpu.VMEM((S, FL), BF), pltpu.VMEM((2, TP, SL, D), BF),
                pltpu.VMEM((2, SL, D), BF), pltpu.VMEM((SL, D), BF), pltpu.VMEM((SL, D), BF),
                pltpu.VMEM((2, SL, D), BF), pltpu.VMEM((SL, D), BF), pltpu.VMEM((SL, D), BF),
                pltpu.VMEM((S, D), F32), pltpu.VMEM((4, 2, D), F32), pltpu.VMEM((S, D), F32), pltpu.VMEM((8, D), F32),
                pltpu.SemaphoreType.DMA((9,)), pltpu.SemaphoreType.DMA((N_SEND,)), pltpu.SemaphoreType.DMA((N_SEND,)),
            ],
            compiler_params=pltpu.CompilerParams(collective_id=0, has_side_effects=True, vmem_limit_bytes=61 * 2**20),
            name='block',
        )(x.reshape(SL, D), grad_y.reshape(SL, D), g1, be1, g2, be2, b_out, b_down, bq, b_up,
          wq, w_out, w_up, w_down)
        y, gx, vec, gb, h, gqkv, ctx, gmid, g, gpre, act, gyf = mids
        vec1 = sds((D,), F32)
        outs = pl.pallas_call(
            grads_kernel,
            out_shape=(sds((SL, D), BF), sds((SL, D), BF), vec1, vec1, sds((3 * HL * HD, D), BF), sds((3, HL, HD), F32),
                       sds((HL * HD, D), BF), vec1, vec1, vec1, sds((D, FL), BF), vec1, sds((FL, D), BF), vec1),
            in_specs=[VM] * 12,
            out_specs=(VM, VM, VM, VM, ANY, VM, ANY, VM, VM, VM, ANY, VM, ANY, VM),
            scratch_shapes=[pltpu.VMEM((3 * HL * HD, D), BF), pltpu.VMEM((HL * HD, D), BF), pltpu.VMEM((D, FL), BF), pltpu.VMEM((FL, D), BF),
                            pltpu.SemaphoreType.DMA((32,))],
            compiler_params=pltpu.CompilerParams(vmem_limit_bytes=22 * 2**20),
            name='grads',
        )(h, gqkv, ctx, gmid, g, gpre, act, gyf, y, gx, vec, gb)
        (y, gx, gl1, bl1, gwqkv, gbqkv, gwout, gbo, gl2, bl2, gwup, gbup, gwdn, gbd) = outs
        gwqkv = jnp.transpose(gwqkv.reshape(HL, 3, HD, D), (3, 0, 1, 2))
        gbqkv = jnp.transpose(gbqkv, (1, 0, 2))
        return (y.reshape(1, SL, D), gx.reshape(1, SL, D), gl1, bl1, gwqkv, gbqkv, gwout, gbo, gl2, bl2, gwup, gbup, gwdn, gbd)

    row_spec = P('dp', 'tp', None)
    in_specs = (row_spec, P(), P(), P(None, 'tp', None, None), P('tp', None, None), P('tp', None), P(), P(), P(),
                P(None, 'tp'), P('tp'), P('tp', None), P(), row_spec)
    out_specs = (row_spec, row_spec, P('dp'), P('dp'), P('dp', 'tp', None, None), P(('dp', 'tp'), None, None),
                 P(('dp', 'tp'), None), P('dp'), P('dp'), P('dp'), P('dp', 'tp'), P(('dp', 'tp')), P(('dp', 'tp'), None), P('dp'))
    return jax.shard_map(local_step, mesh=mesh, in_specs=in_specs, out_specs=out_specs, check_vma=False)
```

```python
import functools
import math

import jax
import jax.numpy as jnp
from jax import lax
from jax.experimental import pallas as pl
from jax.experimental.pallas import tpu as pltpu
from jax.sharding import PartitionSpec as P

EPS = 1e-5
MASK_VALUE = -1e30
BF = jnp.bfloat16
F32 = jnp.float32
MESH = pl.DeviceIdType.MESH

D = 1536
S = 96
SL = 24
TP = 4
HL = 4
HD = 96
FL = 1536
CW = 256
NCH = D // CW
HCH = NCH // 2


def alibi_slopes(n_heads):
    closest = 2 ** int(math.floor(math.log2(n_heads)))
    base_ratio = 2.0 ** (-8.0 / closest)
    extra_ratio = 2.0 ** (-4.0 / closest)
    remaining = min(closest, n_heads - closest)
    slopes = [base_ratio ** (i + 1) for i in range(closest)]
    return slopes + [extra_ratio ** (2 * i + 1) for i in range(remaining)]


def dot(a, b, ca, cb):
    return lax.dot_general(a, b, (((ca,), (cb,)), ((), ())), preferred_element_type=F32)


def gelu_parts(u):
    k = math.sqrt(2.0 / math.pi)
    u2 = u * u
    th = jnp.tanh(k * (u + 0.044715 * (u2 * u)))
    half = 0.5 * (1.0 + th)
    dk = k * (1.0 + 3.0 * 0.044715 * u2)
    return u * half, half + 0.5 * u * (1.0 - th * th) * dk


def rows_stats(v):
    mean = jnp.mean(v, axis=-1, keepdims=True)
    cen = v - mean
    var = jnp.mean(cen * cen, axis=-1, keepdims=True)
    return cen, lax.rsqrt(var + EPS)


def block_kernel(x_hbm, gy_hbm, g1_hbm, be1_hbm, g2_hbm, be2_hbm, bo_hbm, bd_hbm, bqkv_hbm, bup_hbm,
                 wqkv_hbm, wout_hbm, wup_hbm, wdn_hbm,
                 y_ref, gx_ref, vec_ref, gbqkv_ref, gwqkv_ref, gwout_ref, gwup_ref, gwdn_ref,
                 h_ref, gqkv_ref, ctx_ref, gmid_ref, g_ref, gpre_ref, act_ref, gyf_ref,
                 wqkv, wout, wup, wdn, xg, gyg, xf, xhat, rstd_s, biasT, qkvT, probs,
                 a_ps, a_pr, a_hs, a_hr, a_cr, a_fr, b_ps, b_pr, b_hs, b_hr, b_cr, b_fr,
                 gact, ghp, m_pr, m_hs, m_cr, r_pr, r_hs, r_cr, gm_f, ln_x, gg_f, par, bqkv_ref, g1_in, be1_in, g2_in, be2_in, bo_in, bd_in, bup_in,
                 wsem, ssem, rsem, isem):
    t = lax.axis_index('tp')
    core = t % 2
    pt = t + 1 - 2 * core
    ct = (t + 2) % TP
    qt = (pt + 2) % TP

    started = []
    counter = [0]

    def send(src, dst, dev):
        i = counter[0]
        counter[0] += 1
        c = pltpu.make_async_remote_copy(src_ref=src, dst_ref=dst, send_sem=ssem.at[i], recv_sem=rsem.at[i],
                                         device_id={'tp': dev}, device_id_type=MESH)
        c.start()
        started.append(c)
        return c

    in_x = pltpu.make_async_copy(x_hbm, xg.at[t], isem.at[0])
    in_gy = pltpu.make_async_copy(gy_hbm, gyg.at[t], isem.at[1])
    in_b = pltpu.make_async_copy(bqkv_hbm, bqkv_ref, isem.at[2])
    small = ((g1_hbm, g1_in), (be1_hbm, be1_in), (g2_hbm, g2_in), (be2_hbm, be2_in), (bo_hbm, bo_in), (bd_hbm, bd_in), (bup_hbm, bup_in))
    in_p = [pltpu.make_async_copy(a, b, isem.at[3 + i]) for i, (a, b) in enumerate(small)]
    for c in (in_x, in_gy, in_b, *in_p):
        c.start()
    w_cps = {}
    w_cps['qkv'] = [pltpu.make_async_copy(wqkv_hbm, wqkv, wsem.at[0])]
    w_cps['out'] = [pltpu.make_async_copy(wout_hbm.at[:, pl.ds(k * CW, CW)], wout.at[k], wsem.at[1 + k]) for k in range(NCH)]
    w_cps['dn'] = [pltpu.make_async_copy(wdn_hbm, wdn, wsem.at[7])]
    w_cps['up'] = [pltpu.make_async_copy(wup_hbm, wup, wsem.at[8])]

    barrier = pltpu.get_barrier_semaphore()
    for dev in (pt, ct):
        pl.semaphore_signal(barrier, inc=1, device_id={'tp': dev}, device_id_type=MESH)
    for name in ('qkv', 'out', 'dn', 'up'):
        for c in w_cps[name]:
            c.start()
    pl.semaphore_wait(barrier, 2)

    in_x.wait()
    x_c = send(xg.at[t], xg.at[t], ct)
    x_p = send(xg.at[t], xg.at[t], pt)
    in_gy.wait()
    y_c = send(gyg.at[t], gyg.at[t], ct)
    y_p = send(gyg.at[t], gyg.at[t], pt)

    for c in (in_b, *in_p):
        c.wait()
    for i, r in enumerate((g1_in, be1_in, g2_in, be2_in, bo_in, bd_in, bup_in)):
        par[i, :] = r[...]
    g1_ref, be1_ref, g2_ref, be2_ref, bo_ref, bd_ref, bup_ref = (par.at[i:i + 1] for i in range(7))

    for h in range(HL):
        for e in range(3):
            row = jnp.broadcast_to(bqkv_ref[e, h:h + 1, :], (S, HD))
            biasT[pl.ds((h * 3 + e) * HD, HD), :] = row.T

    x_c.wait_recv()
    x_f = send(xg.at[ct], xg.at[ct], pt)
    x_p.wait_recv()
    x_f.wait_recv()

    for i in range(TP):
        xf[pl.ds(i * SL, SL), :] = xg[i].astype(F32)
    for r in range(0, S, 32):
        cen, rstd = rows_stats(xf[r:r + 32, :])
        xh = cen * rstd
        xhat[r:r + 32, :] = xh
        rstd_s[r:r + 32, :] = jnp.broadcast_to(rstd, (32, 128))
        h_ref[r:r + 32, :] = (xh * g1_ref[...] + be1_ref[...]).astype(BF)

    y_c.wait_recv()
    y_f = send(gyg.at[ct], gyg.at[ct], pt)

    w_cps['qkv'][0].wait()
    hv = h_ref[...]
    for h in range(HL):
        rows = slice(h * 3 * HD, (h + 1) * 3 * HD)
        qkvT[rows, :] = (dot(wqkv[rows, :], hv, 1, 1) + biasT[rows, :]).astype(BF)

    scale = HD ** -0.5
    slopes = alibi_slopes(HL * TP)
    j_pos = lax.broadcasted_iota(jnp.int32, (S, S), 0)
    i_pos = lax.broadcasted_iota(jnp.int32, (S, S), 1)
    causal = j_pos <= i_pos
    j_f = j_pos.astype(F32)

    def head(h, e):
        return qkvT[(h * 3 + e) * HD:(h * 3 + e + 1) * HD, :]

    for h in range(HL):
        slope = jnp.where(t == 0, slopes[h], jnp.where(t == 1, slopes[HL + h], jnp.where(t == 2, slopes[2 * HL + h], slopes[3 * HL + h]))).astype(F32)
        s = dot(head(h, 1), head(h, 0), 0, 0) * scale + slope * j_f
        s = jnp.where(causal, s, MASK_VALUE)
        p = jnp.exp(s - jnp.max(s, axis=0, keepdims=True))
        p = p / jnp.sum(p, axis=0, keepdims=True)
        probs[h] = p
        ctx_ref[h * HD:(h + 1) * HD, :] = dot(head(h, 2), p.astype(BF), 1, 0).astype(BF)

    def exchange(part, ps, pr, hs, hr, cr):
        firsts = []
        for k in range(HCH):
            ps[k] = part((1 - core) * HCH + k).astype(BF)
            firsts.append(send(ps.at[k], pr.at[k], pt))
        outs = []
        for k in range(HCH):
            own = part(core * HCH + k)
            firsts[k].wait_recv()
            hs[k] = (own + pr[k].astype(F32)).astype(BF)
            outs.append((send(hs.at[k], cr.at[k], ct), send(hs.at[k], hr.at[k], pt)))
        return outs

    def forward(outs, cr, fr):
        fwd = []
        for k in range(HCH):
            outs[k][0].wait_recv()
            fwd.append(send(cr.at[k], fr.at[k], pt))
        return fwd

    for c in w_cps['out']:
        c.wait()
    ctxT = ctx_ref[...]
    a_outs = exchange(lambda kk: dot(ctxT, wout[kk], 0, 0), a_ps, a_pr, a_hs, a_hr, a_cr)

    y_p.wait_recv()
    y_f.wait_recv()
    for i in range(TP):
        gm_f[pl.ds(i * SL, SL), :] = gyg[i].astype(F32)
    for r in range(0, S, 32):
        gyf_ref[r:r + 32, :] = gm_f[r:r + 32, :].astype(BF)
    w_cps['dn'][0].wait()
    gyv = gyf_ref[...]
    for n in range(NCH):
        gact[:, n * CW:(n + 1) * CW] = dot(gyv, wdn[n * CW:(n + 1) * CW, :], 1, 1).astype(BF)
    vec_ref[0:1, :] = jnp.sum(gm_f[...], axis=0, keepdims=True)

    def gathered(outs, fwd, hs, hr, cr, fr, put):
        for k in range(HCH):
            put(core * HCH + k, (hs[k].astype(F32) + cr[k].astype(F32)).astype(BF).astype(F32))
        for k in range(HCH):
            outs[k][1].wait_recv()
            fwd[k].wait_recv()
            put((1 - core) * HCH + k, (hr[k].astype(F32) + fr[k].astype(F32)).astype(BF).astype(F32))

    a_fwd = forward(a_outs, a_cr, a_fr)

    def put_x(kk, val):
        cols = pl.ds(pl.multiple_of(kk * CW, CW), CW)
        xf[:, cols] = xf[:, cols] + val + bo_ref[:, cols]

    gathered(a_outs, a_fwd, a_hs, a_hr, a_cr, a_fr, put_x)

    for r in range(0, S, 32):
        cen, rstd = rows_stats(xf[r:r + 32, :])
        g_ref[r:r + 32, :] = (cen * rstd * g2_ref[...] + be2_ref[...]).astype(BF)

    w_cps['up'][0].wait()
    gv = g_ref[...]
    for n in range(NCH):
        cols = slice(n * CW, (n + 1) * CW)
        pre = dot(gv, wup[:, cols], 1, 0) + bup_ref[:, cols]
        val, der = gelu_parts(pre)
        act_ref[:, cols] = val.astype(BF)
        gp = gact[:, cols].astype(F32) * der
        vec_ref[1:2, cols] = jnp.sum(gp, axis=0, keepdims=True)
        gpre_ref[:, cols] = gp.astype(BF)

    gprev = gpre_ref[...]

    def part_g(kk):
        return dot(gprev, wup[pl.ds(pl.multiple_of(kk * CW, CW), CW), :], 1, 1)

    g_outs = exchange(part_g, b_ps, b_pr, b_hs, b_hr, b_cr)

    def scatter_first(part, buf, pr, extra=None):
        for n in range(NCH):
            cols = slice(n * CW, (n + 1) * CW)
            v = part(n)
            for i in range(TP):
                buf[i, :, cols] = v[i * SL:(i + 1) * SL, :].astype(BF)
            if extra is not None:
                extra(n, v)
        return (send(buf.at[qt], pr.at[1], pt), send(buf.at[pt], pr.at[0], pt))

    actv = act_ref[...]
    m_first = scatter_first(lambda n: dot(actv, wdn[:, n * CW:(n + 1) * CW], 1, 0), ghp.at[0], m_pr)

    for n in range(NCH):
        gwdn_ref[n * CW:(n + 1) * CW, :] = dot(act_ref[:, n * CW:(n + 1) * CW], gyv, 0, 0).astype(BF)

    m_first[0].wait_recv()
    m_hs[...] = (ghp[0, ct].astype(F32) + m_pr[1].astype(F32)).astype(BF)
    m_out = send(m_hs, m_cr, ct)
    g_fwd = []
    for k in range(HCH):
        g_outs[k][0].wait_recv()
        g_fwd.append(send(b_cr.at[k], b_fr.at[k], pt))
        for n in range(2 * k, 2 * k + 2):
            gwup_ref[n * CW:(n + 1) * CW, :] = dot(g_ref[:, n * CW:(n + 1) * CW], gprev, 0, 0).astype(BF)

    def put_g(kk, val):
        gg_f[:, pl.ds(pl.multiple_of(kk * CW, CW), CW)] = val

    gathered(g_outs, g_fwd, b_hs, b_hr, b_cr, b_fr, put_g)

    gg2 = jnp.zeros((1, D), F32)
    gb2 = jnp.zeros((1, D), F32)
    gbo = jnp.zeros((1, D), F32)
    for r in range(0, S, 32):
        cen, rstd = rows_stats(xf[r:r + 32, :])
        xh = cen * rstd
        gg = gg_f[r:r + 32, :]
        gg2 = gg2 + jnp.sum(gg * xh, axis=0, keepdims=True)
        gb2 = gb2 + jnp.sum(gg, axis=0, keepdims=True)
        dxh = gg * g2_ref[...]
        m1 = jnp.mean(dxh, axis=-1, keepdims=True)
        m2 = jnp.mean(dxh * xh, axis=-1, keepdims=True)
        gm = gm_f[r:r + 32, :] + rstd * (dxh - m1 - xh * m2)
        gm_f[r:r + 32, :] = gm
        gbo = gbo + jnp.sum(gm, axis=0, keepdims=True)
        gmid_ref[r:r + 32, :] = gm.astype(BF)
    vec_ref[2:3, :] = gg2
    vec_ref[3:4, :] = gb2
    vec_ref[4:5, :] = gbo

    gmv = gmid_ref[...]
    gctxT = dot(wout[0], gmv[:, :CW], 1, 1)
    for k in range(1, NCH):
        gctxT = gctxT + dot(wout[k], gmv[:, k * CW:(k + 1) * CW], 1, 1)
    gctxT = gctxT.astype(BF)
    ones = jnp.ones((8, S), BF)
    for h in range(HL):
        go = gctxT[h * HD:(h + 1) * HD, :]
        p = probs[h]
        gp = dot(head(h, 2), go, 0, 0).astype(BF).astype(F32)
        gv_ = dot(go, p.astype(BF), 1, 1).astype(BF)
        gs = (p * (gp - jnp.sum(gp * p, axis=0, keepdims=True))).astype(BF)
        gq = (dot(head(h, 1), gs, 1, 0) * scale).astype(BF)
        gk = (dot(head(h, 0), gs, 1, 1) * scale).astype(BF)
        for e, val in enumerate((gq, gk, gv_)):
            gqkv_ref[(h * 3 + e) * HD:(h * 3 + e + 1) * HD, :] = val
            gbqkv_ref[e, h:h + 1, :] = dot(ones, val, 1, 1)[0:1, :]

    gqv = gqkv_ref[...]

    def ln1_sums(n, v):
        cols = slice(n * CW, (n + 1) * CW)
        v = v.astype(BF).astype(F32)
        ln_s[0:1, cols] = jnp.sum(v * xhat[:, cols], axis=0, keepdims=True)
        ln_s[1:2, cols] = jnp.sum(v, axis=0, keepdims=True)

    ln_s, ln_pr, ln_hs, ln_cr = ln_x.at[0], ln_x.at[1], ln_x.at[2], ln_x.at[3]
    r_first = scatter_first(lambda n: dot(gqv, wqkv[:, n * CW:(n + 1) * CW], 0, 0), ghp.at[1], r_pr, ln1_sums)
    l_first = send(ln_s, ln_pr, pt)

    r_first[0].wait_recv()
    r_hs[...] = (ghp[1, ct].astype(F32) + r_pr[1].astype(F32)).astype(BF)
    r_out = send(r_hs, r_cr, ct)
    l_first.wait_recv()
    ln_hs[...] = ln_s[...] + ln_pr[...]
    l_out = send(ln_hs, ln_cr, ct)

    gwout_ref[...] = dot(ctx_ref[...], gmv, 1, 0).astype(BF)
    for h in range(HL):
        rows = slice(h * 3 * HD, (h + 1) * 3 * HD)
        gwqkv_ref[rows, :] = dot(gqkv_ref[rows, :], h_ref[...], 1, 0).astype(BF)
    own = pl.ds(pl.multiple_of(t * SL, 8), SL)
    m_first[1].wait_recv()
    m_out.wait_recv()
    m_sum = (ghp[0, t].astype(F32) + m_pr[0].astype(F32)).astype(BF).astype(F32) + m_cr[...].astype(F32)
    y_ref[...] = (xf[own, :] + m_sum.astype(BF).astype(F32) + bd_ref[...]).astype(BF)

    r_first[1].wait_recv()
    mine = (ghp[1, t].astype(F32) + r_pr[0].astype(F32)).astype(BF).astype(F32)
    r_out.wait_recv()
    gh = (mine + r_cr[...].astype(F32)).astype(BF).astype(F32)
    xh = xhat[own, :]
    dxh = gh * g1_ref[...]
    m1 = jnp.mean(dxh, axis=-1, keepdims=True)
    m2 = jnp.mean(dxh * xh, axis=-1, keepdims=True)
    gx_ref[...] = (gm_f[own, :] + rstd_s[own, 0:1] * (dxh - m1 - xh * m2)).astype(BF)
    l_out.wait_recv()
    vec_ref[6:8, :] = ln_hs[...] + ln_cr[...]
    for c in started:
        c.wait_send()


N_SEND = 38
VMEM_A = 34 * 2**20
VMEM_B = 8 * 2**20


def write_kernel(yi_ref, gxi_ref, vec_ref, gbi_ref, qkv_ref, out_ref, up_ref, dn_ref,
                 y_ref, gx_ref, gl1_ref, bl1_ref, gwqkv_ref, gbqkv_ref, gwout_ref, gbo_ref, gl2_ref, bl2_ref,
                 gwup_ref, gbup_ref, gwdn_ref, gbd_ref, sem):
    cps = []
    for src, dst in ((dn_ref, gwdn_ref), (up_ref, gwup_ref), (qkv_ref, gwqkv_ref), (out_ref, gwout_ref)):
        rows = src.shape[0] // 4
        for k in range(4):
            part = pl.ds(k * rows, rows)
            c = pltpu.make_async_copy(src.at[part], dst.at[part], sem.at[len(cps)])
            c.start()
            cps.append(c)
    y_ref[...] = yi_ref[...]
    gx_ref[...] = gxi_ref[...]
    gbqkv_ref[...] = gbi_ref[...]
    for i, r in enumerate((gbd_ref, gbup_ref, gl2_ref, bl2_ref, gbo_ref, None, gl1_ref, bl1_ref)):
        if r is not None:
            r[...] = vec_ref[i, :]
    for c in cps:
        c.wait()


def solution(mesh):
    VM = pl.BlockSpec(memory_space=pltpu.VMEM)
    ANY = pl.BlockSpec(memory_space=pltpu.HBM)

    def sds(shape, dt):
        return jax.ShapeDtypeStruct(shape, dt)

    def local_step(x, g1, be1, w_qkv, b_qkv, w_out, b_out, g2, be2, w_up, b_up, w_down, b_down, grad_y):
        wq = jnp.transpose(w_qkv, (1, 2, 3, 0)).reshape(3 * HL * HD, D)
        bq = jnp.transpose(b_qkv, (1, 0, 2))
        half = pltpu.VMEM((HCH, S, CW), BF)
        mids = pl.pallas_call(
            block_kernel,
            out_shape=(pltpu.VMEM((SL, D), BF), pltpu.VMEM((SL, D), BF), pltpu.VMEM((8, D), F32), pltpu.VMEM((3, HL, HD), F32),
                       pltpu.VMEM((3 * HL * HD, D), BF), pltpu.VMEM((HL * HD, D), BF), pltpu.VMEM((D, FL), BF), pltpu.VMEM((FL, D), BF)),
            in_specs=[ANY] * 14,
            out_specs=(VM,) * 8,
            scratch_shapes=[
                pltpu.VMEM((S, D), BF), pltpu.VMEM((3 * HL * HD, S), BF), pltpu.VMEM((HL * HD, S), BF), pltpu.VMEM((S, D), BF),
                pltpu.VMEM((S, D), BF), pltpu.VMEM((S, FL), BF), pltpu.VMEM((S, FL), BF), pltpu.VMEM((S, D), BF),
                pltpu.VMEM((3 * HL * HD, D), BF), pltpu.VMEM((NCH, HL * HD, CW), BF), pltpu.VMEM((D, FL), BF), pltpu.VMEM((FL, D), BF),
                pltpu.VMEM((TP, SL, D), BF), pltpu.VMEM((TP, SL, D), BF), pltpu.VMEM((S, D), F32), pltpu.VMEM((S, D), F32),
                pltpu.VMEM((S, 128), F32), pltpu.VMEM((3 * HL * HD, S), F32), pltpu.VMEM((3 * HL * HD, S), BF), pltpu.VMEM((HL, S, S), F32),
                half, half, half, half, half, half, half, half, half, half, half, half,
                pltpu.VMEM((S, FL), BF), pltpu.VMEM((2, TP, SL, D), BF),
                pltpu.VMEM((2, SL, D), BF), pltpu.VMEM((SL, D), BF), pltpu.VMEM((SL, D), BF),
                pltpu.VMEM((2, SL, D), BF), pltpu.VMEM((SL, D), BF), pltpu.VMEM((SL, D), BF),
                pltpu.VMEM((S, D), F32), pltpu.VMEM((4, 2, D), F32), pltpu.VMEM((S, D), F32), pltpu.VMEM((8, D), F32),
                pltpu.VMEM((3, HL, HD), F32), *[pltpu.VMEM((D,), F32) for _ in range(7)],
                pltpu.SemaphoreType.DMA((9,)), pltpu.SemaphoreType.DMA((N_SEND,)), pltpu.SemaphoreType.DMA((N_SEND,)),
                pltpu.SemaphoreType.DMA((10,)),
            ],
            compiler_params=pltpu.CompilerParams(collective_id=0, has_side_effects=True, vmem_limit_bytes=VMEM_A),
            name='block',
        )(*(pltpu.with_memory_space_constraint(v, pltpu.HBM) for v in (
            x.reshape(SL, D), grad_y.reshape(SL, D), g1, be1, g2, be2, b_out, b_down, bq, b_up, wq, w_out, w_up, w_down)))
        vec1 = sds((D,), F32)
        outs = pl.pallas_call(
            write_kernel,
            out_shape=(sds((SL, D), BF), sds((SL, D), BF), vec1, vec1, sds((3 * HL * HD, D), BF), sds((3, HL, HD), F32),
                       sds((HL * HD, D), BF), vec1, vec1, vec1, sds((D, FL), BF), vec1, sds((FL, D), BF), vec1),
            in_specs=[VM] * 8,
            out_specs=(VM, VM, VM, VM, ANY, VM, ANY, VM, VM, VM, ANY, VM, ANY, VM),
            scratch_shapes=[pltpu.SemaphoreType.DMA((16,))],
            compiler_params=pltpu.CompilerParams(vmem_limit_bytes=VMEM_B),
            name='write',
        )(*mids)
        (y, gx, gl1, bl1, gwqkv, gbqkv, gwout, gbo, gl2, bl2, gwup, gbup, gwdn, gbd) = outs
        gwqkv = jnp.transpose(gwqkv.reshape(HL, 3, HD, D), (3, 0, 1, 2))
        gbqkv = jnp.transpose(gbqkv, (1, 0, 2))
        return (y.reshape(1, SL, D), gx.reshape(1, SL, D), gl1, bl1, gwqkv, gbqkv, gwout, gbo, gl2, bl2, gwup, gbup, gwdn, gbd)

    row_spec = P('dp', 'tp', None)
    in_specs = (row_spec, P(), P(), P(None, 'tp', None, None), P('tp', None, None), P('tp', None), P(), P(), P(),
                P(None, 'tp'), P('tp'), P('tp', None), P(), row_spec)
    out_specs = (row_spec, row_spec, P('dp'), P('dp'), P('dp', 'tp', None, None), P(('dp', 'tp'), None, None),
                 P(('dp', 'tp'), None), P('dp'), P('dp'), P('dp'), P('dp', 'tp'), P(('dp', 'tp')), P(('dp', 'tp'), None), P('dp'))
    return jax.shard_map(local_step, mesh=mesh, in_specs=in_specs, out_specs=out_specs, check_vma=False)
```

```python
import functools
import math

import jax
import jax.numpy as jnp
from jax import lax
from jax.experimental import pallas as pl
from jax.experimental.pallas import tpu as pltpu
from jax.sharding import PartitionSpec as P

EPS = 1e-5
MASK_VALUE = -1e30
BF = jnp.bfloat16
F32 = jnp.float32
MESH = pl.DeviceIdType.MESH

D = 1536
S = 96
SL = 24
TP = 4
HL = 4
HD = 96
FL = 1536
CW = 256
NCH = D // CW
HCH = NCH // 2
HW = D // 2


def alibi_slopes(n_heads):
    closest = 2 ** int(math.floor(math.log2(n_heads)))
    base_ratio = 2.0 ** (-8.0 / closest)
    extra_ratio = 2.0 ** (-4.0 / closest)
    remaining = min(closest, n_heads - closest)
    slopes = [base_ratio ** (i + 1) for i in range(closest)]
    return slopes + [extra_ratio ** (2 * i + 1) for i in range(remaining)]


def dot(a, b, ca, cb):
    return lax.dot_general(a, b, (((ca,), (cb,)), ((), ())), preferred_element_type=F32)


def gelu_parts(u):
    k = math.sqrt(2.0 / math.pi)
    u2 = u * u
    th = jnp.tanh(k * (u + 0.044715 * (u2 * u)))
    half = 0.5 * (1.0 + th)
    dk = k * (1.0 + 3.0 * 0.044715 * u2)
    return u * half, half + 0.5 * u * (1.0 - th * th) * dk


def rows_stats(v):
    mean = jnp.mean(v, axis=-1, keepdims=True)
    cen = v - mean
    var = jnp.mean(cen * cen, axis=-1, keepdims=True)
    return cen, lax.rsqrt(var + EPS)


def block_kernel(x_hbm, gy_hbm, g1_hbm, be1_hbm, g2_hbm, be2_hbm, bo_hbm, bd_hbm, bqkv_hbm, bup_hbm,
                 wqkv_hbm, wout_hbm, wup_hbm, wdn_hbm,
                 y_ref, gx_ref, vec_ref, gbqkv_ref, gwqkv_ref, gwout_ref, gwup_ref, gwdn_ref,
                 h_ref, gqkv_ref, ctx_ref, gmid_ref, g_ref, gpre_ref, act_ref, gyf_ref,
                 wqkv, wout, wup, wdn, xg, gyg, xf, xhat, rstd_s, biasT, qkvT, probs,
                 a_ps, a_pr, a_hs, a_hr, a_cr, a_fr, b_ps, b_pr, b_hs, b_hr, b_cr, b_fr,
                 gact, ghp, m_pr, m_hs, m_cr, r_pr, r_hs, r_cr, gm_f, ln_x, gg_f, par, bqkv_ref, g1_in, be1_in, g2_in, be2_in, bo_in, bd_in, bup_in,
                 wsem, ssem, rsem, isem):
    t = lax.axis_index('tp')
    core = t % 2
    pt = t + 1 - 2 * core
    ct = TP - 1 - t
    qt = TP - 1 - pt
    half = (core + t // 2) % 2

    started = []
    counter = [0]

    def send(src, dst, dev):
        i = counter[0]
        counter[0] += 1
        c = pltpu.make_async_remote_copy(src_ref=src, dst_ref=dst, send_sem=ssem.at[i], recv_sem=rsem.at[i],
                                         device_id={'tp': dev}, device_id_type=MESH)
        c.start()
        started.append(c)
        return c

    in_x = pltpu.make_async_copy(x_hbm, xg.at[t], isem.at[0])
    in_gy = pltpu.make_async_copy(gy_hbm, gyg.at[t], isem.at[1])
    in_b = pltpu.make_async_copy(bqkv_hbm, bqkv_ref, isem.at[2])
    small = ((g1_hbm, g1_in), (be1_hbm, be1_in), (g2_hbm, g2_in), (be2_hbm, be2_in), (bo_hbm, bo_in), (bd_hbm, bd_in), (bup_hbm, bup_in))
    in_p = [pltpu.make_async_copy(a, b, isem.at[3 + i]) for i, (a, b) in enumerate(small)]
    for c in (in_x, in_gy, in_b, *in_p):
        c.start()
    w_cps = {}
    w_cps['qkv'] = [pltpu.make_async_copy(wqkv_hbm, wqkv, wsem.at[0])]
    w_cps['out'] = [pltpu.make_async_copy(wout_hbm.at[:, pl.ds(k * HW, HW)], wout.at[k], wsem.at[1 + k]) for k in range(2)]
    w_cps['dn'] = [pltpu.make_async_copy(wdn_hbm, wdn, wsem.at[7])]
    w_cps['up'] = [pltpu.make_async_copy(wup_hbm, wup, wsem.at[8])]

    barrier = pltpu.get_barrier_semaphore()
    for dev in (pt, ct):
        pl.semaphore_signal(barrier, inc=1, device_id={'tp': dev}, device_id_type=MESH)
    for name in ('qkv', 'out', 'dn', 'up'):
        for c in w_cps[name]:
            c.start()
    pl.semaphore_wait(barrier, 2)

    in_x.wait()
    x_c = send(xg.at[t], xg.at[t], ct)
    x_p = send(xg.at[t], xg.at[t], pt)
    in_gy.wait()
    y_c = send(gyg.at[t], gyg.at[t], ct)
    y_p = send(gyg.at[t], gyg.at[t], pt)

    for c in (in_b, *in_p):
        c.wait()
    for i, r in enumerate((g1_in, be1_in, g2_in, be2_in, bo_in, bd_in, bup_in)):
        par[i, :] = r[...]
    g1_ref, be1_ref, g2_ref, be2_ref, bo_ref, bd_ref, bup_ref = (par.at[i:i + 1] for i in range(7))

    for h in range(HL):
        for e in range(3):
            row = jnp.broadcast_to(bqkv_ref[e, h:h + 1, :], (S, HD))
            biasT[pl.ds((h * 3 + e) * HD, HD), :] = row.T

    x_c.wait_recv()
    x_f = send(xg.at[ct], xg.at[ct], pt)
    x_p.wait_recv()
    x_f.wait_recv()

    for i in range(TP):
        xf[pl.ds(i * SL, SL), :] = xg[i].astype(F32)
    for r in range(0, S, 32):
        cen, rstd = rows_stats(xf[r:r + 32, :])
        xh = cen * rstd
        xhat[r:r + 32, :] = xh
        rstd_s[r:r + 32, :] = jnp.broadcast_to(rstd, (32, 128))
        h_ref[r:r + 32, :] = (xh * g1_ref[...] + be1_ref[...]).astype(BF)

    y_c.wait_recv()
    y_f = send(gyg.at[ct], gyg.at[ct], pt)

    w_cps['qkv'][0].wait()
    hv = h_ref[...]
    for h in range(HL):
        rows = slice(h * 3 * HD, (h + 1) * 3 * HD)
        qkvT[rows, :] = (dot(wqkv[rows, :], hv, 1, 1) + biasT[rows, :]).astype(BF)

    scale = HD ** -0.5
    slopes = alibi_slopes(HL * TP)
    j_pos = lax.broadcasted_iota(jnp.int32, (S, S), 0)
    i_pos = lax.broadcasted_iota(jnp.int32, (S, S), 1)
    causal = j_pos <= i_pos
    j_f = j_pos.astype(F32)

    def head(h, e):
        return qkvT[(h * 3 + e) * HD:(h * 3 + e + 1) * HD, :]

    for h in range(HL):
        slope = jnp.where(t == 0, slopes[h], jnp.where(t == 1, slopes[HL + h], jnp.where(t == 2, slopes[2 * HL + h], slopes[3 * HL + h]))).astype(F32)
        s = dot(head(h, 1), head(h, 0), 0, 0) * scale + slope * j_f
        s = jnp.where(causal, s, MASK_VALUE)
        p = jnp.exp(s - jnp.max(s, axis=0, keepdims=True))
        p = p / jnp.sum(p, axis=0, keepdims=True)
        probs[h] = p
        ctx_ref[h * HD:(h + 1) * HD, :] = dot(head(h, 2), p.astype(BF), 1, 0).astype(BF)

    def exchange(part, ps, pr, hs, hr, cr):
        firsts = []
        theirs = part(1 - half)
        for k in range(HCH):
            ps[k] = theirs[:, k * CW:(k + 1) * CW].astype(BF)
            firsts.append(send(ps.at[k], pr.at[k], pt))
        ours = part(half)
        outs = []
        for k in range(HCH):
            own = ours[:, k * CW:(k + 1) * CW]
            firsts[k].wait_recv()
            hs[k] = (own + pr[k].astype(F32)).astype(BF)
            outs.append((send(hs.at[k], cr.at[k], ct), send(hs.at[k], hr.at[k], pt)))
        return outs

    def forward(outs, cr, fr):
        fwd = []
        for k in range(HCH):
            outs[k][0].wait_recv()
            fwd.append(send(cr.at[k], fr.at[k], pt))
        return fwd

    for c in w_cps['out']:
        c.wait()
    ctxT = ctx_ref[...]
    a_outs = exchange(lambda kk: dot(ctxT, wout[kk], 0, 0), a_ps, a_pr, a_hs, a_hr, a_cr)

    y_p.wait_recv()
    y_f.wait_recv()
    for i in range(TP):
        gm_f[pl.ds(i * SL, SL), :] = gyg[i].astype(F32)
    for r in range(0, S, 32):
        gyf_ref[r:r + 32, :] = gm_f[r:r + 32, :].astype(BF)
    w_cps['dn'][0].wait()
    gyv = gyf_ref[...]
    for n in range(NCH):
        gact[:, n * CW:(n + 1) * CW] = dot(gyv, wdn[n * CW:(n + 1) * CW, :], 1, 1).astype(BF)
    vec_ref[0:1, :] = jnp.sum(gm_f[...], axis=0, keepdims=True)

    def gathered(outs, fwd, hs, hr, cr, fr, put):
        for k in range(HCH):
            put(half * HCH + k, (hs[k].astype(F32) + cr[k].astype(F32)).astype(BF).astype(F32))
        for k in range(HCH):
            outs[k][1].wait_recv()
            fwd[k].wait_recv()
            put((1 - half) * HCH + k, (hr[k].astype(F32) + fr[k].astype(F32)).astype(BF).astype(F32))

    a_fwd = forward(a_outs, a_cr, a_fr)

    def put_x(kk, val):
        cols = pl.ds(pl.multiple_of(kk * CW, CW), CW)
        xf[:, cols] = xf[:, cols] + val + bo_ref[:, cols]

    gathered(a_outs, a_fwd, a_hs, a_hr, a_cr, a_fr, put_x)

    for r in range(0, S, 32):
        cen, rstd = rows_stats(xf[r:r + 32, :])
        g_ref[r:r + 32, :] = (cen * rstd * g2_ref[...] + be2_ref[...]).astype(BF)

    w_cps['up'][0].wait()
    gv = g_ref[...]
    for n in range(NCH):
        cols = slice(n * CW, (n + 1) * CW)
        pre = dot(gv, wup[:, cols], 1, 0) + bup_ref[:, cols]
        val, der = gelu_parts(pre)
        act_ref[:, cols] = val.astype(BF)
        gp = gact[:, cols].astype(F32) * der
        vec_ref[1:2, cols] = jnp.sum(gp, axis=0, keepdims=True)
        gpre_ref[:, cols] = gp.astype(BF)

    gprev = gpre_ref[...]

    def part_g(kk):
        return dot(gprev, wup[pl.ds(pl.multiple_of(kk * HW, HW), HW), :], 1, 1)

    g_outs = exchange(part_g, b_ps, b_pr, b_hs, b_hr, b_cr)

    def scatter_first(part, buf, pr):
        for n in range(NCH):
            cols = slice(n * CW, (n + 1) * CW)
            v = part(n)
            for i in range(TP):
                buf[i, :, cols] = v[i * SL:(i + 1) * SL, :].astype(BF)
        return (send(buf.at[qt], pr.at[1], pt), send(buf.at[pt], pr.at[0], pt))

    actv = act_ref[...]
    m_first = scatter_first(lambda n: dot(actv, wdn[:, n * CW:(n + 1) * CW], 1, 0), ghp.at[0], m_pr)

    for n in range(NCH):
        gwdn_ref[n * CW:(n + 1) * CW, :] = dot(act_ref[:, n * CW:(n + 1) * CW], gyv, 0, 0).astype(BF)

    m_first[0].wait_recv()
    m_hs[...] = (ghp[0, ct].astype(F32) + m_pr[1].astype(F32)).astype(BF)
    m_out = send(m_hs, m_cr, ct)
    g_fwd = []
    for k in range(HCH):
        g_outs[k][0].wait_recv()
        g_fwd.append(send(b_cr.at[k], b_fr.at[k], pt))
        for n in range(2 * k, 2 * k + 2):
            gwup_ref[n * CW:(n + 1) * CW, :] = dot(g_ref[:, n * CW:(n + 1) * CW], gprev, 0, 0).astype(BF)

    def put_g(kk, val):
        gg_f[:, pl.ds(pl.multiple_of(kk * CW, CW), CW)] = val

    gathered(g_outs, g_fwd, b_hs, b_hr, b_cr, b_fr, put_g)

    gg2 = jnp.zeros((1, D), F32)
    gb2 = jnp.zeros((1, D), F32)
    gbo = jnp.zeros((1, D), F32)
    for r in range(0, S, 32):
        cen, rstd = rows_stats(xf[r:r + 32, :])
        xh = cen * rstd
        gg = gg_f[r:r + 32, :]
        gg2 = gg2 + jnp.sum(gg * xh, axis=0, keepdims=True)
        gb2 = gb2 + jnp.sum(gg, axis=0, keepdims=True)
        dxh = gg * g2_ref[...]
        m1 = jnp.mean(dxh, axis=-1, keepdims=True)
        m2 = jnp.mean(dxh * xh, axis=-1, keepdims=True)
        gm = gm_f[r:r + 32, :] + rstd * (dxh - m1 - xh * m2)
        gm_f[r:r + 32, :] = gm
        gbo = gbo + jnp.sum(gm, axis=0, keepdims=True)
        gmid_ref[r:r + 32, :] = gm.astype(BF)
    vec_ref[2:3, :] = gg2
    vec_ref[3:4, :] = gb2
    vec_ref[4:5, :] = gbo

    gmv = gmid_ref[...]
    gctxT = (dot(wout[0], gmv[:, :HW], 1, 1) + dot(wout[1], gmv[:, HW:], 1, 1)).astype(BF)
    heads = range(HL)
    gos = [gctxT[h * HD:(h + 1) * HD, :] for h in heads]
    gps = [dot(head(h, 2), gos[h], 0, 0).astype(BF).astype(F32) for h in heads]
    gvs = [dot(gos[h], probs[h].astype(BF), 1, 1).astype(BF) for h in heads]
    gss = [(probs[h] * (gps[h] - jnp.sum(gps[h] * probs[h], axis=0, keepdims=True))).astype(BF) for h in heads]
    gqs = [(dot(head(h, 1), gss[h], 1, 0) * scale).astype(BF) for h in heads]
    gks = [(dot(head(h, 0), gss[h], 1, 1) * scale).astype(BF) for h in heads]
    for h in heads:
        for e, val in enumerate((gqs[h], gks[h], gvs[h])):
            gqkv_ref[(h * 3 + e) * HD:(h * 3 + e + 1) * HD, :] = val

    gqv = gqkv_ref[...]

    ln_s, ln_pr, ln_hs, ln_cr = ln_x.at[0], ln_x.at[1], ln_x.at[2], ln_x.at[3]
    r_first = scatter_first(lambda n: dot(gqv, wqkv[:, n * CW:(n + 1) * CW], 0, 0), ghp.at[1], r_pr)
    gg1 = jnp.zeros((1, D), F32)
    gb1 = jnp.zeros((1, D), F32)
    for i in range(TP):
        v = ghp[1, i].astype(F32)
        gg1 = gg1 + jnp.sum(v * xhat[i * SL:(i + 1) * SL, :], axis=0, keepdims=True)
        gb1 = gb1 + jnp.sum(v, axis=0, keepdims=True)
    ln_s[0:1, :] = gg1
    ln_s[1:2, :] = gb1
    l_first = send(ln_s, ln_pr, pt)

    r_first[0].wait_recv()
    r_hs[...] = (ghp[1, ct].astype(F32) + r_pr[1].astype(F32)).astype(BF)
    r_out = send(r_hs, r_cr, ct)
    l_first.wait_recv()
    ln_hs[...] = ln_s[...] + ln_pr[...]
    l_out = send(ln_hs, ln_cr, ct)

    ones = jnp.ones((8, S), BF)
    for h in heads:
        for e in range(3):
            gbqkv_ref[e, h:h + 1, :] = dot(ones, gqkv_ref[(h * 3 + e) * HD:(h * 3 + e + 1) * HD, :], 1, 1)[0:1, :]
    gwout_ref[...] = dot(ctx_ref[...], gmv, 1, 0).astype(BF)
    for h in range(HL):
        rows = slice(h * 3 * HD, (h + 1) * 3 * HD)
        gwqkv_ref[rows, :] = dot(gqkv_ref[rows, :], h_ref[...], 1, 0).astype(BF)
    own = pl.ds(pl.multiple_of(t * SL, 8), SL)
    m_first[1].wait_recv()
    m_out.wait_recv()
    m_sum = (ghp[0, t].astype(F32) + m_pr[0].astype(F32)).astype(BF).astype(F32) + m_cr[...].astype(F32)
    y_ref[...] = (xf[own, :] + m_sum.astype(BF).astype(F32) + bd_ref[...]).astype(BF)

    r_first[1].wait_recv()
    mine = (ghp[1, t].astype(F32) + r_pr[0].astype(F32)).astype(BF).astype(F32)
    r_out.wait_recv()
    gh = (mine + r_cr[...].astype(F32)).astype(BF).astype(F32)
    xh = xhat[own, :]
    dxh = gh * g1_ref[...]
    m1 = jnp.mean(dxh, axis=-1, keepdims=True)
    m2 = jnp.mean(dxh * xh, axis=-1, keepdims=True)
    gx_ref[...] = (gm_f[own, :] + rstd_s[own, 0:1] * (dxh - m1 - xh * m2)).astype(BF)
    l_out.wait_recv()
    vec_ref[6:8, :] = ln_hs[...] + ln_cr[...]
    for c in started:
        c.wait_send()


N_SEND = 38
VMEM_A = 34 * 2**20
VMEM_B = 8 * 2**20


def write_kernel(yi_ref, gxi_ref, vec_ref, gbi_ref, qkv_ref, out_ref, up_ref, dn_ref,
                 y_ref, gx_ref, gl1_ref, bl1_ref, gwqkv_ref, gbqkv_ref, gwout_ref, gbo_ref, gl2_ref, bl2_ref,
                 gwup_ref, gbup_ref, gwdn_ref, gbd_ref, sem):
    cps = []
    for src, dst in ((dn_ref, gwdn_ref), (up_ref, gwup_ref), (qkv_ref, gwqkv_ref), (out_ref, gwout_ref)):
        rows = src.shape[0] // 4
        for k in range(4):
            part = pl.ds(k * rows, rows)
            c = pltpu.make_async_copy(src.at[part], dst.at[part], sem.at[len(cps)])
            c.start()
            cps.append(c)
    y_ref[...] = yi_ref[...]
    gx_ref[...] = gxi_ref[...]
    gbqkv_ref[...] = gbi_ref[...]
    for i, r in enumerate((gbd_ref, gbup_ref, gl2_ref, bl2_ref, gbo_ref, None, gl1_ref, bl1_ref)):
        if r is not None:
            r[...] = vec_ref[i, :]
    for c in cps:
        c.wait()


def solution(mesh):
    VM = pl.BlockSpec(memory_space=pltpu.VMEM)
    ANY = pl.BlockSpec(memory_space=pltpu.HBM)

    def sds(shape, dt):
        return jax.ShapeDtypeStruct(shape, dt)

    def local_step(x, g1, be1, w_qkv, b_qkv, w_out, b_out, g2, be2, w_up, b_up, w_down, b_down, grad_y):
        wq = jnp.transpose(w_qkv, (1, 2, 3, 0)).reshape(3 * HL * HD, D)
        bq = jnp.transpose(b_qkv, (1, 0, 2))
        part = pltpu.VMEM((HCH, S, CW), BF)
        mids = pl.pallas_call(
            block_kernel,
            out_shape=(pltpu.VMEM((SL, D), BF), pltpu.VMEM((SL, D), BF), pltpu.VMEM((8, D), F32), pltpu.VMEM((3, HL, HD), F32),
                       pltpu.VMEM((3 * HL * HD, D), BF), pltpu.VMEM((HL * HD, D), BF), pltpu.VMEM((D, FL), BF), pltpu.VMEM((FL, D), BF)),
            in_specs=[ANY] * 14,
            out_specs=(VM,) * 8,
            scratch_shapes=[
                pltpu.VMEM((S, D), BF), pltpu.VMEM((3 * HL * HD, S), BF), pltpu.VMEM((HL * HD, S), BF), pltpu.VMEM((S, D), BF),
                pltpu.VMEM((S, D), BF), pltpu.VMEM((S, FL), BF), pltpu.VMEM((S, FL), BF), pltpu.VMEM((S, D), BF),
                pltpu.VMEM((3 * HL * HD, D), BF), pltpu.VMEM((2, HL * HD, HW), BF), pltpu.VMEM((D, FL), BF), pltpu.VMEM((FL, D), BF),
                pltpu.VMEM((TP, SL, D), BF), pltpu.VMEM((TP, SL, D), BF), pltpu.VMEM((S, D), F32), pltpu.VMEM((S, D), F32),
                pltpu.VMEM((S, 128), F32), pltpu.VMEM((3 * HL * HD, S), F32), pltpu.VMEM((3 * HL * HD, S), BF), pltpu.VMEM((HL, S, S), F32),
                *[part] * 12,
                pltpu.VMEM((S, FL), BF), pltpu.VMEM((2, TP, SL, D), BF),
                pltpu.VMEM((2, SL, D), BF), pltpu.VMEM((SL, D), BF), pltpu.VMEM((SL, D), BF),
                pltpu.VMEM((2, SL, D), BF), pltpu.VMEM((SL, D), BF), pltpu.VMEM((SL, D), BF),
                pltpu.VMEM((S, D), F32), pltpu.VMEM((4, 2, D), F32), pltpu.VMEM((S, D), F32), pltpu.VMEM((8, D), F32),
                pltpu.VMEM((3, HL, HD), F32), *[pltpu.VMEM((D,), F32) for _ in range(7)],
                pltpu.SemaphoreType.DMA((9,)), pltpu.SemaphoreType.DMA((N_SEND,)), pltpu.SemaphoreType.DMA((N_SEND,)),
                pltpu.SemaphoreType.DMA((10,)),
            ],
            compiler_params=pltpu.CompilerParams(collective_id=0, has_side_effects=True, vmem_limit_bytes=VMEM_A),
            name='block',
        )(*(pltpu.with_memory_space_constraint(v, pltpu.HBM) for v in (
            x.reshape(SL, D), grad_y.reshape(SL, D), g1, be1, g2, be2, b_out, b_down, bq, b_up, wq, w_out, w_up, w_down)))
        vec1 = sds((D,), F32)
        outs = pl.pallas_call(
            write_kernel,
            out_shape=(sds((SL, D), BF), sds((SL, D), BF), vec1, vec1, sds((3 * HL * HD, D), BF), sds((3, HL, HD), F32),
                       sds((HL * HD, D), BF), vec1, vec1, vec1, sds((D, FL), BF), vec1, sds((FL, D), BF), vec1),
            in_specs=[VM] * 8,
            out_specs=(VM, VM, VM, VM, ANY, VM, ANY, VM, VM, VM, ANY, VM, ANY, VM),
            scratch_shapes=[pltpu.SemaphoreType.DMA((16,))],
            compiler_params=pltpu.CompilerParams(vmem_limit_bytes=VMEM_B),
            name='write',
        )(*mids)
        (y, gx, gl1, bl1, gwqkv, gbqkv, gwout, gbo, gl2, bl2, gwup, gbup, gwdn, gbd) = outs
        gwqkv = jnp.transpose(gwqkv.reshape(HL, 3, HD, D), (3, 0, 1, 2))
        gbqkv = jnp.transpose(gbqkv, (1, 0, 2))
        return (y.reshape(1, SL, D), gx.reshape(1, SL, D), gl1, bl1, gwqkv, gbqkv, gwout, gbo, gl2, bl2, gwup, gbup, gwdn, gbd)

    row_spec = P('dp', 'tp', None)
    in_specs = (row_spec, P(), P(), P(None, 'tp', None, None), P('tp', None, None), P('tp', None), P(), P(), P(),
                P(None, 'tp'), P('tp'), P('tp', None), P(), row_spec)
    out_specs = (row_spec, row_spec, P('dp'), P('dp'), P('dp', 'tp', None, None), P(('dp', 'tp'), None, None),
                 P(('dp', 'tp'), None), P('dp'), P('dp'), P('dp'), P('dp', 'tp'), P(('dp', 'tp')), P(('dp', 'tp'), None), P('dp'))
    return jax.shard_map(local_step, mesh=mesh, in_specs=in_specs, out_specs=out_specs, check_vma=False)
```

```python
import functools
import math

import jax
import jax.numpy as jnp
from jax import lax
from jax.experimental import pallas as pl
from jax.experimental.pallas import tpu as pltpu
from jax.sharding import PartitionSpec as P

EPS = 1e-5
MASK_VALUE = -1e30
BF = jnp.bfloat16
F32 = jnp.float32
MESH = pl.DeviceIdType.MESH

D = 1536
S = 96
SL = 24
TP = 4
HL = 4
HD = 96
FL = 1536
CW = 256
NCH = D // CW
HCH = NCH // 2
HW = D // 2


def alibi_slopes(n_heads):
    closest = 2 ** int(math.floor(math.log2(n_heads)))
    base_ratio = 2.0 ** (-8.0 / closest)
    extra_ratio = 2.0 ** (-4.0 / closest)
    remaining = min(closest, n_heads - closest)
    slopes = [base_ratio ** (i + 1) for i in range(closest)]
    return slopes + [extra_ratio ** (2 * i + 1) for i in range(remaining)]


def dot(a, b, ca, cb):
    return lax.dot_general(a, b, (((ca,), (cb,)), ((), ())), preferred_element_type=F32)


def gelu_parts(u):
    k = math.sqrt(2.0 / math.pi)
    u2 = u * u
    th = jnp.tanh(k * (u + 0.044715 * (u2 * u)))
    half = 0.5 * (1.0 + th)
    dk = k * (1.0 + 3.0 * 0.044715 * u2)
    return u * half, half + 0.5 * u * (1.0 - th * th) * dk


def rows_stats(v):
    mean = jnp.mean(v, axis=-1, keepdims=True)
    cen = v - mean
    var = jnp.mean(cen * cen, axis=-1, keepdims=True)
    return cen, lax.rsqrt(var + EPS)


def places():
    t = lax.axis_index('tp')
    core = t % 2
    pt = t + 1 - 2 * core
    ct = TP - 1 - t
    qt = TP - 1 - pt
    half = (core + t // 2) % 2
    return t, pt, ct, qt, half


def sender(ssem, rsem):
    started = []

    def send(src, dst, dev):
        i = len(started)
        c = pltpu.make_async_remote_copy(src_ref=src, dst_ref=dst, send_sem=ssem.at[i], recv_sem=rsem.at[i],
                                         device_id={'tp': dev}, device_id_type=MESH)
        c.start()
        started.append(c)
        return c

    return send, started


def head_rows(h, e):
    return slice((h * 3 + e) * HD, (h * 3 + e + 1) * HD)


def row_blocks(buf, cols, v):
    for i in range(TP):
        buf[i, :, cols] = v[i * SL:(i + 1) * SL, :].astype(BF)


def block_kernel(x_hbm, gy_hbm, g1_hbm, be1_hbm, g2_hbm, be2_hbm, bo_hbm, bd_hbm, bqkv_hbm, bup_hbm,
                 wqkv_hbm, wout_hbm, wup_hbm, wdn_hbm,
                 y_ref, vec_ref, gwup_ref, gwdn_ref, gqkv_ref, h_ref, ctx_ref, gmid_ref, mine_ref, xh_ref, gm_ref, rs_ref, g1_out, r_hs, ln_hs,
                 wqkv, wout, xf, gm_f, gg_f, xhat, rstd_s, probs, qkvT, par, mp,
                 wup, wdn, xg, gyg, biasT, a_ps, a_pr, a_hs, a_hr, a_cr, a_fr, b_ps, b_pr, b_hs, b_hr, b_cr, b_fr,
                 gact, g_ref, gpre_ref, act_ref, gyf_ref, bqkv_ref, g1_in, be1_in, g2_in, be2_in, bo_in, bd_in, bup_in,
                 rp, m_pr, m_hs, m_cr, r_pr, ln_x,
                 wsem, ssem, rsem, isem):
    t, pt, ct, qt, half = places()
    send, started = sender(ssem, rsem)

    in_x = pltpu.make_async_copy(x_hbm, xg.at[t], isem.at[0])
    in_gy = pltpu.make_async_copy(gy_hbm, gyg.at[t], isem.at[1])
    in_b = pltpu.make_async_copy(bqkv_hbm, bqkv_ref, isem.at[2])
    small = ((g1_hbm, g1_in), (be1_hbm, be1_in), (g2_hbm, g2_in), (be2_hbm, be2_in), (bo_hbm, bo_in), (bd_hbm, bd_in), (bup_hbm, bup_in))
    in_p = [pltpu.make_async_copy(a, b, isem.at[3 + i]) for i, (a, b) in enumerate(small)]
    for c in (in_x, in_gy, in_b, *in_p):
        c.start()
    w_cps = {}
    w_cps['qkv'] = [pltpu.make_async_copy(wqkv_hbm, wqkv, wsem.at[0])]
    w_cps['out'] = [pltpu.make_async_copy(wout_hbm.at[:, pl.ds(k * HW, HW)], wout.at[k], wsem.at[1 + k]) for k in range(2)]
    w_cps['dn'] = [pltpu.make_async_copy(wdn_hbm, wdn, wsem.at[7])]
    w_cps['up'] = [pltpu.make_async_copy(wup_hbm, wup, wsem.at[8])]

    barrier = pltpu.get_barrier_semaphore()
    for dev in (pt, ct):
        pl.semaphore_signal(barrier, inc=1, device_id={'tp': dev}, device_id_type=MESH)
    for name in ('qkv', 'out', 'dn', 'up'):
        for c in w_cps[name]:
            c.start()
    pl.semaphore_wait(barrier, 2)

    in_x.wait()
    x_c = send(xg.at[t], xg.at[t], ct)
    x_p = send(xg.at[t], xg.at[t], pt)
    in_gy.wait()
    y_c = send(gyg.at[t], gyg.at[t], ct)
    y_p = send(gyg.at[t], gyg.at[t], pt)

    for c in (in_b, *in_p):
        c.wait()
    for i, r in enumerate((g1_in, be1_in, g2_in, be2_in, bo_in, bd_in, bup_in)):
        par[i, :] = r[...]
    g1_ref, be1_ref, g2_ref, be2_ref, bo_ref, bd_ref, bup_ref = (par.at[i:i + 1] for i in range(7))

    for h in range(HL):
        for e in range(3):
            row = jnp.broadcast_to(bqkv_ref[e, h:h + 1, :], (S, HD))
            biasT[pl.ds((h * 3 + e) * HD, HD), :] = row.T

    x_c.wait_recv()
    x_f = send(xg.at[ct], xg.at[ct], pt)
    x_p.wait_recv()
    x_f.wait_recv()

    for i in range(TP):
        xf[pl.ds(i * SL, SL), :] = xg[i].astype(F32)
    for r in range(0, S, 32):
        cen, rstd = rows_stats(xf[r:r + 32, :])
        xh = cen * rstd
        xhat[r:r + 32, :] = xh
        rstd_s[r:r + 32, :] = jnp.broadcast_to(rstd, (32, 128))
        h_ref[r:r + 32, :] = (xh * g1_ref[...] + be1_ref[...]).astype(BF)

    y_c.wait_recv()
    y_f = send(gyg.at[ct], gyg.at[ct], pt)

    w_cps['qkv'][0].wait()
    hv = h_ref[...]
    for h in range(HL):
        rows = slice(h * 3 * HD, (h + 1) * 3 * HD)
        qkvT[rows, :] = (dot(wqkv[rows, :], hv, 1, 1) + biasT[rows, :]).astype(BF)

    scale = HD ** -0.5
    slopes = alibi_slopes(HL * TP)
    j_pos = lax.broadcasted_iota(jnp.int32, (S, S), 0)
    i_pos = lax.broadcasted_iota(jnp.int32, (S, S), 1)
    causal = j_pos <= i_pos
    j_f = j_pos.astype(F32)

    def head(h, e):
        return qkvT[head_rows(h, e), :]

    for h in range(HL):
        slope = jnp.where(t == 0, slopes[h], jnp.where(t == 1, slopes[HL + h], jnp.where(t == 2, slopes[2 * HL + h], slopes[3 * HL + h]))).astype(F32)
        s = dot(head(h, 1), head(h, 0), 0, 0) * scale + slope * j_f
        s = jnp.where(causal, s, MASK_VALUE)
        p = jnp.exp(s - jnp.max(s, axis=0, keepdims=True))
        p = p / jnp.sum(p, axis=0, keepdims=True)
        probs[h] = p
        ctx_ref[h * HD:(h + 1) * HD, :] = dot(head(h, 2), p.astype(BF), 1, 0).astype(BF)

    def exchange(part, groups, ps, pr, hs, hr, cr):
        firsts = []
        for k0, k1 in groups:
            theirs = part(1 - half, k0 * CW, k1 * CW)
            for k in range(k0, k1):
                ps[k] = theirs[:, (k - k0) * CW:(k - k0 + 1) * CW].astype(BF)
                firsts.append(send(ps.at[k], pr.at[k], pt))
        outs = []
        for k0, k1 in groups:
            ours = part(half, k0 * CW, k1 * CW)
            for k in range(k0, k1):
                own = ours[:, (k - k0) * CW:(k - k0 + 1) * CW]
                firsts[k].wait_recv()
                hs[k] = (own + pr[k].astype(F32)).astype(BF)
                outs.append((send(hs.at[k], cr.at[k], ct), send(hs.at[k], hr.at[k], pt)))
        return outs

    def forward(outs, cr, fr):
        fwd = []
        for k in range(HCH):
            outs[k][0].wait_recv()
            fwd.append(send(cr.at[k], fr.at[k], pt))
        return fwd

    for c in w_cps['out']:
        c.wait()
    ctxT = ctx_ref[...]
    a_outs = exchange(lambda hh, c0, c1: dot(ctxT, wout[hh, :, c0:c1], 0, 0), ((0, HCH),), a_ps, a_pr, a_hs, a_hr, a_cr)

    y_p.wait_recv()
    y_f.wait_recv()
    for i in range(TP):
        gm_f[pl.ds(i * SL, SL), :] = gyg[i].astype(F32)
    for r in range(0, S, 32):
        gyf_ref[r:r + 32, :] = gm_f[r:r + 32, :].astype(BF)
    w_cps['dn'][0].wait()
    gyv = gyf_ref[...]
    for n in range(NCH):
        gact[:, n * CW:(n + 1) * CW] = dot(gyv, wdn[n * CW:(n + 1) * CW, :], 1, 1).astype(BF)
    vec_ref[0:1, :] = jnp.sum(gm_f[...], axis=0, keepdims=True)

    def gathered(outs, fwd, hs, hr, cr, fr, put):
        for k in range(HCH):
            put(half * HCH + k, (hs[k].astype(F32) + cr[k].astype(F32)).astype(BF).astype(F32))
        for k in range(HCH):
            outs[k][1].wait_recv()
            fwd[k].wait_recv()
            put((1 - half) * HCH + k, (hr[k].astype(F32) + fr[k].astype(F32)).astype(BF).astype(F32))

    a_fwd = forward(a_outs, a_cr, a_fr)

    def put_x(kk, val):
        cols = pl.ds(pl.multiple_of(kk * CW, CW), CW)
        xf[:, cols] = xf[:, cols] + val + bo_ref[:, cols]

    gathered(a_outs, a_fwd, a_hs, a_hr, a_cr, a_fr, put_x)

    for r in range(0, S, 32):
        cen, rstd = rows_stats(xf[r:r + 32, :])
        g_ref[r:r + 32, :] = (cen * rstd * g2_ref[...] + be2_ref[...]).astype(BF)

    w_cps['up'][0].wait()
    gv = g_ref[...]
    for n in range(NCH):
        cols = slice(n * CW, (n + 1) * CW)
        pre = dot(gv, wup[:, cols], 1, 0) + bup_ref[:, cols]
        val, der = gelu_parts(pre)
        act_ref[:, cols] = val.astype(BF)
        gp = gact[:, cols].astype(F32) * der
        vec_ref[1:2, cols] = jnp.sum(gp, axis=0, keepdims=True)
        gpre_ref[:, cols] = gp.astype(BF)

    gprev = gpre_ref[...]

    def part_g(hh, c0, c1):
        return dot(gprev, wup[pl.ds(pl.multiple_of(hh * HW + c0, CW), c1 - c0), :], 1, 1)

    g_outs = exchange(part_g, ((0, 1), (1, HCH)), b_ps, b_pr, b_hs, b_hr, b_cr)

    actv = act_ref[...]
    for n in range(NCH):
        cols = slice(n * CW, (n + 1) * CW)
        row_blocks(mp, cols, dot(actv, wdn[:, cols], 1, 0))
    m_first = (send(mp.at[qt], m_pr.at[1], pt), send(mp.at[pt], m_pr.at[0], pt))
    for n in range(NCH):
        gwdn_ref[n * CW:(n + 1) * CW, :] = dot(act_ref[:, n * CW:(n + 1) * CW], gyv, 0, 0).astype(BF)
    g_fwd = []
    for k in range(HCH):
        g_outs[k][0].wait_recv()
        g_fwd.append(send(b_cr.at[k], b_fr.at[k], pt))
        for n in range(2 * k, 2 * k + 2):
            gwup_ref[n * CW:(n + 1) * CW, :] = dot(g_ref[:, n * CW:(n + 1) * CW], gprev, 0, 0).astype(BF)

    m_first[0].wait_recv()
    m_hs[...] = (mp[ct].astype(F32) + m_pr[1].astype(F32)).astype(BF)
    m_out = send(m_hs, m_cr, ct)

    def put_g(kk, val):
        gg_f[:, pl.ds(pl.multiple_of(kk * CW, CW), CW)] = val

    gathered(g_outs, g_fwd, b_hs, b_hr, b_cr, b_fr, put_g)

    gg2 = jnp.zeros((1, D), F32)
    gb2 = jnp.zeros((1, D), F32)
    gbo = jnp.zeros((1, D), F32)
    for r in range(0, S, 32):
        cen, rstd = rows_stats(xf[r:r + 32, :])
        xh = cen * rstd
        gg = gg_f[r:r + 32, :]
        gg2 = gg2 + jnp.sum(gg * xh, axis=0, keepdims=True)
        gb2 = gb2 + jnp.sum(gg, axis=0, keepdims=True)
        dxh = gg * g2_ref[...]
        m1 = jnp.mean(dxh, axis=-1, keepdims=True)
        m2 = jnp.mean(dxh * xh, axis=-1, keepdims=True)
        gm = gm_f[r:r + 32, :] + rstd * (dxh - m1 - xh * m2)
        gm_f[r:r + 32, :] = gm
        gbo = gbo + jnp.sum(gm, axis=0, keepdims=True)
        gmid_ref[r:r + 32, :] = gm.astype(BF)
    vec_ref[2:3, :] = gg2
    vec_ref[3:4, :] = gb2
    vec_ref[4:5, :] = gbo

    gmv = gmid_ref[...]
    gctxT = (dot(wout[0], gmv[:, :HW], 1, 1) + dot(wout[1], gmv[:, HW:], 1, 1)).astype(BF)
    heads = range(HL)
    gos = [gctxT[h * HD:(h + 1) * HD, :] for h in heads]
    gps = [dot(head(h, 2), gos[h], 0, 0).astype(BF).astype(F32) for h in heads]
    gvs = [dot(gos[h], probs[h].astype(BF), 1, 1).astype(BF) for h in heads]
    gss = [(probs[h] * (gps[h] - jnp.sum(gps[h] * probs[h], axis=0, keepdims=True))).astype(BF) for h in heads]
    gqs = [(dot(head(h, 1), gss[h], 1, 0) * scale).astype(BF) for h in heads]
    gks = [(dot(head(h, 0), gss[h], 1, 1) * scale).astype(BF) for h in heads]
    for h in heads:
        for e, val in enumerate((gqs[h], gks[h], gvs[h])):
            gqkv_ref[head_rows(h, e), :] = val

    gqv = gqkv_ref[...]
    r_first = []
    for k in range(2):
        row_blocks(rp.at[k], slice(0, HW), dot(gqv, wqkv[:, k * HW:(k + 1) * HW], 0, 0))
        r_first.append((send(rp.at[k, qt], r_pr.at[k, 1], pt), send(rp.at[k, pt], r_pr.at[k, 0], pt)))

    ln_s, ln_pr = ln_x.at[0], ln_x.at[1]
    for k in range(2):
        cols = slice(k * HW, (k + 1) * HW)
        gg1 = jnp.zeros((1, HW), F32)
        gb1 = jnp.zeros((1, HW), F32)
        for i in range(TP):
            v = rp[k, i].astype(F32)
            gg1 = gg1 + jnp.sum(v * xhat[i * SL:(i + 1) * SL, cols], axis=0, keepdims=True)
            gb1 = gb1 + jnp.sum(v, axis=0, keepdims=True)
        ln_s[0:1, cols] = gg1
        ln_s[1:2, cols] = gb1
    l_first = send(ln_s, ln_pr, pt)

    own = pl.ds(pl.multiple_of(t * SL, 8), SL)
    xh_ref[...] = xhat[own, :]
    gm_ref[...] = gm_f[own, :]
    rs_ref[...] = rstd_s[own, :]
    g1_out[...] = par[0:1, :]

    for k in range(2):
        cols = slice(k * HW, (k + 1) * HW)
        r_first[k][0].wait_recv()
        r_hs[:, cols] = (rp[k, ct].astype(F32) + r_pr[k, 1].astype(F32)).astype(BF)
        r_first[k][1].wait_recv()
        mine_ref[:, cols] = (rp[k, t].astype(F32) + r_pr[k, 0].astype(F32)).astype(BF)
    l_first.wait_recv()
    ln_hs[...] = ln_s[...] + ln_pr[...]
    m_first[1].wait_recv()
    m_out.wait_recv()
    m_sum = (mp[t].astype(F32) + m_pr[0].astype(F32)).astype(BF).astype(F32) + m_cr[...].astype(F32)
    y_ref[...] = (xf[own, :] + m_sum.astype(BF).astype(F32) + bd_ref[...]).astype(BF)
    for c in started:
        c.wait_send()


N_SEND = 6 + 12 + 12 + 3 + 4 + 1
VMEM_A = 36 * 2**20
VMEM_B = 8 * 2**20
VMEM_C = 4 * 2**20


def write_kernel(yi_ref, vec_ref, up_ref, dn_ref, gqkv_ref, h_ref, ctx_ref, gmid_ref,
                 y_ref, gwqkv_ref, gbqkv_ref, gwout_ref, gbo_ref, gl2_ref, bl2_ref, gwup_ref, gbup_ref, gwdn_ref, gbd_ref,
                 s_qkv, s_out, sem):
    cps = []

    def out(src, dst, n=1):
        rows = src.shape[0] // n
        for k in range(n):
            c = pltpu.make_async_copy(src.at[pl.ds(k * rows, rows)], dst.at[pl.ds(k * rows, rows)], sem.at[len(cps)])
            c.start()
            cps.append(c)

    out(dn_ref, gwdn_ref, 4)
    out(up_ref, gwup_ref, 4)
    hv = h_ref[...]
    s_out[...] = dot(ctx_ref[...], gmid_ref[...], 1, 0).astype(BF)
    out(s_out, gwout_ref)
    for n in range(HL):
        rows = slice(n * 3 * HD, (n + 1) * 3 * HD)
        s_qkv[rows, :] = dot(gqkv_ref[rows, :], hv, 1, 0).astype(BF)
        out(s_qkv.at[rows], gwqkv_ref.at[rows])
    y_ref[...] = yi_ref[...]
    ones = jnp.ones((8, S), BF)
    for h in range(HL):
        for e in range(3):
            gbqkv_ref[e, h:h + 1, :] = dot(ones, gqkv_ref[head_rows(h, e), :], 1, 1)[0:1, :]
    for i, r in enumerate((gbd_ref, gbup_ref, gl2_ref, bl2_ref, gbo_ref)):
        r[...] = vec_ref[i, :]
    for c in cps:
        c.wait()


def last_kernel(mine_ref, xh_ref, gm_ref, rs_ref, g1_ref, rc_ref, ln_ref, lc_ref, gx_ref, gl1_ref, bl1_ref):
    gh = (mine_ref[...].astype(F32) + rc_ref[...].astype(F32)).astype(BF).astype(F32)
    xh = xh_ref[...]
    dxh = gh * g1_ref[...]
    m1 = jnp.mean(dxh, axis=-1, keepdims=True)
    m2 = jnp.mean(dxh * xh, axis=-1, keepdims=True)
    gx_ref[...] = (gm_ref[...] + rs_ref[:, 0:1] * (dxh - m1 - xh * m2)).astype(BF)
    ln = ln_ref[...] + lc_ref[...]
    gl1_ref[...] = ln[0, :]
    bl1_ref[...] = ln[1, :]


def solution(mesh):
    VM = pl.BlockSpec(memory_space=pltpu.VMEM)
    ANY = pl.BlockSpec(memory_space=pltpu.HBM)

    def sds(shape, dt):
        return jax.ShapeDtypeStruct(shape, dt)

    def local_step(x, g1, be1, w_qkv, b_qkv, w_out, b_out, g2, be2, w_up, b_up, w_down, b_down, grad_y):
        wq = jnp.transpose(w_qkv, (1, 2, 3, 0)).reshape(3 * HL * HD, D)
        bq = jnp.transpose(b_qkv, (1, 0, 2))
        part = pltpu.VMEM((HCH, S, CW), BF)
        vec1 = sds((D,), F32)
        mids = pl.pallas_call(
            block_kernel,
            out_shape=(pltpu.VMEM((SL, D), BF), pltpu.VMEM((8, D), F32), pltpu.VMEM((D, FL), BF), pltpu.VMEM((FL, D), BF),
                       pltpu.VMEM((3 * HL * HD, S), BF), pltpu.VMEM((S, D), BF), pltpu.VMEM((HL * HD, S), BF), pltpu.VMEM((S, D), BF),
                       pltpu.VMEM((SL, D), BF), pltpu.VMEM((SL, D), F32), pltpu.VMEM((SL, D), F32), pltpu.VMEM((SL, 128), F32),
                       pltpu.VMEM((1, D), F32), sds((SL, D), BF), sds((2, D), F32)),
            in_specs=[ANY] * 14,
            out_specs=(VM,) * 15,
            scratch_shapes=[
                pltpu.VMEM((3 * HL * HD, D), BF), pltpu.VMEM((2, HL * HD, HW), BF), pltpu.VMEM((S, D), F32), pltpu.VMEM((S, D), F32),
                pltpu.VMEM((S, D), F32), pltpu.VMEM((S, D), F32), pltpu.VMEM((S, 128), F32), pltpu.VMEM((HL, S, S), F32),
                pltpu.VMEM((3 * HL * HD, S), BF), pltpu.VMEM((8, D), F32), pltpu.VMEM((TP, SL, D), BF),
                pltpu.VMEM((D, FL), BF), pltpu.VMEM((FL, D), BF), pltpu.VMEM((TP, SL, D), BF), pltpu.VMEM((TP, SL, D), BF),
                pltpu.VMEM((3 * HL * HD, S), F32), *[part] * 12,
                pltpu.VMEM((S, FL), BF), pltpu.VMEM((S, D), BF), pltpu.VMEM((S, FL), BF), pltpu.VMEM((S, FL), BF), pltpu.VMEM((S, D), BF),
                pltpu.VMEM((3, HL, HD), F32), *[pltpu.VMEM((D,), F32) for _ in range(7)],
                pltpu.VMEM((2, TP, SL, HW), BF), pltpu.VMEM((2, SL, D), BF), pltpu.VMEM((SL, D), BF), pltpu.VMEM((SL, D), BF),
                pltpu.VMEM((2, 2, SL, HW), BF), pltpu.VMEM((2, 2, D), F32),
                pltpu.SemaphoreType.DMA((9,)), pltpu.SemaphoreType.DMA((N_SEND,)), pltpu.SemaphoreType.DMA((N_SEND,)),
                pltpu.SemaphoreType.DMA((10,)),
            ],
            compiler_params=pltpu.CompilerParams(collective_id=0, has_side_effects=True, vmem_limit_bytes=VMEM_A),
            name='block',
        )(*(pltpu.with_memory_space_constraint(v, pltpu.HBM) for v in (
            x.reshape(SL, D), grad_y.reshape(SL, D), g1, be1, g2, be2, b_out, b_down, bq, b_up, wq, w_out, w_up, w_down)))
        mine, xh, gm, rs, g1v, r_hs, ln_hs = mids[8:]
        across = [(i, TP - 1 - i) for i in range(TP)]
        r_cr = lax.ppermute(r_hs, 'tp', across)
        ln_cr = lax.ppermute(ln_hs, 'tp', across)
        y, gwqkv, gbqkv, gwout, gbo, gl2, bl2, gwup, gbup, gwdn, gbd = pl.pallas_call(
            write_kernel,
            out_shape=(sds((SL, D), BF), sds((3 * HL * HD, D), BF), sds((3, HL, HD), F32), sds((HL * HD, D), BF), vec1, vec1, vec1,
                       sds((D, FL), BF), vec1, sds((FL, D), BF), vec1),
            in_specs=[VM] * 8,
            out_specs=(VM, ANY, VM, ANY, VM, VM, VM, ANY, VM, ANY, VM),
            scratch_shapes=[pltpu.VMEM((3 * HL * HD, D), BF), pltpu.VMEM((HL * HD, D), BF), pltpu.SemaphoreType.DMA((16,))],
            compiler_params=pltpu.CompilerParams(vmem_limit_bytes=VMEM_B),
            cost_estimate=pl.CostEstimate(flops=600_000_000, bytes_accessed=14_200_000, transcendentals=0),
            name='write',
        )(*mids[:8])
        gx, gl1, bl1 = pl.pallas_call(
            last_kernel,
            out_shape=(sds((SL, D), BF), vec1, vec1),
            in_specs=[VM] * 8,
            out_specs=(VM,) * 3,
            compiler_params=pltpu.CompilerParams(vmem_limit_bytes=VMEM_C),
            name='last',
        )(mine, xh, gm, rs, g1v, r_cr, ln_hs, ln_cr)
        gwqkv = jnp.transpose(gwqkv.reshape(HL, 3, HD, D), (3, 0, 1, 2))
        gbqkv = jnp.transpose(gbqkv, (1, 0, 2))
        return (y.reshape(1, SL, D), gx.reshape(1, SL, D), gl1, bl1, gwqkv, gbqkv, gwout, gbo, gl2, bl2, gwup, gbup, gwdn, gbd)

    row_spec = P('dp', 'tp', None)
    in_specs = (row_spec, P(), P(), P(None, 'tp', None, None), P('tp', None, None), P('tp', None), P(), P(), P(),
                P(None, 'tp'), P('tp'), P('tp', None), P(), row_spec)
    out_specs = (row_spec, row_spec, P('dp'), P('dp'), P('dp', 'tp', None, None), P(('dp', 'tp'), None, None),
                 P(('dp', 'tp'), None), P('dp'), P('dp'), P('dp'), P('dp', 'tp'), P(('dp', 'tp')), P(('dp', 'tp'), None), P('dp'))
    return jax.shard_map(local_step, mesh=mesh, in_specs=in_specs, out_specs=out_specs, check_vma=False)
```

```python
import functools
import math

import jax
import jax.numpy as jnp
from jax import lax
from jax.experimental import pallas as pl
from jax.experimental.pallas import tpu as pltpu
from jax.sharding import PartitionSpec as P

EPS = 1e-5
MASK_VALUE = -1e30
BF = jnp.bfloat16
F32 = jnp.float32
MESH = pl.DeviceIdType.MESH

D = 1536
S = 96
SL = 24
TP = 4
HL = 4
HD = 96
FL = 1536
CW = 256
NCH = D // CW
HCH = NCH // 2
HW = D // 2


def alibi_slopes(n_heads):
    closest = 2 ** int(math.floor(math.log2(n_heads)))
    base_ratio = 2.0 ** (-8.0 / closest)
    extra_ratio = 2.0 ** (-4.0 / closest)
    remaining = min(closest, n_heads - closest)
    slopes = [base_ratio ** (i + 1) for i in range(closest)]
    return slopes + [extra_ratio ** (2 * i + 1) for i in range(remaining)]


def dot(a, b, ca, cb):
    return lax.dot_general(a, b, (((ca,), (cb,)), ((), ())), preferred_element_type=F32)


def gelu_parts(u):
    k = math.sqrt(2.0 / math.pi)
    u2 = u * u
    th = jnp.tanh(k * (u + 0.044715 * (u2 * u)))
    half = 0.5 * (1.0 + th)
    dk = k * (1.0 + 3.0 * 0.044715 * u2)
    return u * half, half + 0.5 * u * (1.0 - th * th) * dk


def rows_stats(v):
    mean = jnp.mean(v, axis=-1, keepdims=True)
    cen = v - mean
    var = jnp.mean(cen * cen, axis=-1, keepdims=True)
    return cen, lax.rsqrt(var + EPS)


def places():
    t = lax.axis_index('tp')
    core = t % 2
    pt = t + 1 - 2 * core
    ct = TP - 1 - t
    qt = TP - 1 - pt
    half = (core + t // 2) % 2
    return t, pt, ct, qt, half


def sender(ssem, rsem):
    started = []

    def send(src, dst, dev):
        i = len(started)
        c = pltpu.make_async_remote_copy(src_ref=src, dst_ref=dst, send_sem=ssem.at[i], recv_sem=rsem.at[i],
                                         device_id={'tp': dev}, device_id_type=MESH)
        c.start()
        started.append(c)
        return c

    return send, started


def head_rows(h, e):
    return slice((h * 3 + e) * HD, (h * 3 + e + 1) * HD)


def row_blocks(buf, cols, v):
    for i in range(TP):
        buf[i, :, cols] = v[i * SL:(i + 1) * SL, :].astype(BF)


def block_kernel(x_hbm, gy_hbm, g1_hbm, be1_hbm, g2_hbm, be2_hbm, bo_hbm, bd_hbm, bqkv_hbm, bup_hbm,
                 wqkv_hbm, wout_hbm, wup_hbm, wdn_hbm,
                 y_ref, vec_ref, gwup_ref, gwdn_ref, gqkv_ref, h_ref, ctx_ref, gmid_ref, mine_ref, xh_ref, gm_ref, rs_ref, g1_out, r_hs, ln_hs,
                 wqkv, wout, xf, gm_f, gg_f, xhat, rstd_s, probs, qkvT, par, mp,
                 wup, wdn, xg, gyg, biasT, a_ps, a_pr, a_hs, a_hr, a_cr, a_fr, b_ps, b_pr, b_hs, b_hr, b_cr, b_fr,
                 gact, g_ref, gpre_ref, act_ref, gyf_ref, bqkv_ref, g1_in, be1_in, g2_in, be2_in, bo_in, bd_in, bup_in,
                 rp, m_pr, m_hs, m_cr, r_pr, ln_x,
                 wsem, ssem, rsem, isem):
    t, pt, ct, qt, half = places()
    send, started = sender(ssem, rsem)

    in_x = pltpu.make_async_copy(x_hbm, xg.at[t], isem.at[0])
    in_gy = pltpu.make_async_copy(gy_hbm, gyg.at[t], isem.at[1])
    in_b = pltpu.make_async_copy(bqkv_hbm, bqkv_ref, isem.at[2])
    small = ((g1_hbm, g1_in), (be1_hbm, be1_in), (g2_hbm, g2_in), (be2_hbm, be2_in), (bo_hbm, bo_in), (bd_hbm, bd_in), (bup_hbm, bup_in))
    in_p = [pltpu.make_async_copy(a, b, isem.at[3 + i]) for i, (a, b) in enumerate(small)]
    for c in (in_x, in_gy, in_b, *in_p):
        c.start()
    w_cps = {}
    w_cps['qkv'] = [pltpu.make_async_copy(wqkv_hbm, wqkv, wsem.at[0])]
    w_cps['out'] = [pltpu.make_async_copy(wout_hbm.at[:, pl.ds(k * HW, HW)], wout.at[k], wsem.at[1 + k]) for k in range(2)]
    w_cps['dn'] = [pltpu.make_async_copy(wdn_hbm, wdn, wsem.at[7])]
    w_cps['up'] = [pltpu.make_async_copy(wup_hbm, wup, wsem.at[8])]

    barrier = pltpu.get_barrier_semaphore()
    for dev in (pt, ct):
        pl.semaphore_signal(barrier, inc=1, device_id={'tp': dev}, device_id_type=MESH)
    for name in ('qkv', 'out', 'dn', 'up'):
        for c in w_cps[name]:
            c.start()
    pl.semaphore_wait(barrier, 2)

    in_x.wait()
    x_c = send(xg.at[t], xg.at[t], ct)
    x_p = send(xg.at[t], xg.at[t], pt)
    in_gy.wait()
    y_c = send(gyg.at[t], gyg.at[t], ct)
    y_p = send(gyg.at[t], gyg.at[t], pt)

    for c in (in_b, *in_p):
        c.wait()
    for i, r in enumerate((g1_in, be1_in, g2_in, be2_in, bo_in, bd_in, bup_in)):
        par[i, :] = r[...]
    g1_ref, be1_ref, g2_ref, be2_ref, bo_ref, bd_ref, bup_ref = (par.at[i:i + 1] for i in range(7))

    for h in range(HL):
        for e in range(3):
            row = jnp.broadcast_to(bqkv_ref[e, h:h + 1, :], (S, HD))
            biasT[pl.ds((h * 3 + e) * HD, HD), :] = row.T

    x_c.wait_recv()
    x_f = send(xg.at[ct], xg.at[ct], pt)
    x_p.wait_recv()
    x_f.wait_recv()

    for i in range(TP):
        xf[pl.ds(i * SL, SL), :] = xg[i].astype(F32)
    for r in range(0, S, 32):
        cen, rstd = rows_stats(xf[r:r + 32, :])
        xh = cen * rstd
        xhat[r:r + 32, :] = xh
        rstd_s[r:r + 32, :] = jnp.broadcast_to(rstd, (32, 128))
        h_ref[r:r + 32, :] = (xh * g1_ref[...] + be1_ref[...]).astype(BF)

    y_c.wait_recv()
    y_f = send(gyg.at[ct], gyg.at[ct], pt)

    w_cps['qkv'][0].wait()
    hv = h_ref[...]
    for h in range(HL):
        rows = slice(h * 3 * HD, (h + 1) * 3 * HD)
        qkvT[rows, :] = (dot(wqkv[rows, :], hv, 1, 1) + biasT[rows, :]).astype(BF)

    scale = HD ** -0.5
    slopes = alibi_slopes(HL * TP)
    j_pos = lax.broadcasted_iota(jnp.int32, (S, S), 0)
    i_pos = lax.broadcasted_iota(jnp.int32, (S, S), 1)
    causal = j_pos <= i_pos
    j_f = j_pos.astype(F32)

    def head(h, e):
        return qkvT[head_rows(h, e), :]

    for h in range(HL):
        slope = jnp.where(t == 0, slopes[h], jnp.where(t == 1, slopes[HL + h], jnp.where(t == 2, slopes[2 * HL + h], slopes[3 * HL + h]))).astype(F32)
        s = dot(head(h, 1), head(h, 0), 0, 0) * scale + slope * j_f
        s = jnp.where(causal, s, MASK_VALUE)
        p = jnp.exp(s - jnp.max(s, axis=0, keepdims=True))
        p = p / jnp.sum(p, axis=0, keepdims=True)
        probs[h] = p
        ctx_ref[h * HD:(h + 1) * HD, :] = dot(head(h, 2), p.astype(BF), 1, 0).astype(BF)

    def exchange(part, groups, ps, pr, hs, hr, cr):
        firsts = []
        for k0, k1 in groups:
            theirs = part(1 - half, k0 * CW, k1 * CW)
            for k in range(k0, k1):
                ps[k] = theirs[:, (k - k0) * CW:(k - k0 + 1) * CW].astype(BF)
                firsts.append(send(ps.at[k], pr.at[k], pt))
        outs = []
        for k0, k1 in groups:
            ours = part(half, k0 * CW, k1 * CW)
            for k in range(k0, k1):
                own = ours[:, (k - k0) * CW:(k - k0 + 1) * CW]
                firsts[k].wait_recv()
                hs[k] = (own + pr[k].astype(F32)).astype(BF)
                outs.append((send(hs.at[k], cr.at[k], ct), send(hs.at[k], hr.at[k], pt)))
        return outs

    def forward(outs, cr, fr):
        fwd = []
        for k in range(HCH):
            outs[k][0].wait_recv()
            fwd.append(send(cr.at[k], fr.at[k], pt))
        return fwd

    for c in w_cps['out']:
        c.wait()
    ctxT = ctx_ref[...]
    a_outs = exchange(lambda hh, c0, c1: dot(ctxT, wout[hh, :, c0:c1], 0, 0), ((0, HCH),), a_ps, a_pr, a_hs, a_hr, a_cr)

    y_p.wait_recv()
    y_f.wait_recv()
    for i in range(TP):
        gm_f[pl.ds(i * SL, SL), :] = gyg[i].astype(F32)
    for r in range(0, S, 32):
        gyf_ref[r:r + 32, :] = gm_f[r:r + 32, :].astype(BF)
    w_cps['dn'][0].wait()
    gyv = gyf_ref[...]
    for n in range(NCH):
        gact[:, n * CW:(n + 1) * CW] = dot(gyv, wdn[n * CW:(n + 1) * CW, :], 1, 1).astype(BF)
    vec_ref[0:1, :] = jnp.sum(gm_f[...], axis=0, keepdims=True)

    def gathered(outs, fwd, hs, hr, cr, fr, put):
        for k in range(HCH):
            put(half * HCH + k, (hs[k].astype(F32) + cr[k].astype(F32)).astype(BF).astype(F32))
        for k in range(HCH):
            outs[k][1].wait_recv()
            fwd[k].wait_recv()
            put((1 - half) * HCH + k, (hr[k].astype(F32) + fr[k].astype(F32)).astype(BF).astype(F32))

    a_fwd = forward(a_outs, a_cr, a_fr)

    def put_x(kk, val):
        cols = pl.ds(pl.multiple_of(kk * CW, CW), CW)
        xf[:, cols] = xf[:, cols] + val + bo_ref[:, cols]

    gathered(a_outs, a_fwd, a_hs, a_hr, a_cr, a_fr, put_x)

    for r in range(0, S, 32):
        cen, rstd = rows_stats(xf[r:r + 32, :])
        g_ref[r:r + 32, :] = (cen * rstd * g2_ref[...] + be2_ref[...]).astype(BF)

    w_cps['up'][0].wait()
    gv = g_ref[...]
    for n in range(NCH):
        cols = slice(n * CW, (n + 1) * CW)
        pre = dot(gv, wup[:, cols], 1, 0) + bup_ref[:, cols]
        val, der = gelu_parts(pre)
        act_ref[:, cols] = val.astype(BF)
        gp = gact[:, cols].astype(F32) * der
        vec_ref[1:2, cols] = jnp.sum(gp, axis=0, keepdims=True)
        gpre_ref[:, cols] = gp.astype(BF)

    gprev = gpre_ref[...]

    def part_g(hh, c0, c1):
        return dot(gprev, wup[pl.ds(pl.multiple_of(hh * HW + c0, CW), c1 - c0), :], 1, 1)

    g_outs = exchange(part_g, ((0, 1), (1, HCH)), b_ps, b_pr, b_hs, b_hr, b_cr)

    actv = act_ref[...]
    for n in range(NCH):
        cols = slice(n * CW, (n + 1) * CW)
        row_blocks(mp, cols, dot(actv, wdn[:, cols], 1, 0))
    m_first = (send(mp.at[qt], m_pr.at[1], pt), send(mp.at[pt], m_pr.at[0], pt))
    for n in range(NCH):
        gwdn_ref[n * CW:(n + 1) * CW, :] = dot(act_ref[:, n * CW:(n + 1) * CW], gyv, 0, 0).astype(BF)
    g_fwd = []
    for k in range(HCH):
        g_outs[k][0].wait_recv()
        g_fwd.append(send(b_cr.at[k], b_fr.at[k], pt))
        for n in range(2 * k, 2 * k + 2):
            gwup_ref[n * CW:(n + 1) * CW, :] = dot(g_ref[:, n * CW:(n + 1) * CW], gprev, 0, 0).astype(BF)

    m_first[0].wait_recv()
    m_hs[...] = (mp[ct].astype(F32) + m_pr[1].astype(F32)).astype(BF)
    m_out = send(m_hs, m_cr, ct)

    def put_g(kk, val):
        gg_f[:, pl.ds(pl.multiple_of(kk * CW, CW), CW)] = val

    gathered(g_outs, g_fwd, b_hs, b_hr, b_cr, b_fr, put_g)

    gg2 = jnp.zeros((1, D), F32)
    gb2 = jnp.zeros((1, D), F32)
    gbo = jnp.zeros((1, D), F32)
    for r in range(0, S, 32):
        cen, rstd = rows_stats(xf[r:r + 32, :])
        xh = cen * rstd
        gg = gg_f[r:r + 32, :]
        gg2 = gg2 + jnp.sum(gg * xh, axis=0, keepdims=True)
        gb2 = gb2 + jnp.sum(gg, axis=0, keepdims=True)
        dxh = gg * g2_ref[...]
        m1 = jnp.mean(dxh, axis=-1, keepdims=True)
        m2 = jnp.mean(dxh * xh, axis=-1, keepdims=True)
        gm = gm_f[r:r + 32, :] + rstd * (dxh - m1 - xh * m2)
        gm_f[r:r + 32, :] = gm
        gbo = gbo + jnp.sum(gm, axis=0, keepdims=True)
        gmid_ref[r:r + 32, :] = gm.astype(BF)
    vec_ref[2:3, :] = gg2
    vec_ref[3:4, :] = gb2
    vec_ref[4:5, :] = gbo

    gmv = gmid_ref[...]
    gctxT = (dot(wout[0], gmv[:, :HW], 1, 1) + dot(wout[1], gmv[:, HW:], 1, 1)).astype(BF)
    heads = range(HL)
    gos = [gctxT[h * HD:(h + 1) * HD, :] for h in heads]
    gps = [dot(head(h, 2), gos[h], 0, 0).astype(BF).astype(F32) for h in heads]
    gvs = [dot(gos[h], probs[h].astype(BF), 1, 1).astype(BF) for h in heads]
    gss = [(probs[h] * (gps[h] - jnp.sum(gps[h] * probs[h], axis=0, keepdims=True))).astype(BF) for h in heads]
    gqs = [(dot(head(h, 1), gss[h], 1, 0) * scale).astype(BF) for h in heads]
    gks = [(dot(head(h, 0), gss[h], 1, 1) * scale).astype(BF) for h in heads]
    for h in heads:
        for e, val in enumerate((gqs[h], gks[h], gvs[h])):
            gqkv_ref[head_rows(h, e), :] = val

    gqv = gqkv_ref[...]
    r_first = []
    for k in range(2):
        row_blocks(rp.at[k], slice(0, HW), dot(gqv, wqkv[:, k * HW:(k + 1) * HW], 0, 0))
        r_first.append((send(rp.at[k, qt], r_pr.at[k, 1], pt), send(rp.at[k, pt], r_pr.at[k, 0], pt)))

    ln_s, ln_pr = ln_x.at[0], ln_x.at[1]
    for k in range(2):
        cols = slice(k * HW, (k + 1) * HW)
        gg1 = jnp.zeros((1, HW), F32)
        gb1 = jnp.zeros((1, HW), F32)
        for i in range(TP):
            v = rp[k, i].astype(F32)
            gg1 = gg1 + jnp.sum(v * xhat[i * SL:(i + 1) * SL, cols], axis=0, keepdims=True)
            gb1 = gb1 + jnp.sum(v, axis=0, keepdims=True)
        ln_s[0:1, cols] = gg1
        ln_s[1:2, cols] = gb1
    l_first = send(ln_s, ln_pr, pt)

    own = pl.ds(pl.multiple_of(t * SL, 8), SL)
    xh_ref[...] = xhat[own, :]
    gm_ref[...] = gm_f[own, :]
    rs_ref[...] = rstd_s[own, :]
    g1_out[...] = par[0:1, :]

    for k in range(2):
        cols = slice(k * HW, (k + 1) * HW)
        r_first[k][0].wait_recv()
        r_hs[0:SL, cols] = (rp[k, ct].astype(F32) + r_pr[k, 1].astype(F32)).astype(BF)
        r_first[k][1].wait_recv()
        mine_ref[:, cols] = (rp[k, t].astype(F32) + r_pr[k, 0].astype(F32)).astype(BF)
    l_first.wait_recv()
    ln = ln_s[...] + ln_pr[...]
    ln_hs[...] = ln
    ln_rows = []
    for _ in range(3):
        ln_rows.append(ln.astype(BF).astype(F32))
        ln = ln - ln_rows[-1]
    r_hs[SL:SL + 8, :] = jnp.concatenate(ln_rows + [jnp.zeros((2, D), F32)], axis=0).astype(BF)
    m_first[1].wait_recv()
    m_out.wait_recv()
    m_sum = (mp[t].astype(F32) + m_pr[0].astype(F32)).astype(BF).astype(F32) + m_cr[...].astype(F32)
    y_ref[...] = (xf[own, :] + m_sum.astype(BF).astype(F32) + bd_ref[...]).astype(BF)
    for c in started:
        c.wait_send()


N_SEND = 6 + 12 + 12 + 3 + 4 + 1
VMEM_A = 36 * 2**20
VMEM_B = 8 * 2**20
VMEM_C = 4 * 2**20


def write_kernel(yi_ref, vec_ref, up_ref, dn_ref, gqkv_ref, h_ref, ctx_ref, gmid_ref,
                 y_ref, gwqkv_ref, gbqkv_ref, gwout_ref, gbo_ref, gl2_ref, bl2_ref, gwup_ref, gbup_ref, gwdn_ref, gbd_ref,
                 s_qkv, s_out, s_gb, s0, s1, s2, s3, s4, sem):
    cps = []

    def out(src, dst, n=1):
        rows = src.shape[0] // n
        for k in range(n):
            c = pltpu.make_async_copy(src.at[pl.ds(k * rows, rows)], dst.at[pl.ds(k * rows, rows)], sem.at[len(cps)])
            c.start()
            cps.append(c)

    out(dn_ref, gwdn_ref, 4)
    out(up_ref, gwup_ref, 4)
    out(yi_ref, y_ref)
    for i, (sv, r) in enumerate(((s0, gbd_ref), (s1, gbup_ref), (s2, gl2_ref), (s3, bl2_ref), (s4, gbo_ref))):
        sv[...] = vec_ref[i, :]
        out(sv, r)
    ones = jnp.ones((8, S), BF)
    for h in range(HL):
        for e in range(3):
            s_gb[e, h:h + 1, :] = dot(ones, gqkv_ref[head_rows(h, e), :], 1, 1)[0:1, :]
    out(s_gb, gbqkv_ref)
    hv = h_ref[...]
    s_out[...] = dot(ctx_ref[...], gmid_ref[...], 1, 0).astype(BF)
    out(s_out, gwout_ref)
    for n in range(HL):
        rows = slice(n * 3 * HD, (n + 1) * 3 * HD)
        s_qkv[rows, :] = dot(gqkv_ref[rows, :], hv, 1, 0).astype(BF)
        out(s_qkv.at[rows], gwqkv_ref.at[rows])
    for c in cps:
        c.wait()


def last_kernel(mine_ref, xh_ref, gm_ref, rs_ref, g1_ref, rc_ref, ln_ref, gx_ref, gl1_ref, bl1_ref):
    gh = (mine_ref[...].astype(F32) + rc_ref[0:SL, :].astype(F32)).astype(BF).astype(F32)
    xh = xh_ref[...]
    dxh = gh * g1_ref[...]
    m1 = jnp.mean(dxh, axis=-1, keepdims=True)
    m2 = jnp.mean(dxh * xh, axis=-1, keepdims=True)
    gx_ref[...] = (gm_ref[...] + rs_ref[:, 0:1] * (dxh - m1 - xh * m2)).astype(BF)
    lc = rc_ref[SL:SL + 8, :].astype(F32)
    ln = ln_ref[...] + (lc[0:2, :] + lc[2:4, :] + lc[4:6, :])
    gl1_ref[...] = ln[0, :]
    bl1_ref[...] = ln[1, :]


def solution(mesh):
    VM = pl.BlockSpec(memory_space=pltpu.VMEM)
    ANY = pl.BlockSpec(memory_space=pltpu.HBM)

    def sds(shape, dt):
        return jax.ShapeDtypeStruct(shape, dt)

    def local_step(x, g1, be1, w_qkv, b_qkv, w_out, b_out, g2, be2, w_up, b_up, w_down, b_down, grad_y):
        wq = jnp.transpose(w_qkv, (1, 2, 3, 0)).reshape(3 * HL * HD, D)
        bq = jnp.transpose(b_qkv, (1, 0, 2))
        part = pltpu.VMEM((HCH, S, CW), BF)
        vec1 = sds((D,), F32)
        mids = pl.pallas_call(
            block_kernel,
            out_shape=(pltpu.VMEM((SL, D), BF), pltpu.VMEM((8, D), F32), pltpu.VMEM((D, FL), BF), pltpu.VMEM((FL, D), BF),
                       pltpu.VMEM((3 * HL * HD, S), BF), pltpu.VMEM((S, D), BF), pltpu.VMEM((HL * HD, S), BF), pltpu.VMEM((S, D), BF),
                       pltpu.VMEM((SL, D), BF), pltpu.VMEM((SL, D), F32), pltpu.VMEM((SL, D), F32), pltpu.VMEM((SL, 128), F32),
                       pltpu.VMEM((1, D), F32), sds((SL + 8, D), BF), pltpu.VMEM((2, D), F32)),
            in_specs=[ANY] * 14,
            out_specs=(VM,) * 15,
            scratch_shapes=[
                pltpu.VMEM((3 * HL * HD, D), BF), pltpu.VMEM((2, HL * HD, HW), BF), pltpu.VMEM((S, D), F32), pltpu.VMEM((S, D), F32),
                pltpu.VMEM((S, D), F32), pltpu.VMEM((S, D), F32), pltpu.VMEM((S, 128), F32), pltpu.VMEM((HL, S, S), F32),
                pltpu.VMEM((3 * HL * HD, S), BF), pltpu.VMEM((8, D), F32), pltpu.VMEM((TP, SL, D), BF),
                pltpu.VMEM((D, FL), BF), pltpu.VMEM((FL, D), BF), pltpu.VMEM((TP, SL, D), BF), pltpu.VMEM((TP, SL, D), BF),
                pltpu.VMEM((3 * HL * HD, S), F32), *[part] * 12,
                pltpu.VMEM((S, FL), BF), pltpu.VMEM((S, D), BF), pltpu.VMEM((S, FL), BF), pltpu.VMEM((S, FL), BF), pltpu.VMEM((S, D), BF),
                pltpu.VMEM((3, HL, HD), F32), *[pltpu.VMEM((D,), F32) for _ in range(7)],
                pltpu.VMEM((2, TP, SL, HW), BF), pltpu.VMEM((2, SL, D), BF), pltpu.VMEM((SL, D), BF), pltpu.VMEM((SL, D), BF),
                pltpu.VMEM((2, 2, SL, HW), BF), pltpu.VMEM((2, 2, D), F32),
                pltpu.SemaphoreType.DMA((9,)), pltpu.SemaphoreType.DMA((N_SEND,)), pltpu.SemaphoreType.DMA((N_SEND,)),
                pltpu.SemaphoreType.DMA((10,)),
            ],
            compiler_params=pltpu.CompilerParams(collective_id=0, has_side_effects=True, vmem_limit_bytes=VMEM_A),
            name='block',
        )(*(pltpu.with_memory_space_constraint(v, pltpu.HBM) for v in (
            x.reshape(SL, D), grad_y.reshape(SL, D), g1, be1, g2, be2, b_out, b_down, bq, b_up, wq, w_out, w_up, w_down)))
        mine, xh, gm, rs, g1v, r_hs, ln_hs = mids[8:]
        across = [(i, TP - 1 - i) for i in range(TP)]
        r_cr = lax.ppermute(r_hs, 'tp', across)
        y, gwqkv, gbqkv, gwout, gbo, gl2, bl2, gwup, gbup, gwdn, gbd = pl.pallas_call(
            write_kernel,
            out_shape=(sds((SL, D), BF), sds((3 * HL * HD, D), BF), sds((3, HL, HD), F32), sds((HL * HD, D), BF), vec1, vec1, vec1,
                       sds((D, FL), BF), vec1, sds((FL, D), BF), vec1),
            in_specs=[VM] * 8,
            out_specs=(ANY,) * 11,
            scratch_shapes=[pltpu.VMEM((3 * HL * HD, D), BF), pltpu.VMEM((HL * HD, D), BF), pltpu.VMEM((3, HL, HD), F32),
                            *[pltpu.VMEM((D,), F32) for _ in range(5)], pltpu.SemaphoreType.DMA((20,))],
            compiler_params=pltpu.CompilerParams(vmem_limit_bytes=VMEM_B),
            cost_estimate=pl.CostEstimate(flops=600_000_000, bytes_accessed=14_200_000, transcendentals=0),
            name='write',
        )(*mids[:8])
        gx, gl1, bl1 = pl.pallas_call(
            last_kernel,
            out_shape=(sds((SL, D), BF), vec1, vec1),
            in_specs=[VM] * 7,
            out_specs=(VM,) * 3,
            compiler_params=pltpu.CompilerParams(vmem_limit_bytes=VMEM_C),
            name='last',
        )(mine, xh, gm, rs, g1v, r_cr, ln_hs)
        gwqkv = jnp.transpose(gwqkv.reshape(HL, 3, HD, D), (3, 0, 1, 2))
        gbqkv = jnp.transpose(gbqkv, (1, 0, 2))
        return (y.reshape(1, SL, D), gx.reshape(1, SL, D), gl1, bl1, gwqkv, gbqkv, gwout, gbo, gl2, bl2, gwup, gbup, gwdn, gbd)

    row_spec = P('dp', 'tp', None)
    in_specs = (row_spec, P(), P(), P(None, 'tp', None, None), P('tp', None, None), P('tp', None), P(), P(), P(),
                P(None, 'tp'), P('tp'), P('tp', None), P(), row_spec)
    out_specs = (row_spec, row_spec, P('dp'), P('dp'), P('dp', 'tp', None, None), P(('dp', 'tp'), None, None),
                 P(('dp', 'tp'), None), P('dp'), P('dp'), P('dp'), P('dp', 'tp'), P(('dp', 'tp')), P(('dp', 'tp'), None), P('dp'))
    return jax.shard_map(local_step, mesh=mesh, in_specs=in_specs, out_specs=out_specs, check_vma=False)
```

```python
import functools
import math

import jax
import jax.numpy as jnp
from jax import lax
from jax.experimental import pallas as pl
from jax.experimental.pallas import tpu as pltpu
from jax.sharding import PartitionSpec as P

EPS = 1e-5
MASK_VALUE = -1e30
BF = jnp.bfloat16
F32 = jnp.float32
MESH = pl.DeviceIdType.MESH

D = 1536
S = 96
SL = 24
TP = 4
HL = 4
HD = 96
FL = 1536
CW = 256
NCH = D // CW
HCH = NCH // 2
HW = D // 2
CUT = (0, 256, 512, 640, 768)
NCUT = len(CUT) - 1


def alibi_slopes(n_heads):
    closest = 2 ** int(math.floor(math.log2(n_heads)))
    base_ratio = 2.0 ** (-8.0 / closest)
    extra_ratio = 2.0 ** (-4.0 / closest)
    remaining = min(closest, n_heads - closest)
    slopes = [base_ratio ** (i + 1) for i in range(closest)]
    return slopes + [extra_ratio ** (2 * i + 1) for i in range(remaining)]


def dot(a, b, ca, cb):
    return lax.dot_general(a, b, (((ca,), (cb,)), ((), ())), preferred_element_type=F32)


def gelu_parts(u):
    k = math.sqrt(2.0 / math.pi)
    u2 = u * u
    th = jnp.tanh(u * (k + (k * 0.044715) * u2))
    half = 0.5 + 0.5 * th
    val = u * half
    return val, half + val * (1.0 - th) * (k + (3.0 * 0.044715 * k) * u2)


def rows_stats(v):
    mean = jnp.mean(v, axis=-1, keepdims=True)
    cen = v - mean
    var = jnp.mean(cen * cen, axis=-1, keepdims=True)
    return cen, lax.rsqrt(var + EPS)


def places():
    t = lax.axis_index('tp')
    core = t % 2
    pt = t + 1 - 2 * core
    ct = TP - 1 - t
    qt = TP - 1 - pt
    half = (core + t // 2) % 2
    return t, pt, ct, qt, half


def sender(ssem, rsem):
    started = []

    def send(src, dst, dev):
        i = len(started)
        c = pltpu.make_async_remote_copy(src_ref=src, dst_ref=dst, send_sem=ssem.at[i], recv_sem=rsem.at[i],
                                         device_id={'tp': dev}, device_id_type=MESH)
        c.start()
        started.append(c)
        return c

    return send, started


def head_rows(h, e):
    return slice((h * 3 + e) * HD, (h * 3 + e + 1) * HD)


def row_blocks(buf, cols, v):
    for i in range(TP):
        buf[i, :, cols] = v[i * SL:(i + 1) * SL, :].astype(BF)


def block_kernel(x_hbm, gy_hbm, g1_hbm, be1_hbm, g2_hbm, be2_hbm, bo_hbm, bd_hbm, bqkv_hbm, bup_hbm,
                 wqkv_hbm, wout_hbm, wup_hbm, wdn_hbm,
                 y_ref, vec_ref, gwup_ref, gwdn_ref, gqkv_ref, h_ref, ctx_ref, gmid_ref, mine_ref, xh_ref, gm_ref, rs_ref, g1_out, r_hs, ln_hs,
                 wqkv, wout, xf, gm_f, gg_f, xhat, rstd_s, probs, qkvT, par, mp,
                 wup, wdn, xg, gyg, biasT, a_ps, a_pr, a_hs, a_hr, a_cr, a_fr, b_ps, b_pr, b_hs, b_hr, b_cr, b_fr,
                 gact, g_ref, gpre_ref, act_ref, gyf_ref, bqkv_ref, g1_in, be1_in, g2_in, be2_in, bo_in, bd_in, bup_in,
                 rp, m_pr, m_hs, m_cr, r_pr, ln_x,
                 wsem, ssem, rsem, isem):
    t, pt, ct, qt, half = places()
    send, started = sender(ssem, rsem)

    in_x = pltpu.make_async_copy(x_hbm, xg.at[t], isem.at[0])
    in_gy = pltpu.make_async_copy(gy_hbm, gyg.at[t], isem.at[1])
    in_b = pltpu.make_async_copy(bqkv_hbm, bqkv_ref, isem.at[2])
    small = ((g1_hbm, g1_in), (be1_hbm, be1_in), (g2_hbm, g2_in), (be2_hbm, be2_in), (bo_hbm, bo_in), (bd_hbm, bd_in), (bup_hbm, bup_in))
    in_p = [pltpu.make_async_copy(a, b, isem.at[3 + i]) for i, (a, b) in enumerate(small)]
    for c in (in_x, in_gy, in_b, *in_p):
        c.start()
    w_cps = {}
    w_cps['qkv'] = [pltpu.make_async_copy(wqkv_hbm, wqkv, wsem.at[0])]
    w_cps['out'] = [pltpu.make_async_copy(wout_hbm.at[:, pl.ds(k * HW, HW)], wout.at[k], wsem.at[1 + k]) for k in range(2)]
    w_cps['dn'] = [pltpu.make_async_copy(wdn_hbm, wdn, wsem.at[7])]
    w_cps['up'] = [pltpu.make_async_copy(wup_hbm, wup, wsem.at[8])]

    barrier = pltpu.get_barrier_semaphore()
    for dev in (pt, ct, qt):
        pl.semaphore_signal(barrier, inc=1, device_id={'tp': dev}, device_id_type=MESH)
    for name in ('qkv', 'out', 'dn', 'up'):
        for c in w_cps[name]:
            c.start()
    pl.semaphore_wait(barrier, 3)

    in_x.wait()
    x_c = send(xg.at[t], xg.at[t], ct)
    x_p = send(xg.at[t], xg.at[t], pt)

    for c in (in_b, *in_p):
        c.wait()
    for i, r in enumerate((g1_in, be1_in, g2_in, be2_in, bo_in, bd_in, bup_in)):
        par[i, :] = r[...]
    g1_ref, be1_ref, g2_ref, be2_ref, bo_ref, bd_ref, bup_ref = (par.at[i:i + 1] for i in range(7))

    for h in range(HL):
        for e in range(3):
            row = jnp.broadcast_to(bqkv_ref[e, h:h + 1, :], (S, HD))
            biasT[pl.ds((h * 3 + e) * HD, HD), :] = row.T

    x_c.wait_recv()
    x_f = send(xg.at[ct], xg.at[ct], pt)
    in_gy.wait()
    y_c = send(gyg.at[t], gyg.at[t], ct)
    y_p = send(gyg.at[t], gyg.at[t], pt)
    x_p.wait_recv()
    x_f.wait_recv()

    for i in range(TP):
        xf[pl.ds(i * SL, SL), :] = xg[i].astype(F32)
    for r in range(0, S, 32):
        cen, rstd = rows_stats(xf[r:r + 32, :])
        xh = cen * rstd
        xhat[r:r + 32, :] = xh
        rstd_s[r:r + 32, :] = jnp.broadcast_to(rstd, (32, 128))
        h_ref[r:r + 32, :] = (xh * g1_ref[...] + be1_ref[...]).astype(BF)

    w_cps['qkv'][0].wait()
    hv = h_ref[...]
    for h in range(HL):
        rows = slice(h * 3 * HD, (h + 1) * 3 * HD)
        qkvT[rows, :] = (dot(wqkv[rows, :], hv, 1, 1) + biasT[rows, :]).astype(BF)

    scale = HD ** -0.5
    slopes = alibi_slopes(HL * TP)
    j_pos = lax.broadcasted_iota(jnp.int32, (S, S), 0)
    i_pos = lax.broadcasted_iota(jnp.int32, (S, S), 1)
    causal = j_pos <= i_pos
    j_f = j_pos.astype(F32)

    def head(h, e):
        return qkvT[head_rows(h, e), :]

    for h in range(HL):
        slope = jnp.where(t == 0, slopes[h], jnp.where(t == 1, slopes[HL + h], jnp.where(t == 2, slopes[2 * HL + h], slopes[3 * HL + h]))).astype(F32)
        s = dot(head(h, 1), head(h, 0), 0, 0) * scale + slope * j_f
        s = jnp.where(causal, s, MASK_VALUE)
        p = jnp.exp(s - jnp.max(s, axis=0, keepdims=True))
        p = p / jnp.sum(p, axis=0, keepdims=True)
        probs[h] = p
        ctx_ref[h * HD:(h + 1) * HD, :] = dot(head(h, 2), p.astype(BF), 1, 0).astype(BF)

    def exchange(part, groups, ps, pr, hs, hr, cr, fr):
        firsts = []
        for k0, k1 in groups:
            cols = slice(CUT[k0], CUT[k1])
            ps[:, cols] = part(1 - half, CUT[k0], CUT[k1]).astype(BF)
            firsts.append(send(ps.at[:, cols], pr.at[:, cols], pt))
        outs = []
        for (k0, k1), first in zip(groups, firsts):
            cols = slice(CUT[k0], CUT[k1])
            ours = part(half, CUT[k0], CUT[k1])
            first.wait_recv()
            hs[:, cols] = (ours + pr[:, cols].astype(F32)).astype(BF)
            for k in range(k0, k1):
                c = slice(CUT[k], CUT[k + 1])
                outs.append([send(hs.at[:, c], cr.at[:, c], ct)])
                if k == NCUT - 1:
                    outs[-1].append(send(hs.at[:, c], fr.at[:, c], qt))
        local = send(hs, hr, pt)
        return outs, local

    def forward(out, k, cr, fr):
        if k < NCUT - 1:
            c = slice(CUT[k], CUT[k + 1])
            out[0].wait_recv()
            out.append(send(cr.at[:, c], fr.at[:, c], pt))

    for c in w_cps['out']:
        c.wait()
    ctxT = ctx_ref[...]
    a_outs, a_local = exchange(lambda hh, c0, c1: dot(ctxT, wout[hh, :, c0:c1], 0, 0), ((0, NCUT),), a_ps, a_pr, a_hs, a_hr, a_cr, a_fr)

    y_c.wait_recv()
    y_f = send(gyg.at[ct], gyg.at[ct], pt)
    y_p.wait_recv()
    y_f.wait_recv()
    for i in range(TP):
        gm_f[pl.ds(i * SL, SL), :] = gyg[i].astype(F32)
    for r in range(0, S, 32):
        gyf_ref[r:r + 32, :] = gm_f[r:r + 32, :].astype(BF)
    w_cps['dn'][0].wait()
    gyv = gyf_ref[...]
    for n in range(NCH):
        gact[:, n * CW:(n + 1) * CW] = dot(gyv, wdn[n * CW:(n + 1) * CW, :], 1, 1).astype(BF)
    vec_ref[0:1, :] = jnp.sum(gm_f[...], axis=0, keepdims=True)

    def gathered(outs, local, hs, hr, cr, fr, put):
        outs[-1][0].wait_recv()
        for k in range(HCH):
            c = slice(k * CW, (k + 1) * CW)
            put(half * HCH + k, (hs[:, c].astype(F32) + cr[:, c].astype(F32)).astype(BF).astype(F32))
        local.wait_recv()
        for out in outs:
            out[1].wait_recv()
        for k in range(HCH):
            c = slice(k * CW, (k + 1) * CW)
            put((1 - half) * HCH + k, (hr[:, c].astype(F32) + fr[:, c].astype(F32)).astype(BF).astype(F32))

    for k, out in enumerate(a_outs):
        forward(out, k, a_cr, a_fr)

    def put_x(kk, val):
        cols = pl.ds(pl.multiple_of(kk * CW, CW), CW)
        xf[:, cols] = xf[:, cols] + val + bo_ref[:, cols]

    gathered(a_outs, a_local, a_hs, a_hr, a_cr, a_fr, put_x)

    for r in range(0, S, 32):
        cen, rstd = rows_stats(xf[r:r + 32, :])
        g_ref[r:r + 32, :] = (cen * rstd * g2_ref[...] + be2_ref[...]).astype(BF)

    w_cps['up'][0].wait()
    gv = g_ref[...]
    for n in range(NCH):
        cols = slice(n * CW, (n + 1) * CW)
        pre = dot(gv, wup[:, cols], 1, 0) + bup_ref[:, cols]
        val, der = gelu_parts(pre)
        act_ref[:, cols] = val.astype(BF)
        gp = gact[:, cols].astype(F32) * der
        vec_ref[1:2, cols] = jnp.sum(gp, axis=0, keepdims=True)
        gpre_ref[:, cols] = gp.astype(BF)

    gprev = gpre_ref[...]

    def part_g(hh, c0, c1):
        return dot(gprev, wup[pl.ds(pl.multiple_of(hh * HW + c0, CW), c1 - c0), :], 1, 1)

    g_outs, g_local = exchange(part_g, ((0, 1), (1, NCUT)), b_ps, b_pr, b_hs, b_hr, b_cr, b_fr)

    actv = act_ref[...]
    for n in range(NCH):
        cols = slice(n * CW, (n + 1) * CW)
        row_blocks(mp, cols, dot(actv, wdn[:, cols], 1, 0))
    m_first = (send(mp.at[qt], m_pr.at[1], pt), send(mp.at[pt], m_pr.at[0], pt))
    for n in range(NCH):
        gwdn_ref[n * CW:(n + 1) * CW, :] = dot(act_ref[:, n * CW:(n + 1) * CW], gyv, 0, 0).astype(BF)
    for k in range(HCH):
        forward(g_outs[k], k, b_cr, b_fr)
        for n in range(2 * k, 2 * k + 2):
            gwup_ref[n * CW:(n + 1) * CW, :] = dot(g_ref[:, n * CW:(n + 1) * CW], gprev, 0, 0).astype(BF)

    m_first[0].wait_recv()
    m_hs[...] = (mp[ct].astype(F32) + m_pr[1].astype(F32)).astype(BF)
    m_out = send(m_hs, m_cr, ct)

    def put_g(kk, val):
        gg_f[:, pl.ds(pl.multiple_of(kk * CW, CW), CW)] = val

    gathered(g_outs, g_local, b_hs, b_hr, b_cr, b_fr, put_g)

    gg2 = jnp.zeros((1, D), F32)
    gb2 = jnp.zeros((1, D), F32)
    gbo = jnp.zeros((1, D), F32)
    for r in range(0, S, 32):
        cen, rstd = rows_stats(xf[r:r + 32, :])
        xh = cen * rstd
        gg = gg_f[r:r + 32, :]
        gg2 = gg2 + jnp.sum(gg * xh, axis=0, keepdims=True)
        gb2 = gb2 + jnp.sum(gg, axis=0, keepdims=True)
        dxh = gg * g2_ref[...]
        m1 = jnp.mean(dxh, axis=-1, keepdims=True)
        m2 = jnp.mean(dxh * xh, axis=-1, keepdims=True)
        gm = gm_f[r:r + 32, :] + rstd * (dxh - m1 - xh * m2)
        gm_f[r:r + 32, :] = gm
        gbo = gbo + jnp.sum(gm, axis=0, keepdims=True)
        gmid_ref[r:r + 32, :] = gm.astype(BF)
    vec_ref[2:3, :] = gg2
    vec_ref[3:4, :] = gb2
    vec_ref[4:5, :] = gbo

    gmv = gmid_ref[...]
    gctxT = (dot(wout[0], gmv[:, :HW], 1, 1) + dot(wout[1], gmv[:, HW:], 1, 1)).astype(BF)
    heads = range(HL)
    gos = [gctxT[h * HD:(h + 1) * HD, :] for h in heads]
    gps = [dot(head(h, 2), gos[h], 0, 0).astype(BF).astype(F32) for h in heads]
    gvs = [dot(gos[h], probs[h].astype(BF), 1, 1).astype(BF) for h in heads]
    gss = [(probs[h] * (gps[h] - jnp.sum(gps[h] * probs[h], axis=0, keepdims=True))).astype(BF) for h in heads]
    gqs = [(dot(head(h, 1), gss[h], 1, 0) * scale).astype(BF) for h in heads]
    gks = [(dot(head(h, 0), gss[h], 1, 1) * scale).astype(BF) for h in heads]
    for h in heads:
        for e, val in enumerate((gqs[h], gks[h], gvs[h])):
            gqkv_ref[head_rows(h, e), :] = val

    gqv = gqkv_ref[...]
    r_first = []
    for k in range(2):
        row_blocks(rp.at[k], slice(0, HW), dot(gqv, wqkv[:, k * HW:(k + 1) * HW], 0, 0))
        r_first.append((send(rp.at[k, qt], r_pr.at[k, 1], pt), send(rp.at[k, pt], r_pr.at[k, 0], pt)))

    ln_s, ln_pr = ln_x.at[0], ln_x.at[1]
    for k in range(2):
        cols = slice(k * HW, (k + 1) * HW)
        gg1 = jnp.zeros((1, HW), F32)
        gb1 = jnp.zeros((1, HW), F32)
        for i in range(TP):
            v = rp[k, i].astype(F32)
            gg1 = gg1 + jnp.sum(v * xhat[i * SL:(i + 1) * SL, cols], axis=0, keepdims=True)
            gb1 = gb1 + jnp.sum(v, axis=0, keepdims=True)
        ln_s[0:1, cols] = gg1
        ln_s[1:2, cols] = gb1
    l_first = send(ln_s, ln_pr, pt)

    own = pl.ds(pl.multiple_of(t * SL, 8), SL)
    xh_ref[...] = xhat[own, :]
    gm_ref[...] = gm_f[own, :]
    rs_ref[...] = rstd_s[own, :]
    g1_out[...] = par[0:1, :]

    for k in range(2):
        cols = slice(k * HW, (k + 1) * HW)
        r_first[k][0].wait_recv()
        r_hs[0:SL, cols] = (rp[k, ct].astype(F32) + r_pr[k, 1].astype(F32)).astype(BF)
        r_first[k][1].wait_recv()
        mine_ref[:, cols] = (rp[k, t].astype(F32) + r_pr[k, 0].astype(F32)).astype(BF)
    l_first.wait_recv()
    ln = ln_s[...] + ln_pr[...]
    ln_hs[...] = ln
    ln_rows = []
    for _ in range(3):
        ln_rows.append(ln.astype(BF).astype(F32))
        ln = ln - ln_rows[-1]
    r_hs[SL:SL + 8, :] = jnp.concatenate(ln_rows + [jnp.zeros((2, D), F32)], axis=0).astype(BF)
    m_first[1].wait_recv()
    m_out.wait_recv()
    m_sum = (mp[t].astype(F32) + m_pr[0].astype(F32)).astype(BF).astype(F32) + m_cr[...].astype(F32)
    y_ref[...] = (xf[own, :] + m_sum.astype(BF).astype(F32) + bd_ref[...]).astype(BF)
    for c in started:
        c.wait_send()


N_SEND = 6 + 2 * (2 + 4 + 1 + 1 + 3) + 3 + 4 + 1
VMEM_A = 36 * 2**20
VMEM_B = 8 * 2**20
VMEM_C = 4 * 2**20


def write_kernel(yi_ref, vec_ref, up_ref, dn_ref, gqkv_ref, h_ref, ctx_ref, gmid_ref,
                 y_ref, gwqkv_ref, gbqkv_ref, gwout_ref, gbo_ref, gl2_ref, bl2_ref, gwup_ref, gbup_ref, gwdn_ref, gbd_ref,
                 s_qkv, s_out, s_gb, s0, s1, s2, s3, s4, sem):
    cps = []

    def out(src, dst, n=1):
        rows = src.shape[0] // n
        for k in range(n):
            c = pltpu.make_async_copy(src.at[pl.ds(k * rows, rows)], dst.at[pl.ds(k * rows, rows)], sem.at[len(cps)])
            c.start()
            cps.append(c)

    out(dn_ref, gwdn_ref, 4)
    out(up_ref, gwup_ref, 4)
    out(yi_ref, y_ref)
    for i, (sv, r) in enumerate(((s0, gbd_ref), (s1, gbup_ref), (s2, gl2_ref), (s3, bl2_ref), (s4, gbo_ref))):
        sv[...] = vec_ref[i, :]
        out(sv, r)
    ones = jnp.ones((8, S), BF)
    for h in range(HL):
        for e in range(3):
            s_gb[e, h:h + 1, :] = dot(ones, gqkv_ref[head_rows(h, e), :], 1, 1)[0:1, :]
    out(s_gb, gbqkv_ref)
    hv = h_ref[...]
    s_out[...] = dot(ctx_ref[...], gmid_ref[...], 1, 0).astype(BF)
    out(s_out, gwout_ref)
    for n in range(HL):
        rows = slice(n * 3 * HD, (n + 1) * 3 * HD)
        s_qkv[rows, :] = dot(gqkv_ref[rows, :], hv, 1, 0).astype(BF)
        out(s_qkv.at[rows], gwqkv_ref.at[rows])
    for c in cps:
        c.wait()


def last_kernel(mine_ref, xh_ref, gm_ref, rs_ref, g1_ref, rc_ref, ln_ref, gx_ref, gl1_ref, bl1_ref):
    gh = (mine_ref[...].astype(F32) + rc_ref[0:SL, :].astype(F32)).astype(BF).astype(F32)
    xh = xh_ref[...]
    dxh = gh * g1_ref[...]
    m1 = jnp.mean(dxh, axis=-1, keepdims=True)
    m2 = jnp.mean(dxh * xh, axis=-1, keepdims=True)
    gx_ref[...] = (gm_ref[...] + rs_ref[:, 0:1] * (dxh - m1 - xh * m2)).astype(BF)
    lc = rc_ref[SL:SL + 8, :].astype(F32)
    ln = ln_ref[...] + (lc[0:2, :] + lc[2:4, :] + lc[4:6, :])
    gl1_ref[...] = ln[0, :]
    bl1_ref[...] = ln[1, :]


def solution(mesh):
    VM = pl.BlockSpec(memory_space=pltpu.VMEM)
    ANY = pl.BlockSpec(memory_space=pltpu.HBM)

    def sds(shape, dt):
        return jax.ShapeDtypeStruct(shape, dt)

    def local_step(x, g1, be1, w_qkv, b_qkv, w_out, b_out, g2, be2, w_up, b_up, w_down, b_down, grad_y):
        wq = jnp.transpose(w_qkv, (1, 2, 3, 0)).reshape(3 * HL * HD, D)
        bq = jnp.transpose(b_qkv, (1, 0, 2))
        part = pltpu.VMEM((S, HW), BF)
        vec1 = sds((D,), F32)
        mids = pl.pallas_call(
            block_kernel,
            out_shape=(pltpu.VMEM((SL, D), BF), pltpu.VMEM((8, D), F32), pltpu.VMEM((D, FL), BF), pltpu.VMEM((FL, D), BF),
                       pltpu.VMEM((3 * HL * HD, S), BF), pltpu.VMEM((S, D), BF), pltpu.VMEM((HL * HD, S), BF), pltpu.VMEM((S, D), BF),
                       pltpu.VMEM((SL, D), BF), pltpu.VMEM((SL, D), F32), pltpu.VMEM((SL, D), F32), pltpu.VMEM((SL, 128), F32),
                       pltpu.VMEM((1, D), F32), sds((SL + 8, D), BF), pltpu.VMEM((2, D), F32)),
            in_specs=[ANY] * 14,
            out_specs=(VM,) * 15,
            scratch_shapes=[
                pltpu.VMEM((3 * HL * HD, D), BF), pltpu.VMEM((2, HL * HD, HW), BF), pltpu.VMEM((S, D), F32), pltpu.VMEM((S, D), F32),
                pltpu.VMEM((S, D), F32), pltpu.VMEM((S, D), F32), pltpu.VMEM((S, 128), F32), pltpu.VMEM((HL, S, S), F32),
                pltpu.VMEM((3 * HL * HD, S), BF), pltpu.VMEM((8, D), F32), pltpu.VMEM((TP, SL, D), BF),
                pltpu.VMEM((D, FL), BF), pltpu.VMEM((FL, D), BF), pltpu.VMEM((TP, SL, D), BF), pltpu.VMEM((TP, SL, D), BF),
                pltpu.VMEM((3 * HL * HD, S), F32), *[part] * 12,
                pltpu.VMEM((S, FL), BF), pltpu.VMEM((S, D), BF), pltpu.VMEM((S, FL), BF), pltpu.VMEM((S, FL), BF), pltpu.VMEM((S, D), BF),
                pltpu.VMEM((3, HL, HD), F32), *[pltpu.VMEM((D,), F32) for _ in range(7)],
                pltpu.VMEM((2, TP, SL, HW), BF), pltpu.VMEM((2, SL, D), BF), pltpu.VMEM((SL, D), BF), pltpu.VMEM((SL, D), BF),
                pltpu.VMEM((2, 2, SL, HW), BF), pltpu.VMEM((2, 2, D), F32),
                pltpu.SemaphoreType.DMA((9,)), pltpu.SemaphoreType.DMA((N_SEND,)), pltpu.SemaphoreType.DMA((N_SEND,)),
                pltpu.SemaphoreType.DMA((10,)),
            ],
            compiler_params=pltpu.CompilerParams(collective_id=0, has_side_effects=True, vmem_limit_bytes=VMEM_A),
            name='block',
        )(*(pltpu.with_memory_space_constraint(v, pltpu.HBM) for v in (
            x.reshape(SL, D), grad_y.reshape(SL, D), g1, be1, g2, be2, b_out, b_down, bq, b_up, wq, w_out, w_up, w_down)))
        mine, xh, gm, rs, g1v, r_hs, ln_hs = mids[8:]
        across = [(i, TP - 1 - i) for i in range(TP)]
        r_cr = lax.ppermute(r_hs, 'tp', across)
        y, gwqkv, gbqkv, gwout, gbo, gl2, bl2, gwup, gbup, gwdn, gbd = pl.pallas_call(
            write_kernel,
            out_shape=(sds((SL, D), BF), sds((3 * HL * HD, D), BF), sds((3, HL, HD), F32), sds((HL * HD, D), BF), vec1, vec1, vec1,
                       sds((D, FL), BF), vec1, sds((FL, D), BF), vec1),
            in_specs=[VM] * 8,
            out_specs=(ANY,) * 11,
            scratch_shapes=[pltpu.VMEM((3 * HL * HD, D), BF), pltpu.VMEM((HL * HD, D), BF), pltpu.VMEM((3, HL, HD), F32),
                            *[pltpu.VMEM((D,), F32) for _ in range(5)], pltpu.SemaphoreType.DMA((20,))],
            compiler_params=pltpu.CompilerParams(vmem_limit_bytes=VMEM_B),
            cost_estimate=pl.CostEstimate(flops=600_000_000, bytes_accessed=14_200_000, transcendentals=0),
            name='write',
        )(*mids[:8])
        gx, gl1, bl1 = pl.pallas_call(
            last_kernel,
            out_shape=(sds((SL, D), BF), vec1, vec1),
            in_specs=[VM] * 7,
            out_specs=(VM,) * 3,
            compiler_params=pltpu.CompilerParams(vmem_limit_bytes=VMEM_C),
            name='last',
        )(mine, xh, gm, rs, g1v, r_cr, ln_hs)
        gwqkv = jnp.transpose(gwqkv.reshape(HL, 3, HD, D), (3, 0, 1, 2))
        gbqkv = jnp.transpose(gbqkv, (1, 0, 2))
        return (y.reshape(1, SL, D), gx.reshape(1, SL, D), gl1, bl1, gwqkv, gbqkv, gwout, gbo, gl2, bl2, gwup, gbup, gwdn, gbd)

    row_spec = P('dp', 'tp', None)
    in_specs = (row_spec, P(), P(), P(None, 'tp', None, None), P('tp', None, None), P('tp', None), P(), P(), P(),
                P(None, 'tp'), P('tp'), P('tp', None), P(), row_spec)
    out_specs = (row_spec, row_spec, P('dp'), P('dp'), P('dp', 'tp', None, None), P(('dp', 'tp'), None, None),
                 P(('dp', 'tp'), None), P('dp'), P('dp'), P('dp'), P('dp', 'tp'), P(('dp', 'tp')), P(('dp', 'tp'), None), P('dp'))
    return jax.shard_map(local_step, mesh=mesh, in_specs=in_specs, out_specs=out_specs, check_vma=False)
```

```python
import functools
import math

import jax
import jax.numpy as jnp
from jax import lax
from jax.experimental import pallas as pl
from jax.experimental.pallas import tpu as pltpu
from jax.sharding import PartitionSpec as P

EPS = 1e-5
MASK_VALUE = -1e30
BF = jnp.bfloat16
F32 = jnp.float32
MESH = pl.DeviceIdType.MESH

D = 1536
S = 96
SL = 24
TP = 4
HL = 4
HD = 96
FL = 1536
CW = 256
NCH = D // CW
HCH = NCH // 2
HW = D // 2
CUT = (0, 256, 512, 640, 768)
NCUT = len(CUT) - 1


def alibi_slopes(n_heads):
    closest = 2 ** int(math.floor(math.log2(n_heads)))
    base_ratio = 2.0 ** (-8.0 / closest)
    extra_ratio = 2.0 ** (-4.0 / closest)
    remaining = min(closest, n_heads - closest)
    slopes = [base_ratio ** (i + 1) for i in range(closest)]
    return slopes + [extra_ratio ** (2 * i + 1) for i in range(remaining)]


def dot(a, b, ca, cb):
    return lax.dot_general(a, b, (((ca,), (cb,)), ((), ())), preferred_element_type=F32)


def gelu_parts(u):
    k = math.sqrt(2.0 / math.pi)
    u2 = u * u
    th = jnp.tanh(u * (k + (k * 0.044715) * u2))
    half = 0.5 + 0.5 * th
    val = u * half
    return val, half + val * (1.0 - th) * (k + (3.0 * 0.044715 * k) * u2)


def rows_stats(v):
    mean = jnp.mean(v, axis=-1, keepdims=True)
    cen = v - mean
    var = jnp.mean(cen * cen, axis=-1, keepdims=True)
    return cen, lax.rsqrt(var + EPS)


def places():
    t = lax.axis_index('tp')
    core = t % 2
    pt = t + 1 - 2 * core
    ct = TP - 1 - t
    qt = TP - 1 - pt
    half = (core + t // 2) % 2
    return t, pt, ct, qt, half


def sender(ssem, rsem):
    started = []

    def send(src, dst, dev):
        i = len(started)
        c = pltpu.make_async_remote_copy(src_ref=src, dst_ref=dst, send_sem=ssem.at[i], recv_sem=rsem.at[i],
                                         device_id={'tp': dev}, device_id_type=MESH)
        c.start()
        started.append(c)
        return c

    return send, started


def head_rows(h, e):
    return slice((h * 3 + e) * HD, (h * 3 + e + 1) * HD)


def row_blocks(buf, cols, v):
    for i in range(TP):
        buf[i, :, cols] = v[i * SL:(i + 1) * SL, :].astype(BF)


def block_kernel(x_hbm, gy_hbm, g1_hbm, be1_hbm, g2_hbm, be2_hbm, bo_hbm, bd_hbm, bqkv_hbm, bup_hbm,
                 wqkv_hbm, wout_hbm, wup_hbm, wdn_hbm,
                 y_ref, vec_ref, gwup_ref, gwdn_ref, gqkv_ref, h_ref, ctx_ref, gmid_ref, mine_ref, xh_ref, gm_ref, rs_ref, g1_out, r_hs, ln_hs,
                 wqkv, wout, xf, gm_f, gg_f, xhat, rstd_s, probs, qkvT, par, mp,
                 wup, wdn, xg, gyg, biasT, a_ps, a_pr, a_hs, a_hr, a_cr, a_fr, b_ps, b_pr, b_hs, b_hr, b_cr, b_fr,
                 gact, g_ref, gpre_ref, act_ref, gyf_ref, bqkv_ref, g1_in, be1_in, g2_in, be2_in, bo_in, bd_in, bup_in,
                 rp, m_pr, m_hs, m_cr, r_pr, ln_x,
                 wsem, ssem, rsem, isem):
    t, pt, ct, qt, half = places()
    send, started = sender(ssem, rsem)

    in_x = pltpu.make_async_copy(x_hbm, xg.at[t], isem.at[0])
    in_gy = pltpu.make_async_copy(gy_hbm, gyg.at[t], isem.at[1])
    in_b = pltpu.make_async_copy(bqkv_hbm, bqkv_ref, isem.at[2])
    small = ((g1_hbm, g1_in), (be1_hbm, be1_in), (g2_hbm, g2_in), (be2_hbm, be2_in), (bo_hbm, bo_in), (bd_hbm, bd_in), (bup_hbm, bup_in))
    in_p = [pltpu.make_async_copy(a, b, isem.at[3 + i]) for i, (a, b) in enumerate(small)]
    for c in (in_x, in_gy, in_b, *in_p):
        c.start()
    w_cps = {}
    w_cps['qkv'] = [pltpu.make_async_copy(wqkv_hbm, wqkv, wsem.at[0])]
    w_cps['out'] = [pltpu.make_async_copy(wout_hbm.at[:, pl.ds(k * HW, HW)], wout.at[k], wsem.at[1 + k]) for k in range(2)]
    w_cps['dn'] = [pltpu.make_async_copy(wdn_hbm, wdn, wsem.at[7])]
    w_cps['up'] = [pltpu.make_async_copy(wup_hbm, wup, wsem.at[8])]

    barrier = pltpu.get_barrier_semaphore()
    for dev in (pt, ct, qt):
        pl.semaphore_signal(barrier, inc=1, device_id={'tp': dev}, device_id_type=MESH)
    for name in ('qkv', 'out', 'dn', 'up'):
        for c in w_cps[name]:
            c.start()
    pl.semaphore_wait(barrier, 3)

    in_x.wait()
    x_c = send(xg.at[t], xg.at[t], ct)
    x_p = send(xg.at[t], xg.at[t], pt)

    for c in (in_b, *in_p):
        c.wait()
    for i, r in enumerate((g1_in, be1_in, g2_in, be2_in, bo_in, bd_in, bup_in)):
        par[i, :] = r[...]
    g1_ref, be1_ref, g2_ref, be2_ref, bo_ref, bd_ref, bup_ref = (par.at[i:i + 1] for i in range(7))

    for h in range(HL):
        for e in range(3):
            row = jnp.broadcast_to(bqkv_ref[e, h:h + 1, :], (S, HD))
            biasT[pl.ds((h * 3 + e) * HD, HD), :] = row.T

    x_p.wait_recv()
    in_gy.wait()
    y_c = send(gyg.at[t], gyg.at[t], ct)
    y_p = send(gyg.at[t], gyg.at[t], pt)
    x_c.wait_recv()
    x_f = send(xg.at[ct], xg.at[ct], pt)
    x_f.wait_recv()

    for i in range(TP):
        xf[pl.ds(i * SL, SL), :] = xg[i].astype(F32)
    for r in range(0, S, 32):
        cen, rstd = rows_stats(xf[r:r + 32, :])
        xh = cen * rstd
        xhat[r:r + 32, :] = xh
        rstd_s[r:r + 32, :] = jnp.broadcast_to(rstd, (32, 128))
        h_ref[r:r + 32, :] = (xh * g1_ref[...] + be1_ref[...]).astype(BF)

    w_cps['qkv'][0].wait()
    hv = h_ref[...]
    for h in range(HL):
        rows = slice(h * 3 * HD, (h + 1) * 3 * HD)
        qkvT[rows, :] = (dot(wqkv[rows, :], hv, 1, 1) + biasT[rows, :]).astype(BF)

    scale = HD ** -0.5
    slopes = alibi_slopes(HL * TP)
    j_pos = lax.broadcasted_iota(jnp.int32, (S, S), 0)
    i_pos = lax.broadcasted_iota(jnp.int32, (S, S), 1)
    causal = j_pos <= i_pos
    j_f = j_pos.astype(F32)

    def head(h, e):
        return qkvT[head_rows(h, e), :]

    for h in range(HL):
        slope = jnp.where(t == 0, slopes[h], jnp.where(t == 1, slopes[HL + h], jnp.where(t == 2, slopes[2 * HL + h], slopes[3 * HL + h]))).astype(F32)
        s = dot(head(h, 1), head(h, 0), 0, 0) * scale + slope * j_f
        s = jnp.where(causal, s, MASK_VALUE)
        p = jnp.exp(s - jnp.max(s, axis=0, keepdims=True))
        p = p / jnp.sum(p, axis=0, keepdims=True)
        probs[h] = p
        ctx_ref[h * HD:(h + 1) * HD, :] = dot(head(h, 2), p.astype(BF), 1, 0).astype(BF)

    def exchange(part, groups, ps, pr, hs, hr, cr, fr):
        firsts = []
        for k0, k1 in groups:
            cols = slice(CUT[k0], CUT[k1])
            ps[:, cols] = part(1 - half, CUT[k0], CUT[k1]).astype(BF)
            firsts.append(send(ps.at[:, cols], pr.at[:, cols], pt))
        outs = []
        for (k0, k1), first in zip(groups, firsts):
            cols = slice(CUT[k0], CUT[k1])
            ours = part(half, CUT[k0], CUT[k1])
            first.wait_recv()
            hs[:, cols] = (ours + pr[:, cols].astype(F32)).astype(BF)
            for k in range(k0, k1):
                c = slice(CUT[k], CUT[k + 1])
                outs.append([send(hs.at[:, c], cr.at[:, c], ct)])
                if k == NCUT - 1:
                    outs[-1].append(send(hs.at[:, c], fr.at[:, c], qt))
        local = send(hs, hr, pt)
        return outs, local

    def arrived(out, k, hs, cr, fr, put):
        c = slice(CUT[k], CUT[k + 1])
        out[0].wait_recv()
        if k < NCUT - 1:
            out.append(send(cr.at[:, c], fr.at[:, c], pt))
        put(half * HW + CUT[k], CUT[k + 1] - CUT[k], (hs[:, c].astype(F32) + cr[:, c].astype(F32)).astype(BF).astype(F32))

    def passed_on(outs, local, hr, fr, put):
        local.wait_recv()
        for k, out in enumerate(outs):
            c = slice(CUT[k], CUT[k + 1])
            out[1].wait_recv()
            put((1 - half) * HW + CUT[k], CUT[k + 1] - CUT[k], (hr[:, c].astype(F32) + fr[:, c].astype(F32)).astype(BF).astype(F32))

    for c in w_cps['out']:
        c.wait()
    ctxT = ctx_ref[...]
    a_outs, a_local = exchange(lambda hh, c0, c1: dot(ctxT, wout[hh, :, c0:c1], 0, 0), ((0, NCUT),), a_ps, a_pr, a_hs, a_hr, a_cr, a_fr)

    y_c.wait_recv()
    y_f = send(gyg.at[ct], gyg.at[ct], pt)
    y_p.wait_recv()
    y_f.wait_recv()
    for i in range(TP):
        gm_f[pl.ds(i * SL, SL), :] = gyg[i].astype(F32)
    for r in range(0, S, 32):
        gyf_ref[r:r + 32, :] = gm_f[r:r + 32, :].astype(BF)
    w_cps['dn'][0].wait()
    gyv = gyf_ref[...]
    for n in range(NCH):
        gact[:, n * CW:(n + 1) * CW] = dot(gyv, wdn[n * CW:(n + 1) * CW, :], 1, 1).astype(BF)
    vec_ref[0:1, :] = jnp.sum(gm_f[...], axis=0, keepdims=True)

    def put_x(start, width, val):
        cols = pl.ds(pl.multiple_of(start, 128), width)
        xf[:, cols] = xf[:, cols] + val + bo_ref[:, cols]

    for k, out in enumerate(a_outs):
        arrived(out, k, a_hs, a_cr, a_fr, put_x)
    passed_on(a_outs, a_local, a_hr, a_fr, put_x)

    for r in range(0, S, 32):
        cen, rstd = rows_stats(xf[r:r + 32, :])
        g_ref[r:r + 32, :] = (cen * rstd * g2_ref[...] + be2_ref[...]).astype(BF)

    w_cps['up'][0].wait()
    gv = g_ref[...]
    for n in range(NCH):
        cols = slice(n * CW, (n + 1) * CW)
        pre = dot(gv, wup[:, cols], 1, 0) + bup_ref[:, cols]
        val, der = gelu_parts(pre)
        act_ref[:, cols] = val.astype(BF)
        gp = gact[:, cols].astype(F32) * der
        vec_ref[1:2, cols] = jnp.sum(gp, axis=0, keepdims=True)
        gpre_ref[:, cols] = gp.astype(BF)

    gprev = gpre_ref[...]

    def part_g(hh, c0, c1):
        return dot(gprev, wup[pl.ds(pl.multiple_of(hh * HW + c0, CW), c1 - c0), :], 1, 1)

    g_outs, g_local = exchange(part_g, ((0, 1), (1, NCUT)), b_ps, b_pr, b_hs, b_hr, b_cr, b_fr)

    actv = act_ref[...]
    for n in range(NCH):
        cols = slice(n * CW, (n + 1) * CW)
        row_blocks(mp, cols, dot(actv, wdn[:, cols], 1, 0))
    m_first = (send(mp.at[qt], m_pr.at[1], pt), send(mp.at[pt], m_pr.at[0], pt))
    for n in range(NCH):
        gwdn_ref[n * CW:(n + 1) * CW, :] = dot(act_ref[:, n * CW:(n + 1) * CW], gyv, 0, 0).astype(BF)
    def put_g(start, width, val):
        gg_f[:, pl.ds(pl.multiple_of(start, 128), width)] = val

    for k in range(HCH):
        arrived(g_outs[k], k, b_hs, b_cr, b_fr, put_g)
        for n in range(2 * k, 2 * k + 2):
            gwup_ref[n * CW:(n + 1) * CW, :] = dot(g_ref[:, n * CW:(n + 1) * CW], gprev, 0, 0).astype(BF)
    arrived(g_outs[-1], NCUT - 1, b_hs, b_cr, b_fr, put_g)

    m_first[0].wait_recv()
    m_hs[...] = (mp[ct].astype(F32) + m_pr[1].astype(F32)).astype(BF)
    m_out = send(m_hs, m_cr, ct)

    passed_on(g_outs, g_local, b_hr, b_fr, put_g)

    gg2 = jnp.zeros((1, D), F32)
    gb2 = jnp.zeros((1, D), F32)
    gbo = jnp.zeros((1, D), F32)
    for r in range(0, S, 32):
        cen, rstd = rows_stats(xf[r:r + 32, :])
        xh = cen * rstd
        gg = gg_f[r:r + 32, :]
        gg2 = gg2 + jnp.sum(gg * xh, axis=0, keepdims=True)
        gb2 = gb2 + jnp.sum(gg, axis=0, keepdims=True)
        dxh = gg * g2_ref[...]
        m1 = jnp.mean(dxh, axis=-1, keepdims=True)
        m2 = jnp.mean(dxh * xh, axis=-1, keepdims=True)
        gm = gm_f[r:r + 32, :] + rstd * (dxh - m1 - xh * m2)
        gm_f[r:r + 32, :] = gm
        gbo = gbo + jnp.sum(gm, axis=0, keepdims=True)
        gmid_ref[r:r + 32, :] = gm.astype(BF)
    vec_ref[2:3, :] = gg2
    vec_ref[3:4, :] = gb2
    vec_ref[4:5, :] = gbo

    gmv = gmid_ref[...]
    gctxT = (dot(wout[0], gmv[:, :HW], 1, 1) + dot(wout[1], gmv[:, HW:], 1, 1)).astype(BF)
    heads = range(HL)
    gos = [gctxT[h * HD:(h + 1) * HD, :] for h in heads]
    gps = [dot(head(h, 2), gos[h], 0, 0).astype(BF).astype(F32) for h in heads]
    gvs = [dot(gos[h], probs[h].astype(BF), 1, 1).astype(BF) for h in heads]
    gss = [(probs[h] * (gps[h] - jnp.sum(gps[h] * probs[h], axis=0, keepdims=True))).astype(BF) for h in heads]
    gqs = [(dot(head(h, 1), gss[h], 1, 0) * scale).astype(BF) for h in heads]
    gks = [(dot(head(h, 0), gss[h], 1, 1) * scale).astype(BF) for h in heads]
    for h in heads:
        for e, val in enumerate((gqs[h], gks[h], gvs[h])):
            gqkv_ref[head_rows(h, e), :] = val

    gqv = gqkv_ref[...]
    r_first = []
    for k in range(2):
        row_blocks(rp.at[k], slice(0, HW), dot(gqv, wqkv[:, k * HW:(k + 1) * HW], 0, 0))
        r_first.append((send(rp.at[k, qt], r_pr.at[k, 1], pt), send(rp.at[k, pt], r_pr.at[k, 0], pt)))

    ln_s, ln_pr = ln_x.at[0], ln_x.at[1]
    for k in range(2):
        cols = slice(k * HW, (k + 1) * HW)
        gg1 = jnp.zeros((1, HW), F32)
        gb1 = jnp.zeros((1, HW), F32)
        for i in range(TP):
            v = rp[k, i].astype(F32)
            gg1 = gg1 + jnp.sum(v * xhat[i * SL:(i + 1) * SL, cols], axis=0, keepdims=True)
            gb1 = gb1 + jnp.sum(v, axis=0, keepdims=True)
        ln_s[0:1, cols] = gg1
        ln_s[1:2, cols] = gb1
    l_first = send(ln_s, ln_pr, pt)

    own = pl.ds(pl.multiple_of(t * SL, 8), SL)
    xh_ref[...] = xhat[own, :]
    gm_ref[...] = gm_f[own, :]
    rs_ref[...] = rstd_s[own, :]
    g1_out[...] = par[0:1, :]

    for k in range(2):
        cols = slice(k * HW, (k + 1) * HW)
        r_first[k][0].wait_recv()
        r_hs[0:SL, cols] = (rp[k, ct].astype(F32) + r_pr[k, 1].astype(F32)).astype(BF)
        r_first[k][1].wait_recv()
        mine_ref[:, cols] = (rp[k, t].astype(F32) + r_pr[k, 0].astype(F32)).astype(BF)
    l_first.wait_recv()
    ln = ln_s[...] + ln_pr[...]
    ln_hs[...] = ln
    ln_rows = []
    for _ in range(3):
        ln_rows.append(ln.astype(BF).astype(F32))
        ln = ln - ln_rows[-1]
    r_hs[SL:SL + 8, :] = jnp.concatenate(ln_rows + [jnp.zeros((2, D), F32)], axis=0).astype(BF)
    m_first[1].wait_recv()
    m_out.wait_recv()
    m_sum = (mp[t].astype(F32) + m_pr[0].astype(F32)).astype(BF).astype(F32) + m_cr[...].astype(F32)
    y_ref[...] = (xf[own, :] + m_sum.astype(BF).astype(F32) + bd_ref[...]).astype(BF)
    for c in started:
        c.wait_send()


N_SEND = 6 + 2 * (2 + 4 + 1 + 1 + 3) + 3 + 4 + 1
VMEM_A = 36 * 2**20
VMEM_B = 8 * 2**20
VMEM_C = 4 * 2**20


def write_kernel(yi_ref, vec_ref, up_ref, dn_ref, gqkv_ref, h_ref, ctx_ref, gmid_ref,
                 y_ref, gwqkv_ref, gbqkv_ref, gwout_ref, gbo_ref, gl2_ref, bl2_ref, gwup_ref, gbup_ref, gwdn_ref, gbd_ref,
                 s_qkv, s_out, s_gb, s0, s1, s2, s3, s4, sem):
    cps = []

    def out(src, dst, n=1):
        rows = src.shape[0] // n
        for k in range(n):
            c = pltpu.make_async_copy(src.at[pl.ds(k * rows, rows)], dst.at[pl.ds(k * rows, rows)], sem.at[len(cps)])
            c.start()
            cps.append(c)

    out(dn_ref, gwdn_ref, 4)
    out(up_ref, gwup_ref, 4)
    out(yi_ref, y_ref)
    for i, (sv, r) in enumerate(((s0, gbd_ref), (s1, gbup_ref), (s2, gl2_ref), (s3, bl2_ref), (s4, gbo_ref))):
        sv[...] = vec_ref[i, :]
        out(sv, r)
    ones = jnp.ones((8, S), BF)
    for h in range(HL):
        for e in range(3):
            s_gb[e, h:h + 1, :] = dot(ones, gqkv_ref[head_rows(h, e), :], 1, 1)[0:1, :]
    out(s_gb, gbqkv_ref)
    hv = h_ref[...]
    s_out[...] = dot(ctx_ref[...], gmid_ref[...], 1, 0).astype(BF)
    out(s_out, gwout_ref)
    for n in range(HL):
        rows = slice(n * 3 * HD, (n + 1) * 3 * HD)
        s_qkv[rows, :] = dot(gqkv_ref[rows, :], hv, 1, 0).astype(BF)
        out(s_qkv.at[rows], gwqkv_ref.at[rows])
    for c in cps:
        c.wait()


def last_kernel(mine_ref, xh_ref, gm_ref, rs_ref, g1_ref, rc_ref, ln_ref, gx_ref, gl1_ref, bl1_ref):
    gh = (mine_ref[...].astype(F32) + rc_ref[0:SL, :].astype(F32)).astype(BF).astype(F32)
    xh = xh_ref[...]
    dxh = gh * g1_ref[...]
    m1 = jnp.mean(dxh, axis=-1, keepdims=True)
    m2 = jnp.mean(dxh * xh, axis=-1, keepdims=True)
    gx_ref[...] = (gm_ref[...] + rs_ref[:, 0:1] * (dxh - m1 - xh * m2)).astype(BF)
    lc = rc_ref[SL:SL + 8, :].astype(F32)
    ln = ln_ref[...] + (lc[0:2, :] + lc[2:4, :] + lc[4:6, :])
    gl1_ref[...] = ln[0, :]
    bl1_ref[...] = ln[1, :]


def solution(mesh):
    VM = pl.BlockSpec(memory_space=pltpu.VMEM)
    ANY = pl.BlockSpec(memory_space=pltpu.HBM)

    def sds(shape, dt):
        return jax.ShapeDtypeStruct(shape, dt)

    def local_step(x, g1, be1, w_qkv, b_qkv, w_out, b_out, g2, be2, w_up, b_up, w_down, b_down, grad_y):
        wq = jnp.transpose(w_qkv, (1, 2, 3, 0)).reshape(3 * HL * HD, D)
        bq = jnp.transpose(b_qkv, (1, 0, 2))
        part = pltpu.VMEM((S, HW), BF)
        vec1 = sds((D,), F32)
        mids = pl.pallas_call(
            block_kernel,
            out_shape=(pltpu.VMEM((SL, D), BF), pltpu.VMEM((8, D), F32), pltpu.VMEM((D, FL), BF), pltpu.VMEM((FL, D), BF),
                       pltpu.VMEM((3 * HL * HD, S), BF), pltpu.VMEM((S, D), BF), pltpu.VMEM((HL * HD, S), BF), pltpu.VMEM((S, D), BF),
                       pltpu.VMEM((SL, D), BF), pltpu.VMEM((SL, D), F32), pltpu.VMEM((SL, D), F32), pltpu.VMEM((SL, 128), F32),
                       pltpu.VMEM((1, D), F32), sds((SL + 8, D), BF), pltpu.VMEM((2, D), F32)),
            in_specs=[ANY] * 14,
            out_specs=(VM,) * 15,
            scratch_shapes=[
                pltpu.VMEM((3 * HL * HD, D), BF), pltpu.VMEM((2, HL * HD, HW), BF), pltpu.VMEM((S, D), F32), pltpu.VMEM((S, D), F32),
                pltpu.VMEM((S, D), F32), pltpu.VMEM((S, D), F32), pltpu.VMEM((S, 128), F32), pltpu.VMEM((HL, S, S), F32),
                pltpu.VMEM((3 * HL * HD, S), BF), pltpu.VMEM((8, D), F32), pltpu.VMEM((TP, SL, D), BF),
                pltpu.VMEM((D, FL), BF), pltpu.VMEM((FL, D), BF), pltpu.VMEM((TP, SL, D), BF), pltpu.VMEM((TP, SL, D), BF),
                pltpu.VMEM((3 * HL * HD, S), F32), *[part] * 12,
                pltpu.VMEM((S, FL), BF), pltpu.VMEM((S, D), BF), pltpu.VMEM((S, FL), BF), pltpu.VMEM((S, FL), BF), pltpu.VMEM((S, D), BF),
                pltpu.VMEM((3, HL, HD), F32), *[pltpu.VMEM((D,), F32) for _ in range(7)],
                pltpu.VMEM((2, TP, SL, HW), BF), pltpu.VMEM((2, SL, D), BF), pltpu.VMEM((SL, D), BF), pltpu.VMEM((SL, D), BF),
                pltpu.VMEM((2, 2, SL, HW), BF), pltpu.VMEM((2, 2, D), F32),
                pltpu.SemaphoreType.DMA((9,)), pltpu.SemaphoreType.DMA((N_SEND,)), pltpu.SemaphoreType.DMA((N_SEND,)),
                pltpu.SemaphoreType.DMA((10,)),
            ],
            compiler_params=pltpu.CompilerParams(collective_id=0, has_side_effects=True, vmem_limit_bytes=VMEM_A),
            name='block',
        )(*(pltpu.with_memory_space_constraint(v, pltpu.HBM) for v in (
            x.reshape(SL, D), grad_y.reshape(SL, D), g1, be1, g2, be2, b_out, b_down, bq, b_up, wq, w_out, w_up, w_down)))
        mine, xh, gm, rs, g1v, r_hs, ln_hs = mids[8:]
        across = [(i, TP - 1 - i) for i in range(TP)]
        r_cr = lax.ppermute(r_hs, 'tp', across)
        y, gwqkv, gbqkv, gwout, gbo, gl2, bl2, gwup, gbup, gwdn, gbd = pl.pallas_call(
            write_kernel,
            out_shape=(sds((SL, D), BF), sds((3 * HL * HD, D), BF), sds((3, HL, HD), F32), sds((HL * HD, D), BF), vec1, vec1, vec1,
                       sds((D, FL), BF), vec1, sds((FL, D), BF), vec1),
            in_specs=[VM] * 8,
            out_specs=(ANY,) * 11,
            scratch_shapes=[pltpu.VMEM((3 * HL * HD, D), BF), pltpu.VMEM((HL * HD, D), BF), pltpu.VMEM((3, HL, HD), F32),
                            *[pltpu.VMEM((D,), F32) for _ in range(5)], pltpu.SemaphoreType.DMA((20,))],
            compiler_params=pltpu.CompilerParams(vmem_limit_bytes=VMEM_B),
            cost_estimate=pl.CostEstimate(flops=600_000_000, bytes_accessed=14_200_000, transcendentals=0),
            name='write',
        )(*mids[:8])
        gx, gl1, bl1 = pl.pallas_call(
            last_kernel,
            out_shape=(sds((SL, D), BF), vec1, vec1),
            in_specs=[VM] * 7,
            out_specs=(VM,) * 3,
            compiler_params=pltpu.CompilerParams(vmem_limit_bytes=VMEM_C),
            name='last',
        )(mine, xh, gm, rs, g1v, r_cr, ln_hs)
        gwqkv = jnp.transpose(gwqkv.reshape(HL, 3, HD, D), (3, 0, 1, 2))
        gbqkv = jnp.transpose(gbqkv, (1, 0, 2))
        return (y.reshape(1, SL, D), gx.reshape(1, SL, D), gl1, bl1, gwqkv, gbqkv, gwout, gbo, gl2, bl2, gwup, gbup, gwdn, gbd)

    row_spec = P('dp', 'tp', None)
    in_specs = (row_spec, P(), P(), P(None, 'tp', None, None), P('tp', None, None), P('tp', None), P(), P(), P(),
                P(None, 'tp'), P('tp'), P('tp', None), P(), row_spec)
    out_specs = (row_spec, row_spec, P('dp'), P('dp'), P('dp', 'tp', None, None), P(('dp', 'tp'), None, None),
                 P(('dp', 'tp'), None), P('dp'), P('dp'), P('dp'), P('dp', 'tp'), P(('dp', 'tp')), P(('dp', 'tp'), None), P('dp'))
    return jax.shard_map(local_step, mesh=mesh, in_specs=in_specs, out_specs=out_specs, check_vma=False)
```

```python
import functools
import math

import jax
import jax.numpy as jnp
from jax import lax
from jax.experimental import pallas as pl
from jax.experimental.pallas import tpu as pltpu
from jax.sharding import PartitionSpec as P

EPS = 1e-5
MASK_VALUE = -1e30
BF = jnp.bfloat16
F32 = jnp.float32
MESH = pl.DeviceIdType.MESH

D = 1536
S = 96
SL = 24
TP = 4
HL = 4
HD = 96
FL = 1536
CW = 256
NCH = D // CW
HCH = NCH // 2
HW = D // 2
CUT = (0, 256, 512, 640, 768)
NCUT = len(CUT) - 1


def alibi_slopes(n_heads):
    closest = 2 ** int(math.floor(math.log2(n_heads)))
    base_ratio = 2.0 ** (-8.0 / closest)
    extra_ratio = 2.0 ** (-4.0 / closest)
    remaining = min(closest, n_heads - closest)
    slopes = [base_ratio ** (i + 1) for i in range(closest)]
    return slopes + [extra_ratio ** (2 * i + 1) for i in range(remaining)]


def dot(a, b, ca, cb):
    return lax.dot_general(a, b, (((ca,), (cb,)), ((), ())), preferred_element_type=F32)


def gelu_parts(u):
    k = math.sqrt(2.0 / math.pi)
    u2 = u * u
    th = jnp.tanh(u * (k + (k * 0.044715) * u2))
    half = 0.5 + 0.5 * th
    val = u * half
    return val, half + val * (1.0 - th) * (k + (3.0 * 0.044715 * k) * u2)


def rows_stats(v):
    mean = jnp.mean(v, axis=-1, keepdims=True)
    cen = v - mean
    var = jnp.mean(cen * cen, axis=-1, keepdims=True)
    return cen, lax.rsqrt(var + EPS)


def places():
    t = lax.axis_index('tp')
    core = t % 2
    pt = t + 1 - 2 * core
    ct = TP - 1 - t
    qt = TP - 1 - pt
    half = (core + t // 2) % 2
    return t, pt, ct, qt, half


def sender(ssem, rsem):
    started = []

    def send(src, dst, dev):
        i = len(started)
        c = pltpu.make_async_remote_copy(src_ref=src, dst_ref=dst, send_sem=ssem.at[i], recv_sem=rsem.at[i],
                                         device_id={'tp': dev}, device_id_type=MESH)
        c.start()
        started.append(c)
        return c

    return send, started


def head_rows(h, e):
    return slice((h * 3 + e) * HD, (h * 3 + e + 1) * HD)


def row_blocks(buf, cols, v):
    for i in range(TP):
        buf[i, :, cols] = v[i * SL:(i + 1) * SL, :].astype(BF)


def block_kernel(x_hbm, gy_hbm, g1_hbm, be1_hbm, g2_hbm, be2_hbm, bo_hbm, bd_hbm, bqkv_hbm, bup_hbm,
                 wqkv_hbm, wout_hbm, wup_hbm, wdn_hbm,
                 y_ref, vec_ref, gwup_ref, gwdn_ref, gqkv_ref, h_ref, ctx_ref, gmid_ref, mine_ref, xh_ref, gm_ref, rs_ref, g1_out, r_hs, ln_hs,
                 wqkv, wout, xf, gm_f, gg_f, xhat, rstd_s, probs, qkvT, par, mp,
                 wup, wdn, xg, gyg, biasT, a_ps, a_pr, a_hs, a_hr, a_cr, a_fr, b_ps, b_pr, b_hs, b_hr, b_cr, b_fr,
                 gact, g_ref, gpre_ref, act_ref, gyf_ref, bqkv_ref, g1_in, be1_in, g2_in, be2_in, bo_in, bd_in, bup_in,
                 rp, m_pr, m_hs, m_cr, r_pr, ln_x,
                 wsem, ssem, rsem, isem):
    t, pt, ct, qt, half = places()
    send, started = sender(ssem, rsem)

    in_x = pltpu.make_async_copy(x_hbm, xg.at[t], isem.at[0])
    in_gy = pltpu.make_async_copy(gy_hbm, gyg.at[t], isem.at[1])
    in_b = pltpu.make_async_copy(bqkv_hbm, bqkv_ref, isem.at[2])
    small = ((g1_hbm, g1_in), (be1_hbm, be1_in), (g2_hbm, g2_in), (be2_hbm, be2_in), (bo_hbm, bo_in), (bd_hbm, bd_in), (bup_hbm, bup_in))
    in_p = [pltpu.make_async_copy(a, b, isem.at[3 + i]) for i, (a, b) in enumerate(small)]
    for c in (in_x, in_gy, in_b, *in_p):
        c.start()
    w_cps = {}
    w_cps['qkv'] = [pltpu.make_async_copy(wqkv_hbm, wqkv, wsem.at[0])]
    w_cps['out'] = [pltpu.make_async_copy(wout_hbm.at[:, pl.ds(k * HW, HW)], wout.at[k], wsem.at[1 + k]) for k in range(2)]
    w_cps['dn'] = [pltpu.make_async_copy(wdn_hbm, wdn, wsem.at[7])]
    w_cps['up'] = [pltpu.make_async_copy(wup_hbm, wup, wsem.at[8])]

    barrier = pltpu.get_barrier_semaphore()
    for dev in (pt, ct, qt):
        pl.semaphore_signal(barrier, inc=1, device_id={'tp': dev}, device_id_type=MESH)
    for name in ('qkv', 'out', 'dn', 'up'):
        for c in w_cps[name]:
            c.start()
    pl.semaphore_wait(barrier, 3)

    in_x.wait()
    x_c = send(xg.at[t], xg.at[t], ct)
    x_p = send(xg.at[t], xg.at[t], pt)

    for c in (in_b, *in_p):
        c.wait()
    for i, r in enumerate((g1_in, be1_in, g2_in, be2_in, bo_in, bd_in, bup_in)):
        par[i, :] = r[...]
    g1_ref, be1_ref, g2_ref, be2_ref, bo_ref, bd_ref, bup_ref = (par.at[i:i + 1] for i in range(7))

    for h in range(HL):
        for e in range(3):
            row = jnp.broadcast_to(bqkv_ref[e, h:h + 1, :], (S, HD))
            biasT[pl.ds((h * 3 + e) * HD, HD), :] = row.T

    x_p.wait_recv()
    in_gy.wait()
    y_c = send(gyg.at[t], gyg.at[t], ct)
    y_p = send(gyg.at[t], gyg.at[t], pt)
    x_c.wait_recv()
    x_f = send(xg.at[ct], xg.at[ct], pt)
    x_f.wait_recv()

    for i in range(TP):
        xf[pl.ds(i * SL, SL), :] = xg[i].astype(F32)
    for r in range(0, S, 32):
        cen, rstd = rows_stats(xf[r:r + 32, :])
        xh = cen * rstd
        xhat[r:r + 32, :] = xh
        rstd_s[r:r + 32, :] = jnp.broadcast_to(rstd, (32, 128))
        h_ref[r:r + 32, :] = (xh * g1_ref[...] + be1_ref[...]).astype(BF)

    w_cps['qkv'][0].wait()
    hv = h_ref[...]
    for h in range(HL):
        rows = slice(h * 3 * HD, (h + 1) * 3 * HD)
        qkvT[rows, :] = (dot(wqkv[rows, :], hv, 1, 1) + biasT[rows, :]).astype(BF)

    scale = HD ** -0.5
    slopes = alibi_slopes(HL * TP)
    j_pos = lax.broadcasted_iota(jnp.int32, (S, S), 0)
    i_pos = lax.broadcasted_iota(jnp.int32, (S, S), 1)
    causal = j_pos <= i_pos
    j_f = j_pos.astype(F32)

    def head(h, e):
        return qkvT[head_rows(h, e), :]

    for h in range(HL):
        slope = jnp.where(t == 0, slopes[h], jnp.where(t == 1, slopes[HL + h], jnp.where(t == 2, slopes[2 * HL + h], slopes[3 * HL + h]))).astype(F32)
        s = dot(head(h, 1), head(h, 0), 0, 0) * scale + slope * j_f
        s = jnp.where(causal, s, MASK_VALUE)
        p = jnp.exp(s - jnp.max(s, axis=0, keepdims=True))
        p = p / jnp.sum(p, axis=0, keepdims=True)
        probs[h] = p
        ctx_ref[h * HD:(h + 1) * HD, :] = dot(head(h, 2), p.astype(BF), 1, 0).astype(BF)

    def exchange(part, groups, ps, pr, hs, hr, cr, fr):
        firsts = []
        for k0, k1 in groups:
            cols = slice(CUT[k0], CUT[k1])
            ps[:, cols] = part(1 - half, CUT[k0], CUT[k1]).astype(BF)
            firsts.append(send(ps.at[:, cols], pr.at[:, cols], pt))
        outs = []
        for (k0, k1), first in zip(groups, firsts):
            cols = slice(CUT[k0], CUT[k1])
            ours = part(half, CUT[k0], CUT[k1])
            first.wait_recv()
            hs[:, cols] = (ours + pr[:, cols].astype(F32)).astype(BF)
            for k in range(k0, k1):
                c = slice(CUT[k], CUT[k + 1])
                outs.append([send(hs.at[:, c], cr.at[:, c], ct)])
                if k == NCUT - 1:
                    outs[-1].append(send(hs.at[:, c], fr.at[:, c], qt))
        local = send(hs, hr, pt)
        return outs, local

    def forward(out, k, cr, fr):
        if k < NCUT - 1:
            c = slice(CUT[k], CUT[k + 1])
            out[0].wait_recv()
            out.append(send(cr.at[:, c], fr.at[:, c], pt))

    for c in w_cps['out']:
        c.wait()
    ctxT = ctx_ref[...]
    a_outs, a_local = exchange(lambda hh, c0, c1: dot(ctxT, wout[hh, :, c0:c1], 0, 0), ((0, NCUT),), a_ps, a_pr, a_hs, a_hr, a_cr, a_fr)

    y_c.wait_recv()
    y_f = send(gyg.at[ct], gyg.at[ct], pt)
    y_p.wait_recv()
    y_f.wait_recv()
    for i in range(TP):
        gm_f[pl.ds(i * SL, SL), :] = gyg[i].astype(F32)
    for r in range(0, S, 32):
        gyf_ref[r:r + 32, :] = gm_f[r:r + 32, :].astype(BF)
    w_cps['dn'][0].wait()
    gyv = gyf_ref[...]
    for n in range(NCH):
        gact[:, n * CW:(n + 1) * CW] = dot(gyv, wdn[n * CW:(n + 1) * CW, :], 1, 1).astype(BF)
    vec_ref[0:1, :] = jnp.sum(gm_f[...], axis=0, keepdims=True)

    def gathered(outs, local, hs, hr, cr, fr, put):
        outs[-1][0].wait_recv()
        for k in range(HCH):
            c = slice(k * CW, (k + 1) * CW)
            put(half * HCH + k, (hs[:, c].astype(F32) + cr[:, c].astype(F32)).astype(BF).astype(F32))
        local.wait_recv()
        for out in outs:
            out[1].wait_recv()
        for k in range(HCH):
            c = slice(k * CW, (k + 1) * CW)
            put((1 - half) * HCH + k, (hr[:, c].astype(F32) + fr[:, c].astype(F32)).astype(BF).astype(F32))

    for k, out in enumerate(a_outs):
        forward(out, k, a_cr, a_fr)

    def put_x(kk, val):
        cols = pl.ds(pl.multiple_of(kk * CW, CW), CW)
        xf[:, cols] = xf[:, cols] + val + bo_ref[:, cols]

    gathered(a_outs, a_local, a_hs, a_hr, a_cr, a_fr, put_x)

    for r in range(0, S, 32):
        cen, rstd = rows_stats(xf[r:r + 32, :])
        g_ref[r:r + 32, :] = (cen * rstd * g2_ref[...] + be2_ref[...]).astype(BF)

    w_cps['up'][0].wait()
    gv = g_ref[...]
    for n in range(NCH):
        cols = slice(n * CW, (n + 1) * CW)
        pre = dot(gv, wup[:, cols], 1, 0) + bup_ref[:, cols]
        val, der = gelu_parts(pre)
        act_ref[:, cols] = val.astype(BF)
        gp = gact[:, cols].astype(F32) * der
        vec_ref[1:2, cols] = jnp.sum(gp, axis=0, keepdims=True)
        gpre_ref[:, cols] = gp.astype(BF)

    gprev = gpre_ref[...]

    def part_g(hh, c0, c1):
        return dot(gprev, wup[pl.ds(pl.multiple_of(hh * HW + c0, CW), c1 - c0), :], 1, 1)

    g_outs, g_local = exchange(part_g, ((0, 1), (1, NCUT)), b_ps, b_pr, b_hs, b_hr, b_cr, b_fr)

    actv = act_ref[...]
    for n in range(NCH):
        cols = slice(n * CW, (n + 1) * CW)
        row_blocks(mp, cols, dot(actv, wdn[:, cols], 1, 0))
    m_first = (send(mp.at[qt], m_pr.at[1], pt), send(mp.at[pt], m_pr.at[0], pt))
    for n in range(NCH):
        gwdn_ref[n * CW:(n + 1) * CW, :] = dot(act_ref[:, n * CW:(n + 1) * CW], gyv, 0, 0).astype(BF)
    for k in range(HCH):
        forward(g_outs[k], k, b_cr, b_fr)
        for n in range(2 * k, 2 * k + 2):
            gwup_ref[n * CW:(n + 1) * CW, :] = dot(g_ref[:, n * CW:(n + 1) * CW], gprev, 0, 0).astype(BF)

    m_first[0].wait_recv()
    m_hs[...] = (mp[ct].astype(F32) + m_pr[1].astype(F32)).astype(BF)
    m_out = send(m_hs, m_cr, ct)

    def put_g(kk, val):
        gg_f[:, pl.ds(pl.multiple_of(kk * CW, CW), CW)] = val

    gathered(g_outs, g_local, b_hs, b_hr, b_cr, b_fr, put_g)

    gg2 = jnp.zeros((1, D), F32)
    gb2 = jnp.zeros((1, D), F32)
    gbo = jnp.zeros((1, D), F32)
    for r in range(0, S, 32):
        cen, rstd = rows_stats(xf[r:r + 32, :])
        xh = cen * rstd
        gg = gg_f[r:r + 32, :]
        gg2 = gg2 + jnp.sum(gg * xh, axis=0, keepdims=True)
        gb2 = gb2 + jnp.sum(gg, axis=0, keepdims=True)
        dxh = gg * g2_ref[...]
        m1 = jnp.mean(dxh, axis=-1, keepdims=True)
        m2 = jnp.mean(dxh * xh, axis=-1, keepdims=True)
        gm = gm_f[r:r + 32, :] + rstd * (dxh - m1 - xh * m2)
        gm_f[r:r + 32, :] = gm
        gbo = gbo + jnp.sum(gm, axis=0, keepdims=True)
        gmid_ref[r:r + 32, :] = gm.astype(BF)
    vec_ref[2:3, :] = gg2
    vec_ref[3:4, :] = gb2
    vec_ref[4:5, :] = gbo

    gmv = gmid_ref[...]
    gctxT = (dot(wout[0], gmv[:, :HW], 1, 1) + dot(wout[1], gmv[:, HW:], 1, 1)).astype(BF)
    heads = range(HL)
    gos = [gctxT[h * HD:(h + 1) * HD, :] for h in heads]
    gps = [dot(head(h, 2), gos[h], 0, 0).astype(BF).astype(F32) for h in heads]
    gvs = [dot(gos[h], probs[h].astype(BF), 1, 1).astype(BF) for h in heads]
    gss = [(probs[h] * (gps[h] - jnp.sum(gps[h] * probs[h], axis=0, keepdims=True))).astype(BF) for h in heads]
    gqs = [(dot(head(h, 1), gss[h], 1, 0) * scale).astype(BF) for h in heads]
    gks = [(dot(head(h, 0), gss[h], 1, 1) * scale).astype(BF) for h in heads]
    for h in heads:
        for e, val in enumerate((gqs[h], gks[h], gvs[h])):
            gqkv_ref[head_rows(h, e), :] = val

    gqv = gqkv_ref[...]
    r_first = []
    for k in range(2):
        row_blocks(rp.at[k], slice(0, HW), dot(gqv, wqkv[:, k * HW:(k + 1) * HW], 0, 0))
        r_first.append((send(rp.at[k, qt], r_pr.at[k, 1], pt), send(rp.at[k, pt], r_pr.at[k, 0], pt)))

    ln_s, ln_pr = ln_x.at[0], ln_x.at[1]
    for k in range(2):
        cols = slice(k * HW, (k + 1) * HW)
        gg1 = jnp.zeros((1, HW), F32)
        gb1 = jnp.zeros((1, HW), F32)
        for i in range(TP):
            v = rp[k, i].astype(F32)
            gg1 = gg1 + jnp.sum(v * xhat[i * SL:(i + 1) * SL, cols], axis=0, keepdims=True)
            gb1 = gb1 + jnp.sum(v, axis=0, keepdims=True)
        ln_s[0:1, cols] = gg1
        ln_s[1:2, cols] = gb1
    l_first = send(ln_s, ln_pr, pt)

    own = pl.ds(pl.multiple_of(t * SL, 8), SL)
    xh_ref[...] = xhat[own, :]
    gm_ref[...] = gm_f[own, :]
    rs_ref[...] = rstd_s[own, :]
    g1_out[...] = par[0:1, :]

    for k in range(2):
        cols = slice(k * HW, (k + 1) * HW)
        r_first[k][0].wait_recv()
        r_hs[0:SL, cols] = (rp[k, ct].astype(F32) + r_pr[k, 1].astype(F32)).astype(BF)
        r_first[k][1].wait_recv()
        mine_ref[:, cols] = (rp[k, t].astype(F32) + r_pr[k, 0].astype(F32)).astype(BF)
    l_first.wait_recv()
    ln = ln_s[...] + ln_pr[...]
    ln_hs[...] = ln
    ln_rows = []
    for _ in range(3):
        ln_rows.append(ln.astype(BF).astype(F32))
        ln = ln - ln_rows[-1]
    r_hs[SL:SL + 8, :] = jnp.concatenate(ln_rows + [jnp.zeros((2, D), F32)], axis=0).astype(BF)
    m_first[1].wait_recv()
    m_out.wait_recv()
    m_sum = (mp[t].astype(F32) + m_pr[0].astype(F32)).astype(BF).astype(F32) + m_cr[...].astype(F32)
    y_ref[...] = (xf[own, :] + m_sum.astype(BF).astype(F32) + bd_ref[...]).astype(BF)
    for c in started:
        c.wait_send()


N_SEND = 6 + 2 * (2 + 4 + 1 + 1 + 3) + 3 + 4 + 1
VMEM_A = 36 * 2**20
VMEM_B = 8 * 2**20
VMEM_C = 4 * 2**20


def write_kernel(yi_ref, vec_ref, up_ref, dn_ref, gqkv_ref, h_ref, ctx_ref, gmid_ref,
                 y_ref, gwqkv_ref, gbqkv_ref, gwout_ref, gbo_ref, gl2_ref, bl2_ref, gwup_ref, gbup_ref, gwdn_ref, gbd_ref,
                 s_qkv, s_out, s_gb, s0, s1, s2, s3, s4, sem):
    cps = []

    def out(src, dst, n=1):
        rows = src.shape[0] // n
        for k in range(n):
            c = pltpu.make_async_copy(src.at[pl.ds(k * rows, rows)], dst.at[pl.ds(k * rows, rows)], sem.at[len(cps)])
            c.start()
            cps.append(c)

    out(dn_ref, gwdn_ref, 4)
    out(up_ref, gwup_ref, 4)
    out(yi_ref, y_ref)
    for i, (sv, r) in enumerate(((s0, gbd_ref), (s1, gbup_ref), (s2, gl2_ref), (s3, bl2_ref), (s4, gbo_ref))):
        sv[...] = vec_ref[i, :]
        out(sv, r)
    ones = jnp.ones((8, S), BF)
    for h in range(HL):
        for e in range(3):
            s_gb[e, h:h + 1, :] = dot(ones, gqkv_ref[head_rows(h, e), :], 1, 1)[0:1, :]
    out(s_gb, gbqkv_ref)
    hv = h_ref[...]
    s_out[...] = dot(ctx_ref[...], gmid_ref[...], 1, 0).astype(BF)
    out(s_out, gwout_ref)
    for n in range(HL):
        rows = slice(n * 3 * HD, (n + 1) * 3 * HD)
        s_qkv[rows, :] = dot(gqkv_ref[rows, :], hv, 1, 0).astype(BF)
        out(s_qkv.at[rows], gwqkv_ref.at[rows])
    for c in cps:
        c.wait()


def last_kernel(mine_ref, xh_ref, gm_ref, rs_ref, g1_ref, rc_ref, ln_ref, gx_ref, gl1_ref, bl1_ref):
    gh = (mine_ref[...].astype(F32) + rc_ref[0:SL, :].astype(F32)).astype(BF).astype(F32)
    xh = xh_ref[...]
    dxh = gh * g1_ref[...]
    m1 = jnp.mean(dxh, axis=-1, keepdims=True)
    m2 = jnp.mean(dxh * xh, axis=-1, keepdims=True)
    gx_ref[...] = (gm_ref[...] + rs_ref[:, 0:1] * (dxh - m1 - xh * m2)).astype(BF)
    lc = rc_ref[SL:SL + 8, :].astype(F32)
    ln = ln_ref[...] + (lc[0:2, :] + lc[2:4, :] + lc[4:6, :])
    gl1_ref[...] = ln[0, :]
    bl1_ref[...] = ln[1, :]


def solution(mesh):
    VM = pl.BlockSpec(memory_space=pltpu.VMEM)
    ANY = pl.BlockSpec(memory_space=pltpu.HBM)

    def sds(shape, dt):
        return jax.ShapeDtypeStruct(shape, dt)

    def local_step(x, g1, be1, w_qkv, b_qkv, w_out, b_out, g2, be2, w_up, b_up, w_down, b_down, grad_y):
        wq = jnp.transpose(w_qkv, (1, 2, 3, 0)).reshape(3 * HL * HD, D)
        bq = jnp.transpose(b_qkv, (1, 0, 2))
        part = pltpu.VMEM((S, HW), BF)
        vec1 = sds((D,), F32)
        mids = pl.pallas_call(
            block_kernel,
            out_shape=(pltpu.VMEM((SL, D), BF), pltpu.VMEM((8, D), F32), pltpu.VMEM((D, FL), BF), pltpu.VMEM((FL, D), BF),
                       pltpu.VMEM((3 * HL * HD, S), BF), pltpu.VMEM((S, D), BF), pltpu.VMEM((HL * HD, S), BF), pltpu.VMEM((S, D), BF),
                       pltpu.VMEM((SL, D), BF), pltpu.VMEM((SL, D), F32), pltpu.VMEM((SL, D), F32), pltpu.VMEM((SL, 128), F32),
                       pltpu.VMEM((1, D), F32), sds((SL + 8, D), BF), pltpu.VMEM((2, D), F32)),
            in_specs=[ANY] * 14,
            out_specs=(VM,) * 15,
            scratch_shapes=[
                pltpu.VMEM((3 * HL * HD, D), BF), pltpu.VMEM((2, HL * HD, HW), BF), pltpu.VMEM((S, D), F32), pltpu.VMEM((S, D), F32),
                pltpu.VMEM((S, D), F32), pltpu.VMEM((S, D), F32), pltpu.VMEM((S, 128), F32), pltpu.VMEM((HL, S, S), F32),
                pltpu.VMEM((3 * HL * HD, S), BF), pltpu.VMEM((8, D), F32), pltpu.VMEM((TP, SL, D), BF),
                pltpu.VMEM((D, FL), BF), pltpu.VMEM((FL, D), BF), pltpu.VMEM((TP, SL, D), BF), pltpu.VMEM((TP, SL, D), BF),
                pltpu.VMEM((3 * HL * HD, S), F32), *[part] * 12,
                pltpu.VMEM((S, FL), BF), pltpu.VMEM((S, D), BF), pltpu.VMEM((S, FL), BF), pltpu.VMEM((S, FL), BF), pltpu.VMEM((S, D), BF),
                pltpu.VMEM((3, HL, HD), F32), *[pltpu.VMEM((D,), F32) for _ in range(7)],
                pltpu.VMEM((2, TP, SL, HW), BF), pltpu.VMEM((2, SL, D), BF), pltpu.VMEM((SL, D), BF), pltpu.VMEM((SL, D), BF),
                pltpu.VMEM((2, 2, SL, HW), BF), pltpu.VMEM((2, 2, D), F32),
                pltpu.SemaphoreType.DMA((9,)), pltpu.SemaphoreType.DMA((N_SEND,)), pltpu.SemaphoreType.DMA((N_SEND,)),
                pltpu.SemaphoreType.DMA((10,)),
            ],
            compiler_params=pltpu.CompilerParams(collective_id=0, has_side_effects=True, vmem_limit_bytes=VMEM_A),
            name='block',
        )(*(pltpu.with_memory_space_constraint(v, pltpu.HBM) for v in (
            x.reshape(SL, D), grad_y.reshape(SL, D), g1, be1, g2, be2, b_out, b_down, bq, b_up, wq, w_out, w_up, w_down)))
        mine, xh, gm, rs, g1v, r_hs, ln_hs = mids[8:]
        across = [(i, TP - 1 - i) for i in range(TP)]
        r_cr = lax.ppermute(r_hs, 'tp', across)
        y, gwqkv, gbqkv, gwout, gbo, gl2, bl2, gwup, gbup, gwdn, gbd = pl.pallas_call(
            write_kernel,
            out_shape=(sds((SL, D), BF), sds((3 * HL * HD, D), BF), sds((3, HL, HD), F32), sds((HL * HD, D), BF), vec1, vec1, vec1,
                       sds((D, FL), BF), vec1, sds((FL, D), BF), vec1),
            in_specs=[VM] * 8,
            out_specs=(ANY,) * 11,
            scratch_shapes=[pltpu.VMEM((3 * HL * HD, D), BF), pltpu.VMEM((HL * HD, D), BF), pltpu.VMEM((3, HL, HD), F32),
                            *[pltpu.VMEM((D,), F32) for _ in range(5)], pltpu.SemaphoreType.DMA((20,))],
            compiler_params=pltpu.CompilerParams(vmem_limit_bytes=VMEM_B),
            cost_estimate=pl.CostEstimate(flops=600_000_000, bytes_accessed=14_200_000, transcendentals=0),
            name='write',
        )(*mids[:8])
        gx, gl1, bl1 = pl.pallas_call(
            last_kernel,
            out_shape=(sds((SL, D), BF), vec1, vec1),
            in_specs=[VM] * 7,
            out_specs=(VM,) * 3,
            compiler_params=pltpu.CompilerParams(vmem_limit_bytes=VMEM_C),
            name='last',
        )(mine, xh, gm, rs, g1v, r_cr, ln_hs)
        gwqkv = jnp.transpose(gwqkv.reshape(HL, 3, HD, D), (3, 0, 1, 2))
        gbqkv = jnp.transpose(gbqkv, (1, 0, 2))
        return (y.reshape(1, SL, D), gx.reshape(1, SL, D), gl1, bl1, gwqkv, gbqkv, gwout, gbo, gl2, bl2, gwup, gbup, gwdn, gbd)

    row_spec = P('dp', 'tp', None)
    in_specs = (row_spec, P(), P(), P(None, 'tp', None, None), P('tp', None, None), P('tp', None), P(), P(), P(),
                P(None, 'tp'), P('tp'), P('tp', None), P(), row_spec)
    out_specs = (row_spec, row_spec, P('dp'), P('dp'), P('dp', 'tp', None, None), P(('dp', 'tp'), None, None),
                 P(('dp', 'tp'), None), P('dp'), P('dp'), P('dp'), P('dp', 'tp'), P(('dp', 'tp')), P(('dp', 'tp'), None), P('dp'))
    return jax.shard_map(local_step, mesh=mesh, in_specs=in_specs, out_specs=out_specs, check_vma=False)
```

```python
import functools
import math

import jax
import jax.numpy as jnp
from jax import lax
from jax.experimental import pallas as pl
from jax.experimental.pallas import tpu as pltpu
from jax.sharding import PartitionSpec as P

EPS = 1e-5
MASK_VALUE = -1e30
BF = jnp.bfloat16
F32 = jnp.float32
MESH = pl.DeviceIdType.MESH

D = 1536
S = 96
SL = 24
TP = 4
HL = 4
HD = 96
FL = 1536
CW = 256
NCH = D // CW
HCH = NCH // 2
HW = D // 2
CUT = (0, 256, 512, 768)
NCUT = len(CUT) - 1


def alibi_slopes(n_heads):
    closest = 2 ** int(math.floor(math.log2(n_heads)))
    base_ratio = 2.0 ** (-8.0 / closest)
    extra_ratio = 2.0 ** (-4.0 / closest)
    remaining = min(closest, n_heads - closest)
    slopes = [base_ratio ** (i + 1) for i in range(closest)]
    return slopes + [extra_ratio ** (2 * i + 1) for i in range(remaining)]


def dot(a, b, ca, cb):
    return lax.dot_general(a, b, (((ca,), (cb,)), ((), ())), preferred_element_type=F32)


def gelu_parts(u):
    k = math.sqrt(2.0 / math.pi)
    u2 = u * u
    th = jnp.tanh(u * (k + (k * 0.044715) * u2))
    half = 0.5 + 0.5 * th
    val = u * half
    return val, half + val * (1.0 - th) * (k + (3.0 * 0.044715 * k) * u2)


def rows_stats(v):
    mean = jnp.mean(v, axis=-1, keepdims=True)
    cen = v - mean
    var = jnp.mean(cen * cen, axis=-1, keepdims=True)
    return cen, lax.rsqrt(var + EPS)


def places():
    t = lax.axis_index('tp')
    core = t % 2
    pt = t + 1 - 2 * core
    ct = TP - 1 - t
    qt = TP - 1 - pt
    half = (core + t // 2) % 2
    return t, pt, ct, qt, half


def sender(ssem, rsem):
    started = []

    def send(src, dst, dev):
        i = len(started)
        c = pltpu.make_async_remote_copy(src_ref=src, dst_ref=dst, send_sem=ssem.at[i], recv_sem=rsem.at[i],
                                         device_id={'tp': dev}, device_id_type=MESH)
        c.start()
        started.append(c)
        return c

    return send, started


def head_rows(h, e):
    return slice((h * 3 + e) * HD, (h * 3 + e + 1) * HD)


def row_blocks(buf, cols, v):
    for i in range(TP):
        buf[i, :, cols] = v[i * SL:(i + 1) * SL, :].astype(BF)


def block_kernel(x_hbm, gy_hbm, g1_hbm, be1_hbm, g2_hbm, be2_hbm, bo_hbm, bd_hbm, bqkv_hbm, bup_hbm,
                 wqkv_hbm, wout_hbm, wup_hbm, wdn_hbm,
                 y_ref, vec_ref, gwup_ref, gwdn_ref, gqkv_ref, h_ref, ctx_ref, gmid_ref, mine_ref, xh_ref, gm_ref, rs_ref, g1_out, r_hs, ln_hs,
                 wqkv, wout, xf, gm_f, gg_f, xhat, rstd_s, probs, qkvT, par, mp,
                 wup, wdn, xg, gyg, biasT, a_ps, a_pr, a_hs, a_hr, a_cr, a_fr, b_ps, b_pr, b_hs, b_hr, b_cr, b_fr,
                 gact, g_ref, gpre_ref, act_ref, gyf_ref, bqkv_ref, g1_in, be1_in, g2_in, be2_in, bo_in, bd_in, bup_in,
                 rp, m_pr, m_hs, m_cr, r_pr, ln_x,
                 wsem, ssem, rsem, isem):
    t, pt, ct, qt, half = places()
    send, started = sender(ssem, rsem)

    in_x = pltpu.make_async_copy(x_hbm, xg.at[t], isem.at[0])
    in_gy = pltpu.make_async_copy(gy_hbm, gyg.at[t], isem.at[1])
    in_b = pltpu.make_async_copy(bqkv_hbm, bqkv_ref, isem.at[2])
    small = ((g1_hbm, g1_in), (be1_hbm, be1_in), (g2_hbm, g2_in), (be2_hbm, be2_in), (bo_hbm, bo_in), (bd_hbm, bd_in), (bup_hbm, bup_in))
    in_p = [pltpu.make_async_copy(a, b, isem.at[3 + i]) for i, (a, b) in enumerate(small)]
    for c in (in_x, in_gy, in_b, *in_p):
        c.start()
    w_cps = {}
    w_cps['qkv'] = [pltpu.make_async_copy(wqkv_hbm, wqkv, wsem.at[0])]
    w_cps['out'] = [pltpu.make_async_copy(wout_hbm.at[:, pl.ds(k * HW, HW)], wout.at[k], wsem.at[1 + k]) for k in range(2)]
    w_cps['dn'] = [pltpu.make_async_copy(wdn_hbm, wdn, wsem.at[7])]
    w_cps['up'] = [pltpu.make_async_copy(wup_hbm, wup, wsem.at[8])]

    barrier = pltpu.get_barrier_semaphore()
    for dev in (pt, ct):
        pl.semaphore_signal(barrier, inc=1, device_id={'tp': dev}, device_id_type=MESH)
    for name in ('qkv', 'out', 'dn', 'up'):
        for c in w_cps[name]:
            c.start()
    pl.semaphore_wait(barrier, 2)

    in_x.wait()
    x_c = send(xg.at[t], xg.at[t], ct)
    x_p = send(xg.at[t], xg.at[t], pt)

    for c in (in_b, *in_p):
        c.wait()
    for i, r in enumerate((g1_in, be1_in, g2_in, be2_in, bo_in, bd_in, bup_in)):
        par[i, :] = r[...]
    g1_ref, be1_ref, g2_ref, be2_ref, bo_ref, bd_ref, bup_ref = (par.at[i:i + 1] for i in range(7))

    for h in range(HL):
        for e in range(3):
            row = jnp.broadcast_to(bqkv_ref[e, h:h + 1, :], (S, HD))
            biasT[pl.ds((h * 3 + e) * HD, HD), :] = row.T

    x_c.wait_recv()
    x_f = send(xg.at[ct], xg.at[ct], pt)
    in_gy.wait()
    y_c = send(gyg.at[t], gyg.at[t], ct)
    y_p = send(gyg.at[t], gyg.at[t], pt)
    x_p.wait_recv()
    x_f.wait_recv()

    for i in range(TP):
        xf[pl.ds(i * SL, SL), :] = xg[i].astype(F32)
    for r in range(0, S, 32):
        cen, rstd = rows_stats(xf[r:r + 32, :])
        xh = cen * rstd
        xhat[r:r + 32, :] = xh
        rstd_s[r:r + 32, :] = jnp.broadcast_to(rstd, (32, 128))
        h_ref[r:r + 32, :] = (xh * g1_ref[...] + be1_ref[...]).astype(BF)

    w_cps['qkv'][0].wait()
    hv = h_ref[...]
    for h in range(HL):
        rows = slice(h * 3 * HD, (h + 1) * 3 * HD)
        qkvT[rows, :] = (dot(wqkv[rows, :], hv, 1, 1) + biasT[rows, :]).astype(BF)

    scale = HD ** -0.5
    slopes = alibi_slopes(HL * TP)
    j_pos = lax.broadcasted_iota(jnp.int32, (S, S), 0)
    i_pos = lax.broadcasted_iota(jnp.int32, (S, S), 1)
    causal = j_pos <= i_pos
    j_f = j_pos.astype(F32)

    def head(h, e):
        return qkvT[head_rows(h, e), :]

    for h in range(HL):
        slope = jnp.where(t == 0, slopes[h], jnp.where(t == 1, slopes[HL + h], jnp.where(t == 2, slopes[2 * HL + h], slopes[3 * HL + h]))).astype(F32)
        s = dot(head(h, 1), head(h, 0), 0, 0) * scale + slope * j_f
        s = jnp.where(causal, s, MASK_VALUE)
        p = jnp.exp(s - jnp.max(s, axis=0, keepdims=True))
        p = p / jnp.sum(p, axis=0, keepdims=True)
        probs[h] = p
        ctx_ref[h * HD:(h + 1) * HD, :] = dot(head(h, 2), p.astype(BF), 1, 0).astype(BF)

    def exchange(part, groups, ps, pr, hs, hr, cr, fr):
        firsts = []
        for k0, k1 in groups:
            cols = slice(CUT[k0], CUT[k1])
            ps[:, cols] = part(1 - half, CUT[k0], CUT[k1]).astype(BF)
            firsts.append(send(ps.at[:, cols], pr.at[:, cols], pt))
        outs = []
        for (k0, k1), first in zip(groups, firsts):
            cols = slice(CUT[k0], CUT[k1])
            ours = part(half, CUT[k0], CUT[k1])
            first.wait_recv()
            hs[:, cols] = (ours + pr[:, cols].astype(F32)).astype(BF)
            for k in range(k0, k1):
                c = slice(CUT[k], CUT[k + 1])
                outs.append([send(hs.at[:, c], cr.at[:, c], ct)])
        local = send(hs, hr, pt)
        return outs, local

    def arrived(out, k, hs, cr, fr, put):
        c = slice(CUT[k], CUT[k + 1])
        out[0].wait_recv()
        out.append(send(cr.at[:, c], fr.at[:, c], pt))
        put(half * HW + CUT[k], CUT[k + 1] - CUT[k], (hs[:, c].astype(F32) + cr[:, c].astype(F32)).astype(BF).astype(F32))

    def passed_on(outs, local, hr, fr, put):
        local.wait_recv()
        for k, out in enumerate(outs):
            c = slice(CUT[k], CUT[k + 1])
            out[1].wait_recv()
            put((1 - half) * HW + CUT[k], CUT[k + 1] - CUT[k], (hr[:, c].astype(F32) + fr[:, c].astype(F32)).astype(BF).astype(F32))

    for c in w_cps['out']:
        c.wait()
    ctxT = ctx_ref[...]
    a_outs, a_local = exchange(lambda hh, c0, c1: dot(ctxT, wout[hh, :, c0:c1], 0, 0), ((0, NCUT),), a_ps, a_pr, a_hs, a_hr, a_cr, a_fr)

    y_c.wait_recv()
    y_f = send(gyg.at[ct], gyg.at[ct], pt)
    y_p.wait_recv()
    y_f.wait_recv()
    for i in range(TP):
        gm_f[pl.ds(i * SL, SL), :] = gyg[i].astype(F32)
    for r in range(0, S, 32):
        gyf_ref[r:r + 32, :] = gm_f[r:r + 32, :].astype(BF)
    w_cps['dn'][0].wait()
    gyv = gyf_ref[...]
    for n in range(NCH):
        gact[:, n * CW:(n + 1) * CW] = dot(gyv, wdn[n * CW:(n + 1) * CW, :], 1, 1).astype(BF)
    vec_ref[0:1, :] = jnp.sum(gm_f[...], axis=0, keepdims=True)

    def put_x(start, width, val):
        cols = pl.ds(pl.multiple_of(start, 128), width)
        xf[:, cols] = xf[:, cols] + val + bo_ref[:, cols]

    for k, out in enumerate(a_outs):
        arrived(out, k, a_hs, a_cr, a_fr, put_x)
    passed_on(a_outs, a_local, a_hr, a_fr, put_x)

    for r in range(0, S, 32):
        cen, rstd = rows_stats(xf[r:r + 32, :])
        g_ref[r:r + 32, :] = (cen * rstd * g2_ref[...] + be2_ref[...]).astype(BF)

    w_cps['up'][0].wait()
    gv = g_ref[...]
    for n in range(NCH):
        cols = slice(n * CW, (n + 1) * CW)
        pre = dot(gv, wup[:, cols], 1, 0) + bup_ref[:, cols]
        val, der = gelu_parts(pre)
        act_ref[:, cols] = val.astype(BF)
        gp = gact[:, cols].astype(F32) * der
        vec_ref[1:2, cols] = jnp.sum(gp, axis=0, keepdims=True)
        gpre_ref[:, cols] = gp.astype(BF)

    gprev = gpre_ref[...]

    def part_g(hh, c0, c1):
        return dot(gprev, wup[pl.ds(pl.multiple_of(hh * HW + c0, CW), c1 - c0), :], 1, 1)

    g_outs, g_local = exchange(part_g, ((0, 1), (1, NCUT)), b_ps, b_pr, b_hs, b_hr, b_cr, b_fr)

    actv = act_ref[...]
    for n in range(NCH):
        cols = slice(n * CW, (n + 1) * CW)
        row_blocks(mp, cols, dot(actv, wdn[:, cols], 1, 0))
    m_first = (send(mp.at[qt], m_pr.at[1], pt), send(mp.at[pt], m_pr.at[0], pt))
    for n in range(NCH):
        gwdn_ref[n * CW:(n + 1) * CW, :] = dot(act_ref[:, n * CW:(n + 1) * CW], gyv, 0, 0).astype(BF)
    def put_g(start, width, val):
        gg_f[:, pl.ds(pl.multiple_of(start, 128), width)] = val

    for k in range(HCH):
        arrived(g_outs[k], k, b_hs, b_cr, b_fr, put_g)
        for n in range(2 * k, 2 * k + 2):
            gwup_ref[n * CW:(n + 1) * CW, :] = dot(g_ref[:, n * CW:(n + 1) * CW], gprev, 0, 0).astype(BF)

    m_first[0].wait_recv()
    m_hs[...] = (mp[ct].astype(F32) + m_pr[1].astype(F32)).astype(BF)
    m_out = send(m_hs, m_cr, ct)

    passed_on(g_outs, g_local, b_hr, b_fr, put_g)

    gg2 = jnp.zeros((1, D), F32)
    gb2 = jnp.zeros((1, D), F32)
    gbo = jnp.zeros((1, D), F32)
    for r in range(0, S, 32):
        cen, rstd = rows_stats(xf[r:r + 32, :])
        xh = cen * rstd
        gg = gg_f[r:r + 32, :]
        gg2 = gg2 + jnp.sum(gg * xh, axis=0, keepdims=True)
        gb2 = gb2 + jnp.sum(gg, axis=0, keepdims=True)
        dxh = gg * g2_ref[...]
        m1 = jnp.mean(dxh, axis=-1, keepdims=True)
        m2 = jnp.mean(dxh * xh, axis=-1, keepdims=True)
        gm = gm_f[r:r + 32, :] + rstd * (dxh - m1 - xh * m2)
        gm_f[r:r + 32, :] = gm
        gbo = gbo + jnp.sum(gm, axis=0, keepdims=True)
        gmid_ref[r:r + 32, :] = gm.astype(BF)
    vec_ref[2:3, :] = gg2
    vec_ref[3:4, :] = gb2
    vec_ref[4:5, :] = gbo

    gmv = gmid_ref[...]
    gctxT = (dot(wout[0], gmv[:, :HW], 1, 1) + dot(wout[1], gmv[:, HW:], 1, 1)).astype(BF)
    heads = range(HL)
    gos = [gctxT[h * HD:(h + 1) * HD, :] for h in heads]
    gps = [dot(head(h, 2), gos[h], 0, 0).astype(BF).astype(F32) for h in heads]
    gvs = [dot(gos[h], probs[h].astype(BF), 1, 1).astype(BF) for h in heads]
    gss = [(probs[h] * (gps[h] - jnp.sum(gps[h] * probs[h], axis=0, keepdims=True))).astype(BF) for h in heads]
    gqs = [(dot(head(h, 1), gss[h], 1, 0) * scale).astype(BF) for h in heads]
    gks = [(dot(head(h, 0), gss[h], 1, 1) * scale).astype(BF) for h in heads]
    for h in heads:
        for e, val in enumerate((gqs[h], gks[h], gvs[h])):
            gqkv_ref[head_rows(h, e), :] = val

    gqv = gqkv_ref[...]
    r_first = []
    for k in range(2):
        row_blocks(rp.at[k], slice(0, HW), dot(gqv, wqkv[:, k * HW:(k + 1) * HW], 0, 0))
        r_first.append((send(rp.at[k, qt], r_pr.at[k, 1], pt), send(rp.at[k, pt], r_pr.at[k, 0], pt)))

    ln_s, ln_pr = ln_x.at[0], ln_x.at[1]
    for k in range(2):
        cols = slice(k * HW, (k + 1) * HW)
        gg1 = jnp.zeros((1, HW), F32)
        gb1 = jnp.zeros((1, HW), F32)
        for i in range(TP):
            v = rp[k, i].astype(F32)
            gg1 = gg1 + jnp.sum(v * xhat[i * SL:(i + 1) * SL, cols], axis=0, keepdims=True)
            gb1 = gb1 + jnp.sum(v, axis=0, keepdims=True)
        ln_s[0:1, cols] = gg1
        ln_s[1:2, cols] = gb1
    l_first = send(ln_s, ln_pr, pt)

    own = pl.ds(pl.multiple_of(t * SL, 8), SL)
    xh_ref[...] = xhat[own, :]
    gm_ref[...] = gm_f[own, :]
    rs_ref[...] = rstd_s[own, :]
    g1_out[...] = par[0:1, :]

    for k in range(2):
        cols = slice(k * HW, (k + 1) * HW)
        r_first[k][0].wait_recv()
        r_hs[0:SL, cols] = (rp[k, ct].astype(F32) + r_pr[k, 1].astype(F32)).astype(BF)
        r_first[k][1].wait_recv()
        mine_ref[:, cols] = (rp[k, t].astype(F32) + r_pr[k, 0].astype(F32)).astype(BF)
    l_first.wait_recv()
    ln = ln_s[...] + ln_pr[...]
    ln_hs[...] = ln
    ln_rows = []
    for _ in range(3):
        ln_rows.append(ln.astype(BF).astype(F32))
        ln = ln - ln_rows[-1]
    r_hs[SL:SL + 8, :] = jnp.concatenate(ln_rows + [jnp.zeros((2, D), F32)], axis=0).astype(BF)
    m_first[1].wait_recv()
    m_out.wait_recv()
    m_sum = (mp[t].astype(F32) + m_pr[0].astype(F32)).astype(BF).astype(F32) + m_cr[...].astype(F32)
    y_ref[...] = (xf[own, :] + m_sum.astype(BF).astype(F32) + bd_ref[...]).astype(BF)
    for c in started:
        c.wait_send()


N_SEND = 6 + 2 * (2 + 3 + 1 + 3) + 3 + 4 + 1
VMEM_A = 36 * 2**20
VMEM_B = 8 * 2**20
VMEM_C = 4 * 2**20


def write_kernel(yi_ref, vec_ref, up_ref, dn_ref, gqkv_ref, h_ref, ctx_ref, gmid_ref,
                 y_ref, gwqkv_ref, gbqkv_ref, gwout_ref, gbo_ref, gl2_ref, bl2_ref, gwup_ref, gbup_ref, gwdn_ref, gbd_ref,
                 s_qkv, s_out, s_gb, s0, s1, s2, s3, s4, sem):
    cps = []

    def out(src, dst, n=1):
        rows = src.shape[0] // n
        for k in range(n):
            c = pltpu.make_async_copy(src.at[pl.ds(k * rows, rows)], dst.at[pl.ds(k * rows, rows)], sem.at[len(cps)])
            c.start()
            cps.append(c)

    out(dn_ref, gwdn_ref, 4)
    out(up_ref, gwup_ref, 4)
    out(yi_ref, y_ref)
    for i, (sv, r) in enumerate(((s0, gbd_ref), (s1, gbup_ref), (s2, gl2_ref), (s3, bl2_ref), (s4, gbo_ref))):
        sv[...] = vec_ref[i, :]
        out(sv, r)
    ones = jnp.ones((8, S), BF)
    for h in range(HL):
        for e in range(3):
            s_gb[e, h:h + 1, :] = dot(ones, gqkv_ref[head_rows(h, e), :], 1, 1)[0:1, :]
    out(s_gb, gbqkv_ref)
    hv = h_ref[...]
    s_out[...] = dot(ctx_ref[...], gmid_ref[...], 1, 0).astype(BF)
    out(s_out, gwout_ref)
    for n in range(HL):
        rows = slice(n * 3 * HD, (n + 1) * 3 * HD)
        s_qkv[rows, :] = dot(gqkv_ref[rows, :], hv, 1, 0).astype(BF)
        out(s_qkv.at[rows], gwqkv_ref.at[rows])
    for c in cps:
        c.wait()


def last_kernel(mine_ref, xh_ref, gm_ref, rs_ref, g1_ref, rc_ref, ln_ref, gx_ref, gl1_ref, bl1_ref):
    gh = (mine_ref[...].astype(F32) + rc_ref[0:SL, :].astype(F32)).astype(BF).astype(F32)
    xh = xh_ref[...]
    dxh = gh * g1_ref[...]
    m1 = jnp.mean(dxh, axis=-1, keepdims=True)
    m2 = jnp.mean(dxh * xh, axis=-1, keepdims=True)
    gx_ref[...] = (gm_ref[...] + rs_ref[:, 0:1] * (dxh - m1 - xh * m2)).astype(BF)
    lc = rc_ref[SL:SL + 8, :].astype(F32)
    ln = ln_ref[...] + (lc[0:2, :] + lc[2:4, :] + lc[4:6, :])
    gl1_ref[...] = ln[0, :]
    bl1_ref[...] = ln[1, :]


def solution(mesh):
    VM = pl.BlockSpec(memory_space=pltpu.VMEM)
    ANY = pl.BlockSpec(memory_space=pltpu.HBM)

    def sds(shape, dt):
        return jax.ShapeDtypeStruct(shape, dt)

    def local_step(x, g1, be1, w_qkv, b_qkv, w_out, b_out, g2, be2, w_up, b_up, w_down, b_down, grad_y):
        wq = jnp.transpose(w_qkv, (1, 2, 3, 0)).reshape(3 * HL * HD, D)
        bq = jnp.transpose(b_qkv, (1, 0, 2))
        part = pltpu.VMEM((S, HW), BF)
        vec1 = sds((D,), F32)
        mids = pl.pallas_call(
            block_kernel,
            out_shape=(pltpu.VMEM((SL, D), BF), pltpu.VMEM((8, D), F32), pltpu.VMEM((D, FL), BF), pltpu.VMEM((FL, D), BF),
                       pltpu.VMEM((3 * HL * HD, S), BF), pltpu.VMEM((S, D), BF), pltpu.VMEM((HL * HD, S), BF), pltpu.VMEM((S, D), BF),
                       pltpu.VMEM((SL, D), BF), pltpu.VMEM((SL, D), F32), pltpu.VMEM((SL, D), F32), pltpu.VMEM((SL, 128), F32),
                       pltpu.VMEM((1, D), F32), sds((SL + 8, D), BF), pltpu.VMEM((2, D), F32)),
            in_specs=[ANY] * 14,
            out_specs=(VM,) * 15,
            scratch_shapes=[
                pltpu.VMEM((3 * HL * HD, D), BF), pltpu.VMEM((2, HL * HD, HW), BF), pltpu.VMEM((S, D), F32), pltpu.VMEM((S, D), F32),
                pltpu.VMEM((S, D), F32), pltpu.VMEM((S, D), F32), pltpu.VMEM((S, 128), F32), pltpu.VMEM((HL, S, S), F32),
                pltpu.VMEM((3 * HL * HD, S), BF), pltpu.VMEM((8, D), F32), pltpu.VMEM((TP, SL, D), BF),
                pltpu.VMEM((D, FL), BF), pltpu.VMEM((FL, D), BF), pltpu.VMEM((TP, SL, D), BF), pltpu.VMEM((TP, SL, D), BF),
                pltpu.VMEM((3 * HL * HD, S), F32), *[part] * 12,
                pltpu.VMEM((S, FL), BF), pltpu.VMEM((S, D), BF), pltpu.VMEM((S, FL), BF), pltpu.VMEM((S, FL), BF), pltpu.VMEM((S, D), BF),
                pltpu.VMEM((3, HL, HD), F32), *[pltpu.VMEM((D,), F32) for _ in range(7)],
                pltpu.VMEM((2, TP, SL, HW), BF), pltpu.VMEM((2, SL, D), BF), pltpu.VMEM((SL, D), BF), pltpu.VMEM((SL, D), BF),
                pltpu.VMEM((2, 2, SL, HW), BF), pltpu.VMEM((2, 2, D), F32),
                pltpu.SemaphoreType.DMA((9,)), pltpu.SemaphoreType.DMA((N_SEND,)), pltpu.SemaphoreType.DMA((N_SEND,)),
                pltpu.SemaphoreType.DMA((10,)),
            ],
            compiler_params=pltpu.CompilerParams(collective_id=0, has_side_effects=True, vmem_limit_bytes=VMEM_A),
            name='block',
        )(*(pltpu.with_memory_space_constraint(v, pltpu.HBM) for v in (
            x.reshape(SL, D), grad_y.reshape(SL, D), g1, be1, g2, be2, b_out, b_down, bq, b_up, wq, w_out, w_up, w_down)))
        mine, xh, gm, rs, g1v, r_hs, ln_hs = mids[8:]
        across = [(i, TP - 1 - i) for i in range(TP)]
        r_cr = lax.ppermute(r_hs, 'tp', across)
        y, gwqkv, gbqkv, gwout, gbo, gl2, bl2, gwup, gbup, gwdn, gbd = pl.pallas_call(
            write_kernel,
            out_shape=(sds((SL, D), BF), sds((3 * HL * HD, D), BF), sds((3, HL, HD), F32), sds((HL * HD, D), BF), vec1, vec1, vec1,
                       sds((D, FL), BF), vec1, sds((FL, D), BF), vec1),
            in_specs=[VM] * 8,
            out_specs=(ANY,) * 11,
            scratch_shapes=[pltpu.VMEM((3 * HL * HD, D), BF), pltpu.VMEM((HL * HD, D), BF), pltpu.VMEM((3, HL, HD), F32),
                            *[pltpu.VMEM((D,), F32) for _ in range(5)], pltpu.SemaphoreType.DMA((20,))],
            compiler_params=pltpu.CompilerParams(vmem_limit_bytes=VMEM_B),
            cost_estimate=pl.CostEstimate(flops=600_000_000, bytes_accessed=14_200_000, transcendentals=0),
            name='write',
        )(*mids[:8])
        gx, gl1, bl1 = pl.pallas_call(
            last_kernel,
            out_shape=(sds((SL, D), BF), vec1, vec1),
            in_specs=[VM] * 7,
            out_specs=(VM,) * 3,
            compiler_params=pltpu.CompilerParams(vmem_limit_bytes=VMEM_C),
            name='last',
        )(mine, xh, gm, rs, g1v, r_cr, ln_hs)
        gwqkv = jnp.transpose(gwqkv.reshape(HL, 3, HD, D), (3, 0, 1, 2))
        gbqkv = jnp.transpose(gbqkv, (1, 0, 2))
        return (y.reshape(1, SL, D), gx.reshape(1, SL, D), gl1, bl1, gwqkv, gbqkv, gwout, gbo, gl2, bl2, gwup, gbup, gwdn, gbd)

    row_spec = P('dp', 'tp', None)
    in_specs = (row_spec, P(), P(), P(None, 'tp', None, None), P('tp', None, None), P('tp', None), P(), P(), P(),
                P(None, 'tp'), P('tp'), P('tp', None), P(), row_spec)
    out_specs = (row_spec, row_spec, P('dp'), P('dp'), P('dp', 'tp', None, None), P(('dp', 'tp'), None, None),
                 P(('dp', 'tp'), None), P('dp'), P('dp'), P('dp'), P('dp', 'tp'), P(('dp', 'tp')), P(('dp', 'tp'), None), P('dp'))
    return jax.shard_map(local_step, mesh=mesh, in_specs=in_specs, out_specs=out_specs, check_vma=False)
```

```python
import functools
import math

import jax
import jax.numpy as jnp
from jax import lax
from jax.experimental import pallas as pl
from jax.experimental.pallas import tpu as pltpu
from jax.sharding import PartitionSpec as P

EPS = 1e-5
MASK_VALUE = -1e30
BF = jnp.bfloat16
F32 = jnp.float32
MESH = pl.DeviceIdType.MESH

D = 1536
S = 96
SL = 24
TP = 4
HL = 4
HD = 96
FL = 1536
CW = 256
NCH = D // CW
HCH = NCH // 2
HW = D // 2
CUT = (0, 256, 512, 640, 768)
NCUT = len(CUT) - 1
XCUT = 1024


def alibi_slopes(n_heads):
    closest = 2 ** int(math.floor(math.log2(n_heads)))
    base_ratio = 2.0 ** (-8.0 / closest)
    extra_ratio = 2.0 ** (-4.0 / closest)
    remaining = min(closest, n_heads - closest)
    slopes = [base_ratio ** (i + 1) for i in range(closest)]
    return slopes + [extra_ratio ** (2 * i + 1) for i in range(remaining)]


def dot(a, b, ca, cb):
    return lax.dot_general(a, b, (((ca,), (cb,)), ((), ())), preferred_element_type=F32)


def gelu_parts(u):
    k = math.sqrt(2.0 / math.pi)
    u2 = u * u
    th = jnp.tanh(u * (k + (k * 0.044715) * u2))
    half = 0.5 + 0.5 * th
    val = u * half
    return val, half + val * (1.0 - th) * (k + (3.0 * 0.044715 * k) * u2)


def rows_stats(v):
    mean = jnp.mean(v, axis=-1, keepdims=True)
    cen = v - mean
    var = jnp.mean(cen * cen, axis=-1, keepdims=True)
    return cen, lax.rsqrt(var + EPS)


def places():
    t = lax.axis_index('tp')
    core = t % 2
    pt = t + 1 - 2 * core
    ct = TP - 1 - t
    qt = TP - 1 - pt
    half = (core + t // 2) % 2
    return t, pt, ct, qt, half


def sender(ssem, rsem):
    started = []

    def send(src, dst, dev):
        i = len(started)
        c = pltpu.make_async_remote_copy(src_ref=src, dst_ref=dst, send_sem=ssem.at[i], recv_sem=rsem.at[i],
                                         device_id={'tp': dev}, device_id_type=MESH)
        c.start()
        started.append(c)
        return c

    return send, started


def head_rows(h, e):
    return slice((h * 3 + e) * HD, (h * 3 + e + 1) * HD)


def row_blocks(buf, cols, v):
    for i in range(TP):
        buf[i, :, cols] = v[i * SL:(i + 1) * SL, :].astype(BF)


def block_kernel(x_hbm, gy_hbm, g1_hbm, be1_hbm, g2_hbm, be2_hbm, bo_hbm, bd_hbm, bqkv_hbm, bup_hbm,
                 wqkv_hbm, wout_hbm, wup_hbm, wdn_hbm,
                 y_ref, vec_ref, gwup_ref, gwdn_ref, gqkv_ref, h_ref, ctx_ref, gmid_ref, mine_ref, xh_ref, gm_ref, rs_ref, g1_out, r_hs, ln_hs,
                 wqkv, wout, xf, gm_f, gg_f, xhat, rstd_s, probs, qkvT, par, mp,
                 wup, wdn, xg, gyg, biasT, a_ps, a_pr, a_hs, a_hr, a_cr, a_fr, b_ps, b_pr, b_hs, b_hr, b_cr, b_fr,
                 gact, g_ref, gpre_ref, act_ref, gyf_ref, bqkv_ref, g1_in, be1_in, g2_in, be2_in, bo_in, bd_in, bup_in,
                 rp, m_pr, m_hs, m_cr, r_pr, ln_x,
                 wsem, ssem, rsem, isem):
    t, pt, ct, qt, half = places()
    send, started = sender(ssem, rsem)

    in_x = pltpu.make_async_copy(x_hbm, xg.at[t], isem.at[0])
    in_gy = pltpu.make_async_copy(gy_hbm, gyg.at[t], isem.at[1])
    in_b = pltpu.make_async_copy(bqkv_hbm, bqkv_ref, isem.at[2])
    small = ((g1_hbm, g1_in), (be1_hbm, be1_in), (g2_hbm, g2_in), (be2_hbm, be2_in), (bo_hbm, bo_in), (bd_hbm, bd_in), (bup_hbm, bup_in))
    in_p = [pltpu.make_async_copy(a, b, isem.at[3 + i]) for i, (a, b) in enumerate(small)]
    for c in (in_x, in_gy, in_b, *in_p):
        c.start()
    w_cps = {}
    w_cps['qkv'] = [pltpu.make_async_copy(wqkv_hbm, wqkv, wsem.at[0])]
    w_cps['out'] = [pltpu.make_async_copy(wout_hbm.at[:, pl.ds(k * HW, HW)], wout.at[k], wsem.at[1 + k]) for k in range(2)]
    w_cps['dn'] = [pltpu.make_async_copy(wdn_hbm, wdn, wsem.at[7])]
    w_cps['up'] = [pltpu.make_async_copy(wup_hbm, wup, wsem.at[8])]

    barrier = pltpu.get_barrier_semaphore()
    for dev in (pt, ct, qt):
        pl.semaphore_signal(barrier, inc=1, device_id={'tp': dev}, device_id_type=MESH)
    for name in ('qkv', 'out', 'dn', 'up'):
        for c in w_cps[name]:
            c.start()
    pl.semaphore_wait(barrier, 3)

    in_x.wait()
    lo, hi = slice(0, XCUT), slice(XCUT, D)
    x_c = send(xg.at[t, :, lo], xg.at[t, :, lo], ct)
    x_p = send(xg.at[t], xg.at[t], pt)
    x_d = [send(xg.at[t, :, hi], xg.at[t, :, hi], dev) for dev in (ct, qt)]

    for c in (in_b, *in_p):
        c.wait()
    for i, r in enumerate((g1_in, be1_in, g2_in, be2_in, bo_in, bd_in, bup_in)):
        par[i, :] = r[...]
    g1_ref, be1_ref, g2_ref, be2_ref, bo_ref, bd_ref, bup_ref = (par.at[i:i + 1] for i in range(7))

    for h in range(HL):
        for e in range(3):
            row = jnp.broadcast_to(bqkv_ref[e, h:h + 1, :], (S, HD))
            biasT[pl.ds((h * 3 + e) * HD, HD), :] = row.T

    x_c.wait_recv()
    x_f = send(xg.at[ct, :, lo], xg.at[ct, :, lo], pt)
    in_gy.wait()
    y_c = send(gyg.at[t], gyg.at[t], ct)
    y_p = send(gyg.at[t], gyg.at[t], pt)
    x_p.wait_recv()
    for c in x_d:
        c.wait_recv()
    x_f.wait_recv()

    for i in range(TP):
        xf[pl.ds(i * SL, SL), :] = xg[i].astype(F32)
    for r in range(0, S, 32):
        cen, rstd = rows_stats(xf[r:r + 32, :])
        xh = cen * rstd
        xhat[r:r + 32, :] = xh
        rstd_s[r:r + 32, :] = jnp.broadcast_to(rstd, (32, 128))
        h_ref[r:r + 32, :] = (xh * g1_ref[...] + be1_ref[...]).astype(BF)

    w_cps['qkv'][0].wait()
    hv = h_ref[...]
    for h in range(HL):
        rows = slice(h * 3 * HD, (h + 1) * 3 * HD)
        qkvT[rows, :] = (dot(wqkv[rows, :], hv, 1, 1) + biasT[rows, :]).astype(BF)

    scale = HD ** -0.5
    slopes = alibi_slopes(HL * TP)
    j_pos = lax.broadcasted_iota(jnp.int32, (S, S), 0)
    i_pos = lax.broadcasted_iota(jnp.int32, (S, S), 1)
    causal = j_pos <= i_pos
    j_f = j_pos.astype(F32)

    def head(h, e):
        return qkvT[head_rows(h, e), :]

    for h in range(HL):
        slope = jnp.where(t == 0, slopes[h], jnp.where(t == 1, slopes[HL + h], jnp.where(t == 2, slopes[2 * HL + h], slopes[3 * HL + h]))).astype(F32)
        s = dot(head(h, 1), head(h, 0), 0, 0) * scale + slope * j_f
        s = jnp.where(causal, s, MASK_VALUE)
        p = jnp.exp(s - jnp.max(s, axis=0, keepdims=True))
        p = p / jnp.sum(p, axis=0, keepdims=True)
        probs[h] = p
        ctx_ref[h * HD:(h + 1) * HD, :] = dot(head(h, 2), p.astype(BF), 1, 0).astype(BF)

    def exchange(part, groups, ps, pr, hs, hr, cr, fr):
        firsts = []
        for k0, k1 in groups:
            cols = slice(CUT[k0], CUT[k1])
            ps[:, cols] = part(1 - half, CUT[k0], CUT[k1]).astype(BF)
            firsts.append(send(ps.at[:, cols], pr.at[:, cols], pt))
        outs = []
        for (k0, k1), first in zip(groups, firsts):
            cols = slice(CUT[k0], CUT[k1])
            ours = part(half, CUT[k0], CUT[k1])
            first.wait_recv()
            hs[:, cols] = (ours + pr[:, cols].astype(F32)).astype(BF)
            for k in range(k0, k1):
                c = slice(CUT[k], CUT[k + 1])
                outs.append([send(hs.at[:, c], cr.at[:, c], ct)])
                if k == NCUT - 1:
                    outs[-1].append(send(hs.at[:, c], fr.at[:, c], qt))
        local = send(hs, hr, pt)
        return outs, local

    def arrived(out, k, hs, cr, fr, put):
        c = slice(CUT[k], CUT[k + 1])
        out[0].wait_recv()
        if k < NCUT - 1:
            out.append(send(cr.at[:, c], fr.at[:, c], pt))
        put(half * HW + CUT[k], CUT[k + 1] - CUT[k], (hs[:, c].astype(F32) + cr[:, c].astype(F32)).astype(BF).astype(F32))

    def passed_on(outs, local, hr, fr, put):
        local.wait_recv()
        for k, out in enumerate(outs):
            c = slice(CUT[k], CUT[k + 1])
            out[1].wait_recv()
            put((1 - half) * HW + CUT[k], CUT[k + 1] - CUT[k], (hr[:, c].astype(F32) + fr[:, c].astype(F32)).astype(BF).astype(F32))

    for c in w_cps['out']:
        c.wait()
    ctxT = ctx_ref[...]
    a_outs, a_local = exchange(lambda hh, c0, c1: dot(ctxT, wout[hh, :, c0:c1], 0, 0), ((0, NCUT),), a_ps, a_pr, a_hs, a_hr, a_cr, a_fr)

    y_c.wait_recv()
    y_f = send(gyg.at[ct], gyg.at[ct], pt)
    y_p.wait_recv()
    y_f.wait_recv()
    for i in range(TP):
        gm_f[pl.ds(i * SL, SL), :] = gyg[i].astype(F32)
    for r in range(0, S, 32):
        gyf_ref[r:r + 32, :] = gm_f[r:r + 32, :].astype(BF)
    w_cps['dn'][0].wait()
    gyv = gyf_ref[...]
    for n in range(NCH):
        gact[:, n * CW:(n + 1) * CW] = dot(gyv, wdn[n * CW:(n + 1) * CW, :], 1, 1).astype(BF)
    vec_ref[0:1, :] = jnp.sum(gm_f[...], axis=0, keepdims=True)

    def put_x(start, width, val):
        cols = pl.ds(pl.multiple_of(start, 128), width)
        xf[:, cols] = xf[:, cols] + val + bo_ref[:, cols]

    for k, out in enumerate(a_outs):
        arrived(out, k, a_hs, a_cr, a_fr, put_x)
    passed_on(a_outs, a_local, a_hr, a_fr, put_x)

    for r in range(0, S, 32):
        cen, rstd = rows_stats(xf[r:r + 32, :])
        g_ref[r:r + 32, :] = (cen * rstd * g2_ref[...] + be2_ref[...]).astype(BF)

    w_cps['up'][0].wait()
    gv = g_ref[...]
    for n in range(NCH):
        cols = slice(n * CW, (n + 1) * CW)
        pre = dot(gv, wup[:, cols], 1, 0) + bup_ref[:, cols]
        val, der = gelu_parts(pre)
        act_ref[:, cols] = val.astype(BF)
        gp = gact[:, cols].astype(F32) * der
        vec_ref[1:2, cols] = jnp.sum(gp, axis=0, keepdims=True)
        gpre_ref[:, cols] = gp.astype(BF)

    gprev = gpre_ref[...]

    def part_g(hh, c0, c1):
        return dot(gprev, wup[pl.ds(pl.multiple_of(hh * HW + c0, CW), c1 - c0), :], 1, 1)

    g_outs, g_local = exchange(part_g, ((0, 1), (1, NCUT)), b_ps, b_pr, b_hs, b_hr, b_cr, b_fr)

    actv = act_ref[...]
    for n in range(NCH):
        cols = slice(n * CW, (n + 1) * CW)
        row_blocks(mp, cols, dot(actv, wdn[:, cols], 1, 0))
    m_first = (send(mp.at[qt], m_pr.at[1], pt), send(mp.at[pt], m_pr.at[0], pt))
    for n in range(NCH):
        gwdn_ref[n * CW:(n + 1) * CW, :] = dot(act_ref[:, n * CW:(n + 1) * CW], gyv, 0, 0).astype(BF)
    def put_g(start, width, val):
        gg_f[:, pl.ds(pl.multiple_of(start, 128), width)] = val

    for k in range(HCH):
        arrived(g_outs[k], k, b_hs, b_cr, b_fr, put_g)
        for n in range(2 * k, 2 * k + 2):
            gwup_ref[n * CW:(n + 1) * CW, :] = dot(g_ref[:, n * CW:(n + 1) * CW], gprev, 0, 0).astype(BF)
    arrived(g_outs[-1], NCUT - 1, b_hs, b_cr, b_fr, put_g)

    m_first[0].wait_recv()
    m_hs[...] = (mp[ct].astype(F32) + m_pr[1].astype(F32)).astype(BF)
    m_out = send(m_hs, m_cr, ct)

    passed_on(g_outs, g_local, b_hr, b_fr, put_g)

    gg2 = jnp.zeros((1, D), F32)
    gb2 = jnp.zeros((1, D), F32)
    gbo = jnp.zeros((1, D), F32)
    for r in range(0, S, 32):
        cen, rstd = rows_stats(xf[r:r + 32, :])
        xh = cen * rstd
        gg = gg_f[r:r + 32, :]
        gg2 = gg2 + jnp.sum(gg * xh, axis=0, keepdims=True)
        gb2 = gb2 + jnp.sum(gg, axis=0, keepdims=True)
        dxh = gg * g2_ref[...]
        m1 = jnp.mean(dxh, axis=-1, keepdims=True)
        m2 = jnp.mean(dxh * xh, axis=-1, keepdims=True)
        gm = gm_f[r:r + 32, :] + rstd * (dxh - m1 - xh * m2)
        gm_f[r:r + 32, :] = gm
        gbo = gbo + jnp.sum(gm, axis=0, keepdims=True)
        gmid_ref[r:r + 32, :] = gm.astype(BF)
    vec_ref[2:3, :] = gg2
    vec_ref[3:4, :] = gb2
    vec_ref[4:5, :] = gbo

    gmv = gmid_ref[...]
    gctxT = (dot(wout[0], gmv[:, :HW], 1, 1) + dot(wout[1], gmv[:, HW:], 1, 1)).astype(BF)
    heads = range(HL)
    gos = [gctxT[h * HD:(h + 1) * HD, :] for h in heads]
    gps = [dot(head(h, 2), gos[h], 0, 0).astype(BF).astype(F32) for h in heads]
    gvs = [dot(gos[h], probs[h].astype(BF), 1, 1).astype(BF) for h in heads]
    gss = [(probs[h] * (gps[h] - jnp.sum(gps[h] * probs[h], axis=0, keepdims=True))).astype(BF) for h in heads]
    gqs = [(dot(head(h, 1), gss[h], 1, 0) * scale).astype(BF) for h in heads]
    gks = [(dot(head(h, 0), gss[h], 1, 1) * scale).astype(BF) for h in heads]
    for h in heads:
        for e, val in enumerate((gqs[h], gks[h], gvs[h])):
            gqkv_ref[head_rows(h, e), :] = val

    gqv = gqkv_ref[...]
    r_first = []
    for k in range(2):
        row_blocks(rp.at[k], slice(0, HW), dot(gqv, wqkv[:, k * HW:(k + 1) * HW], 0, 0))
        r_first.append((send(rp.at[k, qt], r_pr.at[k, 1], pt), send(rp.at[k, pt], r_pr.at[k, 0], pt)))

    ln_s, ln_pr = ln_x.at[0], ln_x.at[1]
    for k in range(2):
        cols = slice(k * HW, (k + 1) * HW)
        gg1 = jnp.zeros((1, HW), F32)
        gb1 = jnp.zeros((1, HW), F32)
        for i in range(TP):
            v = rp[k, i].astype(F32)
            gg1 = gg1 + jnp.sum(v * xhat[i * SL:(i + 1) * SL, cols], axis=0, keepdims=True)
            gb1 = gb1 + jnp.sum(v, axis=0, keepdims=True)
        ln_s[0:1, cols] = gg1
        ln_s[1:2, cols] = gb1
    l_first = send(ln_s, ln_pr, pt)

    own = pl.ds(pl.multiple_of(t * SL, 8), SL)
    xh_ref[...] = xhat[own, :]
    gm_ref[...] = gm_f[own, :]
    rs_ref[...] = rstd_s[own, :]
    g1_out[...] = par[0:1, :]

    for k in range(2):
        cols = slice(k * HW, (k + 1) * HW)
        r_first[k][0].wait_recv()
        r_hs[0:SL, cols] = (rp[k, ct].astype(F32) + r_pr[k, 1].astype(F32)).astype(BF)
        r_first[k][1].wait_recv()
        mine_ref[:, cols] = (rp[k, t].astype(F32) + r_pr[k, 0].astype(F32)).astype(BF)
    l_first.wait_recv()
    ln = ln_s[...] + ln_pr[...]
    ln_hs[...] = ln
    ln_rows = []
    for _ in range(3):
        ln_rows.append(ln.astype(BF).astype(F32))
        ln = ln - ln_rows[-1]
    r_hs[SL:SL + 8, :] = jnp.concatenate(ln_rows + [jnp.zeros((2, D), F32)], axis=0).astype(BF)
    m_first[1].wait_recv()
    m_out.wait_recv()
    m_sum = (mp[t].astype(F32) + m_pr[0].astype(F32)).astype(BF).astype(F32) + m_cr[...].astype(F32)
    y_ref[...] = (xf[own, :] + m_sum.astype(BF).astype(F32) + bd_ref[...]).astype(BF)
    for c in started:
        c.wait_send()


N_SEND = 8 + 2 * (2 + 4 + 1 + 1 + 3) + 3 + 4 + 1
VMEM_A = 36 * 2**20
VMEM_B = 8 * 2**20
VMEM_C = 4 * 2**20


def write_kernel(yi_ref, vec_ref, up_ref, dn_ref, gqkv_ref, h_ref, ctx_ref, gmid_ref,
                 y_ref, gwqkv_ref, gbqkv_ref, gwout_ref, gbo_ref, gl2_ref, bl2_ref, gwup_ref, gbup_ref, gwdn_ref, gbd_ref,
                 s_qkv, s_out, s_gb, s0, s1, s2, s3, s4, sem):
    cps = []

    def out(src, dst, n=1):
        rows = src.shape[0] // n
        for k in range(n):
            c = pltpu.make_async_copy(src.at[pl.ds(k * rows, rows)], dst.at[pl.ds(k * rows, rows)], sem.at[len(cps)])
            c.start()
            cps.append(c)

    out(dn_ref, gwdn_ref, 4)
    out(up_ref, gwup_ref, 4)
    out(yi_ref, y_ref)
    for i, (sv, r) in enumerate(((s0, gbd_ref), (s1, gbup_ref), (s2, gl2_ref), (s3, bl2_ref), (s4, gbo_ref))):
        sv[...] = vec_ref[i, :]
        out(sv, r)
    ones = jnp.ones((8, S), BF)
    for h in range(HL):
        for e in range(3):
            s_gb[e, h:h + 1, :] = dot(ones, gqkv_ref[head_rows(h, e), :], 1, 1)[0:1, :]
    out(s_gb, gbqkv_ref)
    hv = h_ref[...]
    s_out[...] = dot(ctx_ref[...], gmid_ref[...], 1, 0).astype(BF)
    out(s_out, gwout_ref)
    for n in range(HL):
        rows = slice(n * 3 * HD, (n + 1) * 3 * HD)
        s_qkv[rows, :] = dot(gqkv_ref[rows, :], hv, 1, 0).astype(BF)
        out(s_qkv.at[rows], gwqkv_ref.at[rows])
    for c in cps:
        c.wait()


def last_kernel(mine_ref, xh_ref, gm_ref, rs_ref, g1_ref, rc_ref, ln_ref, gx_ref, gl1_ref, bl1_ref):
    gh = (mine_ref[...].astype(F32) + rc_ref[0:SL, :].astype(F32)).astype(BF).astype(F32)
    xh = xh_ref[...]
    dxh = gh * g1_ref[...]
    m1 = jnp.mean(dxh, axis=-1, keepdims=True)
    m2 = jnp.mean(dxh * xh, axis=-1, keepdims=True)
    gx_ref[...] = (gm_ref[...] + rs_ref[:, 0:1] * (dxh - m1 - xh * m2)).astype(BF)
    lc = rc_ref[SL:SL + 8, :].astype(F32)
    ln = ln_ref[...] + (lc[0:2, :] + lc[2:4, :] + lc[4:6, :])
    gl1_ref[...] = ln[0, :]
    bl1_ref[...] = ln[1, :]


def solution(mesh):
    VM = pl.BlockSpec(memory_space=pltpu.VMEM)
    ANY = pl.BlockSpec(memory_space=pltpu.HBM)

    def sds(shape, dt):
        return jax.ShapeDtypeStruct(shape, dt)

    def local_step(x, g1, be1, w_qkv, b_qkv, w_out, b_out, g2, be2, w_up, b_up, w_down, b_down, grad_y):
        wq = jnp.transpose(w_qkv, (1, 2, 3, 0)).reshape(3 * HL * HD, D)
        bq = jnp.transpose(b_qkv, (1, 0, 2))
        part = pltpu.VMEM((S, HW), BF)
        vec1 = sds((D,), F32)
        mids = pl.pallas_call(
            block_kernel,
            out_shape=(pltpu.VMEM((SL, D), BF), pltpu.VMEM((8, D), F32), pltpu.VMEM((D, FL), BF), pltpu.VMEM((FL, D), BF),
                       pltpu.VMEM((3 * HL * HD, S), BF), pltpu.VMEM((S, D), BF), pltpu.VMEM((HL * HD, S), BF), pltpu.VMEM((S, D), BF),
                       pltpu.VMEM((SL, D), BF), pltpu.VMEM((SL, D), F32), pltpu.VMEM((SL, D), F32), pltpu.VMEM((SL, 128), F32),
                       pltpu.VMEM((1, D), F32), sds((SL + 8, D), BF), pltpu.VMEM((2, D), F32)),
            in_specs=[ANY] * 14,
            out_specs=(VM,) * 15,
            scratch_shapes=[
                pltpu.VMEM((3 * HL * HD, D), BF), pltpu.VMEM((2, HL * HD, HW), BF), pltpu.VMEM((S, D), F32), pltpu.VMEM((S, D), F32),
                pltpu.VMEM((S, D), F32), pltpu.VMEM((S, D), F32), pltpu.VMEM((S, 128), F32), pltpu.VMEM((HL, S, S), F32),
                pltpu.VMEM((3 * HL * HD, S), BF), pltpu.VMEM((8, D), F32), pltpu.VMEM((TP, SL, D), BF),
                pltpu.VMEM((D, FL), BF), pltpu.VMEM((FL, D), BF), pltpu.VMEM((TP, SL, D), BF), pltpu.VMEM((TP, SL, D), BF),
                pltpu.VMEM((3 * HL * HD, S), F32), *[part] * 12,
                pltpu.VMEM((S, FL), BF), pltpu.VMEM((S, D), BF), pltpu.VMEM((S, FL), BF), pltpu.VMEM((S, FL), BF), pltpu.VMEM((S, D), BF),
                pltpu.VMEM((3, HL, HD), F32), *[pltpu.VMEM((D,), F32) for _ in range(7)],
                pltpu.VMEM((2, TP, SL, HW), BF), pltpu.VMEM((2, SL, D), BF), pltpu.VMEM((SL, D), BF), pltpu.VMEM((SL, D), BF),
                pltpu.VMEM((2, 2, SL, HW), BF), pltpu.VMEM((2, 2, D), F32),
                pltpu.SemaphoreType.DMA((9,)), pltpu.SemaphoreType.DMA((N_SEND,)), pltpu.SemaphoreType.DMA((N_SEND,)),
                pltpu.SemaphoreType.DMA((10,)),
            ],
            compiler_params=pltpu.CompilerParams(collective_id=0, has_side_effects=True, vmem_limit_bytes=VMEM_A),
            name='block',
        )(*(pltpu.with_memory_space_constraint(v, pltpu.HBM) for v in (
            x.reshape(SL, D), grad_y.reshape(SL, D), g1, be1, g2, be2, b_out, b_down, bq, b_up, wq, w_out, w_up, w_down)))
        mine, xh, gm, rs, g1v, r_hs, ln_hs = mids[8:]
        across = [(i, TP - 1 - i) for i in range(TP)]
        r_cr = lax.ppermute(r_hs, 'tp', across)
        y, gwqkv, gbqkv, gwout, gbo, gl2, bl2, gwup, gbup, gwdn, gbd = pl.pallas_call(
            write_kernel,
            out_shape=(sds((SL, D), BF), sds((3 * HL * HD, D), BF), sds((3, HL, HD), F32), sds((HL * HD, D), BF), vec1, vec1, vec1,
                       sds((D, FL), BF), vec1, sds((FL, D), BF), vec1),
            in_specs=[VM] * 8,
            out_specs=(ANY,) * 11,
            scratch_shapes=[pltpu.VMEM((3 * HL * HD, D), BF), pltpu.VMEM((HL * HD, D), BF), pltpu.VMEM((3, HL, HD), F32),
                            *[pltpu.VMEM((D,), F32) for _ in range(5)], pltpu.SemaphoreType.DMA((20,))],
            compiler_params=pltpu.CompilerParams(vmem_limit_bytes=VMEM_B),
            cost_estimate=pl.CostEstimate(flops=600_000_000, bytes_accessed=14_200_000, transcendentals=0),
            name='write',
        )(*mids[:8])
        gx, gl1, bl1 = pl.pallas_call(
            last_kernel,
            out_shape=(sds((SL, D), BF), vec1, vec1),
            in_specs=[VM] * 7,
            out_specs=(VM,) * 3,
            compiler_params=pltpu.CompilerParams(vmem_limit_bytes=VMEM_C),
            name='last',
        )(mine, xh, gm, rs, g1v, r_cr, ln_hs)
        gwqkv = jnp.transpose(gwqkv.reshape(HL, 3, HD, D), (3, 0, 1, 2))
        gbqkv = jnp.transpose(gbqkv, (1, 0, 2))
        return (y.reshape(1, SL, D), gx.reshape(1, SL, D), gl1, bl1, gwqkv, gbqkv, gwout, gbo, gl2, bl2, gwup, gbup, gwdn, gbd)

    row_spec = P('dp', 'tp', None)
    in_specs = (row_spec, P(), P(), P(None, 'tp', None, None), P('tp', None, None), P('tp', None), P(), P(), P(),
                P(None, 'tp'), P('tp'), P('tp', None), P(), row_spec)
    out_specs = (row_spec, row_spec, P('dp'), P('dp'), P('dp', 'tp', None, None), P(('dp', 'tp'), None, None),
                 P(('dp', 'tp'), None), P('dp'), P('dp'), P('dp'), P('dp', 'tp'), P(('dp', 'tp')), P(('dp', 'tp'), None), P('dp'))
    return jax.shard_map(local_step, mesh=mesh, in_specs=in_specs, out_specs=out_specs, check_vma=False)
```

```python
import functools
import math

import jax
import jax.numpy as jnp
from jax import lax
from jax.experimental import pallas as pl
from jax.experimental.pallas import tpu as pltpu
from jax.sharding import PartitionSpec as P

EPS = 1e-5
MASK_VALUE = -1e30
BF = jnp.bfloat16
F32 = jnp.float32
MESH = pl.DeviceIdType.MESH

D = 1536
S = 96
SL = 24
TP = 4
HL = 4
HD = 96
FL = 1536
CW = 256
NCH = D // CW
HCH = NCH // 2
HW = D // 2
CUT = (0, 256, 512, 640, 768)
NCUT = len(CUT) - 1


def alibi_slopes(n_heads):
    closest = 2 ** int(math.floor(math.log2(n_heads)))
    base_ratio = 2.0 ** (-8.0 / closest)
    extra_ratio = 2.0 ** (-4.0 / closest)
    remaining = min(closest, n_heads - closest)
    slopes = [base_ratio ** (i + 1) for i in range(closest)]
    return slopes + [extra_ratio ** (2 * i + 1) for i in range(remaining)]


def dot(a, b, ca, cb):
    return lax.dot_general(a, b, (((ca,), (cb,)), ((), ())), preferred_element_type=F32)


def gelu_parts(u):
    k = math.sqrt(2.0 / math.pi)
    u2 = u * u
    th = jnp.tanh(u * (k + (k * 0.044715) * u2))
    half = 0.5 + 0.5 * th
    val = u * half
    return val, half + val * (1.0 - th) * (k + (3.0 * 0.044715 * k) * u2)


def rows_stats(v):
    mean = jnp.mean(v, axis=-1, keepdims=True)
    cen = v - mean
    var = jnp.mean(cen * cen, axis=-1, keepdims=True)
    return cen, lax.rsqrt(var + EPS)


def places():
    t = lax.axis_index('tp')
    core = t % 2
    pt = t + 1 - 2 * core
    ct = TP - 1 - t
    qt = TP - 1 - pt
    half = (core + t // 2) % 2
    return t, pt, ct, qt, half


def sender(ssem, rsem):
    started = []

    def send(src, dst, dev):
        i = len(started)
        c = pltpu.make_async_remote_copy(src_ref=src, dst_ref=dst, send_sem=ssem.at[i], recv_sem=rsem.at[i],
                                         device_id={'tp': dev}, device_id_type=MESH)
        c.start()
        started.append(c)
        return c

    return send, started


def head_rows(h, e):
    return slice((h * 3 + e) * HD, (h * 3 + e + 1) * HD)


def row_blocks(buf, cols, v):
    for i in range(TP):
        buf[i, :, cols] = v[i * SL:(i + 1) * SL, :].astype(BF)


def block_kernel(x_hbm, gy_hbm, g1_hbm, be1_hbm, g2_hbm, be2_hbm, bo_hbm, bd_hbm, bqkv_hbm, bup_hbm,
                 wqkv_hbm, wout_hbm, wup_hbm, wdn_hbm,
                 y_ref, vec_ref, gwup_ref, gwdn_ref, gqkv_ref, h_ref, ctx_ref, gmid_ref, mine_ref, xh_ref, gm_ref, rs_ref, g1_out, r_hs, ln_hs,
                 wqkv, wout, xf, gm_f, gg_f, xhat, rstd_s, probs, qkvT, par, mp,
                 wup, wdn, xg, gyg, biasT, a_ps, a_pr, a_hs, a_hr, a_cr, a_fr, b_ps, b_pr, b_hs, b_hr, b_cr, b_fr,
                 gact, g_ref, gpre_ref, act_ref, gyf_ref, bqkv_ref, g1_in, be1_in, g2_in, be2_in, bo_in, bd_in, bup_in,
                 rp, m_pr, m_hs, m_cr, r_pr, ln_x, xh2, rstd2,
                 wsem, ssem, rsem, isem):
    t, pt, ct, qt, half = places()
    send, started = sender(ssem, rsem)

    in_x = pltpu.make_async_copy(x_hbm, xg.at[t], isem.at[0])
    in_gy = pltpu.make_async_copy(gy_hbm, gyg.at[t], isem.at[1])
    in_b = pltpu.make_async_copy(bqkv_hbm, bqkv_ref, isem.at[2])
    small = ((g1_hbm, g1_in), (be1_hbm, be1_in), (g2_hbm, g2_in), (be2_hbm, be2_in), (bo_hbm, bo_in), (bd_hbm, bd_in), (bup_hbm, bup_in))
    in_p = [pltpu.make_async_copy(a, b, isem.at[3 + i]) for i, (a, b) in enumerate(small)]
    for c in (in_x, in_gy, in_b, *in_p):
        c.start()
    w_cps = {}
    w_cps['qkv'] = [pltpu.make_async_copy(wqkv_hbm, wqkv, wsem.at[0])]
    w_cps['out'] = [pltpu.make_async_copy(wout_hbm.at[:, pl.ds(k * HW, HW)], wout.at[k], wsem.at[1 + k]) for k in range(2)]
    w_cps['dn'] = [pltpu.make_async_copy(wdn_hbm, wdn, wsem.at[7])]
    w_cps['up'] = [pltpu.make_async_copy(wup_hbm, wup, wsem.at[8])]

    barrier = pltpu.get_barrier_semaphore()
    for dev in (pt, ct, qt):
        pl.semaphore_signal(barrier, inc=1, device_id={'tp': dev}, device_id_type=MESH)
    for name in ('qkv', 'out', 'dn', 'up'):
        for c in w_cps[name]:
            c.start()
    pl.semaphore_wait(barrier, 3)

    in_x.wait()
    x_c = send(xg.at[t], xg.at[t], ct)
    x_p = send(xg.at[t], xg.at[t], pt)

    for c in (in_b, *in_p):
        c.wait()
    for i, r in enumerate((g1_in, be1_in, g2_in, be2_in, bo_in, bd_in, bup_in)):
        par[i, :] = r[...]
    g1_ref, be1_ref, g2_ref, be2_ref, bo_ref, bd_ref, bup_ref = (par.at[i:i + 1] for i in range(7))

    for h in range(HL):
        for e in range(3):
            row = jnp.broadcast_to(bqkv_ref[e, h:h + 1, :], (S, HD))
            biasT[pl.ds((h * 3 + e) * HD, HD), :] = row.T

    x_c.wait_recv()
    x_f = send(xg.at[ct], xg.at[ct], pt)
    in_gy.wait()
    y_c = send(gyg.at[t], gyg.at[t], ct)
    y_p = send(gyg.at[t], gyg.at[t], pt)
    x_p.wait_recv()
    x_f.wait_recv()

    for i in range(TP):
        xf[pl.ds(i * SL, SL), :] = xg[i].astype(F32)
    for r in range(0, S, 32):
        cen, rstd = rows_stats(xf[r:r + 32, :])
        xh = cen * rstd
        xhat[r:r + 32, :] = xh
        rstd_s[r:r + 32, :] = jnp.broadcast_to(rstd, (32, 128))
        h_ref[r:r + 32, :] = (xh * g1_ref[...] + be1_ref[...]).astype(BF)

    w_cps['qkv'][0].wait()
    hv = h_ref[...]
    for h in range(HL):
        rows = slice(h * 3 * HD, (h + 1) * 3 * HD)
        qkvT[rows, :] = (dot(wqkv[rows, :], hv, 1, 1) + biasT[rows, :]).astype(BF)

    scale = HD ** -0.5
    slopes = alibi_slopes(HL * TP)
    j_pos = lax.broadcasted_iota(jnp.int32, (S, S), 0)
    i_pos = lax.broadcasted_iota(jnp.int32, (S, S), 1)
    causal = j_pos <= i_pos
    j_f = j_pos.astype(F32)

    def head(h, e):
        return qkvT[head_rows(h, e), :]

    for h in range(HL):
        slope = jnp.where(t == 0, slopes[h], jnp.where(t == 1, slopes[HL + h], jnp.where(t == 2, slopes[2 * HL + h], slopes[3 * HL + h]))).astype(F32)
        s = dot(head(h, 1), head(h, 0), 0, 0) * scale + slope * j_f
        s = jnp.where(causal, s, MASK_VALUE)
        p = jnp.exp(s - jnp.max(s, axis=0, keepdims=True))
        p = p / jnp.sum(p, axis=0, keepdims=True)
        probs[h] = p
        ctx_ref[h * HD:(h + 1) * HD, :] = dot(head(h, 2), p.astype(BF), 1, 0).astype(BF)

    def exchange(part, groups, ps, pr, hs, hr, cr, fr):
        firsts = []
        for k0, k1 in groups:
            cols = slice(CUT[k0], CUT[k1])
            ps[:, cols] = part(1 - half, CUT[k0], CUT[k1]).astype(BF)
            firsts.append(send(ps.at[:, cols], pr.at[:, cols], pt))
        outs = []
        for (k0, k1), first in zip(groups, firsts):
            cols = slice(CUT[k0], CUT[k1])
            ours = part(half, CUT[k0], CUT[k1])
            first.wait_recv()
            hs[:, cols] = (ours + pr[:, cols].astype(F32)).astype(BF)
            for k in range(k0, k1):
                c = slice(CUT[k], CUT[k + 1])
                outs.append([send(hs.at[:, c], cr.at[:, c], ct)])
                if k == NCUT - 1:
                    outs[-1].append(send(hs.at[:, c], fr.at[:, c], qt))
        local = send(hs, hr, pt)
        return outs, local

    def arrived(out, k, hs, cr, fr, put):
        c = slice(CUT[k], CUT[k + 1])
        out[0].wait_recv()
        if k < NCUT - 1:
            out.append(send(cr.at[:, c], fr.at[:, c], pt))
        put(half * HW + CUT[k], CUT[k + 1] - CUT[k], (hs[:, c].astype(F32) + cr[:, c].astype(F32)).astype(BF).astype(F32))

    def passed_on(outs, local, hr, fr, put):
        local.wait_recv()
        for k, out in enumerate(outs):
            c = slice(CUT[k], CUT[k + 1])
            out[1].wait_recv()
            put((1 - half) * HW + CUT[k], CUT[k + 1] - CUT[k], (hr[:, c].astype(F32) + fr[:, c].astype(F32)).astype(BF).astype(F32))

    for c in w_cps['out']:
        c.wait()
    ctxT = ctx_ref[...]
    a_outs, a_local = exchange(lambda hh, c0, c1: dot(ctxT, wout[hh, :, c0:c1], 0, 0), ((0, NCUT),), a_ps, a_pr, a_hs, a_hr, a_cr, a_fr)

    y_c.wait_recv()
    y_f = send(gyg.at[ct], gyg.at[ct], pt)
    y_p.wait_recv()
    y_f.wait_recv()
    for i in range(TP):
        gm_f[pl.ds(i * SL, SL), :] = gyg[i].astype(F32)
    for r in range(0, S, 32):
        gyf_ref[r:r + 32, :] = gm_f[r:r + 32, :].astype(BF)
    w_cps['dn'][0].wait()
    gyv = gyf_ref[...]
    for n in range(NCH):
        gact[:, n * CW:(n + 1) * CW] = dot(gyv, wdn[n * CW:(n + 1) * CW, :], 1, 1).astype(BF)
    vec_ref[0:1, :] = jnp.sum(gm_f[...], axis=0, keepdims=True)

    def put_x(start, width, val):
        cols = pl.ds(pl.multiple_of(start, 128), width)
        xf[:, cols] = xf[:, cols] + val + bo_ref[:, cols]

    for k, out in enumerate(a_outs):
        arrived(out, k, a_hs, a_cr, a_fr, put_x)
    passed_on(a_outs, a_local, a_hr, a_fr, put_x)

    for r in range(0, S, 32):
        cen, rstd = rows_stats(xf[r:r + 32, :])
        xh = cen * rstd
        xh2[r:r + 32, :] = xh
        rstd2[r:r + 32, :] = jnp.broadcast_to(rstd, (32, 128))
        g_ref[r:r + 32, :] = (xh * g2_ref[...] + be2_ref[...]).astype(BF)

    w_cps['up'][0].wait()
    gv = g_ref[...]
    for n in range(NCH):
        cols = slice(n * CW, (n + 1) * CW)
        pre = dot(gv, wup[:, cols], 1, 0) + bup_ref[:, cols]
        val, der = gelu_parts(pre)
        act_ref[:, cols] = val.astype(BF)
        gp = gact[:, cols].astype(F32) * der
        vec_ref[1:2, cols] = jnp.sum(gp, axis=0, keepdims=True)
        gpre_ref[:, cols] = gp.astype(BF)

    gprev = gpre_ref[...]

    def part_g(hh, c0, c1):
        return dot(gprev, wup[pl.ds(pl.multiple_of(hh * HW + c0, CW), c1 - c0), :], 1, 1)

    g_outs, g_local = exchange(part_g, ((0, 1), (1, NCUT)), b_ps, b_pr, b_hs, b_hr, b_cr, b_fr)

    actv = act_ref[...]
    for n in range(NCH):
        cols = slice(n * CW, (n + 1) * CW)
        row_blocks(mp, cols, dot(actv, wdn[:, cols], 1, 0))
    m_first = (send(mp.at[qt], m_pr.at[1], pt), send(mp.at[pt], m_pr.at[0], pt))
    for n in range(NCH):
        gwdn_ref[n * CW:(n + 1) * CW, :] = dot(act_ref[:, n * CW:(n + 1) * CW], gyv, 0, 0).astype(BF)
    def put_g(start, width, val):
        gg_f[:, pl.ds(pl.multiple_of(start, 128), width)] = val

    for k in range(HCH):
        arrived(g_outs[k], k, b_hs, b_cr, b_fr, put_g)
        for n in range(2 * k, 2 * k + 2):
            gwup_ref[n * CW:(n + 1) * CW, :] = dot(g_ref[:, n * CW:(n + 1) * CW], gprev, 0, 0).astype(BF)
    arrived(g_outs[-1], NCUT - 1, b_hs, b_cr, b_fr, put_g)

    m_first[0].wait_recv()
    m_hs[...] = (mp[ct].astype(F32) + m_pr[1].astype(F32)).astype(BF)
    m_out = send(m_hs, m_cr, ct)

    passed_on(g_outs, g_local, b_hr, b_fr, put_g)

    for r in range(0, S, 32):
        xh = xh2[r:r + 32, :]
        dxh = gg_f[r:r + 32, :] * g2_ref[...]
        m1 = jnp.mean(dxh, axis=-1, keepdims=True)
        m2 = jnp.mean(dxh * xh, axis=-1, keepdims=True)
        gm = gm_f[r:r + 32, :] + rstd2[r:r + 32, 0:1] * (dxh - m1 - xh * m2)
        gm_f[r:r + 32, :] = gm
        gmid_ref[r:r + 32, :] = gm.astype(BF)

    gmv = gmid_ref[...]
    gctxT = (dot(wout[0], gmv[:, :HW], 1, 1) + dot(wout[1], gmv[:, HW:], 1, 1)).astype(BF)
    heads = range(HL)
    gos = [gctxT[h * HD:(h + 1) * HD, :] for h in heads]
    gps = [dot(head(h, 2), gos[h], 0, 0).astype(BF).astype(F32) for h in heads]
    gvs = [dot(gos[h], probs[h].astype(BF), 1, 1).astype(BF) for h in heads]
    gss = [(probs[h] * (gps[h] - jnp.sum(gps[h] * probs[h], axis=0, keepdims=True))).astype(BF) for h in heads]
    gqs = [(dot(head(h, 1), gss[h], 1, 0) * scale).astype(BF) for h in heads]
    gks = [(dot(head(h, 0), gss[h], 1, 1) * scale).astype(BF) for h in heads]
    for h in heads:
        for e, val in enumerate((gqs[h], gks[h], gvs[h])):
            gqkv_ref[head_rows(h, e), :] = val

    gqv = gqkv_ref[...]
    r_first = []
    for k in range(2):
        row_blocks(rp.at[k], slice(0, HW), dot(gqv, wqkv[:, k * HW:(k + 1) * HW], 0, 0))
        r_first.append((send(rp.at[k, qt], r_pr.at[k, 1], pt), send(rp.at[k, pt], r_pr.at[k, 0], pt)))

    ln_s, ln_pr = ln_x.at[0], ln_x.at[1]
    for k in range(2):
        cols = slice(k * HW, (k + 1) * HW)
        gg1 = jnp.zeros((1, HW), F32)
        gb1 = jnp.zeros((1, HW), F32)
        for i in range(TP):
            v = rp[k, i].astype(F32)
            gg1 = gg1 + jnp.sum(v * xhat[i * SL:(i + 1) * SL, cols], axis=0, keepdims=True)
            gb1 = gb1 + jnp.sum(v, axis=0, keepdims=True)
        ln_s[0:1, cols] = gg1
        ln_s[1:2, cols] = gb1
    l_first = send(ln_s, ln_pr, pt)

    vec_ref[2:3, :] = jnp.sum(gg_f[...] * xh2[...], axis=0, keepdims=True)
    vec_ref[3:4, :] = jnp.sum(gg_f[...], axis=0, keepdims=True)
    vec_ref[4:5, :] = jnp.sum(gm_f[...], axis=0, keepdims=True)

    own = pl.ds(pl.multiple_of(t * SL, 8), SL)
    xh_ref[...] = xhat[own, :]
    gm_ref[...] = gm_f[own, :]
    rs_ref[...] = rstd_s[own, :]
    g1_out[...] = par[0:1, :]

    for k in range(2):
        cols = slice(k * HW, (k + 1) * HW)
        r_first[k][0].wait_recv()
        r_hs[0:SL, cols] = (rp[k, ct].astype(F32) + r_pr[k, 1].astype(F32)).astype(BF)
        r_first[k][1].wait_recv()
        mine_ref[:, cols] = (rp[k, t].astype(F32) + r_pr[k, 0].astype(F32)).astype(BF)
    l_first.wait_recv()
    ln = ln_s[...] + ln_pr[...]
    ln_hs[...] = ln
    ln_rows = []
    for _ in range(3):
        ln_rows.append(ln.astype(BF).astype(F32))
        ln = ln - ln_rows[-1]
    r_hs[SL:SL + 8, :] = jnp.concatenate(ln_rows + [jnp.zeros((2, D), F32)], axis=0).astype(BF)
    m_first[1].wait_recv()
    m_out.wait_recv()
    m_sum = (mp[t].astype(F32) + m_pr[0].astype(F32)).astype(BF).astype(F32) + m_cr[...].astype(F32)
    y_ref[...] = (xf[own, :] + m_sum.astype(BF).astype(F32) + bd_ref[...]).astype(BF)
    for c in started:
        c.wait_send()


N_SEND = 6 + 2 * (2 + 4 + 1 + 1 + 3) + 3 + 4 + 1
VMEM_A = 36 * 2**20
VMEM_B = 8 * 2**20
VMEM_C = 4 * 2**20


def write_kernel(yi_ref, vec_ref, up_ref, dn_ref, gqkv_ref, h_ref, ctx_ref, gmid_ref,
                 y_ref, gwqkv_ref, gbqkv_ref, gwout_ref, gbo_ref, gl2_ref, bl2_ref, gwup_ref, gbup_ref, gwdn_ref, gbd_ref,
                 s_qkv, s_out, s_gb, s0, s1, s2, s3, s4, sem):
    cps = []

    def out(src, dst, n=1):
        rows = src.shape[0] // n
        for k in range(n):
            c = pltpu.make_async_copy(src.at[pl.ds(k * rows, rows)], dst.at[pl.ds(k * rows, rows)], sem.at[len(cps)])
            c.start()
            cps.append(c)

    out(dn_ref, gwdn_ref, 4)
    out(up_ref, gwup_ref, 4)
    out(yi_ref, y_ref)
    for i, (sv, r) in enumerate(((s0, gbd_ref), (s1, gbup_ref), (s2, gl2_ref), (s3, bl2_ref), (s4, gbo_ref))):
        sv[...] = vec_ref[i, :]
        out(sv, r)
    ones = jnp.ones((8, S), BF)
    for h in range(HL):
        for e in range(3):
            s_gb[e, h:h + 1, :] = dot(ones, gqkv_ref[head_rows(h, e), :], 1, 1)[0:1, :]
    out(s_gb, gbqkv_ref)
    hv = h_ref[...]
    s_out[...] = dot(ctx_ref[...], gmid_ref[...], 1, 0).astype(BF)
    out(s_out, gwout_ref)
    for n in range(HL):
        rows = slice(n * 3 * HD, (n + 1) * 3 * HD)
        s_qkv[rows, :] = dot(gqkv_ref[rows, :], hv, 1, 0).astype(BF)
        out(s_qkv.at[rows], gwqkv_ref.at[rows])
    for c in cps:
        c.wait()


def last_kernel(mine_ref, xh_ref, gm_ref, rs_ref, g1_ref, rc_ref, ln_ref, gx_ref, gl1_ref, bl1_ref):
    gh = (mine_ref[...].astype(F32) + rc_ref[0:SL, :].astype(F32)).astype(BF).astype(F32)
    xh = xh_ref[...]
    dxh = gh * g1_ref[...]
    m1 = jnp.mean(dxh, axis=-1, keepdims=True)
    m2 = jnp.mean(dxh * xh, axis=-1, keepdims=True)
    gx_ref[...] = (gm_ref[...] + rs_ref[:, 0:1] * (dxh - m1 - xh * m2)).astype(BF)
    lc = rc_ref[SL:SL + 8, :].astype(F32)
    ln = ln_ref[...] + (lc[0:2, :] + lc[2:4, :] + lc[4:6, :])
    gl1_ref[...] = ln[0, :]
    bl1_ref[...] = ln[1, :]


def solution(mesh):
    VM = pl.BlockSpec(memory_space=pltpu.VMEM)
    ANY = pl.BlockSpec(memory_space=pltpu.HBM)

    def sds(shape, dt):
        return jax.ShapeDtypeStruct(shape, dt)

    def local_step(x, g1, be1, w_qkv, b_qkv, w_out, b_out, g2, be2, w_up, b_up, w_down, b_down, grad_y):
        wq = jnp.transpose(w_qkv, (1, 2, 3, 0)).reshape(3 * HL * HD, D)
        bq = jnp.transpose(b_qkv, (1, 0, 2))
        part = pltpu.VMEM((S, HW), BF)
        vec1 = sds((D,), F32)
        mids = pl.pallas_call(
            block_kernel,
            out_shape=(pltpu.VMEM((SL, D), BF), pltpu.VMEM((8, D), F32), pltpu.VMEM((D, FL), BF), pltpu.VMEM((FL, D), BF),
                       pltpu.VMEM((3 * HL * HD, S), BF), pltpu.VMEM((S, D), BF), pltpu.VMEM((HL * HD, S), BF), pltpu.VMEM((S, D), BF),
                       pltpu.VMEM((SL, D), BF), pltpu.VMEM((SL, D), F32), pltpu.VMEM((SL, D), F32), pltpu.VMEM((SL, 128), F32),
                       pltpu.VMEM((1, D), F32), sds((SL + 8, D), BF), pltpu.VMEM((2, D), F32)),
            in_specs=[ANY] * 14,
            out_specs=(VM,) * 15,
            scratch_shapes=[
                pltpu.VMEM((3 * HL * HD, D), BF), pltpu.VMEM((2, HL * HD, HW), BF), pltpu.VMEM((S, D), F32), pltpu.VMEM((S, D), F32),
                pltpu.VMEM((S, D), F32), pltpu.VMEM((S, D), F32), pltpu.VMEM((S, 128), F32), pltpu.VMEM((HL, S, S), F32),
                pltpu.VMEM((3 * HL * HD, S), BF), pltpu.VMEM((8, D), F32), pltpu.VMEM((TP, SL, D), BF),
                pltpu.VMEM((D, FL), BF), pltpu.VMEM((FL, D), BF), pltpu.VMEM((TP, SL, D), BF), pltpu.VMEM((TP, SL, D), BF),
                pltpu.VMEM((3 * HL * HD, S), F32), *[part] * 12,
                pltpu.VMEM((S, FL), BF), pltpu.VMEM((S, D), BF), pltpu.VMEM((S, FL), BF), pltpu.VMEM((S, FL), BF), pltpu.VMEM((S, D), BF),
                pltpu.VMEM((3, HL, HD), F32), *[pltpu.VMEM((D,), F32) for _ in range(7)],
                pltpu.VMEM((2, TP, SL, HW), BF), pltpu.VMEM((2, SL, D), BF), pltpu.VMEM((SL, D), BF), pltpu.VMEM((SL, D), BF),
                pltpu.VMEM((2, 2, SL, HW), BF), pltpu.VMEM((2, 2, D), F32), pltpu.VMEM((S, D), F32), pltpu.VMEM((S, 128), F32),
                pltpu.SemaphoreType.DMA((9,)), pltpu.SemaphoreType.DMA((N_SEND,)), pltpu.SemaphoreType.DMA((N_SEND,)),
                pltpu.SemaphoreType.DMA((10,)),
            ],
            compiler_params=pltpu.CompilerParams(collective_id=0, has_side_effects=True, vmem_limit_bytes=VMEM_A),
            name='block',
        )(*(pltpu.with_memory_space_constraint(v, pltpu.HBM) for v in (
            x.reshape(SL, D), grad_y.reshape(SL, D), g1, be1, g2, be2, b_out, b_down, bq, b_up, wq, w_out, w_up, w_down)))
        mine, xh, gm, rs, g1v, r_hs, ln_hs = mids[8:]
        across = [(i, TP - 1 - i) for i in range(TP)]
        r_cr = lax.ppermute(r_hs, 'tp', across)
        y, gwqkv, gbqkv, gwout, gbo, gl2, bl2, gwup, gbup, gwdn, gbd = pl.pallas_call(
            write_kernel,
            out_shape=(sds((SL, D), BF), sds((3 * HL * HD, D), BF), sds((3, HL, HD), F32), sds((HL * HD, D), BF), vec1, vec1, vec1,
                       sds((D, FL), BF), vec1, sds((FL, D), BF), vec1),
            in_specs=[VM] * 8,
            out_specs=(ANY,) * 11,
            scratch_shapes=[pltpu.VMEM((3 * HL * HD, D), BF), pltpu.VMEM((HL * HD, D), BF), pltpu.VMEM((3, HL, HD), F32),
                            *[pltpu.VMEM((D,), F32) for _ in range(5)], pltpu.SemaphoreType.DMA((20,))],
            compiler_params=pltpu.CompilerParams(vmem_limit_bytes=VMEM_B),
            cost_estimate=pl.CostEstimate(flops=600_000_000, bytes_accessed=14_200_000, transcendentals=0),
            name='write',
        )(*mids[:8])
        gx, gl1, bl1 = pl.pallas_call(
            last_kernel,
            out_shape=(sds((SL, D), BF), vec1, vec1),
            in_specs=[VM] * 7,
            out_specs=(VM,) * 3,
            compiler_params=pltpu.CompilerParams(vmem_limit_bytes=VMEM_C),
            name='last',
        )(mine, xh, gm, rs, g1v, r_cr, ln_hs)
        gwqkv = jnp.transpose(gwqkv.reshape(HL, 3, HD, D), (3, 0, 1, 2))
        gbqkv = jnp.transpose(gbqkv, (1, 0, 2))
        return (y.reshape(1, SL, D), gx.reshape(1, SL, D), gl1, bl1, gwqkv, gbqkv, gwout, gbo, gl2, bl2, gwup, gbup, gwdn, gbd)

    row_spec = P('dp', 'tp', None)
    in_specs = (row_spec, P(), P(), P(None, 'tp', None, None), P('tp', None, None), P('tp', None), P(), P(), P(),
                P(None, 'tp'), P('tp'), P('tp', None), P(), row_spec)
    out_specs = (row_spec, row_spec, P('dp'), P('dp'), P('dp', 'tp', None, None), P(('dp', 'tp'), None, None),
                 P(('dp', 'tp'), None), P('dp'), P('dp'), P('dp'), P('dp', 'tp'), P(('dp', 'tp')), P(('dp', 'tp'), None), P('dp'))
    return jax.shard_map(local_step, mesh=mesh, in_specs=in_specs, out_specs=out_specs, check_vma=False)
```

```python
import functools
import math

import jax
import jax.numpy as jnp
from jax import lax
from jax.experimental import pallas as pl
from jax.experimental.pallas import tpu as pltpu
from jax.sharding import PartitionSpec as P

EPS = 1e-5
MASK_VALUE = -1e30
BF = jnp.bfloat16
F32 = jnp.float32
MESH = pl.DeviceIdType.MESH

D = 1536
S = 96
SL = 24
TP = 4
HL = 4
HD = 96
FL = 1536
CW = 256
NCH = D // CW
HCH = NCH // 2
HW = D // 2
UW = 128
CUT = (128, 384, 640, 768)
NCUT = len(CUT) - 1


def alibi_slopes(n_heads):
    closest = 2 ** int(math.floor(math.log2(n_heads)))
    base_ratio = 2.0 ** (-8.0 / closest)
    extra_ratio = 2.0 ** (-4.0 / closest)
    remaining = min(closest, n_heads - closest)
    slopes = [base_ratio ** (i + 1) for i in range(closest)]
    return slopes + [extra_ratio ** (2 * i + 1) for i in range(remaining)]


def dot(a, b, ca, cb):
    return lax.dot_general(a, b, (((ca,), (cb,)), ((), ())), preferred_element_type=F32)


def gelu_parts(u):
    k = math.sqrt(2.0 / math.pi)
    u2 = u * u
    th = jnp.tanh(u * (k + (k * 0.044715) * u2))
    half = 0.5 + 0.5 * th
    val = u * half
    return val, half + val * (1.0 - th) * (k + (3.0 * 0.044715 * k) * u2)


def rows_stats(v):
    mean = jnp.mean(v, axis=-1, keepdims=True)
    cen = v - mean
    var = jnp.mean(cen * cen, axis=-1, keepdims=True)
    return cen, lax.rsqrt(var + EPS)


def places():
    t = lax.axis_index('tp')
    core = t % 2
    pt = t + 1 - 2 * core
    ct = TP - 1 - t
    qt = TP - 1 - pt
    half = (core + t // 2) % 2
    return t, pt, ct, qt, half


def sender(ssem, rsem):
    started = []

    def send(src, dst, dev):
        i = len(started)
        c = pltpu.make_async_remote_copy(src_ref=src, dst_ref=dst, send_sem=ssem.at[i], recv_sem=rsem.at[i],
                                         device_id={'tp': dev}, device_id_type=MESH)
        c.start()
        started.append(c)
        return c

    return send, started


def columns(start, width):
    return pl.ds(start if isinstance(start, int) else pl.multiple_of(start, 128), width)


def head_rows(h, e):
    return slice((h * 3 + e) * HD, (h * 3 + e + 1) * HD)


def row_blocks(buf, cols, v):
    for i in range(TP):
        buf[i, :, cols] = v[i * SL:(i + 1) * SL, :].astype(BF)


def block_kernel(x_hbm, gy_hbm, g1_hbm, be1_hbm, g2_hbm, be2_hbm, bo_hbm, bd_hbm, bqkv_hbm, bup_hbm,
                 wqkv_hbm, wout_hbm, wup_hbm, wdn_hbm,
                 y_ref, vec_ref, gwup_ref, gwdn_ref, gqkv_ref, h_ref, ctx_ref, gmid_ref, mine_ref, xh_ref, gm_ref, rs_ref, g1_out, r_hs, ln_hs,
                 wqkv, wout, xf, gm_f, gg_f, xhat, rstd_s, probs, qkvT, par, mp,
                 wup, wdn, xg, gyg, biasT, a_ps, a_pr, a_hs, a_hr, a_cr, a_fr, b_ps, b_pr, b_hs, b_hr, b_cr, b_fr,
                 gact, g_ref, gpre_ref, act_ref, gyf_ref, bqkv_ref, g1_in, be1_in, g2_in, be2_in, bo_in, bd_in, bup_in,
                 rp, m_pr, m_hs, m_cr, r_pr, ln_x, xh2, rstd2, a_un, b_un,
                 wsem, ssem, rsem, isem):
    t, pt, ct, qt, half = places()
    send, started = sender(ssem, rsem)

    in_x = pltpu.make_async_copy(x_hbm, xg.at[t], isem.at[0])
    in_gy = pltpu.make_async_copy(gy_hbm, gyg.at[t], isem.at[1])
    in_b = pltpu.make_async_copy(bqkv_hbm, bqkv_ref, isem.at[2])
    small = ((g1_hbm, g1_in), (be1_hbm, be1_in), (g2_hbm, g2_in), (be2_hbm, be2_in), (bo_hbm, bo_in), (bd_hbm, bd_in), (bup_hbm, bup_in))
    in_p = [pltpu.make_async_copy(a, b, isem.at[3 + i]) for i, (a, b) in enumerate(small)]
    for c in (in_x, in_gy, in_b, *in_p):
        c.start()
    w_cps = {}
    w_cps['qkv'] = [pltpu.make_async_copy(wqkv_hbm, wqkv, wsem.at[0])]
    w_cps['out'] = [pltpu.make_async_copy(wout_hbm.at[:, pl.ds(k * HW, HW)], wout.at[k], wsem.at[1 + k]) for k in range(2)]
    w_cps['dn'] = [pltpu.make_async_copy(wdn_hbm, wdn, wsem.at[7])]
    w_cps['up'] = [pltpu.make_async_copy(wup_hbm, wup, wsem.at[8])]

    barrier = pltpu.get_barrier_semaphore()
    for dev in (pt, ct, qt):
        pl.semaphore_signal(barrier, inc=1, device_id={'tp': dev}, device_id_type=MESH)
    for name in ('qkv', 'out', 'dn', 'up'):
        for c in w_cps[name]:
            c.start()
    pl.semaphore_wait(barrier, 3)

    in_x.wait()
    x_c = send(xg.at[t], xg.at[t], ct)
    x_p = send(xg.at[t], xg.at[t], pt)

    for c in (in_b, *in_p):
        c.wait()
    for i, r in enumerate((g1_in, be1_in, g2_in, be2_in, bo_in, bd_in, bup_in)):
        par[i, :] = r[...]
    g1_ref, be1_ref, g2_ref, be2_ref, bo_ref, bd_ref, bup_ref = (par.at[i:i + 1] for i in range(7))

    for h in range(HL):
        for e in range(3):
            row = jnp.broadcast_to(bqkv_ref[e, h:h + 1, :], (S, HD))
            biasT[pl.ds((h * 3 + e) * HD, HD), :] = row.T

    x_c.wait_recv()
    x_f = send(xg.at[ct], xg.at[ct], pt)
    in_gy.wait()
    y_c = send(gyg.at[t], gyg.at[t], ct)
    y_p = send(gyg.at[t], gyg.at[t], pt)
    x_p.wait_recv()
    x_f.wait_recv()

    for i in range(TP):
        xf[pl.ds(i * SL, SL), :] = xg[i].astype(F32)
    for r in range(0, S, 32):
        cen, rstd = rows_stats(xf[r:r + 32, :])
        xh = cen * rstd
        xhat[r:r + 32, :] = xh
        rstd_s[r:r + 32, :] = jnp.broadcast_to(rstd, (32, 128))
        h_ref[r:r + 32, :] = (xh * g1_ref[...] + be1_ref[...]).astype(BF)

    w_cps['qkv'][0].wait()
    hv = h_ref[...]
    for h in range(HL):
        rows = slice(h * 3 * HD, (h + 1) * 3 * HD)
        qkvT[rows, :] = (dot(wqkv[rows, :], hv, 1, 1) + biasT[rows, :]).astype(BF)

    scale = HD ** -0.5
    slopes = alibi_slopes(HL * TP)
    j_pos = lax.broadcasted_iota(jnp.int32, (S, S), 0)
    i_pos = lax.broadcasted_iota(jnp.int32, (S, S), 1)
    causal = j_pos <= i_pos
    j_f = j_pos.astype(F32)

    def head(h, e):
        return qkvT[head_rows(h, e), :]

    for h in range(HL):
        slope = jnp.where(t == 0, slopes[h], jnp.where(t == 1, slopes[HL + h], jnp.where(t == 2, slopes[2 * HL + h], slopes[3 * HL + h]))).astype(F32)
        s = dot(head(h, 1), head(h, 0), 0, 0) * scale + slope * j_f
        s = jnp.where(causal, s, MASK_VALUE)
        p = jnp.exp(s - jnp.max(s, axis=0, keepdims=True))
        p = p / jnp.sum(p, axis=0, keepdims=True)
        probs[h] = p
        ctx_ref[h * HD:(h + 1) * HD, :] = dot(head(h, 2), p.astype(BF), 1, 0).astype(BF)

    def exchange(part, groups, ps, pr, hs, hr, cr, fr, un):
        firsts = []
        for k0, k1 in groups:
            cols = slice(CUT[k0], CUT[k1])
            ps[:, cols] = part(1 - half, CUT[k0], CUT[k1]).astype(BF)
            firsts.append(send(ps.at[:, cols], pr.at[:, cols], pt))
            if k0 == 0:
                for hh in range(2):
                    un[0, hh] = part(hh, 0, UW).astype(BF)
                early = [send(un.at[0], un.at[2], ct), send(un.at[0], un.at[1], pt)]
        outs = []
        for (k0, k1), first in zip(groups, firsts):
            cols = slice(CUT[k0], CUT[k1])
            ours = part(half, CUT[k0], CUT[k1])
            first.wait_recv()
            hs[:, cols] = (ours + pr[:, cols].astype(F32)).astype(BF)
            for k in range(k0, k1):
                c = slice(CUT[k], CUT[k + 1])
                outs.append([send(hs.at[:, c], cr.at[:, c], ct)])
                if k == NCUT - 1:
                    outs[-1].append(send(hs.at[:, c], fr.at[:, c], qt))
        local = send(hs.at[:, UW:], hr.at[:, UW:], pt)
        return outs, local, early

    def early_arrived(early, un):
        early[0].wait_recv()
        early.append(send(un.at[2], un.at[3], pt))

    def early_added(early, un, put):
        early[1].wait_recv()
        early[2].wait_recv()
        for hh in range(2):
            chips = [un[k, hh].astype(F32) + un[k + 1, hh].astype(F32) for k in (0, 2)]
            put(hh * HW, UW, (chips[0] + chips[1]).astype(BF).astype(F32))

    def arrived(out, k, hs, cr, fr, put):
        c = slice(CUT[k], CUT[k + 1])
        out[0].wait_recv()
        if k < NCUT - 1:
            out.append(send(cr.at[:, c], fr.at[:, c], pt))
        put(half * HW + CUT[k], CUT[k + 1] - CUT[k], (hs[:, c].astype(F32) + cr[:, c].astype(F32)).astype(BF).astype(F32))

    def passed_on(outs, local, hr, fr, put):
        local.wait_recv()
        for k, out in enumerate(outs):
            c = slice(CUT[k], CUT[k + 1])
            out[1].wait_recv()
            put((1 - half) * HW + CUT[k], CUT[k + 1] - CUT[k], (hr[:, c].astype(F32) + fr[:, c].astype(F32)).astype(BF).astype(F32))

    for c in w_cps['out']:
        c.wait()
    ctxT = ctx_ref[...]
    a_outs, a_local, a_early = exchange(lambda hh, c0, c1: dot(ctxT, wout[hh, :, c0:c1], 0, 0), ((0, NCUT),), a_ps, a_pr, a_hs, a_hr, a_cr, a_fr, a_un)

    y_c.wait_recv()
    y_f = send(gyg.at[ct], gyg.at[ct], pt)
    y_p.wait_recv()
    y_f.wait_recv()
    for i in range(TP):
        gm_f[pl.ds(i * SL, SL), :] = gyg[i].astype(F32)
    for r in range(0, S, 32):
        gyf_ref[r:r + 32, :] = gm_f[r:r + 32, :].astype(BF)
    w_cps['dn'][0].wait()
    gyv = gyf_ref[...]
    for n in range(NCH):
        gact[:, n * CW:(n + 1) * CW] = dot(gyv, wdn[n * CW:(n + 1) * CW, :], 1, 1).astype(BF)
    vec_ref[0:1, :] = jnp.sum(gm_f[...], axis=0, keepdims=True)

    def put_x(start, width, val):
        cols = columns(start, width)
        xf[:, cols] = xf[:, cols] + val + bo_ref[:, cols]

    early_arrived(a_early, a_un)
    for k, out in enumerate(a_outs):
        arrived(out, k, a_hs, a_cr, a_fr, put_x)
    early_added(a_early, a_un, put_x)
    passed_on(a_outs, a_local, a_hr, a_fr, put_x)

    for r in range(0, S, 32):
        cen, rstd = rows_stats(xf[r:r + 32, :])
        xh = cen * rstd
        xh2[r:r + 32, :] = xh
        rstd2[r:r + 32, :] = jnp.broadcast_to(rstd, (32, 128))
        g_ref[r:r + 32, :] = (xh * g2_ref[...] + be2_ref[...]).astype(BF)

    w_cps['up'][0].wait()
    gv = g_ref[...]
    for n in range(NCH):
        cols = slice(n * CW, (n + 1) * CW)
        pre = dot(gv, wup[:, cols], 1, 0) + bup_ref[:, cols]
        val, der = gelu_parts(pre)
        act_ref[:, cols] = val.astype(BF)
        gp = gact[:, cols].astype(F32) * der
        vec_ref[1:2, cols] = jnp.sum(gp, axis=0, keepdims=True)
        gpre_ref[:, cols] = gp.astype(BF)

    gprev = gpre_ref[...]

    def part_g(hh, c0, c1):
        return dot(gprev, wup[columns(hh * HW + c0, c1 - c0), :], 1, 1)

    g_outs, g_local, g_early = exchange(part_g, ((0, 1), (1, NCUT)), b_ps, b_pr, b_hs, b_hr, b_cr, b_fr, b_un)

    actv = act_ref[...]
    for n in range(NCH):
        cols = slice(n * CW, (n + 1) * CW)
        row_blocks(mp, cols, dot(actv, wdn[:, cols], 1, 0))
    m_first = (send(mp.at[qt], m_pr.at[1], pt), send(mp.at[pt], m_pr.at[0], pt))
    for n in range(NCH):
        gwdn_ref[n * CW:(n + 1) * CW, :] = dot(act_ref[:, n * CW:(n + 1) * CW], gyv, 0, 0).astype(BF)
    def put_g(start, width, val):
        gg_f[:, columns(start, width)] = val

    early_arrived(g_early, b_un)
    for n in range(NCH):
        gwup_ref[n * CW:(n + 1) * CW, :] = dot(g_ref[:, n * CW:(n + 1) * CW], gprev, 0, 0).astype(BF)
        if n % 2:
            arrived(g_outs[n // 2], n // 2, b_hs, b_cr, b_fr, put_g)
    early_added(g_early, b_un, put_g)

    m_first[0].wait_recv()
    m_hs[...] = (mp[ct].astype(F32) + m_pr[1].astype(F32)).astype(BF)
    m_out = send(m_hs, m_cr, ct)

    passed_on(g_outs, g_local, b_hr, b_fr, put_g)

    for r in range(0, S, 32):
        xh = xh2[r:r + 32, :]
        dxh = gg_f[r:r + 32, :] * g2_ref[...]
        m1 = jnp.mean(dxh, axis=-1, keepdims=True)
        m2 = jnp.mean(dxh * xh, axis=-1, keepdims=True)
        gm = gm_f[r:r + 32, :] + rstd2[r:r + 32, 0:1] * (dxh - m1 - xh * m2)
        gm_f[r:r + 32, :] = gm
        gmid_ref[r:r + 32, :] = gm.astype(BF)

    gmv = gmid_ref[...]
    gctxT = (dot(wout[0], gmv[:, :HW], 1, 1) + dot(wout[1], gmv[:, HW:], 1, 1)).astype(BF)
    heads = range(HL)
    gos = [gctxT[h * HD:(h + 1) * HD, :] for h in heads]
    gps = [dot(head(h, 2), gos[h], 0, 0).astype(BF).astype(F32) for h in heads]
    gvs = [dot(gos[h], probs[h].astype(BF), 1, 1).astype(BF) for h in heads]
    gss = [(probs[h] * (gps[h] - jnp.sum(gps[h] * probs[h], axis=0, keepdims=True))).astype(BF) for h in heads]
    gqs = [(dot(head(h, 1), gss[h], 1, 0) * scale).astype(BF) for h in heads]
    gks = [(dot(head(h, 0), gss[h], 1, 1) * scale).astype(BF) for h in heads]
    for h in heads:
        for e, val in enumerate((gqs[h], gks[h], gvs[h])):
            gqkv_ref[head_rows(h, e), :] = val

    gqv = gqkv_ref[...]
    r_first = []
    for k in range(2):
        row_blocks(rp.at[k], slice(0, HW), dot(gqv, wqkv[:, k * HW:(k + 1) * HW], 0, 0))
        r_first.append((send(rp.at[k, qt], r_pr.at[k, 1], pt), send(rp.at[k, pt], r_pr.at[k, 0], pt)))

    ln_s, ln_pr = ln_x.at[0], ln_x.at[1]
    for k in range(2):
        cols = slice(k * HW, (k + 1) * HW)
        gg1 = jnp.zeros((1, HW), F32)
        gb1 = jnp.zeros((1, HW), F32)
        for i in range(TP):
            v = rp[k, i].astype(F32)
            gg1 = gg1 + jnp.sum(v * xhat[i * SL:(i + 1) * SL, cols], axis=0, keepdims=True)
            gb1 = gb1 + jnp.sum(v, axis=0, keepdims=True)
        ln_s[0:1, cols] = gg1
        ln_s[1:2, cols] = gb1
    l_first = send(ln_s, ln_pr, pt)

    vec_ref[2:3, :] = jnp.sum(gg_f[...] * xh2[...], axis=0, keepdims=True)
    vec_ref[3:4, :] = jnp.sum(gg_f[...], axis=0, keepdims=True)
    vec_ref[4:5, :] = jnp.sum(gm_f[...], axis=0, keepdims=True)

    own = pl.ds(pl.multiple_of(t * SL, 8), SL)
    xh_ref[...] = xhat[own, :]
    gm_ref[...] = gm_f[own, :]
    rs_ref[...] = rstd_s[own, :]
    g1_out[...] = par[0:1, :]

    for k in range(2):
        cols = slice(k * HW, (k + 1) * HW)
        r_first[k][0].wait_recv()
        r_hs[0:SL, cols] = (rp[k, ct].astype(F32) + r_pr[k, 1].astype(F32)).astype(BF)
        r_first[k][1].wait_recv()
        mine_ref[:, cols] = (rp[k, t].astype(F32) + r_pr[k, 0].astype(F32)).astype(BF)
    l_first.wait_recv()
    ln = ln_s[...] + ln_pr[...]
    ln_hs[...] = ln
    ln_rows = []
    for _ in range(3):
        ln_rows.append(ln.astype(BF).astype(F32))
        ln = ln - ln_rows[-1]
    r_hs[SL:SL + 8, :] = jnp.concatenate(ln_rows + [jnp.zeros((2, D), F32)], axis=0).astype(BF)
    m_first[1].wait_recv()
    m_out.wait_recv()
    m_sum = (mp[t].astype(F32) + m_pr[0].astype(F32)).astype(BF).astype(F32) + m_cr[...].astype(F32)
    y_ref[...] = (xf[own, :] + m_sum.astype(BF).astype(F32) + bd_ref[...]).astype(BF)
    for c in started:
        c.wait_send()


N_SEND = 37
VMEM_A = 36 * 2**20
VMEM_B = 8 * 2**20
VMEM_C = 4 * 2**20


def write_kernel(yi_ref, vec_ref, up_ref, dn_ref, gqkv_ref, h_ref, ctx_ref, gmid_ref,
                 y_ref, gwqkv_ref, gbqkv_ref, gwout_ref, gbo_ref, gl2_ref, bl2_ref, gwup_ref, gbup_ref, gwdn_ref, gbd_ref,
                 s_qkv, s_out, s_gb, s0, s1, s2, s3, s4, sem):
    cps = []

    def out(src, dst, n=1):
        rows = src.shape[0] // n
        for k in range(n):
            c = pltpu.make_async_copy(src.at[pl.ds(k * rows, rows)], dst.at[pl.ds(k * rows, rows)], sem.at[len(cps)])
            c.start()
            cps.append(c)

    out(dn_ref, gwdn_ref, 4)
    out(up_ref, gwup_ref, 4)
    out(yi_ref, y_ref)
    for i, (sv, r) in enumerate(((s0, gbd_ref), (s1, gbup_ref), (s2, gl2_ref), (s3, bl2_ref), (s4, gbo_ref))):
        sv[...] = vec_ref[i, :]
        out(sv, r)
    ones = jnp.ones((8, S), BF)
    for h in range(HL):
        for e in range(3):
            s_gb[e, h:h + 1, :] = dot(ones, gqkv_ref[head_rows(h, e), :], 1, 1)[0:1, :]
    out(s_gb, gbqkv_ref)
    hv = h_ref[...]
    s_out[...] = dot(ctx_ref[...], gmid_ref[...], 1, 0).astype(BF)
    out(s_out, gwout_ref)
    for n in range(HL):
        rows = slice(n * 3 * HD, (n + 1) * 3 * HD)
        s_qkv[rows, :] = dot(gqkv_ref[rows, :], hv, 1, 0).astype(BF)
        out(s_qkv.at[rows], gwqkv_ref.at[rows])
    for c in cps:
        c.wait()


def last_kernel(mine_ref, xh_ref, gm_ref, rs_ref, g1_ref, rc_ref, ln_ref, gx_ref, gl1_ref, bl1_ref):
    gh = (mine_ref[...].astype(F32) + rc_ref[0:SL, :].astype(F32)).astype(BF).astype(F32)
    xh = xh_ref[...]
    dxh = gh * g1_ref[...]
    m1 = jnp.mean(dxh, axis=-1, keepdims=True)
    m2 = jnp.mean(dxh * xh, axis=-1, keepdims=True)
    gx_ref[...] = (gm_ref[...] + rs_ref[:, 0:1] * (dxh - m1 - xh * m2)).astype(BF)
    lc = rc_ref[SL:SL + 8, :].astype(F32)
    ln = ln_ref[...] + (lc[0:2, :] + lc[2:4, :] + lc[4:6, :])
    gl1_ref[...] = ln[0, :]
    bl1_ref[...] = ln[1, :]


def solution(mesh):
    VM = pl.BlockSpec(memory_space=pltpu.VMEM)
    ANY = pl.BlockSpec(memory_space=pltpu.HBM)

    def sds(shape, dt):
        return jax.ShapeDtypeStruct(shape, dt)

    def local_step(x, g1, be1, w_qkv, b_qkv, w_out, b_out, g2, be2, w_up, b_up, w_down, b_down, grad_y):
        wq = jnp.transpose(w_qkv, (1, 2, 3, 0)).reshape(3 * HL * HD, D)
        bq = jnp.transpose(b_qkv, (1, 0, 2))
        part = pltpu.VMEM((S, HW), BF)
        vec1 = sds((D,), F32)
        mids = pl.pallas_call(
            block_kernel,
            out_shape=(pltpu.VMEM((SL, D), BF), pltpu.VMEM((8, D), F32), pltpu.VMEM((D, FL), BF), pltpu.VMEM((FL, D), BF),
                       pltpu.VMEM((3 * HL * HD, S), BF), pltpu.VMEM((S, D), BF), pltpu.VMEM((HL * HD, S), BF), pltpu.VMEM((S, D), BF),
                       pltpu.VMEM((SL, D), BF), pltpu.VMEM((SL, D), F32), pltpu.VMEM((SL, D), F32), pltpu.VMEM((SL, 128), F32),
                       pltpu.VMEM((1, D), F32), sds((SL + 8, D), BF), pltpu.VMEM((2, D), F32)),
            in_specs=[ANY] * 14,
            out_specs=(VM,) * 15,
            scratch_shapes=[
                pltpu.VMEM((3 * HL * HD, D), BF), pltpu.VMEM((2, HL * HD, HW), BF), pltpu.VMEM((S, D), F32), pltpu.VMEM((S, D), F32),
                pltpu.VMEM((S, D), F32), pltpu.VMEM((S, D), F32), pltpu.VMEM((S, 128), F32), pltpu.VMEM((HL, S, S), F32),
                pltpu.VMEM((3 * HL * HD, S), BF), pltpu.VMEM((8, D), F32), pltpu.VMEM((TP, SL, D), BF),
                pltpu.VMEM((D, FL), BF), pltpu.VMEM((FL, D), BF), pltpu.VMEM((TP, SL, D), BF), pltpu.VMEM((TP, SL, D), BF),
                pltpu.VMEM((3 * HL * HD, S), F32), *[part] * 12,
                pltpu.VMEM((S, FL), BF), pltpu.VMEM((S, D), BF), pltpu.VMEM((S, FL), BF), pltpu.VMEM((S, FL), BF), pltpu.VMEM((S, D), BF),
                pltpu.VMEM((3, HL, HD), F32), *[pltpu.VMEM((D,), F32) for _ in range(7)],
                pltpu.VMEM((2, TP, SL, HW), BF), pltpu.VMEM((2, SL, D), BF), pltpu.VMEM((SL, D), BF), pltpu.VMEM((SL, D), BF),
                pltpu.VMEM((2, 2, SL, HW), BF), pltpu.VMEM((2, 2, D), F32), pltpu.VMEM((S, D), F32), pltpu.VMEM((S, 128), F32),
                pltpu.VMEM((4, 2, S, UW), BF), pltpu.VMEM((4, 2, S, UW), BF),
                pltpu.SemaphoreType.DMA((9,)), pltpu.SemaphoreType.DMA((N_SEND,)), pltpu.SemaphoreType.DMA((N_SEND,)),
                pltpu.SemaphoreType.DMA((10,)),
            ],
            compiler_params=pltpu.CompilerParams(collective_id=0, has_side_effects=True, vmem_limit_bytes=VMEM_A),
            name='block',
        )(*(pltpu.with_memory_space_constraint(v, pltpu.HBM) for v in (
            x.reshape(SL, D), grad_y.reshape(SL, D), g1, be1, g2, be2, b_out, b_down, bq, b_up, wq, w_out, w_up, w_down)))
        mine, xh, gm, rs, g1v, r_hs, ln_hs = mids[8:]
        across = [(i, TP - 1 - i) for i in range(TP)]
        r_cr = lax.ppermute(r_hs, 'tp', across)
        y, gwqkv, gbqkv, gwout, gbo, gl2, bl2, gwup, gbup, gwdn, gbd = pl.pallas_call(
            write_kernel,
            out_shape=(sds((SL, D), BF), sds((3 * HL * HD, D), BF), sds((3, HL, HD), F32), sds((HL * HD, D), BF), vec1, vec1, vec1,
                       sds((D, FL), BF), vec1, sds((FL, D), BF), vec1),
            in_specs=[VM] * 8,
            out_specs=(ANY,) * 11,
            scratch_shapes=[pltpu.VMEM((3 * HL * HD, D), BF), pltpu.VMEM((HL * HD, D), BF), pltpu.VMEM((3, HL, HD), F32),
                            *[pltpu.VMEM((D,), F32) for _ in range(5)], pltpu.SemaphoreType.DMA((20,))],
            compiler_params=pltpu.CompilerParams(vmem_limit_bytes=VMEM_B),
            cost_estimate=pl.CostEstimate(flops=600_000_000, bytes_accessed=14_200_000, transcendentals=0),
            name='write',
        )(*mids[:8])
        gx, gl1, bl1 = pl.pallas_call(
            last_kernel,
            out_shape=(sds((SL, D), BF), vec1, vec1),
            in_specs=[VM] * 7,
            out_specs=(VM,) * 3,
            compiler_params=pltpu.CompilerParams(vmem_limit_bytes=VMEM_C),
            name='last',
        )(mine, xh, gm, rs, g1v, r_cr, ln_hs)
        gwqkv = jnp.transpose(gwqkv.reshape(HL, 3, HD, D), (3, 0, 1, 2))
        gbqkv = jnp.transpose(gbqkv, (1, 0, 2))
        return (y.reshape(1, SL, D), gx.reshape(1, SL, D), gl1, bl1, gwqkv, gbqkv, gwout, gbo, gl2, bl2, gwup, gbup, gwdn, gbd)

    row_spec = P('dp', 'tp', None)
    in_specs = (row_spec, P(), P(), P(None, 'tp', None, None), P('tp', None, None), P('tp', None), P(), P(), P(),
                P(None, 'tp'), P('tp'), P('tp', None), P(), row_spec)
    out_specs = (row_spec, row_spec, P('dp'), P('dp'), P('dp', 'tp', None, None), P(('dp', 'tp'), None, None),
                 P(('dp', 'tp'), None), P('dp'), P('dp'), P('dp'), P('dp', 'tp'), P(('dp', 'tp')), P(('dp', 'tp'), None), P('dp'))
    return jax.shard_map(local_step, mesh=mesh, in_specs=in_specs, out_specs=out_specs, check_vma=False)
```

```python
import functools
import math

import jax
import jax.numpy as jnp
from jax import lax
from jax.experimental import pallas as pl
from jax.experimental.pallas import tpu as pltpu
from jax.sharding import PartitionSpec as P

EPS = 1e-5
MASK_VALUE = -1e30
BF = jnp.bfloat16
F32 = jnp.float32
MESH = pl.DeviceIdType.MESH

D = 1536
S = 96
SL = 24
TP = 4
HL = 4
HD = 96
FL = 1536
CW = 256
NCH = D // CW
HCH = NCH // 2
HW = D // 2
UW = 128
CUT = (128, 384, 640, 768)
NCUT = len(CUT) - 1


def alibi_slopes(n_heads):
    closest = 2 ** int(math.floor(math.log2(n_heads)))
    base_ratio = 2.0 ** (-8.0 / closest)
    extra_ratio = 2.0 ** (-4.0 / closest)
    remaining = min(closest, n_heads - closest)
    slopes = [base_ratio ** (i + 1) for i in range(closest)]
    return slopes + [extra_ratio ** (2 * i + 1) for i in range(remaining)]


def dot(a, b, ca, cb):
    return lax.dot_general(a, b, (((ca,), (cb,)), ((), ())), preferred_element_type=F32)


def gelu_parts(u):
    k = math.sqrt(2.0 / math.pi)
    u2 = u * u
    th = jnp.tanh(u * (k + (k * 0.044715) * u2))
    half = 0.5 + 0.5 * th
    val = u * half
    return val, half + val * (1.0 - th) * (k + (3.0 * 0.044715 * k) * u2)


def rows_stats(v):
    mean = jnp.mean(v, axis=-1, keepdims=True)
    cen = v - mean
    var = jnp.mean(cen * cen, axis=-1, keepdims=True)
    return cen, lax.rsqrt(var + EPS)


def places():
    t = lax.axis_index('tp')
    core = t % 2
    pt = t + 1 - 2 * core
    ct = TP - 1 - t
    qt = TP - 1 - pt
    half = (core + t // 2) % 2
    return t, pt, ct, qt, half


def sender(ssem, rsem):
    started = []

    def send(src, dst, dev):
        i = len(started)
        c = pltpu.make_async_remote_copy(src_ref=src, dst_ref=dst, send_sem=ssem.at[i], recv_sem=rsem.at[i],
                                         device_id={'tp': dev}, device_id_type=MESH)
        c.start()
        started.append(c)
        return c

    return send, started


def columns(start, width):
    return pl.ds(start if isinstance(start, int) else pl.multiple_of(start, 128), width)


def head_rows(h, e):
    return slice((h * 3 + e) * HD, (h * 3 + e + 1) * HD)


def row_blocks(buf, cols, v):
    for i in range(TP):
        buf[i, :, cols] = v[i * SL:(i + 1) * SL, :].astype(BF)


def block_kernel(x_hbm, gy_hbm, g1_hbm, be1_hbm, g2_hbm, be2_hbm, bo_hbm, bd_hbm, bqkv_hbm, bup_hbm,
                 wqkv_hbm, wout_hbm, wup_hbm, wdn_hbm,
                 y_ref, vec_ref, gwup_ref, gwdn_ref, gqkv_ref, h_ref, ctx_ref, gmid_ref, mine_ref, xh_ref, gm_ref, rs_ref, g1_out, r_hs, ln_hs,
                 wqkv, wout, xf, gm_f, gg_f, xhat, rstd_s, probs, qkvT, par, mp,
                 wup, wdn, xg, gyg, biasT, a_ps, a_pr, a_hs, a_hr, a_cr, a_fr, b_ps, b_pr, b_hs, b_hr, b_cr, b_fr,
                 gact, g_ref, gpre_ref, act_ref, gyf_ref, bqkv_ref, g1_in, be1_in, g2_in, be2_in, bo_in, bd_in, bup_in,
                 rp, m_pr, m_hs, m_cr, r_pr, ln_x, xh2, rstd2, a_un, b_un,
                 wsem, ssem, rsem, isem):
    t, pt, ct, qt, half = places()
    send, started = sender(ssem, rsem)

    in_x = pltpu.make_async_copy(x_hbm, xg.at[t], isem.at[0])
    in_gy = pltpu.make_async_copy(gy_hbm, gyg.at[t], isem.at[1])
    in_b = pltpu.make_async_copy(bqkv_hbm, bqkv_ref, isem.at[2])
    small = ((g1_hbm, g1_in), (be1_hbm, be1_in), (g2_hbm, g2_in), (be2_hbm, be2_in), (bo_hbm, bo_in), (bd_hbm, bd_in), (bup_hbm, bup_in))
    in_p = [pltpu.make_async_copy(a, b, isem.at[3 + i]) for i, (a, b) in enumerate(small)]
    for c in (in_x, in_gy, in_b, *in_p):
        c.start()
    w_cps = {}
    w_cps['qkv'] = [pltpu.make_async_copy(wqkv_hbm, wqkv, wsem.at[0])]
    w_cps['out'] = [pltpu.make_async_copy(wout_hbm.at[:, pl.ds(k * HW, HW)], wout.at[k], wsem.at[1 + k]) for k in range(2)]
    w_cps['dn'] = [pltpu.make_async_copy(wdn_hbm, wdn, wsem.at[7])]
    w_cps['up'] = [pltpu.make_async_copy(wup_hbm, wup, wsem.at[8])]

    barrier = pltpu.get_barrier_semaphore()
    for dev in (pt, ct, qt):
        pl.semaphore_signal(barrier, inc=1, device_id={'tp': dev}, device_id_type=MESH)
    for name in ('qkv', 'out', 'dn', 'up'):
        for c in w_cps[name]:
            c.start()
    pl.semaphore_wait(barrier, 3)

    in_x.wait()
    x_c = send(xg.at[t], xg.at[t], ct)
    x_p = send(xg.at[t], xg.at[t], pt)

    for c in (in_b, *in_p):
        c.wait()
    for i, r in enumerate((g1_in, be1_in, g2_in, be2_in, bo_in, bd_in, bup_in)):
        par[i, :] = r[...]
    g1_ref, be1_ref, g2_ref, be2_ref, bo_ref, bd_ref, bup_ref = (par.at[i:i + 1] for i in range(7))

    for h in range(HL):
        for e in range(3):
            row = jnp.broadcast_to(bqkv_ref[e, h:h + 1, :], (S, HD))
            biasT[pl.ds((h * 3 + e) * HD, HD), :] = row.T

    x_c.wait_recv()
    x_f = send(xg.at[ct], xg.at[ct], pt)
    in_gy.wait()
    y_c = send(gyg.at[t], gyg.at[t], ct)
    y_p = send(gyg.at[t], gyg.at[t], pt)
    x_p.wait_recv()
    x_f.wait_recv()

    for i in range(TP):
        xf[pl.ds(i * SL, SL), :] = xg[i].astype(F32)
    for r in range(0, S, 32):
        cen, rstd = rows_stats(xf[r:r + 32, :])
        xh = cen * rstd
        xhat[r:r + 32, :] = xh
        rstd_s[r:r + 32, :] = jnp.broadcast_to(rstd, (32, 128))
        h_ref[r:r + 32, :] = (xh * g1_ref[...] + be1_ref[...]).astype(BF)

    w_cps['qkv'][0].wait()
    hv = h_ref[...]
    for h in range(2):
        rows = slice(h * 6 * HD, (h + 1) * 6 * HD)
        qkvT[rows, :] = (dot(wqkv[rows, :], hv, 1, 1) + biasT[rows, :]).astype(BF)

    scale = HD ** -0.5
    slopes = alibi_slopes(HL * TP)
    j_pos = lax.broadcasted_iota(jnp.int32, (S, S), 0)
    i_pos = lax.broadcasted_iota(jnp.int32, (S, S), 1)
    causal = j_pos <= i_pos
    j_f = j_pos.astype(F32)

    def head(h, e):
        return qkvT[head_rows(h, e), :]

    for h in range(HL):
        slope = jnp.where(t == 0, slopes[h], jnp.where(t == 1, slopes[HL + h], jnp.where(t == 2, slopes[2 * HL + h], slopes[3 * HL + h]))).astype(F32)
        s = dot(head(h, 1), head(h, 0), 0, 0) * scale + slope * j_f
        s = jnp.where(causal, s, MASK_VALUE)
        p = jnp.exp(s - jnp.max(s, axis=0, keepdims=True))
        p = p / jnp.sum(p, axis=0, keepdims=True)
        probs[h] = p
        ctx_ref[h * HD:(h + 1) * HD, :] = dot(head(h, 2), p.astype(BF), 1, 0).astype(BF)

    def exchange(part, groups, ps, pr, hs, hr, cr, fr, un):
        firsts = []
        for k0, k1 in groups:
            cols = slice(CUT[k0], CUT[k1])
            ps[:, cols] = part(1 - half, CUT[k0], CUT[k1]).astype(BF)
            firsts.append(send(ps.at[:, cols], pr.at[:, cols], pt))
            if k0 == 0:
                for hh in range(2):
                    un[0, hh] = part(hh, 0, UW).astype(BF)
                early = [send(un.at[0], un.at[2], ct), send(un.at[0], un.at[1], pt)]
        outs = []
        for (k0, k1), first in zip(groups, firsts):
            cols = slice(CUT[k0], CUT[k1])
            ours = part(half, CUT[k0], CUT[k1])
            first.wait_recv()
            hs[:, cols] = (ours + pr[:, cols].astype(F32)).astype(BF)
            for k in range(k0, k1):
                c = slice(CUT[k], CUT[k + 1])
                outs.append([send(hs.at[:, c], cr.at[:, c], ct)])
                if k == NCUT - 1:
                    outs[-1].append(send(hs.at[:, c], fr.at[:, c], qt))
        local = send(hs.at[:, UW:], hr.at[:, UW:], pt)
        return outs, local, early

    def early_arrived(early, un):
        early[0].wait_recv()
        early.append(send(un.at[2], un.at[3], pt))

    def early_added(early, un, put):
        early[1].wait_recv()
        early[2].wait_recv()
        for hh in range(2):
            chips = [un[k, hh].astype(F32) + un[k + 1, hh].astype(F32) for k in (0, 2)]
            put(hh * HW, UW, (chips[0] + chips[1]).astype(BF).astype(F32))

    def arrived(out, k, hs, cr, fr, put):
        c = slice(CUT[k], CUT[k + 1])
        out[0].wait_recv()
        if k < NCUT - 1:
            out.append(send(cr.at[:, c], fr.at[:, c], pt))
        put(half * HW + CUT[k], CUT[k + 1] - CUT[k], (hs[:, c].astype(F32) + cr[:, c].astype(F32)).astype(BF).astype(F32))

    def passed_on(outs, local, hr, fr, put):
        local.wait_recv()
        for k, out in enumerate(outs):
            c = slice(CUT[k], CUT[k + 1])
            out[1].wait_recv()
            put((1 - half) * HW + CUT[k], CUT[k + 1] - CUT[k], (hr[:, c].astype(F32) + fr[:, c].astype(F32)).astype(BF).astype(F32))

    for c in w_cps['out']:
        c.wait()
    ctxT = ctx_ref[...]
    a_outs, a_local, a_early = exchange(lambda hh, c0, c1: dot(ctxT, wout[hh, :, c0:c1], 0, 0), ((0, NCUT),), a_ps, a_pr, a_hs, a_hr, a_cr, a_fr, a_un)

    y_c.wait_recv()
    y_f = send(gyg.at[ct], gyg.at[ct], pt)
    y_p.wait_recv()
    y_f.wait_recv()
    for i in range(TP):
        gm_f[pl.ds(i * SL, SL), :] = gyg[i].astype(F32)
    for r in range(0, S, 32):
        gyf_ref[r:r + 32, :] = gm_f[r:r + 32, :].astype(BF)
    w_cps['dn'][0].wait()
    gyv = gyf_ref[...]
    for n in range(NCH):
        gact[:, n * CW:(n + 1) * CW] = dot(gyv, wdn[n * CW:(n + 1) * CW, :], 1, 1).astype(BF)
    vec_ref[0:1, :] = jnp.sum(gm_f[...], axis=0, keepdims=True)

    def put_x(start, width, val):
        cols = columns(start, width)
        xf[:, cols] = xf[:, cols] + val + bo_ref[:, cols]

    early_arrived(a_early, a_un)
    for k, out in enumerate(a_outs):
        arrived(out, k, a_hs, a_cr, a_fr, put_x)
    early_added(a_early, a_un, put_x)
    passed_on(a_outs, a_local, a_hr, a_fr, put_x)

    for r in range(0, S, 32):
        cen, rstd = rows_stats(xf[r:r + 32, :])
        xh = cen * rstd
        xh2[r:r + 32, :] = xh
        rstd2[r:r + 32, :] = jnp.broadcast_to(rstd, (32, 128))
        g_ref[r:r + 32, :] = (xh * g2_ref[...] + be2_ref[...]).astype(BF)

    w_cps['up'][0].wait()
    gv = g_ref[...]
    for n in range(NCH // 2):
        cols = slice(n * 2 * CW, (n + 1) * 2 * CW)
        pre = dot(gv, wup[:, cols], 1, 0) + bup_ref[:, cols]
        val, der = gelu_parts(pre)
        act_ref[:, cols] = val.astype(BF)
        gp = gact[:, cols].astype(F32) * der
        vec_ref[1:2, cols] = jnp.sum(gp, axis=0, keepdims=True)
        gpre_ref[:, cols] = gp.astype(BF)

    gprev = gpre_ref[...]

    def part_g(hh, c0, c1):
        return dot(gprev, wup[columns(hh * HW + c0, c1 - c0), :], 1, 1)

    g_outs, g_local, g_early = exchange(part_g, ((0, 1), (1, NCUT)), b_ps, b_pr, b_hs, b_hr, b_cr, b_fr, b_un)

    actv = act_ref[...]
    for n in range(NCH):
        cols = slice(n * CW, (n + 1) * CW)
        row_blocks(mp, cols, dot(actv, wdn[:, cols], 1, 0))
    m_first = (send(mp.at[qt], m_pr.at[1], pt), send(mp.at[pt], m_pr.at[0], pt))
    for n in range(NCH):
        gwdn_ref[n * CW:(n + 1) * CW, :] = dot(act_ref[:, n * CW:(n + 1) * CW], gyv, 0, 0).astype(BF)
    def put_g(start, width, val):
        gg_f[:, columns(start, width)] = val

    early_arrived(g_early, b_un)
    for n in range(NCH):
        gwup_ref[n * CW:(n + 1) * CW, :] = dot(g_ref[:, n * CW:(n + 1) * CW], gprev, 0, 0).astype(BF)
        if n % 2:
            arrived(g_outs[n // 2], n // 2, b_hs, b_cr, b_fr, put_g)
    early_added(g_early, b_un, put_g)

    m_first[0].wait_recv()
    m_hs[...] = (mp[ct].astype(F32) + m_pr[1].astype(F32)).astype(BF)
    m_out = send(m_hs, m_cr, ct)

    passed_on(g_outs, g_local, b_hr, b_fr, put_g)

    for r in range(0, S, 32):
        xh = xh2[r:r + 32, :]
        dxh = gg_f[r:r + 32, :] * g2_ref[...]
        m1 = jnp.mean(dxh, axis=-1, keepdims=True)
        m2 = jnp.mean(dxh * xh, axis=-1, keepdims=True)
        gm = gm_f[r:r + 32, :] + rstd2[r:r + 32, 0:1] * (dxh - m1 - xh * m2)
        gm_f[r:r + 32, :] = gm
        gmid_ref[r:r + 32, :] = gm.astype(BF)

    gmv = gmid_ref[...]
    gctxT = (dot(wout[0], gmv[:, :HW], 1, 1) + dot(wout[1], gmv[:, HW:], 1, 1)).astype(BF)
    heads = range(HL)
    gos = [gctxT[h * HD:(h + 1) * HD, :] for h in heads]
    gps = [dot(head(h, 2), gos[h], 0, 0).astype(BF).astype(F32) for h in heads]
    gvs = [dot(gos[h], probs[h].astype(BF), 1, 1).astype(BF) for h in heads]
    gss = [(probs[h] * (gps[h] - jnp.sum(gps[h] * probs[h], axis=0, keepdims=True))).astype(BF) for h in heads]
    gqs = [(dot(head(h, 1), gss[h], 1, 0) * scale).astype(BF) for h in heads]
    gks = [(dot(head(h, 0), gss[h], 1, 1) * scale).astype(BF) for h in heads]
    for h in heads:
        for e, val in enumerate((gqs[h], gks[h], gvs[h])):
            gqkv_ref[head_rows(h, e), :] = val

    gqv = gqkv_ref[...]
    r_first = []
    for k in range(2):
        row_blocks(rp.at[k], slice(0, HW), dot(gqv, wqkv[:, k * HW:(k + 1) * HW], 0, 0))
        r_first.append((send(rp.at[k, qt], r_pr.at[k, 1], pt), send(rp.at[k, pt], r_pr.at[k, 0], pt)))

    ln_s, ln_pr = ln_x.at[0], ln_x.at[1]
    for k in range(2):
        cols = slice(k * HW, (k + 1) * HW)
        gg1 = jnp.zeros((1, HW), F32)
        gb1 = jnp.zeros((1, HW), F32)
        for i in range(TP):
            v = rp[k, i].astype(F32)
            gg1 = gg1 + jnp.sum(v * xhat[i * SL:(i + 1) * SL, cols], axis=0, keepdims=True)
            gb1 = gb1 + jnp.sum(v, axis=0, keepdims=True)
        ln_s[0:1, cols] = gg1
        ln_s[1:2, cols] = gb1
    l_first = send(ln_s, ln_pr, pt)

    vec_ref[2:3, :] = jnp.sum(gg_f[...] * xh2[...], axis=0, keepdims=True)
    vec_ref[3:4, :] = jnp.sum(gg_f[...], axis=0, keepdims=True)
    vec_ref[4:5, :] = jnp.sum(gm_f[...], axis=0, keepdims=True)

    own = pl.ds(pl.multiple_of(t * SL, 8), SL)
    xh_ref[...] = xhat[own, :]
    gm_ref[...] = gm_f[own, :]
    rs_ref[...] = rstd_s[own, :]
    g1_out[...] = par[0:1, :]

    for k in range(2):
        cols = slice(k * HW, (k + 1) * HW)
        r_first[k][0].wait_recv()
        r_hs[0:SL, cols] = (rp[k, ct].astype(F32) + r_pr[k, 1].astype(F32)).astype(BF)
        r_first[k][1].wait_recv()
        mine_ref[:, cols] = (rp[k, t].astype(F32) + r_pr[k, 0].astype(F32)).astype(BF)
    l_first.wait_recv()
    ln = ln_s[...] + ln_pr[...]
    ln_hs[...] = ln
    ln_rows = []
    for _ in range(3):
        ln_rows.append(ln.astype(BF).astype(F32))
        ln = ln - ln_rows[-1]
    r_hs[SL:SL + 8, :] = jnp.concatenate(ln_rows + [jnp.zeros((2, D), F32)], axis=0).astype(BF)
    m_first[1].wait_recv()
    m_out.wait_recv()
    m_sum = (mp[t].astype(F32) + m_pr[0].astype(F32)).astype(BF).astype(F32) + m_cr[...].astype(F32)
    y_ref[...] = (xf[own, :] + m_sum.astype(BF).astype(F32) + bd_ref[...]).astype(BF)
    for c in started:
        c.wait_send()


N_SEND = 37
VMEM_A = 36 * 2**20
VMEM_B = 8 * 2**20
VMEM_C = 4 * 2**20


def write_kernel(yi_ref, vec_ref, up_ref, dn_ref, gqkv_ref, h_ref, ctx_ref, gmid_ref,
                 y_ref, gwqkv_ref, gbqkv_ref, gwout_ref, gbo_ref, gl2_ref, bl2_ref, gwup_ref, gbup_ref, gwdn_ref, gbd_ref,
                 s_qkv, s_out, s_gb, s0, s1, s2, s3, s4, sem):
    cps = []

    def out(src, dst, n=1):
        rows = src.shape[0] // n
        for k in range(n):
            c = pltpu.make_async_copy(src.at[pl.ds(k * rows, rows)], dst.at[pl.ds(k * rows, rows)], sem.at[len(cps)])
            c.start()
            cps.append(c)

    out(dn_ref, gwdn_ref, 4)
    out(up_ref, gwup_ref, 4)
    out(yi_ref, y_ref)
    for i, (sv, r) in enumerate(((s0, gbd_ref), (s1, gbup_ref), (s2, gl2_ref), (s3, bl2_ref), (s4, gbo_ref))):
        sv[...] = vec_ref[i, :]
        out(sv, r)
    ones = jnp.ones((8, S), BF)
    for h in range(HL):
        for e in range(3):
            s_gb[e, h:h + 1, :] = dot(ones, gqkv_ref[head_rows(h, e), :], 1, 1)[0:1, :]
    out(s_gb, gbqkv_ref)
    hv = h_ref[...]
    s_out[...] = dot(ctx_ref[...], gmid_ref[...], 1, 0).astype(BF)
    out(s_out, gwout_ref)
    for n in range(HL):
        rows = slice(n * 3 * HD, (n + 1) * 3 * HD)
        s_qkv[rows, :] = dot(gqkv_ref[rows, :], hv, 1, 0).astype(BF)
        out(s_qkv.at[rows], gwqkv_ref.at[rows])
    for c in cps:
        c.wait()


def last_kernel(mine_ref, xh_ref, gm_ref, rs_ref, g1_ref, rc_ref, ln_ref, gx_ref, gl1_ref, bl1_ref):
    gh = (mine_ref[...].astype(F32) + rc_ref[0:SL, :].astype(F32)).astype(BF).astype(F32)
    xh = xh_ref[...]
    dxh = gh * g1_ref[...]
    m1 = jnp.mean(dxh, axis=-1, keepdims=True)
    m2 = jnp.mean(dxh * xh, axis=-1, keepdims=True)
    gx_ref[...] = (gm_ref[...] + rs_ref[:, 0:1] * (dxh - m1 - xh * m2)).astype(BF)
    lc = rc_ref[SL:SL + 8, :].astype(F32)
    ln = ln_ref[...] + (lc[0:2, :] + lc[2:4, :] + lc[4:6, :])
    gl1_ref[...] = ln[0, :]
    bl1_ref[...] = ln[1, :]


def solution(mesh):
    VM = pl.BlockSpec(memory_space=pltpu.VMEM)
    ANY = pl.BlockSpec(memory_space=pltpu.HBM)

    def sds(shape, dt):
        return jax.ShapeDtypeStruct(shape, dt)

    def local_step(x, g1, be1, w_qkv, b_qkv, w_out, b_out, g2, be2, w_up, b_up, w_down, b_down, grad_y):
        wq = jnp.transpose(w_qkv, (1, 2, 3, 0)).reshape(3 * HL * HD, D)
        bq = jnp.transpose(b_qkv, (1, 0, 2))
        part = pltpu.VMEM((S, HW), BF)
        vec1 = sds((D,), F32)
        mids = pl.pallas_call(
            block_kernel,
            out_shape=(pltpu.VMEM((SL, D), BF), pltpu.VMEM((8, D), F32), pltpu.VMEM((D, FL), BF), pltpu.VMEM((FL, D), BF),
                       pltpu.VMEM((3 * HL * HD, S), BF), pltpu.VMEM((S, D), BF), pltpu.VMEM((HL * HD, S), BF), pltpu.VMEM((S, D), BF),
                       pltpu.VMEM((SL, D), BF), pltpu.VMEM((SL, D), F32), pltpu.VMEM((SL, D), F32), pltpu.VMEM((SL, 128), F32),
                       pltpu.VMEM((1, D), F32), sds((SL + 8, D), BF), pltpu.VMEM((2, D), F32)),
            in_specs=[ANY] * 14,
            out_specs=(VM,) * 15,
            scratch_shapes=[
                pltpu.VMEM((3 * HL * HD, D), BF), pltpu.VMEM((2, HL * HD, HW), BF), pltpu.VMEM((S, D), F32), pltpu.VMEM((S, D), F32),
                pltpu.VMEM((S, D), F32), pltpu.VMEM((S, D), F32), pltpu.VMEM((S, 128), F32), pltpu.VMEM((HL, S, S), F32),
                pltpu.VMEM((3 * HL * HD, S), BF), pltpu.VMEM((8, D), F32), pltpu.VMEM((TP, SL, D), BF),
                pltpu.VMEM((D, FL), BF), pltpu.VMEM((FL, D), BF), pltpu.VMEM((TP, SL, D), BF), pltpu.VMEM((TP, SL, D), BF),
                pltpu.VMEM((3 * HL * HD, S), F32), *[part] * 12,
                pltpu.VMEM((S, FL), BF), pltpu.VMEM((S, D), BF), pltpu.VMEM((S, FL), BF), pltpu.VMEM((S, FL), BF), pltpu.VMEM((S, D), BF),
                pltpu.VMEM((3, HL, HD), F32), *[pltpu.VMEM((D,), F32) for _ in range(7)],
                pltpu.VMEM((2, TP, SL, HW), BF), pltpu.VMEM((2, SL, D), BF), pltpu.VMEM((SL, D), BF), pltpu.VMEM((SL, D), BF),
                pltpu.VMEM((2, 2, SL, HW), BF), pltpu.VMEM((2, 2, D), F32), pltpu.VMEM((S, D), F32), pltpu.VMEM((S, 128), F32),
                pltpu.VMEM((4, 2, S, UW), BF), pltpu.VMEM((4, 2, S, UW), BF),
                pltpu.SemaphoreType.DMA((9,)), pltpu.SemaphoreType.DMA((N_SEND,)), pltpu.SemaphoreType.DMA((N_SEND,)),
                pltpu.SemaphoreType.DMA((10,)),
            ],
            compiler_params=pltpu.CompilerParams(collective_id=0, has_side_effects=True, vmem_limit_bytes=VMEM_A),
            name='block',
        )(*(pltpu.with_memory_space_constraint(v, pltpu.HBM) for v in (
            x.reshape(SL, D), grad_y.reshape(SL, D), g1, be1, g2, be2, b_out, b_down, bq, b_up, wq, w_out, w_up, w_down)))
        mine, xh, gm, rs, g1v, r_hs, ln_hs = mids[8:]
        across = [(i, TP - 1 - i) for i in range(TP)]
        r_cr = lax.ppermute(r_hs, 'tp', across)
        y, gwqkv, gbqkv, gwout, gbo, gl2, bl2, gwup, gbup, gwdn, gbd = pl.pallas_call(
            write_kernel,
            out_shape=(sds((SL, D), BF), sds((3 * HL * HD, D), BF), sds((3, HL, HD), F32), sds((HL * HD, D), BF), vec1, vec1, vec1,
                       sds((D, FL), BF), vec1, sds((FL, D), BF), vec1),
            in_specs=[VM] * 8,
            out_specs=(ANY,) * 11,
            scratch_shapes=[pltpu.VMEM((3 * HL * HD, D), BF), pltpu.VMEM((HL * HD, D), BF), pltpu.VMEM((3, HL, HD), F32),
                            *[pltpu.VMEM((D,), F32) for _ in range(5)], pltpu.SemaphoreType.DMA((20,))],
            compiler_params=pltpu.CompilerParams(vmem_limit_bytes=VMEM_B),
            cost_estimate=pl.CostEstimate(flops=600_000_000, bytes_accessed=14_200_000, transcendentals=0),
            name='write',
        )(*mids[:8])
        gx, gl1, bl1 = pl.pallas_call(
            last_kernel,
            out_shape=(sds((SL, D), BF), vec1, vec1),
            in_specs=[VM] * 7,
            out_specs=(VM,) * 3,
            compiler_params=pltpu.CompilerParams(vmem_limit_bytes=VMEM_C),
            name='last',
        )(mine, xh, gm, rs, g1v, r_cr, ln_hs)
        gwqkv = jnp.transpose(gwqkv.reshape(HL, 3, HD, D), (3, 0, 1, 2))
        gbqkv = jnp.transpose(gbqkv, (1, 0, 2))
        return (y.reshape(1, SL, D), gx.reshape(1, SL, D), gl1, bl1, gwqkv, gbqkv, gwout, gbo, gl2, bl2, gwup, gbup, gwdn, gbd)

    row_spec = P('dp', 'tp', None)
    in_specs = (row_spec, P(), P(), P(None, 'tp', None, None), P('tp', None, None), P('tp', None), P(), P(), P(),
                P(None, 'tp'), P('tp'), P('tp', None), P(), row_spec)
    out_specs = (row_spec, row_spec, P('dp'), P('dp'), P('dp', 'tp', None, None), P(('dp', 'tp'), None, None),
                 P(('dp', 'tp'), None), P('dp'), P('dp'), P('dp'), P('dp', 'tp'), P(('dp', 'tp')), P(('dp', 'tp'), None), P('dp'))
    return jax.shard_map(local_step, mesh=mesh, in_specs=in_specs, out_specs=out_specs, check_vma=False)
```

```python
import functools
import math

import jax
import jax.numpy as jnp
from jax import lax
from jax.experimental import pallas as pl
from jax.experimental.pallas import tpu as pltpu
from jax.sharding import PartitionSpec as P

EPS = 1e-5
MASK_VALUE = -1e30
BF = jnp.bfloat16
F32 = jnp.float32
MESH = pl.DeviceIdType.MESH

D = 1536
S = 96
SL = 24
TP = 4
HL = 4
HD = 96
FL = 1536
CW = 256
NCH = D // CW
HCH = NCH // 2
HW = D // 2
UW = 128
CUT = (128, 384, 640, 768)
NCUT = len(CUT) - 1


def alibi_slopes(n_heads):
    closest = 2 ** int(math.floor(math.log2(n_heads)))
    base_ratio = 2.0 ** (-8.0 / closest)
    extra_ratio = 2.0 ** (-4.0 / closest)
    remaining = min(closest, n_heads - closest)
    slopes = [base_ratio ** (i + 1) for i in range(closest)]
    return slopes + [extra_ratio ** (2 * i + 1) for i in range(remaining)]


def dot(a, b, ca, cb):
    return lax.dot_general(a, b, (((ca,), (cb,)), ((), ())), preferred_element_type=F32)


def gelu_parts(u):
    k = math.sqrt(2.0 / math.pi)
    u2 = u * u
    th = jnp.tanh(u * (k + (k * 0.044715) * u2))
    half = 0.5 + 0.5 * th
    val = u * half
    return val, half + val * (1.0 - th) * (k + (3.0 * 0.044715 * k) * u2)


def rows_stats(v):
    mean = jnp.mean(v, axis=-1, keepdims=True)
    cen = v - mean
    var = jnp.mean(cen * cen, axis=-1, keepdims=True)
    return cen, lax.rsqrt(var + EPS)


def places():
    t = lax.axis_index('tp')
    core = t % 2
    pt = t + 1 - 2 * core
    ct = TP - 1 - t
    qt = TP - 1 - pt
    half = (core + t // 2) % 2
    return t, pt, ct, qt, half


def sender(ssem, rsem):
    started = []

    def send(src, dst, dev):
        i = len(started)
        c = pltpu.make_async_remote_copy(src_ref=src, dst_ref=dst, send_sem=ssem.at[i], recv_sem=rsem.at[i],
                                         device_id={'tp': dev}, device_id_type=MESH)
        c.start()
        started.append(c)
        return c

    return send, started


def columns(start, width):
    return pl.ds(start if isinstance(start, int) else pl.multiple_of(start, 128), width)


def head_rows(h, e):
    return slice((h * 3 + e) * HD, (h * 3 + e + 1) * HD)


def row_blocks(buf, cols, v):
    for i in range(TP):
        buf[i, :, cols] = v[i * SL:(i + 1) * SL, :].astype(BF)


def block_kernel(x_hbm, gy_hbm, g1_hbm, be1_hbm, g2_hbm, be2_hbm, bo_hbm, bd_hbm, bqkv_hbm, bup_hbm,
                 wqkv_hbm, wout_hbm, wup_hbm, wdn_hbm,
                 y_ref, vec_ref, gwup_ref, gwdn_ref, gqkv_ref, h_ref, ctx_ref, gmid_ref, mine_ref, xh_ref, gm_ref, rs_ref, g1_out, r_hs, ln_hs,
                 wqkv, wout, xf, gm_f, gg_f, xhat, rstd_s, probs, qkvT, par, mp,
                 wup, wdn, xg, gyg, biasT, a_ps, a_pr, a_hs, a_hr, a_cr, a_fr, b_ps, b_pr, b_hs, b_hr, b_cr, b_fr,
                 gact, g_ref, gpre_ref, act_ref, gyf_ref, bqkv_ref, g1_in, be1_in, g2_in, be2_in, bo_in, bd_in, bup_in,
                 rp, m_pr, m_hs, m_cr, r_pr, ln_x, xh2, rstd2, a_un, b_un,
                 wsem, ssem, rsem, isem):
    t, pt, ct, qt, half = places()
    send, started = sender(ssem, rsem)

    in_x = pltpu.make_async_copy(x_hbm, xg.at[t], isem.at[0])
    in_gy = pltpu.make_async_copy(gy_hbm, gyg.at[t], isem.at[1])
    in_b = pltpu.make_async_copy(bqkv_hbm, bqkv_ref, isem.at[2])
    small = ((g1_hbm, g1_in), (be1_hbm, be1_in), (g2_hbm, g2_in), (be2_hbm, be2_in), (bo_hbm, bo_in), (bd_hbm, bd_in), (bup_hbm, bup_in))
    in_p = [pltpu.make_async_copy(a, b, isem.at[3 + i]) for i, (a, b) in enumerate(small)]
    for c in (in_x, in_gy, in_b, *in_p):
        c.start()
    w_cps = {}
    w_cps['qkv'] = [pltpu.make_async_copy(wqkv_hbm, wqkv, wsem.at[0])]
    w_cps['out'] = [pltpu.make_async_copy(wout_hbm.at[:, pl.ds(k * HW, HW)], wout.at[k], wsem.at[1 + k]) for k in range(2)]
    w_cps['dn'] = [pltpu.make_async_copy(wdn_hbm, wdn, wsem.at[7])]
    w_cps['up'] = [pltpu.make_async_copy(wup_hbm, wup, wsem.at[8])]

    barrier = pltpu.get_barrier_semaphore()
    for dev in (pt, ct, qt):
        pl.semaphore_signal(barrier, inc=1, device_id={'tp': dev}, device_id_type=MESH)
    for name in ('qkv', 'out', 'dn', 'up'):
        for c in w_cps[name]:
            c.start()
    pl.semaphore_wait(barrier, 3)

    in_x.wait()
    x_c = send(xg.at[t], xg.at[t], ct)
    x_p = send(xg.at[t], xg.at[t], pt)

    for c in (in_b, *in_p):
        c.wait()
    for i, r in enumerate((g1_in, be1_in, g2_in, be2_in, bo_in, bd_in, bup_in)):
        par[i, :] = r[...]
    g1_ref, be1_ref, g2_ref, be2_ref, bo_ref, bd_ref, bup_ref = (par.at[i:i + 1] for i in range(7))

    for h in range(HL):
        for e in range(3):
            row = jnp.broadcast_to(bqkv_ref[e, h:h + 1, :], (S, HD))
            biasT[pl.ds((h * 3 + e) * HD, HD), :] = row.T

    x_c.wait_recv()
    x_f = send(xg.at[ct], xg.at[ct], pt)
    in_gy.wait()
    y_c = send(gyg.at[t], gyg.at[t], ct)
    y_p = send(gyg.at[t], gyg.at[t], pt)
    x_p.wait_recv()
    x_f.wait_recv()

    for i in range(TP):
        xf[pl.ds(i * SL, SL), :] = xg[i].astype(F32)
    for r in range(0, S, 32):
        cen, rstd = rows_stats(xf[r:r + 32, :])
        xh = cen * rstd
        xhat[r:r + 32, :] = xh
        rstd_s[r:r + 32, :] = jnp.broadcast_to(rstd, (32, 128))
        h_ref[r:r + 32, :] = (xh * g1_ref[...] + be1_ref[...]).astype(BF)

    w_cps['qkv'][0].wait()
    hv = h_ref[...]
    for h in range(HL):
        rows = slice(h * 3 * HD, (h + 1) * 3 * HD)
        qkvT[rows, :] = (dot(wqkv[rows, :], hv, 1, 1) + biasT[rows, :]).astype(BF)

    scale = HD ** -0.5
    slopes = alibi_slopes(HL * TP)
    j_pos = lax.broadcasted_iota(jnp.int32, (S, S), 0)
    i_pos = lax.broadcasted_iota(jnp.int32, (S, S), 1)
    causal = j_pos <= i_pos
    j_f = j_pos.astype(F32)

    def head(h, e):
        return qkvT[head_rows(h, e), :]

    for h in range(HL):
        slope = jnp.where(t == 0, slopes[h], jnp.where(t == 1, slopes[HL + h], jnp.where(t == 2, slopes[2 * HL + h], slopes[3 * HL + h]))).astype(F32)
        s = dot(head(h, 1), head(h, 0), 0, 0) * scale + slope * j_f
        s = jnp.where(causal, s, MASK_VALUE)
        p = jnp.exp(s - jnp.max(s, axis=0, keepdims=True))
        p = p / jnp.sum(p, axis=0, keepdims=True)
        probs[h] = p
        ctx_ref[h * HD:(h + 1) * HD, :] = dot(head(h, 2), p.astype(BF), 1, 0).astype(BF)

    def exchange(part, groups, ps, pr, hs, hr, cr, fr, un):
        firsts = []
        for k0, k1 in groups:
            cols = slice(CUT[k0], CUT[k1])
            ps[:, cols] = part(1 - half, CUT[k0], CUT[k1]).astype(BF)
            firsts.append(send(ps.at[:, cols], pr.at[:, cols], pt))
            if k0 == 0:
                for hh in range(2):
                    un[0, hh] = part(hh, 0, UW).astype(BF)
                early = [send(un.at[0], un.at[2], ct), send(un.at[0], un.at[1], pt)]
        outs = []
        for (k0, k1), first in zip(groups, firsts):
            cols = slice(CUT[k0], CUT[k1])
            ours = part(half, CUT[k0], CUT[k1])
            first.wait_recv()
            hs[:, cols] = (ours + pr[:, cols].astype(F32)).astype(BF)
            for k in range(k0, k1):
                c = slice(CUT[k], CUT[k + 1])
                outs.append([send(hs.at[:, c], cr.at[:, c], ct)])
                if k == NCUT - 1:
                    outs[-1].append(send(hs.at[:, c], fr.at[:, c], qt))
        local = send(hs.at[:, UW:], hr.at[:, UW:], pt)
        return outs, local, early

    def early_arrived(early, un):
        early[0].wait_recv()
        early.append(send(un.at[2], un.at[3], pt))

    def early_added(early, un, put):
        early[1].wait_recv()
        early[2].wait_recv()
        for hh in range(2):
            chips = [un[k, hh].astype(F32) + un[k + 1, hh].astype(F32) for k in (0, 2)]
            put(hh * HW, UW, (chips[0] + chips[1]).astype(BF).astype(F32))

    def arrived(out, k, hs, cr, fr, put):
        c = slice(CUT[k], CUT[k + 1])
        out[0].wait_recv()
        if k < NCUT - 1:
            out.append(send(cr.at[:, c], fr.at[:, c], pt))
        put(half * HW + CUT[k], CUT[k + 1] - CUT[k], (hs[:, c].astype(F32) + cr[:, c].astype(F32)).astype(BF).astype(F32))

    def passed_on(outs, local, hr, fr, put):
        local.wait_recv()
        for k, out in enumerate(outs):
            c = slice(CUT[k], CUT[k + 1])
            out[1].wait_recv()
            put((1 - half) * HW + CUT[k], CUT[k + 1] - CUT[k], (hr[:, c].astype(F32) + fr[:, c].astype(F32)).astype(BF).astype(F32))

    for c in w_cps['out']:
        c.wait()
    ctxT = ctx_ref[...]
    a_outs, a_local, a_early = exchange(lambda hh, c0, c1: dot(ctxT, wout[hh, :, c0:c1], 0, 0), ((0, NCUT),), a_ps, a_pr, a_hs, a_hr, a_cr, a_fr, a_un)

    y_c.wait_recv()
    y_f = send(gyg.at[ct], gyg.at[ct], pt)
    y_p.wait_recv()
    y_f.wait_recv()
    for i in range(TP):
        gm_f[pl.ds(i * SL, SL), :] = gyg[i].astype(F32)
    for r in range(0, S, 32):
        gyf_ref[r:r + 32, :] = gm_f[r:r + 32, :].astype(BF)
    w_cps['dn'][0].wait()
    gyv = gyf_ref[...]
    for n in range(NCH):
        gact[:, n * CW:(n + 1) * CW] = dot(gyv, wdn[n * CW:(n + 1) * CW, :], 1, 1).astype(BF)
    vec_ref[0:1, :] = jnp.sum(gm_f[...], axis=0, keepdims=True)

    def put_x(start, width, val):
        cols = columns(start, width)
        xf[:, cols] = xf[:, cols] + val + bo_ref[:, cols]

    early_arrived(a_early, a_un)
    for k, out in enumerate(a_outs):
        arrived(out, k, a_hs, a_cr, a_fr, put_x)
    early_added(a_early, a_un, put_x)
    passed_on(a_outs, a_local, a_hr, a_fr, put_x)

    for r in range(0, S, 32):
        cen, rstd = rows_stats(xf[r:r + 32, :])
        xh = cen * rstd
        xh2[r:r + 32, :] = xh
        rstd2[r:r + 32, :] = jnp.broadcast_to(rstd, (32, 128))
        g_ref[r:r + 32, :] = (xh * g2_ref[...] + be2_ref[...]).astype(BF)

    w_cps['up'][0].wait()
    gv = g_ref[...]
    for n in range(NCH):
        cols = slice(n * CW, (n + 1) * CW)
        pre = dot(gv, wup[:, cols], 1, 0) + bup_ref[:, cols]
        val, der = gelu_parts(pre)
        act_ref[:, cols] = val.astype(BF)
        gp = gact[:, cols].astype(F32) * der
        vec_ref[1:2, cols] = jnp.sum(gp, axis=0, keepdims=True)
        gpre_ref[:, cols] = gp.astype(BF)

    gprev = gpre_ref[...]

    def part_g(hh, c0, c1):
        return dot(gprev, wup[columns(hh * HW + c0, c1 - c0), :], 1, 1)

    g_outs, g_local, g_early = exchange(part_g, ((0, 1), (1, NCUT)), b_ps, b_pr, b_hs, b_hr, b_cr, b_fr, b_un)

    actv = act_ref[...]
    for n in range(NCH):
        cols = slice(n * CW, (n + 1) * CW)
        row_blocks(mp, cols, dot(actv, wdn[:, cols], 1, 0))
    m_first = (send(mp.at[qt], m_pr.at[1], pt), send(mp.at[pt], m_pr.at[0], pt))
    for n in range(NCH):
        gwdn_ref[n * CW:(n + 1) * CW, :] = dot(act_ref[:, n * CW:(n + 1) * CW], gyv, 0, 0).astype(BF)
    def put_g(start, width, val):
        gg_f[:, columns(start, width)] = val

    early_arrived(g_early, b_un)
    for n in range(NCH):
        gwup_ref[n * CW:(n + 1) * CW, :] = dot(g_ref[:, n * CW:(n + 1) * CW], gprev, 0, 0).astype(BF)
        if n % 2:
            arrived(g_outs[n // 2], n // 2, b_hs, b_cr, b_fr, put_g)
    early_added(g_early, b_un, put_g)

    m_first[0].wait_recv()
    m_hs[...] = (mp[ct].astype(F32) + m_pr[1].astype(F32)).astype(BF)
    m_out = send(m_hs, m_cr, ct)

    passed_on(g_outs, g_local, b_hr, b_fr, put_g)

    for r in range(0, S, 32):
        xh = xh2[r:r + 32, :]
        dxh = gg_f[r:r + 32, :] * g2_ref[...]
        m1 = jnp.mean(dxh, axis=-1, keepdims=True)
        m2 = jnp.mean(dxh * xh, axis=-1, keepdims=True)
        gm = gm_f[r:r + 32, :] + rstd2[r:r + 32, 0:1] * (dxh - m1 - xh * m2)
        gm_f[r:r + 32, :] = gm
        gmid_ref[r:r + 32, :] = gm.astype(BF)

    gmv = gmid_ref[...]
    gctxT = (dot(wout[0], gmv[:, :HW], 1, 1) + dot(wout[1], gmv[:, HW:], 1, 1)).astype(BF)
    heads = range(HL)
    gos = [gctxT[h * HD:(h + 1) * HD, :] for h in heads]
    gps = [dot(head(h, 2), gos[h], 0, 0).astype(BF).astype(F32) for h in heads]
    gvs = [dot(gos[h], probs[h].astype(BF), 1, 1).astype(BF) for h in heads]
    gss = [(probs[h] * (gps[h] - jnp.sum(gps[h] * probs[h], axis=0, keepdims=True))).astype(BF) for h in heads]
    gqs = [(dot(head(h, 1), gss[h], 1, 0) * scale).astype(BF) for h in heads]
    gks = [(dot(head(h, 0), gss[h], 1, 1) * scale).astype(BF) for h in heads]
    for h in heads:
        for e, val in enumerate((gqs[h], gks[h], gvs[h])):
            gqkv_ref[head_rows(h, e), :] = val

    gqv = gqkv_ref[...]
    r_first = []
    for n in range(NCH):
        row_blocks(rp.at[n // HCH], slice(n % HCH * CW, (n % HCH + 1) * CW), dot(gqv, wqkv[:, n * CW:(n + 1) * CW], 0, 0))
    for k in range(2):
        r_first.append((send(rp.at[k, qt], r_pr.at[k, 1], pt), send(rp.at[k, pt], r_pr.at[k, 0], pt)))

    ln_s, ln_pr = ln_x.at[0], ln_x.at[1]
    for k in range(2):
        cols = slice(k * HW, (k + 1) * HW)
        gg1 = jnp.zeros((1, HW), F32)
        gb1 = jnp.zeros((1, HW), F32)
        for i in range(TP):
            v = rp[k, i].astype(F32)
            gg1 = gg1 + jnp.sum(v * xhat[i * SL:(i + 1) * SL, cols], axis=0, keepdims=True)
            gb1 = gb1 + jnp.sum(v, axis=0, keepdims=True)
        ln_s[0:1, cols] = gg1
        ln_s[1:2, cols] = gb1
    l_first = send(ln_s, ln_pr, pt)

    vec_ref[2:3, :] = jnp.sum(gg_f[...] * xh2[...], axis=0, keepdims=True)
    vec_ref[3:4, :] = jnp.sum(gg_f[...], axis=0, keepdims=True)
    vec_ref[4:5, :] = jnp.sum(gm_f[...], axis=0, keepdims=True)

    own = pl.ds(pl.multiple_of(t * SL, 8), SL)
    xh_ref[...] = xhat[own, :]
    gm_ref[...] = gm_f[own, :]
    rs_ref[...] = rstd_s[own, :]
    g1_out[...] = par[0:1, :]

    for k in range(2):
        cols = slice(k * HW, (k + 1) * HW)
        r_first[k][0].wait_recv()
        r_hs[0:SL, cols] = (rp[k, ct].astype(F32) + r_pr[k, 1].astype(F32)).astype(BF)
        r_first[k][1].wait_recv()
        mine_ref[:, cols] = (rp[k, t].astype(F32) + r_pr[k, 0].astype(F32)).astype(BF)
    l_first.wait_recv()
    ln = ln_s[...] + ln_pr[...]
    ln_hs[...] = ln
    ln_rows = []
    for _ in range(3):
        ln_rows.append(ln.astype(BF).astype(F32))
        ln = ln - ln_rows[-1]
    r_hs[SL:SL + 8, :] = jnp.concatenate(ln_rows + [jnp.zeros((2, D), F32)], axis=0).astype(BF)
    m_first[1].wait_recv()
    m_out.wait_recv()
    m_sum = (mp[t].astype(F32) + m_pr[0].astype(F32)).astype(BF).astype(F32) + m_cr[...].astype(F32)
    y_ref[...] = (xf[own, :] + m_sum.astype(BF).astype(F32) + bd_ref[...]).astype(BF)
    for c in started:
        c.wait_send()


N_SEND = 37
VMEM_A = 36 * 2**20
VMEM_B = 8 * 2**20
VMEM_C = 4 * 2**20


def write_kernel(yi_ref, vec_ref, up_ref, dn_ref, gqkv_ref, h_ref, ctx_ref, gmid_ref,
                 y_ref, gwqkv_ref, gbqkv_ref, gwout_ref, gbo_ref, gl2_ref, bl2_ref, gwup_ref, gbup_ref, gwdn_ref, gbd_ref,
                 s_qkv, s_out, s_gb, s0, s1, s2, s3, s4, sem):
    cps = []

    def out(src, dst, n=1):
        rows = src.shape[0] // n
        for k in range(n):
            c = pltpu.make_async_copy(src.at[pl.ds(k * rows, rows)], dst.at[pl.ds(k * rows, rows)], sem.at[len(cps)])
            c.start()
            cps.append(c)

    out(dn_ref, gwdn_ref, 4)
    out(up_ref, gwup_ref, 4)
    out(yi_ref, y_ref)
    for i, (sv, r) in enumerate(((s0, gbd_ref), (s1, gbup_ref), (s2, gl2_ref), (s3, bl2_ref), (s4, gbo_ref))):
        sv[...] = vec_ref[i, :]
        out(sv, r)
    ones = jnp.ones((8, S), BF)
    for h in range(HL):
        for e in range(3):
            s_gb[e, h:h + 1, :] = dot(ones, gqkv_ref[head_rows(h, e), :], 1, 1)[0:1, :]
    out(s_gb, gbqkv_ref)
    hv = h_ref[...]
    s_out[...] = dot(ctx_ref[...], gmid_ref[...], 1, 0).astype(BF)
    out(s_out, gwout_ref)
    for n in range(HL):
        rows = slice(n * 3 * HD, (n + 1) * 3 * HD)
        s_qkv[rows, :] = dot(gqkv_ref[rows, :], hv, 1, 0).astype(BF)
        out(s_qkv.at[rows], gwqkv_ref.at[rows])
    for c in cps:
        c.wait()


def last_kernel(mine_ref, xh_ref, gm_ref, rs_ref, g1_ref, rc_ref, ln_ref, gx_hbm, gl1_hbm, bl1_hbm, gx_ref, gl1_ref, bl1_ref, sem):
    lc = rc_ref[SL:SL + 8, :].astype(F32)
    ln = ln_ref[...] + (lc[0:2, :] + lc[2:4, :] + lc[4:6, :])
    gl1_ref[...] = ln[0, :]
    bl1_ref[...] = ln[1, :]
    cps = [pltpu.make_async_copy(gl1_ref, gl1_hbm, sem.at[0]), pltpu.make_async_copy(bl1_ref, bl1_hbm, sem.at[1]),
           pltpu.make_async_copy(gx_ref, gx_hbm, sem.at[2])]
    cps[0].start()
    cps[1].start()

    gh = (mine_ref[...].astype(F32) + rc_ref[0:SL, :].astype(F32)).astype(BF).astype(F32)
    xh = xh_ref[...]
    dxh = gh * g1_ref[...]
    m1 = jnp.mean(dxh, axis=-1, keepdims=True)
    m2 = jnp.mean(dxh * xh, axis=-1, keepdims=True)
    gx_ref[...] = (gm_ref[...] + rs_ref[:, 0:1] * (dxh - m1 - xh * m2)).astype(BF)
    cps[2].start()
    for c in cps:
        c.wait()


def solution(mesh):
    VM = pl.BlockSpec(memory_space=pltpu.VMEM)
    ANY = pl.BlockSpec(memory_space=pltpu.HBM)

    def sds(shape, dt):
        return jax.ShapeDtypeStruct(shape, dt)

    def local_step(x, g1, be1, w_qkv, b_qkv, w_out, b_out, g2, be2, w_up, b_up, w_down, b_down, grad_y):
        wq = jnp.transpose(w_qkv, (1, 2, 3, 0)).reshape(3 * HL * HD, D)
        bq = jnp.transpose(b_qkv, (1, 0, 2))
        part = pltpu.VMEM((S, HW), BF)
        vec1 = sds((D,), F32)
        mids = pl.pallas_call(
            block_kernel,
            out_shape=(pltpu.VMEM((SL, D), BF), pltpu.VMEM((8, D), F32), pltpu.VMEM((D, FL), BF), pltpu.VMEM((FL, D), BF),
                       pltpu.VMEM((3 * HL * HD, S), BF), pltpu.VMEM((S, D), BF), pltpu.VMEM((HL * HD, S), BF), pltpu.VMEM((S, D), BF),
                       pltpu.VMEM((SL, D), BF), pltpu.VMEM((SL, D), F32), pltpu.VMEM((SL, D), F32), pltpu.VMEM((SL, 128), F32),
                       pltpu.VMEM((1, D), F32), sds((SL + 8, D), BF), pltpu.VMEM((2, D), F32)),
            in_specs=[ANY] * 14,
            out_specs=(VM,) * 15,
            scratch_shapes=[
                pltpu.VMEM((3 * HL * HD, D), BF), pltpu.VMEM((2, HL * HD, HW), BF), pltpu.VMEM((S, D), F32), pltpu.VMEM((S, D), F32),
                pltpu.VMEM((S, D), F32), pltpu.VMEM((S, D), F32), pltpu.VMEM((S, 128), F32), pltpu.VMEM((HL, S, S), F32),
                pltpu.VMEM((3 * HL * HD, S), BF), pltpu.VMEM((8, D), F32), pltpu.VMEM((TP, SL, D), BF),
                pltpu.VMEM((D, FL), BF), pltpu.VMEM((FL, D), BF), pltpu.VMEM((TP, SL, D), BF), pltpu.VMEM((TP, SL, D), BF),
                pltpu.VMEM((3 * HL * HD, S), F32), *[part] * 12,
                pltpu.VMEM((S, FL), BF), pltpu.VMEM((S, D), BF), pltpu.VMEM((S, FL), BF), pltpu.VMEM((S, FL), BF), pltpu.VMEM((S, D), BF),
                pltpu.VMEM((3, HL, HD), F32), *[pltpu.VMEM((D,), F32) for _ in range(7)],
                pltpu.VMEM((2, TP, SL, HW), BF), pltpu.VMEM((2, SL, D), BF), pltpu.VMEM((SL, D), BF), pltpu.VMEM((SL, D), BF),
                pltpu.VMEM((2, 2, SL, HW), BF), pltpu.VMEM((2, 2, D), F32), pltpu.VMEM((S, D), F32), pltpu.VMEM((S, 128), F32),
                pltpu.VMEM((4, 2, S, UW), BF), pltpu.VMEM((4, 2, S, UW), BF),
                pltpu.SemaphoreType.DMA((9,)), pltpu.SemaphoreType.DMA((N_SEND,)), pltpu.SemaphoreType.DMA((N_SEND,)),
                pltpu.SemaphoreType.DMA((10,)),
            ],
            compiler_params=pltpu.CompilerParams(collective_id=0, has_side_effects=True, vmem_limit_bytes=VMEM_A),
            name='block',
        )(*(pltpu.with_memory_space_constraint(v, pltpu.HBM) for v in (
            x.reshape(SL, D), grad_y.reshape(SL, D), g1, be1, g2, be2, b_out, b_down, bq, b_up, wq, w_out, w_up, w_down)))
        mine, xh, gm, rs, g1v, r_hs, ln_hs = mids[8:]
        across = [(i, TP - 1 - i) for i in range(TP)]
        r_cr = lax.ppermute(r_hs, 'tp', across)
        y, gwqkv, gbqkv, gwout, gbo, gl2, bl2, gwup, gbup, gwdn, gbd = pl.pallas_call(
            write_kernel,
            out_shape=(sds((SL, D), BF), sds((3 * HL * HD, D), BF), sds((3, HL, HD), F32), sds((HL * HD, D), BF), vec1, vec1, vec1,
                       sds((D, FL), BF), vec1, sds((FL, D), BF), vec1),
            in_specs=[VM] * 8,
            out_specs=(ANY,) * 11,
            scratch_shapes=[pltpu.VMEM((3 * HL * HD, D), BF), pltpu.VMEM((HL * HD, D), BF), pltpu.VMEM((3, HL, HD), F32),
                            *[pltpu.VMEM((D,), F32) for _ in range(5)], pltpu.SemaphoreType.DMA((20,))],
            compiler_params=pltpu.CompilerParams(vmem_limit_bytes=VMEM_B),
            cost_estimate=pl.CostEstimate(flops=600_000_000, bytes_accessed=14_200_000, transcendentals=0),
            name='write',
        )(*mids[:8])
        gx, gl1, bl1 = pl.pallas_call(
            last_kernel,
            out_shape=(sds((SL, D), BF), vec1, vec1),
            in_specs=[VM] * 7,
            out_specs=(ANY,) * 3,
            scratch_shapes=[pltpu.VMEM((SL, D), BF), pltpu.VMEM((D,), F32), pltpu.VMEM((D,), F32), pltpu.SemaphoreType.DMA((3,))],
            compiler_params=pltpu.CompilerParams(vmem_limit_bytes=VMEM_C),
            name='last',
        )(mine, xh, gm, rs, g1v, r_cr, ln_hs)
        gwqkv = jnp.transpose(gwqkv.reshape(HL, 3, HD, D), (3, 0, 1, 2))
        gbqkv = jnp.transpose(gbqkv, (1, 0, 2))
        return (y.reshape(1, SL, D), gx.reshape(1, SL, D), gl1, bl1, gwqkv, gbqkv, gwout, gbo, gl2, bl2, gwup, gbup, gwdn, gbd)

    row_spec = P('dp', 'tp', None)
    in_specs = (row_spec, P(), P(), P(None, 'tp', None, None), P('tp', None, None), P('tp', None), P(), P(), P(),
                P(None, 'tp'), P('tp'), P('tp', None), P(), row_spec)
    out_specs = (row_spec, row_spec, P('dp'), P('dp'), P('dp', 'tp', None, None), P(('dp', 'tp'), None, None),
                 P(('dp', 'tp'), None), P('dp'), P('dp'), P('dp'), P('dp', 'tp'), P(('dp', 'tp')), P(('dp', 'tp'), None), P('dp'))
    return jax.shard_map(local_step, mesh=mesh, in_specs=in_specs, out_specs=out_specs, check_vma=False)
```

```python
import functools
import math

import jax
import jax.numpy as jnp
from jax import lax
from jax.experimental import pallas as pl
from jax.experimental.pallas import tpu as pltpu
from jax.sharding import PartitionSpec as P

EPS = 1e-5
MASK_VALUE = -1e30
BF = jnp.bfloat16
F32 = jnp.float32
MESH = pl.DeviceIdType.MESH

D = 1536
S = 96
SL = 24
TP = 4
HL = 4
HD = 96
FL = 1536
CW = 256
NCH = D // CW
HCH = NCH // 2
HW = D // 2
UW = 128
CUT = (128, 384, 640, 768)
NCUT = len(CUT) - 1


def alibi_slopes(n_heads):
    closest = 2 ** int(math.floor(math.log2(n_heads)))
    base_ratio = 2.0 ** (-8.0 / closest)
    extra_ratio = 2.0 ** (-4.0 / closest)
    remaining = min(closest, n_heads - closest)
    slopes = [base_ratio ** (i + 1) for i in range(closest)]
    return slopes + [extra_ratio ** (2 * i + 1) for i in range(remaining)]


def dot(a, b, ca, cb):
    return lax.dot_general(a, b, (((ca,), (cb,)), ((), ())), preferred_element_type=F32)


def gelu_parts(u):
    k = math.sqrt(2.0 / math.pi)
    u2 = u * u
    th = jnp.tanh(u * (k + (k * 0.044715) * u2))
    half = 0.5 + 0.5 * th
    val = u * half
    return val, half + val * (1.0 - th) * (k + (3.0 * 0.044715 * k) * u2)


def rows_stats(v):
    mean = jnp.mean(v, axis=-1, keepdims=True)
    cen = v - mean
    var = jnp.mean(cen * cen, axis=-1, keepdims=True)
    return cen, lax.rsqrt(var + EPS)


def places():
    t = lax.axis_index('tp')
    core = t % 2
    pt = t + 1 - 2 * core
    ct = TP - 1 - t
    qt = TP - 1 - pt
    half = (core + t // 2) % 2
    return t, pt, ct, qt, half


def sender(ssem, rsem):
    started = []

    def send(src, dst, dev):
        i = len(started)
        c = pltpu.make_async_remote_copy(src_ref=src, dst_ref=dst, send_sem=ssem.at[i], recv_sem=rsem.at[i],
                                         device_id={'tp': dev}, device_id_type=MESH)
        c.start()
        started.append(c)
        return c

    return send, started


def columns(start, width):
    return pl.ds(start if isinstance(start, int) else pl.multiple_of(start, 128), width)


def head_rows(h, e):
    return slice((h * 3 + e) * HD, (h * 3 + e + 1) * HD)


def row_blocks(buf, cols, v):
    for i in range(TP):
        buf[i, :, cols] = v[i * SL:(i + 1) * SL, :].astype(BF)


def block_kernel(x_hbm, gy_hbm, g1_hbm, be1_hbm, g2_hbm, be2_hbm, bo_hbm, bd_hbm, bqkv_hbm, bup_hbm,
                 wqkv_hbm, wout_hbm, wup_hbm, wdn_hbm,
                 y_ref, vec_ref, gwup_ref, gwdn_ref, gqkv_ref, h_ref, ctx_ref, gmid_ref, mine_ref, xh_ref, gm_ref, rs_ref, g1_out, r_hs, ln_hs,
                 wqkv, wout, xf, gm_f, gg_f, xhat, rstd_s, probs, qkvT, par, mp,
                 wup, wdn, xg, gyg, biasT, a_ps, a_pr, a_hs, a_hr, a_cr, a_fr, b_ps, b_pr, b_hs, b_hr, b_cr, b_fr,
                 gact, g_ref, gpre_ref, act_ref, gyf_ref, bqkv_ref, g1_in, be1_in, g2_in, be2_in, bo_in, bd_in, bup_in,
                 rp, m_pr, m_hs, m_cr, r_pr, ln_x, xh2, rstd2, a_un, b_un,
                 wsem, ssem, rsem, isem):
    t, pt, ct, qt, half = places()
    send, started = sender(ssem, rsem)

    in_x = pltpu.make_async_copy(x_hbm, xg.at[t], isem.at[0])
    in_gy = pltpu.make_async_copy(gy_hbm, gyg.at[t], isem.at[1])
    in_b = pltpu.make_async_copy(bqkv_hbm, bqkv_ref, isem.at[2])
    small = ((g1_hbm, g1_in), (be1_hbm, be1_in), (g2_hbm, g2_in), (be2_hbm, be2_in), (bo_hbm, bo_in), (bd_hbm, bd_in), (bup_hbm, bup_in))
    in_p = [pltpu.make_async_copy(a, b, isem.at[3 + i]) for i, (a, b) in enumerate(small)]
    for c in (in_x, in_gy, in_b, *in_p):
        c.start()
    w_cps = {}
    w_cps['qkv'] = [pltpu.make_async_copy(wqkv_hbm, wqkv, wsem.at[0])]
    w_cps['out'] = [pltpu.make_async_copy(wout_hbm.at[:, pl.ds(k * HW, HW)], wout.at[k], wsem.at[1 + k]) for k in range(2)]
    w_cps['dn'] = [pltpu.make_async_copy(wdn_hbm, wdn, wsem.at[7])]
    w_cps['up'] = [pltpu.make_async_copy(wup_hbm, wup, wsem.at[8])]

    barrier = pltpu.get_barrier_semaphore()
    for dev in (pt, ct, qt):
        pl.semaphore_signal(barrier, inc=1, device_id={'tp': dev}, device_id_type=MESH)
    for name in ('qkv', 'out', 'dn', 'up'):
        for c in w_cps[name]:
            c.start()
    pl.semaphore_wait(barrier, 3)

    in_x.wait()
    x_c = send(xg.at[t], xg.at[t], ct)
    x_p = send(xg.at[t], xg.at[t], pt)

    for c in (in_b, *in_p):
        c.wait()
    for i, r in enumerate((g1_in, be1_in, g2_in, be2_in, bo_in, bd_in, bup_in)):
        par[i, :] = r[...]
    g1_ref, be1_ref, g2_ref, be2_ref, bo_ref, bd_ref, bup_ref = (par.at[i:i + 1] for i in range(7))

    for h in range(HL):
        for e in range(3):
            row = jnp.broadcast_to(bqkv_ref[e, h:h + 1, :], (S, HD))
            biasT[pl.ds((h * 3 + e) * HD, HD), :] = row.T

    x_c.wait_recv()
    x_f = send(xg.at[ct], xg.at[ct], pt)
    in_gy.wait()
    y_c = send(gyg.at[t], gyg.at[t], ct)
    y_p = send(gyg.at[t], gyg.at[t], pt)
    x_p.wait_recv()
    x_f.wait_recv()

    for i in range(TP):
        xf[pl.ds(i * SL, SL), :] = xg[i].astype(F32)
    for r in range(0, S, 32):
        cen, rstd = rows_stats(xf[r:r + 32, :])
        xh = cen * rstd
        xhat[r:r + 32, :] = xh
        rstd_s[r:r + 32, :] = jnp.broadcast_to(rstd, (32, 128))
        h_ref[r:r + 32, :] = (xh * g1_ref[...] + be1_ref[...]).astype(BF)

    w_cps['qkv'][0].wait()
    hv = h_ref[...]
    for h in range(HL):
        rows = slice(h * 3 * HD, (h + 1) * 3 * HD)
        qkvT[rows, :] = (dot(wqkv[rows, :], hv, 1, 1) + biasT[rows, :]).astype(BF)

    scale = HD ** -0.5
    slopes = alibi_slopes(HL * TP)
    j_pos = lax.broadcasted_iota(jnp.int32, (S, S), 0)
    i_pos = lax.broadcasted_iota(jnp.int32, (S, S), 1)
    causal = j_pos <= i_pos
    j_f = j_pos.astype(F32)

    def head(h, e):
        return qkvT[head_rows(h, e), :]

    for h in range(HL):
        slope = jnp.where(t == 0, slopes[h], jnp.where(t == 1, slopes[HL + h], jnp.where(t == 2, slopes[2 * HL + h], slopes[3 * HL + h]))).astype(F32)
        s = dot(head(h, 1), head(h, 0), 0, 0) * scale + slope * j_f
        s = jnp.where(causal, s, MASK_VALUE)
        p = jnp.exp(s - jnp.max(s, axis=0, keepdims=True))
        p = p / jnp.sum(p, axis=0, keepdims=True)
        probs[h] = p
        ctx_ref[h * HD:(h + 1) * HD, :] = dot(head(h, 2), p.astype(BF), 1, 0).astype(BF)

    def exchange(part, groups, ps, pr, hs, hr, cr, fr, un):
        firsts = []
        for k0, k1 in groups:
            cols = slice(CUT[k0], CUT[k1])
            ps[:, cols] = part(1 - half, CUT[k0], CUT[k1]).astype(BF)
            firsts.append(send(ps.at[:, cols], pr.at[:, cols], pt))
            if k0 == 0:
                for hh in range(2):
                    un[0, hh] = part(hh, 0, UW).astype(BF)
                early = [send(un.at[0], un.at[2], ct), send(un.at[0], un.at[1], pt)]
        outs = []
        for (k0, k1), first in zip(groups, firsts):
            cols = slice(CUT[k0], CUT[k1])
            ours = part(half, CUT[k0], CUT[k1])
            first.wait_recv()
            hs[:, cols] = (ours + pr[:, cols].astype(F32)).astype(BF)
            for k in range(k0, k1):
                c = slice(CUT[k], CUT[k + 1])
                outs.append([send(hs.at[:, c], cr.at[:, c], ct)])
                if k == NCUT - 1:
                    outs[-1].append(send(hs.at[:, c], fr.at[:, c], qt))
        local = send(hs.at[:, UW:], hr.at[:, UW:], pt)
        return outs, local, early

    def early_arrived(early, un):
        early[0].wait_recv()
        early.append(send(un.at[2], un.at[3], pt))

    def early_added(early, un, put):
        early[1].wait_recv()
        early[2].wait_recv()
        for hh in range(2):
            chips = [un[k, hh].astype(F32) + un[k + 1, hh].astype(F32) for k in (0, 2)]
            put(hh * HW, UW, (chips[0] + chips[1]).astype(BF).astype(F32))

    def arrived(out, k, hs, cr, fr, put):
        c = slice(CUT[k], CUT[k + 1])
        out[0].wait_recv()
        if k < NCUT - 1:
            out.append(send(cr.at[:, c], fr.at[:, c], pt))
        put(half * HW + CUT[k], CUT[k + 1] - CUT[k], (hs[:, c].astype(F32) + cr[:, c].astype(F32)).astype(BF).astype(F32))

    def passed_on(outs, local, hr, fr, put):
        local.wait_recv()
        for k, out in enumerate(outs):
            c = slice(CUT[k], CUT[k + 1])
            out[1].wait_recv()
            put((1 - half) * HW + CUT[k], CUT[k + 1] - CUT[k], (hr[:, c].astype(F32) + fr[:, c].astype(F32)).astype(BF).astype(F32))

    for c in w_cps['out']:
        c.wait()
    ctxT = ctx_ref[...]
    a_outs, a_local, a_early = exchange(lambda hh, c0, c1: dot(ctxT, wout[hh, :, c0:c1], 0, 0), ((0, NCUT),), a_ps, a_pr, a_hs, a_hr, a_cr, a_fr, a_un)

    y_c.wait_recv()
    y_f = send(gyg.at[ct], gyg.at[ct], pt)
    y_p.wait_recv()
    y_f.wait_recv()
    for i in range(TP):
        gm_f[pl.ds(i * SL, SL), :] = gyg[i].astype(F32)
    for r in range(0, S, 32):
        gyf_ref[r:r + 32, :] = gm_f[r:r + 32, :].astype(BF)
    w_cps['dn'][0].wait()
    gyv = gyf_ref[...]
    for n in range(NCH):
        gact[:, n * CW:(n + 1) * CW] = dot(gyv, wdn[n * CW:(n + 1) * CW, :], 1, 1).astype(BF)
    vec_ref[0:1, :] = jnp.sum(gm_f[...], axis=0, keepdims=True)

    def put_x(start, width, val):
        cols = columns(start, width)
        xf[:, cols] = xf[:, cols] + val + bo_ref[:, cols]

    early_arrived(a_early, a_un)
    for k, out in enumerate(a_outs):
        arrived(out, k, a_hs, a_cr, a_fr, put_x)
    early_added(a_early, a_un, put_x)
    passed_on(a_outs, a_local, a_hr, a_fr, put_x)

    for r in range(0, S, 32):
        cen, rstd = rows_stats(xf[r:r + 32, :])
        xh = cen * rstd
        xh2[r:r + 32, :] = xh
        rstd2[r:r + 32, :] = jnp.broadcast_to(rstd, (32, 128))
        g_ref[r:r + 32, :] = (xh * g2_ref[...] + be2_ref[...]).astype(BF)

    w_cps['up'][0].wait()
    gv = g_ref[...]
    for n in range(NCH):
        cols = slice(n * CW, (n + 1) * CW)
        pre = dot(gv, wup[:, cols], 1, 0) + bup_ref[:, cols]
        val, der = gelu_parts(pre)
        act_ref[:, cols] = val.astype(BF)
        gp = gact[:, cols].astype(F32) * der
        vec_ref[1:2, cols] = jnp.sum(gp, axis=0, keepdims=True)
        gpre_ref[:, cols] = gp.astype(BF)

    gprev = gpre_ref[...]

    def part_g(hh, c0, c1):
        return dot(gprev, wup[columns(hh * HW + c0, c1 - c0), :], 1, 1)

    g_outs, g_local, g_early = exchange(part_g, ((0, 1), (1, NCUT)), b_ps, b_pr, b_hs, b_hr, b_cr, b_fr, b_un)

    actv = act_ref[...]
    for n in range(NCH):
        cols = slice(n * CW, (n + 1) * CW)
        row_blocks(mp, cols, dot(actv, wdn[:, cols], 1, 0))
    m_first = (send(mp.at[qt], m_pr.at[1], pt), send(mp.at[pt], m_pr.at[0], pt))
    for n in range(NCH):
        gwdn_ref[n * CW:(n + 1) * CW, :] = dot(act_ref[:, n * CW:(n + 1) * CW], gyv, 0, 0).astype(BF)
    def put_g(start, width, val):
        gg_f[:, columns(start, width)] = val

    early_arrived(g_early, b_un)
    for n in range(NCH):
        gwup_ref[n * CW:(n + 1) * CW, :] = dot(g_ref[:, n * CW:(n + 1) * CW], gprev, 0, 0).astype(BF)
        if n % 2:
            arrived(g_outs[n // 2], n // 2, b_hs, b_cr, b_fr, put_g)
    early_added(g_early, b_un, put_g)

    m_first[0].wait_recv()
    m_hs[...] = (mp[ct].astype(F32) + m_pr[1].astype(F32)).astype(BF)
    m_out = send(m_hs, m_cr, ct)

    passed_on(g_outs, g_local, b_hr, b_fr, put_g)

    for r in range(0, S, 32):
        xh = xh2[r:r + 32, :]
        dxh = gg_f[r:r + 32, :] * g2_ref[...]
        m1 = jnp.mean(dxh, axis=-1, keepdims=True)
        m2 = jnp.mean(dxh * xh, axis=-1, keepdims=True)
        gm = gm_f[r:r + 32, :] + rstd2[r:r + 32, 0:1] * (dxh - m1 - xh * m2)
        gm_f[r:r + 32, :] = gm
        gmid_ref[r:r + 32, :] = gm.astype(BF)

    gmv = gmid_ref[...]
    gctxT = (dot(wout[0], gmv[:, :HW], 1, 1) + dot(wout[1], gmv[:, HW:], 1, 1)).astype(BF)
    heads = range(HL)
    gos = [gctxT[h * HD:(h + 1) * HD, :] for h in heads]
    gps = [dot(head(h, 2), gos[h], 0, 0).astype(BF).astype(F32) for h in heads]
    gvs = [dot(gos[h], probs[h].astype(BF), 1, 1).astype(BF) for h in heads]
    gss = [(probs[h] * (gps[h] - jnp.sum(gps[h] * probs[h], axis=0, keepdims=True))).astype(BF) for h in heads]
    gqs = [(dot(head(h, 1), gss[h], 1, 0) * scale).astype(BF) for h in heads]
    gks = [(dot(head(h, 0), gss[h], 1, 1) * scale).astype(BF) for h in heads]
    for h in heads:
        for e, val in enumerate((gqs[h], gks[h], gvs[h])):
            gqkv_ref[head_rows(h, e), :] = val

    gqv = gqkv_ref[...]
    r_first = []
    ln_s, ln_pr = ln_x.at[0], ln_x.at[1]
    for n in range(NCH):
        cols = slice(n * CW, (n + 1) * CW)
        v = dot(gqv, wqkv[:, cols], 0, 0)
        row_blocks(rp.at[n // HCH], slice(n % HCH * CW, (n % HCH + 1) * CW), v)
        v = v.astype(BF).astype(F32)
        ln_s[0:1, cols] = jnp.sum(v * xhat[:, cols], axis=0, keepdims=True)
        ln_s[1:2, cols] = jnp.sum(v, axis=0, keepdims=True)
    for k in range(2):
        r_first.append((send(rp.at[k, qt], r_pr.at[k, 1], pt), send(rp.at[k, pt], r_pr.at[k, 0], pt)))

    l_first = send(ln_s, ln_pr, pt)

    vec_ref[2:3, :] = jnp.sum(gg_f[...] * xh2[...], axis=0, keepdims=True)
    vec_ref[3:4, :] = jnp.sum(gg_f[...], axis=0, keepdims=True)
    vec_ref[4:5, :] = jnp.sum(gm_f[...], axis=0, keepdims=True)

    own = pl.ds(pl.multiple_of(t * SL, 8), SL)
    xh_ref[...] = xhat[own, :]
    gm_ref[...] = gm_f[own, :]
    rs_ref[...] = rstd_s[own, :]
    g1_out[...] = par[0:1, :]

    for k in range(2):
        cols = slice(k * HW, (k + 1) * HW)
        r_first[k][0].wait_recv()
        r_hs[0:SL, cols] = (rp[k, ct].astype(F32) + r_pr[k, 1].astype(F32)).astype(BF)
        r_first[k][1].wait_recv()
        mine_ref[:, cols] = (rp[k, t].astype(F32) + r_pr[k, 0].astype(F32)).astype(BF)
    l_first.wait_recv()
    ln = ln_s[...] + ln_pr[...]
    ln_hs[...] = ln
    ln_rows = []
    for _ in range(3):
        ln_rows.append(ln.astype(BF).astype(F32))
        ln = ln - ln_rows[-1]
    r_hs[SL:SL + 8, :] = jnp.concatenate(ln_rows + [jnp.zeros((2, D), F32)], axis=0).astype(BF)
    m_first[1].wait_recv()
    m_out.wait_recv()
    m_sum = (mp[t].astype(F32) + m_pr[0].astype(F32)).astype(BF).astype(F32) + m_cr[...].astype(F32)
    y_ref[...] = (xf[own, :] + m_sum.astype(BF).astype(F32) + bd_ref[...]).astype(BF)
    for c in started:
        c.wait_send()


N_SEND = 37
VMEM_A = 36 * 2**20
VMEM_B = 8 * 2**20
VMEM_C = 4 * 2**20


def write_kernel(yi_ref, vec_ref, up_ref, dn_ref, gqkv_ref, h_ref, ctx_ref, gmid_ref,
                 y_ref, gwqkv_ref, gbqkv_ref, gwout_ref, gbo_ref, gl2_ref, bl2_ref, gwup_ref, gbup_ref, gwdn_ref, gbd_ref,
                 s_qkv, s_out, s_gb, s0, s1, s2, s3, s4, sem):
    cps = []

    def out(src, dst, n=1):
        rows = src.shape[0] // n
        for k in range(n):
            c = pltpu.make_async_copy(src.at[pl.ds(k * rows, rows)], dst.at[pl.ds(k * rows, rows)], sem.at[len(cps)])
            c.start()
            cps.append(c)

    out(dn_ref, gwdn_ref, 4)
    out(up_ref, gwup_ref, 4)
    out(yi_ref, y_ref)
    for i, (sv, r) in enumerate(((s0, gbd_ref), (s1, gbup_ref), (s2, gl2_ref), (s3, bl2_ref), (s4, gbo_ref))):
        sv[...] = vec_ref[i, :]
        out(sv, r)
    ones = jnp.ones((8, S), BF)
    for h in range(HL):
        for e in range(3):
            s_gb[e, h:h + 1, :] = dot(ones, gqkv_ref[head_rows(h, e), :], 1, 1)[0:1, :]
    out(s_gb, gbqkv_ref)
    hv = h_ref[...]
    s_out[...] = dot(ctx_ref[...], gmid_ref[...], 1, 0).astype(BF)
    out(s_out, gwout_ref)
    for n in range(HL):
        rows = slice(n * 3 * HD, (n + 1) * 3 * HD)
        s_qkv[rows, :] = dot(gqkv_ref[rows, :], hv, 1, 0).astype(BF)
        out(s_qkv.at[rows], gwqkv_ref.at[rows])
    for c in cps:
        c.wait()


def last_kernel(mine_ref, xh_ref, gm_ref, rs_ref, g1_ref, rc_ref, ln_ref, gx_ref, gl1_ref, bl1_ref):
    gh = (mine_ref[...].astype(F32) + rc_ref[0:SL, :].astype(F32)).astype(BF).astype(F32)
    xh = xh_ref[...]
    dxh = gh * g1_ref[...]
    m1 = jnp.mean(dxh, axis=-1, keepdims=True)
    m2 = jnp.mean(dxh * xh, axis=-1, keepdims=True)
    gx_ref[...] = (gm_ref[...] + rs_ref[:, 0:1] * (dxh - m1 - xh * m2)).astype(BF)
    lc = rc_ref[SL:SL + 8, :].astype(F32)
    ln = ln_ref[...] + (lc[0:2, :] + lc[2:4, :] + lc[4:6, :])
    gl1_ref[...] = ln[0, :]
    bl1_ref[...] = ln[1, :]


def solution(mesh):
    VM = pl.BlockSpec(memory_space=pltpu.VMEM)
    ANY = pl.BlockSpec(memory_space=pltpu.HBM)

    def sds(shape, dt):
        return jax.ShapeDtypeStruct(shape, dt)

    def local_step(x, g1, be1, w_qkv, b_qkv, w_out, b_out, g2, be2, w_up, b_up, w_down, b_down, grad_y):
        wq = jnp.transpose(w_qkv, (1, 2, 3, 0)).reshape(3 * HL * HD, D)
        bq = jnp.transpose(b_qkv, (1, 0, 2))
        part = pltpu.VMEM((S, HW), BF)
        vec1 = sds((D,), F32)
        mids = pl.pallas_call(
            block_kernel,
            out_shape=(pltpu.VMEM((SL, D), BF), pltpu.VMEM((8, D), F32), pltpu.VMEM((D, FL), BF), pltpu.VMEM((FL, D), BF),
                       pltpu.VMEM((3 * HL * HD, S), BF), pltpu.VMEM((S, D), BF), pltpu.VMEM((HL * HD, S), BF), pltpu.VMEM((S, D), BF),
                       pltpu.VMEM((SL, D), BF), pltpu.VMEM((SL, D), F32), pltpu.VMEM((SL, D), F32), pltpu.VMEM((SL, 128), F32),
                       pltpu.VMEM((1, D), F32), sds((SL + 8, D), BF), pltpu.VMEM((2, D), F32)),
            in_specs=[ANY] * 14,
            out_specs=(VM,) * 15,
            scratch_shapes=[
                pltpu.VMEM((3 * HL * HD, D), BF), pltpu.VMEM((2, HL * HD, HW), BF), pltpu.VMEM((S, D), F32), pltpu.VMEM((S, D), F32),
                pltpu.VMEM((S, D), F32), pltpu.VMEM((S, D), F32), pltpu.VMEM((S, 128), F32), pltpu.VMEM((HL, S, S), F32),
                pltpu.VMEM((3 * HL * HD, S), BF), pltpu.VMEM((8, D), F32), pltpu.VMEM((TP, SL, D), BF),
                pltpu.VMEM((D, FL), BF), pltpu.VMEM((FL, D), BF), pltpu.VMEM((TP, SL, D), BF), pltpu.VMEM((TP, SL, D), BF),
                pltpu.VMEM((3 * HL * HD, S), F32), *[part] * 12,
                pltpu.VMEM((S, FL), BF), pltpu.VMEM((S, D), BF), pltpu.VMEM((S, FL), BF), pltpu.VMEM((S, FL), BF), pltpu.VMEM((S, D), BF),
                pltpu.VMEM((3, HL, HD), F32), *[pltpu.VMEM((D,), F32) for _ in range(7)],
                pltpu.VMEM((2, TP, SL, HW), BF), pltpu.VMEM((2, SL, D), BF), pltpu.VMEM((SL, D), BF), pltpu.VMEM((SL, D), BF),
                pltpu.VMEM((2, 2, SL, HW), BF), pltpu.VMEM((2, 2, D), F32), pltpu.VMEM((S, D), F32), pltpu.VMEM((S, 128), F32),
                pltpu.VMEM((4, 2, S, UW), BF), pltpu.VMEM((4, 2, S, UW), BF),
                pltpu.SemaphoreType.DMA((9,)), pltpu.SemaphoreType.DMA((N_SEND,)), pltpu.SemaphoreType.DMA((N_SEND,)),
                pltpu.SemaphoreType.DMA((10,)),
            ],
            compiler_params=pltpu.CompilerParams(collective_id=0, has_side_effects=True, vmem_limit_bytes=VMEM_A),
            name='block',
        )(*(pltpu.with_memory_space_constraint(v, pltpu.HBM) for v in (
            x.reshape(SL, D), grad_y.reshape(SL, D), g1, be1, g2, be2, b_out, b_down, bq, b_up, wq, w_out, w_up, w_down)))
        mine, xh, gm, rs, g1v, r_hs, ln_hs = mids[8:]
        across = [(i, TP - 1 - i) for i in range(TP)]
        r_cr = lax.ppermute(r_hs, 'tp', across)
        y, gwqkv, gbqkv, gwout, gbo, gl2, bl2, gwup, gbup, gwdn, gbd = pl.pallas_call(
            write_kernel,
            out_shape=(sds((SL, D), BF), sds((3 * HL * HD, D), BF), sds((3, HL, HD), F32), sds((HL * HD, D), BF), vec1, vec1, vec1,
                       sds((D, FL), BF), vec1, sds((FL, D), BF), vec1),
            in_specs=[VM] * 8,
            out_specs=(ANY,) * 11,
            scratch_shapes=[pltpu.VMEM((3 * HL * HD, D), BF), pltpu.VMEM((HL * HD, D), BF), pltpu.VMEM((3, HL, HD), F32),
                            *[pltpu.VMEM((D,), F32) for _ in range(5)], pltpu.SemaphoreType.DMA((20,))],
            compiler_params=pltpu.CompilerParams(vmem_limit_bytes=VMEM_B),
            cost_estimate=pl.CostEstimate(flops=600_000_000, bytes_accessed=14_200_000, transcendentals=0),
            name='write',
        )(*mids[:8])
        gx, gl1, bl1 = pl.pallas_call(
            last_kernel,
            out_shape=(sds((SL, D), BF), vec1, vec1),
            in_specs=[VM] * 7,
            out_specs=(VM,) * 3,
            compiler_params=pltpu.CompilerParams(vmem_limit_bytes=VMEM_C),
            name='last',
        )(mine, xh, gm, rs, g1v, r_cr, ln_hs)
        gwqkv = jnp.transpose(gwqkv.reshape(HL, 3, HD, D), (3, 0, 1, 2))
        gbqkv = jnp.transpose(gbqkv, (1, 0, 2))
        return (y.reshape(1, SL, D), gx.reshape(1, SL, D), gl1, bl1, gwqkv, gbqkv, gwout, gbo, gl2, bl2, gwup, gbup, gwdn, gbd)

    row_spec = P('dp', 'tp', None)
    in_specs = (row_spec, P(), P(), P(None, 'tp', None, None), P('tp', None, None), P('tp', None), P(), P(), P(),
                P(None, 'tp'), P('tp'), P('tp', None), P(), row_spec)
    out_specs = (row_spec, row_spec, P('dp'), P('dp'), P('dp', 'tp', None, None), P(('dp', 'tp'), None, None),
                 P(('dp', 'tp'), None), P('dp'), P('dp'), P('dp'), P('dp', 'tp'), P(('dp', 'tp')), P(('dp', 'tp'), None), P('dp'))
    return jax.shard_map(local_step, mesh=mesh, in_specs=in_specs, out_specs=out_specs, check_vma=False)
```

```python
import functools
import math

import jax
import jax.numpy as jnp
from jax import lax
from jax.experimental import pallas as pl
from jax.experimental.pallas import tpu as pltpu
from jax.sharding import PartitionSpec as P

EPS = 1e-5
MASK_VALUE = -1e30
BF = jnp.bfloat16
F32 = jnp.float32
MESH = pl.DeviceIdType.MESH

D = 1536
S = 96
SL = 24
TP = 4
HL = 4
HD = 96
FL = 1536
CW = 256
NCH = D // CW
HCH = NCH // 2
HW = D // 2
UW = 128
CUT = (128, 384, 640, 768)
NCUT = len(CUT) - 1


def alibi_slopes(n_heads):
    closest = 2 ** int(math.floor(math.log2(n_heads)))
    base_ratio = 2.0 ** (-8.0 / closest)
    extra_ratio = 2.0 ** (-4.0 / closest)
    remaining = min(closest, n_heads - closest)
    slopes = [base_ratio ** (i + 1) for i in range(closest)]
    return slopes + [extra_ratio ** (2 * i + 1) for i in range(remaining)]


def dot(a, b, ca, cb):
    return lax.dot_general(a, b, (((ca,), (cb,)), ((), ())), preferred_element_type=F32)


def gelu_parts(u):
    k = math.sqrt(2.0 / math.pi)
    u2 = u * u
    th = jnp.tanh(u * (k + (k * 0.044715) * u2))
    half = 0.5 + 0.5 * th
    val = u * half
    return val, half + val * (1.0 - th) * (k + (3.0 * 0.044715 * k) * u2)


def rows_stats(v):
    mean = jnp.mean(v, axis=-1, keepdims=True)
    cen = v - mean
    var = jnp.mean(cen * cen, axis=-1, keepdims=True)
    return cen, lax.rsqrt(var + EPS)


def places():
    t = lax.axis_index('tp')
    core = t % 2
    pt = t + 1 - 2 * core
    ct = TP - 1 - t
    qt = TP - 1 - pt
    half = (core + t // 2) % 2
    return t, pt, ct, qt, half


def sender(ssem, rsem):
    started = []

    def send(src, dst, dev):
        i = len(started)
        c = pltpu.make_async_remote_copy(src_ref=src, dst_ref=dst, send_sem=ssem.at[i], recv_sem=rsem.at[i],
                                         device_id={'tp': dev}, device_id_type=MESH)
        c.start()
        started.append(c)
        return c

    return send, started


def columns(start, width):
    return pl.ds(start if isinstance(start, int) else pl.multiple_of(start, 128), width)


def head_rows(h, e):
    return slice((h * 3 + e) * HD, (h * 3 + e + 1) * HD)


def row_blocks(buf, cols, v):
    for i in range(TP):
        buf[i, :, cols] = v[i * SL:(i + 1) * SL, :].astype(BF)


def block_kernel(x_hbm, gy_hbm, g1_hbm, be1_hbm, g2_hbm, be2_hbm, bo_hbm, bd_hbm, bqkv_hbm, bup_hbm,
                 wqkv_hbm, wout_hbm, wup_hbm, wdn_hbm,
                 y_ref, vec_ref, gwup_ref, gwdn_ref, gqkv_ref, h_ref, ctx_ref, gmid_ref, mine_ref, xh_ref, gm_ref, rs_ref, g1_out, r_hs, ln_hs,
                 wqkv, wout, xf, gm_f, gg_f, xhat, rstd_s, probs, qkvT, par, mp,
                 wup, wdn, xg, gyg, biasT, a_ps, a_pr, a_hs, a_hr, a_cr, a_fr, b_ps, b_pr, b_hs, b_hr, b_cr, b_fr,
                 gact, g_ref, gpre_ref, act_ref, gyf_ref, bqkv_ref, g1_in, be1_in, g2_in, be2_in, bo_in, bd_in, bup_in,
                 rp, m_pr, m_hs, m_cr, r_pr, ln_x, xh2, rstd2, a_un, b_un,
                 wsem, ssem, rsem, isem):
    t, pt, ct, qt, half = places()
    send, started = sender(ssem, rsem)

    in_x = pltpu.make_async_copy(x_hbm, xg.at[t], isem.at[0])
    in_gy = pltpu.make_async_copy(gy_hbm, gyg.at[t], isem.at[1])
    in_b = pltpu.make_async_copy(bqkv_hbm, bqkv_ref, isem.at[2])
    small = ((g1_hbm, g1_in), (be1_hbm, be1_in), (g2_hbm, g2_in), (be2_hbm, be2_in), (bo_hbm, bo_in), (bd_hbm, bd_in), (bup_hbm, bup_in))
    in_p = [pltpu.make_async_copy(a, b, isem.at[3 + i]) for i, (a, b) in enumerate(small)]
    for c in (in_x, in_gy, in_b, *in_p):
        c.start()
    w_cps = {}
    w_cps['qkv'] = [pltpu.make_async_copy(wqkv_hbm, wqkv, wsem.at[0])]
    w_cps['out'] = [pltpu.make_async_copy(wout_hbm.at[:, pl.ds(k * HW, HW)], wout.at[k], wsem.at[1 + k]) for k in range(2)]
    w_cps['dn'] = [pltpu.make_async_copy(wdn_hbm, wdn, wsem.at[7])]
    w_cps['up'] = [pltpu.make_async_copy(wup_hbm, wup, wsem.at[8])]

    barrier = pltpu.get_barrier_semaphore()
    for dev in (pt, ct, qt):
        pl.semaphore_signal(barrier, inc=1, device_id={'tp': dev}, device_id_type=MESH)
    for name in ('qkv', 'out', 'dn', 'up'):
        for c in w_cps[name]:
            c.start()
    pl.semaphore_wait(barrier, 3)

    in_x.wait()
    x_c = send(xg.at[t], xg.at[t], ct)
    x_p = send(xg.at[t], xg.at[t], pt)

    for c in (in_b, *in_p):
        c.wait()
    for i, r in enumerate((g1_in, be1_in, g2_in, be2_in, bo_in, bd_in, bup_in)):
        par[i, :] = r[...]
    g1_ref, be1_ref, g2_ref, be2_ref, bo_ref, bd_ref, bup_ref = (par.at[i:i + 1] for i in range(7))

    for h in range(HL):
        for e in range(3):
            row = jnp.broadcast_to(bqkv_ref[e, h:h + 1, :], (S, HD))
            biasT[pl.ds((h * 3 + e) * HD, HD), :] = row.T

    x_c.wait_recv()
    x_f = send(xg.at[ct], xg.at[ct], pt)
    in_gy.wait()
    y_c = send(gyg.at[t], gyg.at[t], ct)
    y_p = send(gyg.at[t], gyg.at[t], pt)
    x_p.wait_recv()
    x_f.wait_recv()

    for i in range(TP):
        xf[pl.ds(i * SL, SL), :] = xg[i].astype(F32)
    for r in range(0, S, 32):
        cen, rstd = rows_stats(xf[r:r + 32, :])
        xh = cen * rstd
        xhat[r:r + 32, :] = xh
        rstd_s[r:r + 32, :] = jnp.broadcast_to(rstd, (32, 128))
        h_ref[r:r + 32, :] = (xh * g1_ref[...] + be1_ref[...]).astype(BF)

    w_cps['qkv'][0].wait()
    hv = h_ref[...]
    for h in range(HL):
        rows = slice(h * 3 * HD, (h + 1) * 3 * HD)
        qkvT[rows, :] = (dot(wqkv[rows, :], hv, 1, 1) + biasT[rows, :]).astype(BF)

    scale = HD ** -0.5
    slopes = alibi_slopes(HL * TP)
    j_pos = lax.broadcasted_iota(jnp.int32, (S, S), 0)
    i_pos = lax.broadcasted_iota(jnp.int32, (S, S), 1)
    causal = j_pos <= i_pos
    j_f = j_pos.astype(F32)

    def head(h, e):
        return qkvT[head_rows(h, e), :]

    for h in range(HL):
        slope = jnp.where(t == 0, slopes[h], jnp.where(t == 1, slopes[HL + h], jnp.where(t == 2, slopes[2 * HL + h], slopes[3 * HL + h]))).astype(F32)
        s = dot(head(h, 1), head(h, 0), 0, 0) * scale + slope * j_f
        s = jnp.where(causal, s, MASK_VALUE)
        p = jnp.exp(s - jnp.max(s, axis=0, keepdims=True))
        p = p / jnp.sum(p, axis=0, keepdims=True)
        probs[h] = p
        ctx_ref[h * HD:(h + 1) * HD, :] = dot(head(h, 2), p.astype(BF), 1, 0).astype(BF)

    def exchange(part, groups, ps, pr, hs, hr, cr, fr, un):
        firsts = []
        for k0, k1 in groups:
            cols = slice(CUT[k0], CUT[k1])
            ps[:, cols] = part(1 - half, CUT[k0], CUT[k1]).astype(BF)
            firsts.append(send(ps.at[:, cols], pr.at[:, cols], pt))
            if k0 == 0:
                for hh in range(2):
                    un[0, hh] = part(hh, 0, UW).astype(BF)
                early = [send(un.at[0], un.at[2], ct), send(un.at[0], un.at[1], pt)]
        outs = []
        for (k0, k1), first in zip(groups, firsts):
            cols = slice(CUT[k0], CUT[k1])
            ours = part(half, CUT[k0], CUT[k1])
            first.wait_recv()
            hs[:, cols] = (ours + pr[:, cols].astype(F32)).astype(BF)
            for k in range(k0, k1):
                c = slice(CUT[k], CUT[k + 1])
                outs.append([send(hs.at[:, c], cr.at[:, c], ct)])
                if k == NCUT - 1:
                    outs[-1].append(send(hs.at[:, c], fr.at[:, c], qt))
        local = send(hs.at[:, UW:], hr.at[:, UW:], pt)
        return outs, local, early

    def early_arrived(early, un):
        early[0].wait_recv()
        early.append(send(un.at[2], un.at[3], pt))

    def early_added(early, un, put):
        early[1].wait_recv()
        early[2].wait_recv()
        for hh in range(2):
            chips = [un[k, hh].astype(F32) + un[k + 1, hh].astype(F32) for k in (0, 2)]
            put(hh * HW, UW, (chips[0] + chips[1]).astype(BF).astype(F32))

    def arrived(out, k, hs, cr, fr, put):
        c = slice(CUT[k], CUT[k + 1])
        out[0].wait_recv()
        if k < NCUT - 1:
            out.append(send(cr.at[:, c], fr.at[:, c], pt))
        put(half * HW + CUT[k], CUT[k + 1] - CUT[k], (hs[:, c].astype(F32) + cr[:, c].astype(F32)).astype(BF).astype(F32))

    def passed_on(outs, local, hr, fr, put):
        local.wait_recv()
        for k, out in enumerate(outs):
            c = slice(CUT[k], CUT[k + 1])
            out[1].wait_recv()
            put((1 - half) * HW + CUT[k], CUT[k + 1] - CUT[k], (hr[:, c].astype(F32) + fr[:, c].astype(F32)).astype(BF).astype(F32))

    for c in w_cps['out']:
        c.wait()
    ctxT = ctx_ref[...]
    a_outs, a_local, a_early = exchange(lambda hh, c0, c1: dot(ctxT, wout[hh, :, c0:c1], 0, 0), ((0, NCUT),), a_ps, a_pr, a_hs, a_hr, a_cr, a_fr, a_un)

    y_c.wait_recv()
    y_f = send(gyg.at[ct], gyg.at[ct], pt)
    y_p.wait_recv()
    y_f.wait_recv()
    for i in range(TP):
        gm_f[pl.ds(i * SL, SL), :] = gyg[i].astype(F32)
    for r in range(0, S, 32):
        gyf_ref[r:r + 32, :] = gm_f[r:r + 32, :].astype(BF)
    w_cps['dn'][0].wait()
    gyv = gyf_ref[...]
    for n in range(NCH):
        gact[:, n * CW:(n + 1) * CW] = dot(gyv, wdn[n * CW:(n + 1) * CW, :], 1, 1).astype(BF)
    vec_ref[0:1, :] = jnp.sum(gm_f[...], axis=0, keepdims=True)

    def put_x(start, width, val):
        cols = columns(start, width)
        xf[:, cols] = xf[:, cols] + val + bo_ref[:, cols]

    early_arrived(a_early, a_un)
    for k, out in enumerate(a_outs):
        arrived(out, k, a_hs, a_cr, a_fr, put_x)
    early_added(a_early, a_un, put_x)
    passed_on(a_outs, a_local, a_hr, a_fr, put_x)

    for r in range(0, S, 32):
        cen, rstd = rows_stats(xf[r:r + 32, :])
        xh = cen * rstd
        xh2[r:r + 32, :] = xh
        rstd2[r:r + 32, :] = jnp.broadcast_to(rstd, (32, 128))
        g_ref[r:r + 32, :] = (xh * g2_ref[...] + be2_ref[...]).astype(BF)

    w_cps['up'][0].wait()
    gv = g_ref[...]
    for n in range(NCH):
        cols = slice(n * CW, (n + 1) * CW)
        pre = dot(gv, wup[:, cols], 1, 0) + bup_ref[:, cols]
        val, der = gelu_parts(pre)
        act_ref[:, cols] = val.astype(BF)
        gp = gact[:, cols].astype(F32) * der
        vec_ref[1:2, cols] = jnp.sum(gp, axis=0, keepdims=True)
        gpre_ref[:, cols] = gp.astype(BF)

    gprev = gpre_ref[...]

    def part_g(hh, c0, c1):
        return dot(gprev, wup[columns(hh * HW + c0, c1 - c0), :], 1, 1)

    g_outs, g_local, g_early = exchange(part_g, ((0, 1), (1, NCUT)), b_ps, b_pr, b_hs, b_hr, b_cr, b_fr, b_un)

    actv = act_ref[...]
    for n in range(NCH):
        cols = slice(n * CW, (n + 1) * CW)
        row_blocks(mp, cols, dot(actv, wdn[:, cols], 1, 0))
    m_first = (send(mp.at[qt], m_pr.at[1], pt), send(mp.at[pt], m_pr.at[0], pt))
    for n in range(NCH):
        gwdn_ref[n * CW:(n + 1) * CW, :] = dot(act_ref[:, n * CW:(n + 1) * CW], gyv, 0, 0).astype(BF)
    def put_g(start, width, val):
        gg_f[:, columns(start, width)] = val

    early_arrived(g_early, b_un)
    for n in range(NCH):
        gwup_ref[n * CW:(n + 1) * CW, :] = dot(g_ref[:, n * CW:(n + 1) * CW], gprev, 0, 0).astype(BF)
        if n % 2:
            arrived(g_outs[n // 2], n // 2, b_hs, b_cr, b_fr, put_g)
        if n == HCH:
            m_first[0].wait_recv()
            m_hs[...] = (mp[ct].astype(F32) + m_pr[1].astype(F32)).astype(BF)
            m_out = send(m_hs, m_cr, ct)
    early_added(g_early, b_un, put_g)


    passed_on(g_outs, g_local, b_hr, b_fr, put_g)

    for r in range(0, S, 32):
        xh = xh2[r:r + 32, :]
        dxh = gg_f[r:r + 32, :] * g2_ref[...]
        m1 = jnp.mean(dxh, axis=-1, keepdims=True)
        m2 = jnp.mean(dxh * xh, axis=-1, keepdims=True)
        gm = gm_f[r:r + 32, :] + rstd2[r:r + 32, 0:1] * (dxh - m1 - xh * m2)
        gm_f[r:r + 32, :] = gm
        gmid_ref[r:r + 32, :] = gm.astype(BF)

    gmv = gmid_ref[...]
    gctxT = (dot(wout[0], gmv[:, :HW], 1, 1) + dot(wout[1], gmv[:, HW:], 1, 1)).astype(BF)
    heads = range(HL)
    gos = [gctxT[h * HD:(h + 1) * HD, :] for h in heads]
    gps = [dot(head(h, 2), gos[h], 0, 0).astype(BF).astype(F32) for h in heads]
    gvs = [dot(gos[h], probs[h].astype(BF), 1, 1).astype(BF) for h in heads]
    gss = [(probs[h] * (gps[h] - jnp.sum(gps[h] * probs[h], axis=0, keepdims=True))).astype(BF) for h in heads]
    gqs = [(dot(head(h, 1), gss[h], 1, 0) * scale).astype(BF) for h in heads]
    gks = [(dot(head(h, 0), gss[h], 1, 1) * scale).astype(BF) for h in heads]
    for h in heads:
        for e, val in enumerate((gqs[h], gks[h], gvs[h])):
            gqkv_ref[head_rows(h, e), :] = val

    gqv = gqkv_ref[...]
    r_first = []
    ln_s, ln_pr = ln_x.at[0], ln_x.at[1]
    for n in range(NCH):
        cols = slice(n * CW, (n + 1) * CW)
        v = dot(gqv, wqkv[:, cols], 0, 0)
        row_blocks(rp.at[n // HCH], slice(n % HCH * CW, (n % HCH + 1) * CW), v)
        v = v.astype(BF).astype(F32)
        ln_s[0:1, cols] = jnp.sum(v * xhat[:, cols], axis=0, keepdims=True)
        ln_s[1:2, cols] = jnp.sum(v, axis=0, keepdims=True)
    for k in range(2):
        r_first.append((send(rp.at[k, qt], r_pr.at[k, 1], pt), send(rp.at[k, pt], r_pr.at[k, 0], pt)))

    l_first = send(ln_s, ln_pr, pt)

    vec_ref[2:3, :] = jnp.sum(gg_f[...] * xh2[...], axis=0, keepdims=True)
    vec_ref[3:4, :] = jnp.sum(gg_f[...], axis=0, keepdims=True)
    vec_ref[4:5, :] = jnp.sum(gm_f[...], axis=0, keepdims=True)

    own = pl.ds(pl.multiple_of(t * SL, 8), SL)
    xh_ref[...] = xhat[own, :]
    gm_ref[...] = gm_f[own, :]
    rs_ref[...] = rstd_s[own, :]
    g1_out[...] = par[0:1, :]

    m_first[1].wait_recv()
    m_out.wait_recv()
    m_sum = (mp[t].astype(F32) + m_pr[0].astype(F32)).astype(BF).astype(F32) + m_cr[...].astype(F32)
    y_ref[...] = (xf[own, :] + m_sum.astype(BF).astype(F32) + bd_ref[...]).astype(BF)

    for k in range(2):
        cols = slice(k * HW, (k + 1) * HW)
        r_first[k][0].wait_recv()
        r_hs[0:SL, cols] = (rp[k, ct].astype(F32) + r_pr[k, 1].astype(F32)).astype(BF)
        r_first[k][1].wait_recv()
        mine_ref[:, cols] = (rp[k, t].astype(F32) + r_pr[k, 0].astype(F32)).astype(BF)
    l_first.wait_recv()
    ln = ln_s[...] + ln_pr[...]
    ln_hs[...] = ln
    ln_rows = []
    for _ in range(3):
        ln_rows.append(ln.astype(BF).astype(F32))
        ln = ln - ln_rows[-1]
    r_hs[SL:SL + 8, :] = jnp.concatenate(ln_rows + [jnp.zeros((2, D), F32)], axis=0).astype(BF)
    for c in started:
        c.wait_send()


N_SEND = 37
VMEM_A = 36 * 2**20
VMEM_B = 8 * 2**20
VMEM_C = 4 * 2**20


def write_kernel(yi_ref, vec_ref, up_ref, dn_ref, gqkv_ref, h_ref, ctx_ref, gmid_ref,
                 y_ref, gwqkv_ref, gbqkv_ref, gwout_ref, gbo_ref, gl2_ref, bl2_ref, gwup_ref, gbup_ref, gwdn_ref, gbd_ref,
                 s_qkv, s_out, s_gb, s0, s1, s2, s3, s4, sem):
    cps = []

    def out(src, dst, n=1):
        rows = src.shape[0] // n
        for k in range(n):
            c = pltpu.make_async_copy(src.at[pl.ds(k * rows, rows)], dst.at[pl.ds(k * rows, rows)], sem.at[len(cps)])
            c.start()
            cps.append(c)

    out(dn_ref, gwdn_ref, 4)
    out(up_ref, gwup_ref, 4)
    out(yi_ref, y_ref)
    for i, (sv, r) in enumerate(((s0, gbd_ref), (s1, gbup_ref), (s2, gl2_ref), (s3, bl2_ref), (s4, gbo_ref))):
        sv[...] = vec_ref[i, :]
        out(sv, r)
    ones = jnp.ones((8, S), BF)
    for h in range(HL):
        for e in range(3):
            s_gb[e, h:h + 1, :] = dot(ones, gqkv_ref[head_rows(h, e), :], 1, 1)[0:1, :]
    out(s_gb, gbqkv_ref)
    hv = h_ref[...]
    s_out[...] = dot(ctx_ref[...], gmid_ref[...], 1, 0).astype(BF)
    out(s_out, gwout_ref)
    for n in range(HL):
        rows = slice(n * 3 * HD, (n + 1) * 3 * HD)
        s_qkv[rows, :] = dot(gqkv_ref[rows, :], hv, 1, 0).astype(BF)
        out(s_qkv.at[rows], gwqkv_ref.at[rows])
    for c in cps:
        c.wait()


def last_kernel(mine_ref, xh_ref, gm_ref, rs_ref, g1_ref, rc_ref, ln_ref, gx_ref, gl1_ref, bl1_ref):
    gh = (mine_ref[...].astype(F32) + rc_ref[0:SL, :].astype(F32)).astype(BF).astype(F32)
    xh = xh_ref[...]
    dxh = gh * g1_ref[...]
    m1 = jnp.mean(dxh, axis=-1, keepdims=True)
    m2 = jnp.mean(dxh * xh, axis=-1, keepdims=True)
    gx_ref[...] = (gm_ref[...] + rs_ref[:, 0:1] * (dxh - m1 - xh * m2)).astype(BF)
    lc = rc_ref[SL:SL + 8, :].astype(F32)
    ln = ln_ref[...] + (lc[0:2, :] + lc[2:4, :] + lc[4:6, :])
    gl1_ref[...] = ln[0, :]
    bl1_ref[...] = ln[1, :]


def solution(mesh):
    VM = pl.BlockSpec(memory_space=pltpu.VMEM)
    ANY = pl.BlockSpec(memory_space=pltpu.HBM)

    def sds(shape, dt):
        return jax.ShapeDtypeStruct(shape, dt)

    def local_step(x, g1, be1, w_qkv, b_qkv, w_out, b_out, g2, be2, w_up, b_up, w_down, b_down, grad_y):
        wq = jnp.transpose(w_qkv, (1, 2, 3, 0)).reshape(3 * HL * HD, D)
        bq = jnp.transpose(b_qkv, (1, 0, 2))
        part = pltpu.VMEM((S, HW), BF)
        vec1 = sds((D,), F32)
        mids = pl.pallas_call(
            block_kernel,
            out_shape=(pltpu.VMEM((SL, D), BF), pltpu.VMEM((8, D), F32), pltpu.VMEM((D, FL), BF), pltpu.VMEM((FL, D), BF),
                       pltpu.VMEM((3 * HL * HD, S), BF), pltpu.VMEM((S, D), BF), pltpu.VMEM((HL * HD, S), BF), pltpu.VMEM((S, D), BF),
                       pltpu.VMEM((SL, D), BF), pltpu.VMEM((SL, D), F32), pltpu.VMEM((SL, D), F32), pltpu.VMEM((SL, 128), F32),
                       pltpu.VMEM((1, D), F32), sds((SL + 8, D), BF), pltpu.VMEM((2, D), F32)),
            in_specs=[ANY] * 14,
            out_specs=(VM,) * 15,
            scratch_shapes=[
                pltpu.VMEM((3 * HL * HD, D), BF), pltpu.VMEM((2, HL * HD, HW), BF), pltpu.VMEM((S, D), F32), pltpu.VMEM((S, D), F32),
                pltpu.VMEM((S, D), F32), pltpu.VMEM((S, D), F32), pltpu.VMEM((S, 128), F32), pltpu.VMEM((HL, S, S), F32),
                pltpu.VMEM((3 * HL * HD, S), BF), pltpu.VMEM((8, D), F32), pltpu.VMEM((TP, SL, D), BF),
                pltpu.VMEM((D, FL), BF), pltpu.VMEM((FL, D), BF), pltpu.VMEM((TP, SL, D), BF), pltpu.VMEM((TP, SL, D), BF),
                pltpu.VMEM((3 * HL * HD, S), F32), *[part] * 12,
                pltpu.VMEM((S, FL), BF), pltpu.VMEM((S, D), BF), pltpu.VMEM((S, FL), BF), pltpu.VMEM((S, FL), BF), pltpu.VMEM((S, D), BF),
                pltpu.VMEM((3, HL, HD), F32), *[pltpu.VMEM((D,), F32) for _ in range(7)],
                pltpu.VMEM((2, TP, SL, HW), BF), pltpu.VMEM((2, SL, D), BF), pltpu.VMEM((SL, D), BF), pltpu.VMEM((SL, D), BF),
                pltpu.VMEM((2, 2, SL, HW), BF), pltpu.VMEM((2, 2, D), F32), pltpu.VMEM((S, D), F32), pltpu.VMEM((S, 128), F32),
                pltpu.VMEM((4, 2, S, UW), BF), pltpu.VMEM((4, 2, S, UW), BF),
                pltpu.SemaphoreType.DMA((9,)), pltpu.SemaphoreType.DMA((N_SEND,)), pltpu.SemaphoreType.DMA((N_SEND,)),
                pltpu.SemaphoreType.DMA((10,)),
            ],
            compiler_params=pltpu.CompilerParams(collective_id=0, has_side_effects=True, vmem_limit_bytes=VMEM_A),
            name='block',
        )(*(pltpu.with_memory_space_constraint(v, pltpu.HBM) for v in (
            x.reshape(SL, D), grad_y.reshape(SL, D), g1, be1, g2, be2, b_out, b_down, bq, b_up, wq, w_out, w_up, w_down)))
        mine, xh, gm, rs, g1v, r_hs, ln_hs = mids[8:]
        across = [(i, TP - 1 - i) for i in range(TP)]
        r_cr = lax.ppermute(r_hs, 'tp', across)
        y, gwqkv, gbqkv, gwout, gbo, gl2, bl2, gwup, gbup, gwdn, gbd = pl.pallas_call(
            write_kernel,
            out_shape=(sds((SL, D), BF), sds((3 * HL * HD, D), BF), sds((3, HL, HD), F32), sds((HL * HD, D), BF), vec1, vec1, vec1,
                       sds((D, FL), BF), vec1, sds((FL, D), BF), vec1),
            in_specs=[VM] * 8,
            out_specs=(ANY,) * 11,
            scratch_shapes=[pltpu.VMEM((3 * HL * HD, D), BF), pltpu.VMEM((HL * HD, D), BF), pltpu.VMEM((3, HL, HD), F32),
                            *[pltpu.VMEM((D,), F32) for _ in range(5)], pltpu.SemaphoreType.DMA((20,))],
            compiler_params=pltpu.CompilerParams(vmem_limit_bytes=VMEM_B),
            cost_estimate=pl.CostEstimate(flops=600_000_000, bytes_accessed=14_200_000, transcendentals=0),
            name='write',
        )(*mids[:8])
        gx, gl1, bl1 = pl.pallas_call(
            last_kernel,
            out_shape=(sds((SL, D), BF), vec1, vec1),
            in_specs=[VM] * 7,
            out_specs=(VM,) * 3,
            compiler_params=pltpu.CompilerParams(vmem_limit_bytes=VMEM_C),
            name='last',
        )(mine, xh, gm, rs, g1v, r_cr, ln_hs)
        gwqkv = jnp.transpose(gwqkv.reshape(HL, 3, HD, D), (3, 0, 1, 2))
        gbqkv = jnp.transpose(gbqkv, (1, 0, 2))
        return (y.reshape(1, SL, D), gx.reshape(1, SL, D), gl1, bl1, gwqkv, gbqkv, gwout, gbo, gl2, bl2, gwup, gbup, gwdn, gbd)

    row_spec = P('dp', 'tp', None)
    in_specs = (row_spec, P(), P(), P(None, 'tp', None, None), P('tp', None, None), P('tp', None), P(), P(), P(),
                P(None, 'tp'), P('tp'), P('tp', None), P(), row_spec)
    out_specs = (row_spec, row_spec, P('dp'), P('dp'), P('dp', 'tp', None, None), P(('dp', 'tp'), None, None),
                 P(('dp', 'tp'), None), P('dp'), P('dp'), P('dp'), P('dp', 'tp'), P(('dp', 'tp')), P(('dp', 'tp'), None), P('dp'))
    return jax.shard_map(local_step, mesh=mesh, in_specs=in_specs, out_specs=out_specs, check_vma=False)
```
